64 devices in a mesh: dp: 4 (over x, y), sp: 16 (over z, core).
Axes of the slice: x: 2, y: 2, z: 8, core: 2. Of those that a mesh axis runs over, the one named last changes fastest.
The devices are a block of a 4x4x8 slice.
Arguments:
- x_in: bfloat16 [8, 4096, 1536], P('dp', 'sp'), parts along dimension 0
- positions: int32 [8, 4096], P('dp', 'sp'), parts along dimension 0
- keep_mask: int32 [8, 4096], P('dp', 'sp'), parts along dimension 0
- ln_gain: float32 [1536], replicated
- ln_bias: float32 [1536], replicated
- w_qkv: bfloat16 [1536, 16, 3, 96], replicated
- b_qkv: float32 [16, 3, 96], replicated
- w_out: bfloat16 [1536, 1536], replicated
- b_out: float32 [1536], replicated
- grad_y: bfloat16 [8, 4096, 1536], P('dp', 'sp'), parts along dimension 0
Outputs:
- output 1: bfloat16 [8, 4096, 1536], P('dp', 'sp'), parts along dimension 0
- output 2: bfloat16 [8, 4096, 1536], P('dp', 'sp'), parts along dimension 0
- output 3: float32 [6144, 16, 3, 96], P('dp'), parts along dimension 0
- output 4: float32 [64, 3, 96], P('dp'), parts along dimension 0
- output 5: float32 [6144, 1536], P('dp'), parts along dimension 0
- output 6: float32 [6144], P('dp'), parts along dimension 0
- output 7: float32 [6144], P('dp'), parts along dimension 0
- output 8: float32 [6144], P('dp'), parts along dimension 0
There are 4 independent parts. The reference program is written for one: setup_inputs(seed, part) draws one part's arguments, and reference() takes and returns one part's arrays. A program takes and returns all parts, laid end to end along the dimension named above; an argument that names none is the same for every part.
All inputs are finite; a program needn't handle non-finite values.
Results may differ from the reference program's by a relative error of at most 0.00974613.
Values are sent between devices in bfloat16 or wider.
A program may use at most 768 MiB of HBM per device.

```python
import jax
import jax.numpy as jnp
import numpy as np
from jax import lax

BATCH_SEQS = 2
SEQ_LEN = 4096
HIDDEN = 1536
NUM_HEADS = 16
HEAD_DIM = HIDDEN // NUM_HEADS
NORM_EPS = 1e-5
MASK_FILL = -1e30
QK_SCALE = HEAD_DIM ** -0.5
SLOPES = 2.0 ** (-8.0 * (np.arange(NUM_HEADS) + 1) / NUM_HEADS)


def setup_inputs(seed: int = 0, part: int = 0) -> dict:
    part_key = jax.random.fold_in(jax.random.key(seed), part)
    k_x, k_dy, k_len, k_gap = jax.random.split(part_key, 4)
    k_g, k_b, k_wq, k_bq, k_wo, k_bo = jax.random.split(jax.random.key(seed + 1), 6)
    shape_act = (BATCH_SEQS, SEQ_LEN, HIDDEN)
    x_in = jax.random.normal(k_x, shape_act, jnp.float32).astype(jnp.bfloat16)
    grad_y = jax.random.normal(k_dy, shape_act, jnp.float32).astype(jnp.bfloat16)
    lengths = jax.random.randint(k_len, (BATCH_SEQS,), SEQ_LEN // 8, SEQ_LEN + 1)
    lengths = lengths.at[0].set(SEQ_LEN)
    keep_mask = (jnp.arange(SEQ_LEN)[None, :] < lengths[:, None]).astype(jnp.int32)
    pos_steps = jax.random.randint(k_gap, (BATCH_SEQS, SEQ_LEN), 1, 3)
    positions = (jnp.cumsum(pos_steps, axis=1) - pos_steps[:, :1]).astype(jnp.int32)
    w_scale = HIDDEN ** -0.5
    return {
        "x_in": x_in,
        "positions": positions,
        "keep_mask": keep_mask,
        "ln_gain": 1.0 + 0.5 * jax.random.normal(k_g, (HIDDEN,), jnp.float32),
        "ln_bias": 0.5 * jax.random.normal(k_b, (HIDDEN,), jnp.float32),
        "w_qkv": (w_scale * jax.random.normal(k_wq, (HIDDEN, NUM_HEADS, 3, HEAD_DIM), jnp.float32)).astype(jnp.bfloat16),
        "b_qkv": 0.5 * jax.random.normal(k_bq, (NUM_HEADS, 3, HEAD_DIM), jnp.float32),
        "w_out": (w_scale * jax.random.normal(k_wo, (HIDDEN, HIDDEN), jnp.float32)).astype(jnp.bfloat16),
        "b_out": 0.5 * jax.random.normal(k_bo, (HIDDEN,), jnp.float32),
        "grad_y": grad_y,
    }


def head_probs(q_head, k_head, pos_row, keep_row, head_slope):
    scores = jnp.dot(q_head, k_head.T, preferred_element_type=jnp.float32) * QK_SCALE
    pos_gap = (pos_row[:, None] - pos_row[None, :]).astype(jnp.float32)
    scores = scores - head_slope * pos_gap
    tok_index = jnp.arange(SEQ_LEN)
    allowed = (tok_index[None, :] <= tok_index[:, None]) & (keep_row[None, :] > 0)
    return jax.nn.softmax(jnp.where(allowed, scores, MASK_FILL), axis=-1)


def head_forward(head_item):
    q_head, k_head, v_head, pos_row, keep_row, head_slope = head_item
    attn_prob = head_probs(q_head, k_head, pos_row, keep_row, head_slope)
    return jnp.dot(attn_prob.astype(jnp.bfloat16), v_head, preferred_element_type=jnp.float32).astype(jnp.bfloat16)


def head_backward(head_item):
    q_head, k_head, v_head, o_head, do_head, pos_row, keep_row, head_slope = head_item
    attn_prob = head_probs(q_head, k_head, pos_row, keep_row, head_slope)
    prob_lo = attn_prob.astype(jnp.bfloat16)
    dv_head = jnp.dot(prob_lo.T, do_head, preferred_element_type=jnp.float32).astype(jnp.bfloat16)
    grad_prob = jnp.dot(do_head, v_head.T, preferred_element_type=jnp.float32)
    row_dot = jnp.sum(do_head.astype(jnp.float32) * o_head.astype(jnp.float32), axis=-1)
    ds_lo = (attn_prob * (grad_prob - row_dot[:, None])).astype(jnp.bfloat16)
    dq_head = (jnp.dot(ds_lo, k_head, preferred_element_type=jnp.float32) * QK_SCALE).astype(jnp.bfloat16)
    dk_head = (jnp.dot(ds_lo.T, q_head, preferred_element_type=jnp.float32) * QK_SCALE).astype(jnp.bfloat16)
    return dq_head, dk_head, dv_head


def reference(x_in, positions, keep_mask, ln_gain, ln_bias, w_qkv, b_qkv, w_out, b_out, grad_y):
    tokens = BATCH_SEQS * SEQ_LEN
    x_f32 = x_in.astype(jnp.float32)
    centered = x_f32 - jnp.mean(x_f32, axis=-1, keepdims=True)
    inv_std = lax.rsqrt(jnp.mean(centered * centered, axis=-1, keepdims=True) + NORM_EPS)
    x_hat = centered * inv_std
    x_norm = (x_hat * ln_gain + ln_bias).astype(jnp.bfloat16).reshape(tokens, HIDDEN)
    w_flat = w_qkv.reshape(HIDDEN, 3 * HIDDEN)
    qkv_flat = (jnp.dot(x_norm, w_flat, preferred_element_type=jnp.float32) + b_qkv.reshape(3 * HIDDEN)).astype(jnp.bfloat16)
    qkv_heads = jnp.transpose(qkv_flat.reshape(BATCH_SEQS, SEQ_LEN, NUM_HEADS, 3, HEAD_DIM), (3, 0, 2, 1, 4))
    qkv_heads = qkv_heads.reshape(3, BATCH_SEQS * NUM_HEADS, SEQ_LEN, HEAD_DIM)
    pos_rows = jnp.repeat(positions, NUM_HEADS, axis=0)
    keep_rows = jnp.repeat(keep_mask, NUM_HEADS, axis=0)
    slope_rows = jnp.tile(jnp.asarray(SLOPES, jnp.float32), BATCH_SEQS)
    o_heads = lax.map(head_forward, (qkv_heads[0], qkv_heads[1], qkv_heads[2], pos_rows, keep_rows, slope_rows))
    o_flat = jnp.transpose(o_heads.reshape(BATCH_SEQS, NUM_HEADS, SEQ_LEN, HEAD_DIM), (0, 2, 1, 3)).reshape(tokens, HIDDEN)
    y_out = (x_f32.reshape(tokens, HIDDEN) + jnp.dot(o_flat, w_out, preferred_element_type=jnp.float32) + b_out).astype(jnp.bfloat16)
    dy_flat = grad_y.reshape(tokens, HIDDEN)
    grad_b_out = jnp.sum(dy_flat.astype(jnp.float32), axis=0)
    grad_w_out = jnp.dot(o_flat.T, dy_flat, preferred_element_type=jnp.float32)
    do_flat = jnp.dot(dy_flat, w_out.T, preferred_element_type=jnp.float32).astype(jnp.bfloat16)
    do_heads = jnp.transpose(do_flat.reshape(BATCH_SEQS, SEQ_LEN, NUM_HEADS, HEAD_DIM), (0, 2, 1, 3)).reshape(BATCH_SEQS * NUM_HEADS, SEQ_LEN, HEAD_DIM)
    dq_heads, dk_heads, dv_heads = lax.map(head_backward, (qkv_heads[0], qkv_heads[1], qkv_heads[2], o_heads, do_heads, pos_rows, keep_rows, slope_rows))
    d_qkv = jnp.stack([dq_heads, dk_heads, dv_heads], axis=0).reshape(3, BATCH_SEQS, NUM_HEADS, SEQ_LEN, HEAD_DIM)
    d_qkv = jnp.transpose(d_qkv, (1, 3, 2, 0, 4)).reshape(tokens, 3 * HIDDEN)
    grad_b_qkv = jnp.sum(d_qkv.astype(jnp.float32), axis=0).reshape(NUM_HEADS, 3, HEAD_DIM)
    grad_w_qkv = jnp.dot(x_norm.T, d_qkv, preferred_element_type=jnp.float32).reshape(HIDDEN, NUM_HEADS, 3, HEAD_DIM)
    d_norm = jnp.dot(d_qkv, w_flat.T, preferred_element_type=jnp.float32).reshape(BATCH_SEQS, SEQ_LEN, HIDDEN)
    grad_gain = jnp.sum(d_norm * x_hat, axis=(0, 1))
    grad_bias = jnp.sum(d_norm, axis=(0, 1))
    d_hat = d_norm * ln_gain
    d_ln = inv_std * (d_hat - jnp.mean(d_hat, axis=-1, keepdims=True) - x_hat * jnp.mean(d_hat * x_hat, axis=-1, keepdims=True))
    grad_x = (grad_y.astype(jnp.float32) + d_ln).astype(jnp.bfloat16)
    return (y_out.reshape(BATCH_SEQS, SEQ_LEN, HIDDEN), grad_x, grad_w_qkv, grad_b_qkv, grad_w_out, grad_b_out, grad_gain, grad_bias)
```

```python
import functools
import jax
import jax.numpy as jnp
from jax import lax
from jax.experimental import pallas as pl
from jax.experimental.pallas import tpu as pltpu
from jax.sharding import PartitionSpec as P

NORM_EPS = 1e-5

LOG2E = 1.4426950408889634
MASKED = -1e30
F32, BF16 = jnp.float32, jnp.bfloat16
NT = (((1,), (1,)), ((), ()))


def attn_body(slope_ref, qkvt_ref, dot_ref, posk_ref, pref_ref, out_ref,
              k_tok, v_tok, s_buf, q_pad, do_pad, o_acc, dq_acc, dk_acc, dv_acc, *, blk, tok):
    dim = dot_ref.shape[0]
    seq = dot_ref.shape[1]
    pad = k_tok.shape[1] - dim
    nq = blk // tok
    scale = dim ** -0.5
    i = pl.program_id(0)
    half = blk // 2

    @pl.when(i == 0)
    def _():
        dk_acc[...] = jnp.zeros_like(dk_acc)
        dv_acc[...] = jnp.zeros_like(dv_acc)
        q_pad[...] = jnp.zeros_like(q_pad)
        do_pad[...] = jnp.zeros_like(do_pad)

        @pl.loop(0, seq // 128)
        def _(t):
            cols = pl.ds(pl.multiple_of(t * 128, 128), 128)
            for base, dst in ((dim, k_tok), (2 * dim, v_tok)):
                part = qkvt_ref[base:base + dim, cols].astype(F32)
                full = jnp.concatenate([part, jnp.zeros((pad, 128), F32)], axis=0)
                dst[cols, :] = jnp.transpose(full).astype(BF16)

    qcols = pl.ds(pl.multiple_of(i * blk, blk), blk)
    q_pad[0:dim, :] = qkvt_ref[0:dim, qcols]
    do_pad[0:dim, :] = dot_ref[:, qcols]
    slope2 = slope_ref[0]
    ref_pos = pref_ref[pl.ds(i, 1), :]
    c = scale * LOG2E

    def scores(j, m8, diag):
        for sub in range(2):
            rows = pl.ds(pl.multiple_of(j * blk + sub * half, half), half)
            st = jnp.dot(k_tok[rows, :], q_pad[...], preferred_element_type=F32)
            bias = (posk_ref[rows, :] - ref_pos) * slope2
            st = st * c + jnp.concatenate([bias] * (blk // 128), axis=1)
            if diag:
                key = lax.broadcasted_iota(jnp.int32, (half, blk), 0) + sub * half
                qry = lax.broadcasted_iota(jnp.int32, (half, blk), 1)
                st = jnp.where(key <= qry, st, MASKED)
            s_buf[rows, :] = st
            m8 = jnp.maximum(m8, jnp.max(st.reshape(half // 8, 8, blk), axis=0))
        return m8

    m8 = lax.fori_loop(0, i, lambda j, m: scores(j, m, False), jnp.full((8, blk), MASKED, F32))
    m8 = scores(i, m8, True)
    m = jnp.max(m8, axis=0, keepdims=True)

    def exps(j, l8):
        for sub in range(2):
            rows = pl.ds(pl.multiple_of(j * blk + sub * half, half), half)
            e = jnp.exp2(s_buf[rows, :] - m)
            s_buf[rows, :] = e
            l8 = l8 + jnp.sum(e.reshape(half // 8, 8, blk), axis=0)
        return l8

    l8 = lax.fori_loop(0, i + 1, exps, jnp.zeros((8, blk), F32))
    inv = 1.0 / jnp.sum(l8, axis=0, keepdims=True)
    o_acc[...] = jnp.zeros_like(o_acc)
    dq_acc[...] = jnp.zeros_like(dq_acc)

    def values(j, _):
        rows = pl.ds(pl.multiple_of(j * blk, blk), blk)
        p = s_buf[rows, :] * inv
        s_buf[rows, :] = p
        pb = p.astype(BF16)
        o_acc[...] += jnp.dot(qkvt_ref[2 * dim:3 * dim, rows], pb, preferred_element_type=F32)
        dv_acc[:, rows] += lax.dot_general(do_pad[0:dim, :], pb, NT, preferred_element_type=F32)
        return 0

    lax.fori_loop(0, i + 1, values, 0)
    o_lo = o_acc[...].astype(BF16)
    do_f = do_pad[0:dim, :].astype(F32)
    r = jnp.sum(do_f * o_lo.astype(F32), axis=0, keepdims=True)

    def grads(j, _):
        rows = pl.ds(pl.multiple_of(j * blk, blk), blk)
        g = jnp.dot(v_tok[rows, :], do_pad[...], preferred_element_type=F32)
        ds = (s_buf[rows, :] * (g - r)).astype(BF16)
        dq_acc[...] += jnp.dot(qkvt_ref[dim:2 * dim, rows], ds, preferred_element_type=F32)
        dk_acc[:, rows] += lax.dot_general(q_pad[0:dim, :], ds, NT, preferred_element_type=F32)
        return 0

    lax.fori_loop(0, i + 1, grads, 0)
    dq_lo = (dq_acc[...] * scale).astype(BF16)
    for t in range(nq):
        out_ref[i * nq + t, 0] = o_lo[:, t * tok:(t + 1) * tok]
        out_ref[i * nq + t, 1] = dq_lo[:, t * tok:(t + 1) * tok]

    @pl.when(i == pl.num_programs(0) - 1)
    def _():
        @pl.loop(0, seq // tok)
        def _(t):
            cols = pl.ds(pl.multiple_of(t * tok, tok), tok)
            out_ref[t, 2] = (dk_acc[:, cols] * scale).astype(BF16)
            out_ref[t, 3] = dv_acc[:, cols].astype(BF16)


def attention(slope2, qkvt, dot_, posk, pref, *, blk, tok):
    dim, seq = dot_.shape
    wide = 128 * pl.cdiv(dim, 128)
    full = lambda a: pl.BlockSpec(a.shape, lambda i: (0,) * a.ndim, pipeline_mode=pl.Buffered(1))
    out = jax.ShapeDtypeStruct((seq // tok, 4, dim, tok), BF16)
    pairs = (seq // blk) * (seq // blk + 1) // 2
    return pl.pallas_call(
        functools.partial(attn_body, blk=blk, tok=tok),
        name="attention",
        out_shape=out,
        grid=(seq // blk,),
        in_specs=[pl.BlockSpec(memory_space=pltpu.SMEM)] + [full(a) for a in (qkvt, dot_, posk, pref)],
        out_specs=pl.BlockSpec(out.shape, lambda i: (0, 0, 0, 0), pipeline_mode=pl.Buffered(1)),
        scratch_shapes=[
            pltpu.VMEM((seq, wide), BF16), pltpu.VMEM((seq, wide), BF16),
            pltpu.VMEM((seq, blk), F32),
            pltpu.VMEM((wide, blk), BF16), pltpu.VMEM((wide, blk), BF16),
            pltpu.VMEM((dim, blk), F32), pltpu.VMEM((dim, blk), F32),
            pltpu.VMEM((dim, seq), F32), pltpu.VMEM((dim, seq), F32)],
        cost_estimate=pl.CostEstimate(flops=pairs * 6 * 2 * blk * blk * 256, bytes_accessed=12 << 20, transcendentals=pairs * blk * blk),
        compiler_params=pltpu.CompilerParams(dimension_semantics=("arbitrary",), vmem_limit_bytes=48 << 20),
    )(slope2, qkvt, dot_, posk, pref)


def exchange_body(x_ref, out_ref, send_sem, recv_sem, *, peers):
    me = lax.axis_index("sp")
    barrier = pltpu.get_barrier_semaphore()
    for d in range(1, peers):
        pl.semaphore_signal(barrier, inc=1, device_id={"sp": lax.rem(me + d, peers)}, device_id_type=pl.DeviceIdType.MESH)
    pl.semaphore_wait(barrier, peers - 1)
    copies = []
    for d in range(1, peers):
        copies.append(pltpu.make_async_remote_copy(
            src_ref=x_ref, dst_ref=out_ref.at[me], send_sem=send_sem.at[d - 1], recv_sem=recv_sem.at[d - 1],
            device_id={"sp": lax.rem(me + d, peers)}, device_id_type=pl.DeviceIdType.MESH))
        copies[-1].start()
    out_ref[me] = x_ref[...]
    for copy in copies:
        copy.wait()


def exchange(x, peers, collective_id, name):
    return pl.pallas_call(
        functools.partial(exchange_body, peers=peers),
        name=name,
        out_shape=jax.ShapeDtypeStruct((peers,) + x.shape, x.dtype),
        in_specs=[pl.BlockSpec(memory_space=pltpu.VMEM)],
        out_specs=pl.BlockSpec(memory_space=pltpu.VMEM),
        scratch_shapes=[pltpu.SemaphoreType.DMA((peers - 1,)), pltpu.SemaphoreType.DMA((peers - 1,))],
        compiler_params=pltpu.CompilerParams(collective_id=collective_id, has_side_effects=True, vmem_limit_bytes=8 << 20),
    )(x)


def swap_body(x_ref, out_ref, own, send_sem, recv_sem, own_sem, *, peers):
    me = lax.axis_index("sp")
    barrier = pltpu.get_barrier_semaphore()
    for d in range(1, peers):
        pl.semaphore_signal(barrier, inc=1, device_id={"sp": lax.rem(me + d, peers)}, device_id_type=pl.DeviceIdType.MESH)
    pl.semaphore_wait(barrier, peers - 1)
    copies = []
    for near in range(peers // 2):
        for d in sorted({peers // 2 - near, peers // 2 + near}):
            peer = lax.rem(me + d, peers)
            copies.append(pltpu.make_async_remote_copy(
                src_ref=x_ref.at[peer], dst_ref=out_ref.at[me], send_sem=send_sem.at[d - 1], recv_sem=recv_sem.at[d - 1],
                device_id={"sp": peer}, device_id_type=pl.DeviceIdType.MESH))
            copies[-1].start()
    take = pltpu.make_async_copy(x_ref.at[me], own, own_sem)
    take.start()
    take.wait()
    put = pltpu.make_async_copy(own, out_ref.at[me], own_sem)
    put.start()
    put.wait()
    for copy in copies:
        copy.wait()


def swap(x, peers, collective_id, name):
    hbm = pl.BlockSpec(memory_space=pltpu.HBM)
    return pl.pallas_call(
        functools.partial(swap_body, peers=peers),
        name=name,
        out_shape=jax.ShapeDtypeStruct(x.shape, x.dtype),
        in_specs=[hbm],
        out_specs=hbm,
        scratch_shapes=[pltpu.VMEM(x.shape[1:], x.dtype), pltpu.SemaphoreType.DMA((peers - 1,)),
                        pltpu.SemaphoreType.DMA((peers - 1,)), pltpu.SemaphoreType.DMA],
        compiler_params=pltpu.CompilerParams(collective_id=collective_id, has_side_effects=True, vmem_limit_bytes=48 << 20),
    )(x)


def norm_forward(x_blk, ln_gain, ln_bias):
    x_f32 = x_blk.astype(F32)
    centered = x_f32 - jnp.mean(x_f32, axis=-1, keepdims=True)
    inv_std = lax.rsqrt(jnp.mean(centered * centered, axis=-1, keepdims=True) + NORM_EPS)
    x_hat = centered * inv_std
    return x_f32, x_hat, inv_std, (x_hat * ln_gain + ln_bias).astype(BF16)


def solution(mesh):
    peers = mesh.shape["sp"]

    def block_fn(x_blk, pos_blk, keep_blk, ln_gain, ln_bias, w_qkv, b_qkv, w_out, b_out, dy_blk):
        batch, tok, hidden = x_blk.shape
        heads, dim = w_qkv.shape[1], w_qkv.shape[3]
        assert heads == peers
        seq = tok * peers
        blk = 2 * tok
        rank = lax.axis_index("sp")
        x_f32, x_hat, inv_std, x_norm = norm_forward(x_blk, ln_gain, ln_bias)
        marks = exchange(jnp.concatenate([pos_blk, keep_blk, jnp.zeros((8 - 2 * batch, tok), jnp.int32)]), peers, 0, "marks")
        w_t = jnp.transpose(w_qkv, (1, 2, 3, 0))
        w_head = lax.dynamic_index_in_dim(w_t, rank, 0, keepdims=False).reshape(3 * dim, hidden)
        b_head = lax.dynamic_index_in_dim(b_qkv, rank, 0, keepdims=False).reshape(3 * dim, 1)
        wo_head = lax.dynamic_slice_in_dim(w_out, rank * dim, dim, 0)
        slope = jnp.exp2(-8.0 * (rank + 1).astype(F32) / heads)
        slope2 = (slope * LOG2E).reshape(1)
        gw = jnp.zeros((3 * dim, hidden), F32)
        go = jnp.zeros((dim, hidden), F32)
        gb = jnp.zeros((3 * dim,), F32)
        got = []
        for b in range(batch):
            xn, dy = x_norm[b], dy_blk[b]
            if b:
                xn, dy, _, _ = lax.optimization_barrier((xn, dy, xf, df))
            xf = lax.all_gather(xn, "sp", axis=0, tiled=True)
            df = lax.all_gather(dy, "sp", axis=0, tiled=True)
            pos = marks[:, b].reshape(seq).astype(F32)
            keep = marks[:, batch + b].reshape(seq)
            posk = jnp.broadcast_to(jnp.where(keep > 0, pos, MASKED)[:, None], (seq, 128))
            pref = jnp.broadcast_to(pos[::blk][:, None], (seq // blk, 128))
            qkvt = (lax.dot_general(w_head, xf, NT, preferred_element_type=F32) + b_head).astype(BF16)
            dot_ = lax.dot_general(wo_head, df, NT, preferred_element_type=F32).astype(BF16)
            if b:
                slope2, _ = lax.optimization_barrier((slope2, got[-1]))
            att = attention(slope2, qkvt, dot_, posk, pref, blk=blk, tok=tok)
            got.append(swap(att, peers, 2 + b, "swap"))
            xf3, df3 = xf.reshape(peers, tok, hidden), df.reshape(peers, tok, hidden)
            gw += jnp.einsum("pcdt,pth->cdh", att[:, 1:], xf3, preferred_element_type=F32).reshape(3 * dim, hidden)
            go += jnp.einsum("pdt,pth->dh", att[:, 0], df3, preferred_element_type=F32)
            gb += jnp.sum(att[:, 1:].astype(F32), axis=(0, 3)).reshape(3 * dim)
        gw_all = lax.all_gather(gw, "sp", axis=0, tiled=True)
        go_all = lax.all_gather(go, "sp", axis=0, tiled=True)
        y, gx, gg, gbias = [], [], 0.0, 0.0
        for b in range(batch):
            o_t = got[b][:, 0].reshape(hidden, tok)
            dqkv_t = got[b][:, 1:].reshape(3 * hidden, tok)
            y.append((x_f32[b] + lax.dot_general(o_t, w_out, (((0,), (0,)), ((), ())), preferred_element_type=F32) + b_out).astype(BF16))
            d_norm = lax.dot_general(dqkv_t, w_t.reshape(3 * hidden, hidden), (((0,), (0,)), ((), ())), preferred_element_type=F32)
            gg += jnp.sum(d_norm * x_hat[b], axis=0)
            gbias += jnp.sum(d_norm, axis=0)
            d_hat = d_norm * ln_gain
            d_mean = jnp.mean(d_hat, axis=-1, keepdims=True)
            d_proj = jnp.mean(d_hat * x_hat[b], axis=-1, keepdims=True)
            gx.append((dy_blk[b].astype(F32) + inv_std[b] * (d_hat - d_mean - x_hat[b] * d_proj)).astype(BF16))
        g_out = jnp.sum(dy_blk.astype(F32), axis=(0, 1))
        rows = jnp.stack([gg, gbias, g_out, jnp.pad(gb, (0, hidden - 3 * dim))] + [jnp.zeros((hidden,), F32)] * 4)
        sums = exchange(rows, peers, 1, "sums")
        total = jnp.sum(sums[:, :3], axis=0)
        gb_all = sums[:, 3, :3 * dim].reshape(heads, 3, dim)
        gw_out = jnp.transpose(gw_all.reshape(heads, 3, dim, hidden), (3, 0, 1, 2))
        return jnp.stack(y), jnp.stack(gx), gw_out, gb_all, go_all, total[2], total[0], total[1]

    act_spec = P("dp", "sp", None)
    tok_spec = P("dp", "sp")
    in_specs = (act_spec, tok_spec, tok_spec, P(), P(), P(), P(), P(), P(), act_spec)
    out_specs = (act_spec, act_spec, P("dp", None, None, None), P("dp", None, None), P("dp", None), P("dp"), P("dp"), P("dp"))
    return jax.shard_map(block_fn, mesh=mesh, in_specs=in_specs, out_specs=out_specs, check_vma=False)
```

```python
import functools
import jax
import jax.numpy as jnp
from jax import lax
from jax.experimental import pallas as pl
from jax.experimental.pallas import tpu as pltpu
from jax.sharding import PartitionSpec as P

NORM_EPS = 1e-5

LOG2E = 1.4426950408889634
MASKED = -1e30
F32, BF16 = jnp.float32, jnp.bfloat16
NT = (((1,), (1,)), ((), ()))


def attn_body(slope_ref, qkvt_ref, dot_ref, posk_ref, pref_ref, *refs, blk, tok, peers):
    if peers:
        old_ref, out_ref, got_ref = refs[:3]
        own, send_sem, recv_sem, own_sem = refs[-4:]
        refs = refs[3:-4]
    else:
        out_ref, refs = refs[0], refs[1:]
    k_tok, v_tok, s_buf, q_pad, do_pad, o_acc, dq_acc, dk_acc, dv_acc = refs
    dim = dot_ref.shape[1]
    seq = dot_ref.shape[0] * tok
    pad = k_tok.shape[1] - dim
    nq = blk // tok
    scale = dim ** -0.5
    i = pl.program_id(0)
    half = blk // 2

    if peers:
        @pl.when(i == 0)
        def _():
            meet(peers)
            swap_start(old_ref, got_ref, own, send_sem, recv_sem, own_sem, peers)

    @pl.when(i == 0)
    def _():
        dk_acc[...] = jnp.zeros_like(dk_acc)
        dv_acc[...] = jnp.zeros_like(dv_acc)
        q_pad[...] = jnp.zeros_like(q_pad)
        do_pad[...] = jnp.zeros_like(do_pad)

        @pl.loop(0, seq // 128)
        def _(t):
            cols = pl.ds(pl.multiple_of(t * 128, 128), 128)
            for base, dst in ((dim, k_tok), (2 * dim, v_tok)):
                part = qkvt_ref[base:base + dim, cols].astype(F32)
                full = jnp.concatenate([part, jnp.zeros((pad, 128), F32)], axis=0)
                dst[cols, :] = jnp.transpose(full).astype(BF16)

    qcols = pl.ds(pl.multiple_of(i * blk, blk), blk)
    q_pad[0:dim, :] = qkvt_ref[0:dim, qcols]
    for t in range(nq):
        do_pad[0:dim, t * tok:(t + 1) * tok] = dot_ref[i * nq + t]
    slope2 = slope_ref[0]
    ref_pos = pref_ref[pl.ds(i, 1), :]
    c = scale * LOG2E

    def scores(j, m8, diag):
        for sub in range(2):
            rows = pl.ds(pl.multiple_of(j * blk + sub * half, half), half)
            st = jnp.dot(k_tok[rows, :], q_pad[...], preferred_element_type=F32)
            bias = (posk_ref[rows, :] - ref_pos) * slope2
            st = st * c + jnp.concatenate([bias] * (blk // 128), axis=1)
            if diag:
                key = lax.broadcasted_iota(jnp.int32, (half, blk), 0) + sub * half
                qry = lax.broadcasted_iota(jnp.int32, (half, blk), 1)
                st = jnp.where(key <= qry, st, MASKED)
            s_buf[rows, :] = st
            m8 = jnp.maximum(m8, jnp.max(st.reshape(half // 8, 8, blk), axis=0))
        return m8

    m8 = lax.fori_loop(0, i, lambda j, m: scores(j, m, False), jnp.full((8, blk), MASKED, F32))
    m8 = scores(i, m8, True)
    m = jnp.max(m8, axis=0, keepdims=True)

    def exps(j, l8):
        for sub in range(2):
            rows = pl.ds(pl.multiple_of(j * blk + sub * half, half), half)
            e = jnp.exp2(s_buf[rows, :] - m)
            s_buf[rows, :] = e
            l8 = l8 + jnp.sum(e.reshape(half // 8, 8, blk), axis=0)
        return l8

    l8 = lax.fori_loop(0, i + 1, exps, jnp.zeros((8, blk), F32))
    inv = 1.0 / jnp.sum(l8, axis=0, keepdims=True)
    o_acc[...] = jnp.zeros_like(o_acc)
    dq_acc[...] = jnp.zeros_like(dq_acc)

    def values(j, _):
        rows = pl.ds(pl.multiple_of(j * blk, blk), blk)
        p = s_buf[rows, :] * inv
        s_buf[rows, :] = p
        pb = p.astype(BF16)
        o_acc[...] += jnp.dot(qkvt_ref[2 * dim:3 * dim, rows], pb, preferred_element_type=F32)
        dv_acc[:, rows] += lax.dot_general(do_pad[0:dim, :], pb, NT, preferred_element_type=F32)
        return 0

    lax.fori_loop(0, i + 1, values, 0)
    o_lo = o_acc[...].astype(BF16)
    do_f = do_pad[0:dim, :].astype(F32)
    r = jnp.sum(do_f * o_lo.astype(F32), axis=0, keepdims=True)

    def grads(j, _):
        rows = pl.ds(pl.multiple_of(j * blk, blk), blk)
        g = jnp.dot(v_tok[rows, :], do_pad[...], preferred_element_type=F32)
        ds = (s_buf[rows, :] * (g - r)).astype(BF16)
        dq_acc[...] += jnp.dot(qkvt_ref[dim:2 * dim, rows], ds, preferred_element_type=F32)
        dk_acc[:, rows] += lax.dot_general(q_pad[0:dim, :], ds, NT, preferred_element_type=F32)
        return 0

    lax.fori_loop(0, i + 1, grads, 0)
    dq_lo = (dq_acc[...] * scale).astype(BF16)
    for t in range(nq):
        out_ref[i * nq + t, 0] = o_lo[:, t * tok:(t + 1) * tok]
        out_ref[i * nq + t, 1] = dq_lo[:, t * tok:(t + 1) * tok]

    @pl.when(i == pl.num_programs(0) - 1)
    def _():
        @pl.loop(0, seq // tok)
        def _(t):
            cols = pl.ds(pl.multiple_of(t * tok, tok), tok)
            out_ref[t, 2] = (dk_acc[:, cols] * scale).astype(BF16)
            out_ref[t, 3] = dv_acc[:, cols].astype(BF16)

        if peers:
            swap_wait(old_ref, got_ref, own, send_sem, recv_sem, own_sem, peers)


def attention(slope2, qkvt, dot_, posk, pref, *, blk, tok, old=None, collective_id=None):
    blocks, dim, _ = dot_.shape
    seq = blocks * tok
    wide = 128 * pl.cdiv(dim, 128)
    hbm = pl.BlockSpec(memory_space=pltpu.HBM)
    full = lambda a: pl.BlockSpec(a.shape, lambda i: (0,) * a.ndim, pipeline_mode=pl.Buffered(1))
    out = jax.ShapeDtypeStruct((blocks, 4, dim, tok), BF16)
    pairs = (seq // blk) * (seq // blk + 1) // 2
    args = (slope2, qkvt, dot_, posk, pref)
    in_specs = [pl.BlockSpec(memory_space=pltpu.SMEM)] + [full(a) for a in (qkvt, dot_, posk, pref)]
    out_shape, out_specs = [out], [pl.BlockSpec(out.shape, lambda i: (0, 0, 0, 0), pipeline_mode=pl.Buffered(1))]
    scratch = [
        pltpu.VMEM((seq, wide), BF16), pltpu.VMEM((seq, wide), BF16),
        pltpu.VMEM((seq, blk), F32),
        pltpu.VMEM((wide, blk), BF16), pltpu.VMEM((wide, blk), BF16),
        pltpu.VMEM((dim, blk), F32), pltpu.VMEM((dim, blk), F32),
        pltpu.VMEM((dim, seq), F32), pltpu.VMEM((dim, seq), F32)]
    peers = 0
    if old is not None:
        peers = old.shape[0]
        args += (old,)
        in_specs.append(hbm)
        out_shape.append(jax.ShapeDtypeStruct(old.shape, old.dtype))
        out_specs.append(hbm)
        scratch += swap_scratch(old)
    res = pl.pallas_call(
        functools.partial(attn_body, blk=blk, tok=tok, peers=peers),
        name="attention",
        out_shape=out_shape,
        grid=(seq // blk,),
        in_specs=in_specs,
        out_specs=out_specs,
        scratch_shapes=scratch,
        cost_estimate=pl.CostEstimate(flops=pairs * 6 * 2 * blk * blk * 256, bytes_accessed=12 << 20, transcendentals=pairs * blk * blk),
        compiler_params=pltpu.CompilerParams(dimension_semantics=("arbitrary",), vmem_limit_bytes=44 << 20,
                                             collective_id=collective_id, has_side_effects=old is not None),
    )(*args)
    return res if old is not None else res[0]


def peer_at(d, peers):
    return {"sp": lax.rem(lax.axis_index("sp") + d, peers)}


def meet(peers):
    barrier = pltpu.get_barrier_semaphore()
    for d in range(1, peers):
        pl.semaphore_signal(barrier, inc=1, device_id=peer_at(d, peers), device_id_type=pl.DeviceIdType.MESH)
    pl.semaphore_wait(barrier, peers - 1)


def swap_copies(x_ref, out_ref, send_sem, recv_sem, peers):
    me = lax.axis_index("sp")
    order = [d for near in range(peers // 2) for d in sorted({peers // 2 - near, peers // 2 + near})]
    return [pltpu.make_async_remote_copy(
        src_ref=x_ref.at[lax.rem(me + d, peers)], dst_ref=out_ref.at[me], send_sem=send_sem.at[d - 1], recv_sem=recv_sem.at[d - 1],
        device_id=peer_at(d, peers), device_id_type=pl.DeviceIdType.MESH) for d in order]


def swap_start(x_ref, out_ref, own, send_sem, recv_sem, own_sem, peers):
    me = lax.axis_index("sp")
    for copy in swap_copies(x_ref, out_ref, send_sem, recv_sem, peers):
        copy.start()
    take = pltpu.make_async_copy(x_ref.at[me], own, own_sem)
    take.start()
    take.wait()
    pltpu.make_async_copy(own, out_ref.at[me], own_sem).start()


def swap_wait(x_ref, out_ref, own, send_sem, recv_sem, own_sem, peers):
    pltpu.make_async_copy(own, out_ref.at[lax.axis_index("sp")], own_sem).wait()
    for copy in swap_copies(x_ref, out_ref, send_sem, recv_sem, peers):
        copy.wait()


def swap_scratch(x):
    peers = x.shape[0]
    return [pltpu.VMEM(x.shape[1:], x.dtype), pltpu.SemaphoreType.DMA((peers - 1,)), pltpu.SemaphoreType.DMA((peers - 1,)),
            pltpu.SemaphoreType.DMA]


def swap_body(*refs, peers, n):
    ins, outs, scratch = refs[:n], refs[n:2 * n], refs[2 * n:]
    meet(peers)
    for k in range(n):
        swap_start(ins[k], outs[k], *scratch[4 * k:4 * k + 4], peers)
    for k in range(n):
        swap_wait(ins[k], outs[k], *scratch[4 * k:4 * k + 4], peers)


def swap(xs, collective_id, name):
    hbm = pl.BlockSpec(memory_space=pltpu.HBM)
    peers = xs[0].shape[0]
    return pl.pallas_call(
        functools.partial(swap_body, peers=peers, n=len(xs)),
        name=name,
        out_shape=[jax.ShapeDtypeStruct(x.shape, x.dtype) for x in xs],
        in_specs=[hbm] * len(xs),
        out_specs=[hbm] * len(xs),
        scratch_shapes=sum((swap_scratch(x) for x in xs), []),
        cost_estimate=pl.CostEstimate(flops=24000 * sum(x.size for x in xs), bytes_accessed=4 * sum(x.size for x in xs), transcendentals=0),
        compiler_params=pltpu.CompilerParams(collective_id=collective_id, has_side_effects=True, vmem_limit_bytes=48 << 20),
    )(*xs)


def exchange_body(x_ref, out_ref, send_sem, recv_sem, *, peers):
    me = lax.axis_index("sp")
    meet(peers)
    copies = [pltpu.make_async_remote_copy(
        src_ref=x_ref, dst_ref=out_ref.at[me], send_sem=send_sem.at[d - 1], recv_sem=recv_sem.at[d - 1],
        device_id=peer_at(d, peers), device_id_type=pl.DeviceIdType.MESH) for d in range(1, peers)]
    for copy in copies:
        copy.start()
    out_ref[me] = x_ref[...]
    for copy in copies:
        copy.wait()


def exchange(x, peers, collective_id, name):
    return pl.pallas_call(
        functools.partial(exchange_body, peers=peers),
        name=name,
        out_shape=jax.ShapeDtypeStruct((peers,) + x.shape, x.dtype),
        in_specs=[pl.BlockSpec(memory_space=pltpu.VMEM)],
        out_specs=pl.BlockSpec(memory_space=pltpu.VMEM),
        scratch_shapes=[pltpu.SemaphoreType.DMA((peers - 1,)), pltpu.SemaphoreType.DMA((peers - 1,))],
        compiler_params=pltpu.CompilerParams(collective_id=collective_id, has_side_effects=True, vmem_limit_bytes=8 << 20),
    )(x)


def copy_body(x_ref, out_ref):
    out_ref[...] = x_ref[...]


def keep_copy(x, steps):
    spec = pl.BlockSpec((x.shape[0] // steps, x.shape[1]), lambda i: (i, 0))
    return pl.pallas_call(
        copy_body, name="keep_copy", out_shape=jax.ShapeDtypeStruct(x.shape, x.dtype), grid=(steps,), in_specs=[spec], out_specs=spec,
        cost_estimate=pl.CostEstimate(flops=10**10, bytes_accessed=8 * x.size, transcendentals=0))(x)


def norm_forward(x_blk, ln_gain, ln_bias):
    x_f32 = x_blk.astype(F32)
    centered = x_f32 - jnp.mean(x_f32, axis=-1, keepdims=True)
    inv_std = lax.rsqrt(jnp.mean(centered * centered, axis=-1, keepdims=True) + NORM_EPS)
    x_hat = centered * inv_std
    return x_f32, x_hat, inv_std, (x_hat * ln_gain + ln_bias).astype(BF16)


def solution(mesh):
    peers = mesh.shape["sp"]

    def block_fn(x_blk, pos_blk, keep_blk, ln_gain, ln_bias, w_qkv, b_qkv, w_out, b_out, dy_blk):
        batch, tok, hidden = x_blk.shape
        heads, dim = w_qkv.shape[1], w_qkv.shape[3]
        assert heads == peers
        seq = tok * peers
        blk = 2 * tok
        rank = lax.axis_index("sp")
        x_f32, x_hat, inv_std, x_norm = norm_forward(x_blk, ln_gain, ln_bias)
        xf = [lax.all_gather(x_norm[0], "sp", axis=0, tiled=True)]
        marks = exchange(jnp.concatenate([pos_blk, keep_blk, jnp.zeros((8 - 2 * batch, tok), jnp.int32)]), peers, 0, "marks")
        do_loc = [lax.dot_general(w_out, dy_blk[b], NT, preferred_element_type=F32).astype(BF16).reshape(heads, dim, tok) for b in range(batch)]
        do_t = swap(do_loc, 1, "swap_do")
        for b in range(1, batch):
            xn, _ = lax.optimization_barrier((x_norm[b], xf[-1]))
            xf.append(lax.all_gather(xn, "sp", axis=0, tiled=True))
        w_t = jnp.transpose(w_qkv, (1, 2, 3, 0))
        w_head = lax.dynamic_index_in_dim(w_t, rank, 0, keepdims=False).reshape(3 * dim, hidden)
        b_head = lax.dynamic_index_in_dim(b_qkv, rank, 0, keepdims=False).reshape(3 * dim, 1)
        slope = jnp.exp2(-8.0 * (rank + 1).astype(F32) / heads)
        slope2 = (slope * LOG2E).reshape(1)
        gw = jnp.zeros((3 * dim, hidden), F32)
        gb = jnp.zeros((3 * dim,), F32)
        att, got = [], []
        for b in range(batch):
            pos = marks[:, b].reshape(seq).astype(F32)
            keep = marks[:, batch + b].reshape(seq)
            posk = jnp.broadcast_to(jnp.where(keep > 0, pos, MASKED)[:, None], (seq, 128))
            pref = jnp.broadcast_to(pos[::blk][:, None], (seq // blk, 128))
            qkvt = (lax.dot_general(w_head, xf[b], NT, preferred_element_type=F32) + b_head).astype(BF16)
            if b:
                slope2, gw = lax.optimization_barrier((slope2, gw))
                cur, prev = attention(slope2, qkvt, do_t[b], posk, pref, blk=blk, tok=tok, old=att[-1], collective_id=2 + b)
                got.append(prev)
            else:
                cur = attention(slope2, qkvt, do_t[b], posk, pref, blk=blk, tok=tok)
            att.append(cur)
            gw += jnp.einsum("pcdt,pth->cdh", cur[:, 1:], xf[b].reshape(peers, tok, hidden), preferred_element_type=F32).reshape(3 * dim, hidden)
            gb += jnp.sum(cur[:, 1:].astype(F32), axis=(0, 3)).reshape(3 * dim)
        gw_all = lax.all_gather(gw, "sp", axis=0, tiled=True)
        last, _ = lax.optimization_barrier((att[-1], gw))
        got += swap([last], 2, "swap_last")
        go = sum(lax.dot_general(got[b][:, 0].reshape(hidden, tok), dy_blk[b], (((1,), (0,)), ((), ())), preferred_element_type=F32) for b in range(batch))
        y, gx, gg, gbias = [], [], 0.0, 0.0
        for b in range(batch):
            o_t = got[b][:, 0].reshape(hidden, tok)
            dqkv_t = got[b][:, 1:].reshape(3 * hidden, tok)
            y.append((x_f32[b] + lax.dot_general(o_t, w_out, (((0,), (0,)), ((), ())), preferred_element_type=F32) + b_out).astype(BF16))
            d_norm = lax.dot_general(dqkv_t, w_t.reshape(3 * hidden, hidden), (((0,), (0,)), ((), ())), preferred_element_type=F32)
            gg += jnp.sum(d_norm * x_hat[b], axis=0)
            gbias += jnp.sum(d_norm, axis=0)
            d_hat = d_norm * ln_gain
            d_mean = jnp.mean(d_hat, axis=-1, keepdims=True)
            d_proj = jnp.mean(d_hat * x_hat[b], axis=-1, keepdims=True)
            gx.append((dy_blk[b].astype(F32) + inv_std[b] * (d_hat - d_mean - x_hat[b] * d_proj)).astype(BF16))
        g_out = jnp.sum(dy_blk.astype(F32), axis=(0, 1))
        rows = jnp.stack([gg, gbias, g_out, jnp.pad(gb, (0, hidden - 3 * dim))] + [jnp.zeros((hidden,), F32)] * 4)
        sums = exchange(rows, peers, 4, "sums")
        total = jnp.sum(sums[:, :3], axis=0)
        gb_all = sums[:, 3, :3 * dim].reshape(heads, 3, dim)
        go, gw_all, _, _ = lax.optimization_barrier((go, gw_all, y, gx))
        part = lax.psum_scatter(go, "sp", scatter_dimension=0, tiled=True)
        gw_all = keep_copy(gw_all, heads)
        part, gw_all = lax.optimization_barrier((part, gw_all))
        go_all = lax.all_gather(part, "sp", axis=0, tiled=True)
        gw_out = jnp.transpose(gw_all.reshape(heads, 3, dim, hidden), (3, 0, 1, 2))
        return jnp.stack(y), jnp.stack(gx), gw_out, gb_all, go_all, total[2], total[0], total[1]

    act_spec = P("dp", "sp", None)
    tok_spec = P("dp", "sp")
    in_specs = (act_spec, tok_spec, tok_spec, P(), P(), P(), P(), P(), P(), act_spec)
    out_specs = (act_spec, act_spec, P("dp", None, None, None), P("dp", None, None), P("dp", None), P("dp"), P("dp"), P("dp"))
    return jax.shard_map(block_fn, mesh=mesh, in_specs=in_specs, out_specs=out_specs, check_vma=False)
```

```python
import functools
import jax
import jax.numpy as jnp
from jax import lax
from jax.experimental import pallas as pl
from jax.experimental.pallas import tpu as pltpu
from jax.sharding import PartitionSpec as P

NORM_EPS = 1e-5

LOG2E = 1.4426950408889634
MASKED = -1e30
F32, BF16 = jnp.float32, jnp.bfloat16
NT = (((1,), (1,)), ((), ()))


def attn_body(slope_ref, qkvt_ref, dot_ref, posk_ref, pref_ref, *refs, blk, tok, peers):
    if peers:
        old, (o_ref, dqkv_ref), got = refs[:2], refs[2:4], refs[4:6]
        swaps = [(old[n], got[n]) + refs[4 * n - 8:(4 * n - 4) or None] for n in range(2)]
        refs = refs[6:-8]
    else:
        (o_ref, dqkv_ref), refs = refs[:2], refs[2:]
    k_tok, v_tok, s_buf, q_pad, do_pad, o_acc, dq_acc, dk_acc, dv_acc = refs
    dim = dot_ref.shape[1]
    seq = dot_ref.shape[0] * tok
    pad = k_tok.shape[1] - dim
    nq = blk // tok
    scale = dim ** -0.5
    i = pl.program_id(0)
    half = blk // 2

    if peers:
        @pl.when(i == 0)
        def _():
            meet(peers)
            for one in swaps:
                swap_start(*one, peers)

    @pl.when(i == 0)
    def _():
        dk_acc[...] = jnp.zeros_like(dk_acc)
        dv_acc[...] = jnp.zeros_like(dv_acc)
        q_pad[...] = jnp.zeros_like(q_pad)
        do_pad[...] = jnp.zeros_like(do_pad)

        @pl.loop(0, seq // 128)
        def _(t):
            cols = pl.ds(pl.multiple_of(t * 128, 128), 128)
            for base, dst in ((dim, k_tok), (2 * dim, v_tok)):
                part = qkvt_ref[base:base + dim, cols].astype(F32)
                full = jnp.concatenate([part, jnp.zeros((pad, 128), F32)], axis=0)
                dst[cols, :] = jnp.transpose(full).astype(BF16)

    qcols = pl.ds(pl.multiple_of(i * blk, blk), blk)
    q_pad[0:dim, :] = qkvt_ref[0:dim, qcols]
    for t in range(nq):
        do_pad[0:dim, t * tok:(t + 1) * tok] = dot_ref[i * nq + t]
    slope2 = slope_ref[0]
    ref_pos = pref_ref[pl.ds(i, 1), :]
    c = scale * LOG2E

    def scores(j, m8, diag):
        for sub in range(2):
            rows = pl.ds(pl.multiple_of(j * blk + sub * half, half), half)
            st = jnp.dot(k_tok[rows, :], q_pad[...], preferred_element_type=F32)
            bias = (posk_ref[rows, :] - ref_pos) * slope2
            st = st * c + jnp.concatenate([bias] * (blk // 128), axis=1)
            if diag:
                key = lax.broadcasted_iota(jnp.int32, (half, blk), 0) + sub * half
                qry = lax.broadcasted_iota(jnp.int32, (half, blk), 1)
                st = jnp.where(key <= qry, st, MASKED)
            s_buf[rows, :] = st
            m8 = jnp.maximum(m8, jnp.max(st.reshape(half // 8, 8, blk), axis=0))
        return m8

    m8 = lax.fori_loop(0, i, lambda j, m: scores(j, m, False), jnp.full((8, blk), MASKED, F32))
    m8 = scores(i, m8, True)
    m = jnp.max(m8, axis=0, keepdims=True)

    def exps(j, l8):
        for sub in range(2):
            rows = pl.ds(pl.multiple_of(j * blk + sub * half, half), half)
            e = jnp.exp2(s_buf[rows, :] - m)
            s_buf[rows, :] = e
            l8 = l8 + jnp.sum(e.reshape(half // 8, 8, blk), axis=0)
        return l8

    l8 = lax.fori_loop(0, i + 1, exps, jnp.zeros((8, blk), F32))
    inv = 1.0 / jnp.sum(l8, axis=0, keepdims=True)
    o_acc[...] = jnp.zeros_like(o_acc)
    dq_acc[...] = jnp.zeros_like(dq_acc)

    def values(j, _):
        rows = pl.ds(pl.multiple_of(j * blk, blk), blk)
        p = s_buf[rows, :] * inv
        s_buf[rows, :] = p
        pb = p.astype(BF16)
        o_acc[...] += jnp.dot(qkvt_ref[2 * dim:3 * dim, rows], pb, preferred_element_type=F32)
        dv_acc[:, rows] += lax.dot_general(do_pad[0:dim, :], pb, NT, preferred_element_type=F32)
        return 0

    lax.fori_loop(0, i + 1, values, 0)
    o_lo = o_acc[...].astype(BF16)
    do_f = do_pad[0:dim, :].astype(F32)
    r = jnp.sum(do_f * o_lo.astype(F32), axis=0, keepdims=True)

    def grads(j, _):
        rows = pl.ds(pl.multiple_of(j * blk, blk), blk)
        g = jnp.dot(v_tok[rows, :], do_pad[...], preferred_element_type=F32)
        ds = (s_buf[rows, :] * (g - r)).astype(BF16)
        dq_acc[...] += jnp.dot(qkvt_ref[dim:2 * dim, rows], ds, preferred_element_type=F32)
        dk_acc[:, rows] += lax.dot_general(q_pad[0:dim, :], ds, NT, preferred_element_type=F32)
        return 0

    lax.fori_loop(0, i + 1, grads, 0)
    dq_lo = (dq_acc[...] * scale).astype(BF16)
    for t in range(nq):
        o_ref[i * nq + t] = o_lo[:, t * tok:(t + 1) * tok]
        dqkv_ref[i * nq + t, 0] = dq_lo[:, t * tok:(t + 1) * tok]

    @pl.when(i == pl.num_programs(0) - 1)
    def _():
        @pl.loop(0, seq // tok)
        def _(t):
            cols = pl.ds(pl.multiple_of(t * tok, tok), tok)
            dqkv_ref[t, 1] = (dk_acc[:, cols] * scale).astype(BF16)
            dqkv_ref[t, 2] = dv_acc[:, cols].astype(BF16)

        if peers:
            for one in swaps:
                swap_wait(*one, peers)


def attention(slope2, qkvt, dot_, posk, pref, *, blk, tok, old=None, collective_id=None):
    blocks, dim, _ = dot_.shape
    seq = blocks * tok
    wide = 128 * pl.cdiv(dim, 128)
    hbm = pl.BlockSpec(memory_space=pltpu.HBM)
    full = lambda a: pl.BlockSpec(a.shape, lambda i: (0,) * a.ndim, pipeline_mode=pl.Buffered(1))
    outs = [jax.ShapeDtypeStruct((blocks, dim, tok), BF16), jax.ShapeDtypeStruct((blocks, 3, dim, tok), BF16)]
    pairs = (seq // blk) * (seq // blk + 1) // 2
    args = (slope2, qkvt, dot_, posk, pref)
    in_specs = [pl.BlockSpec(memory_space=pltpu.SMEM)] + [full(a) for a in (qkvt, dot_, posk, pref)]
    out_shape, out_specs = list(outs), [full(a) for a in outs]
    scratch = [
        pltpu.VMEM((seq, wide), BF16), pltpu.VMEM((seq, wide), BF16),
        pltpu.VMEM((seq, blk), F32),
        pltpu.VMEM((wide, blk), BF16), pltpu.VMEM((wide, blk), BF16),
        pltpu.VMEM((dim, blk), F32), pltpu.VMEM((dim, blk), F32),
        pltpu.VMEM((dim, seq), F32), pltpu.VMEM((dim, seq), F32)]
    peers = 0
    if old is not None:
        peers = blocks
        args += tuple(old)
        in_specs += [hbm] * 2
        out_shape += outs
        out_specs += [hbm] * 2
        scratch += swap_scratch(old[0]) + swap_scratch(old[1])
    res = pl.pallas_call(
        functools.partial(attn_body, blk=blk, tok=tok, peers=peers),
        name="attention",
        out_shape=out_shape,
        grid=(seq // blk,),
        in_specs=in_specs,
        out_specs=out_specs,
        scratch_shapes=scratch,
        cost_estimate=pl.CostEstimate(flops=pairs * 6 * 2 * blk * blk * 256, bytes_accessed=12 << 20, transcendentals=pairs * blk * blk),
        compiler_params=pltpu.CompilerParams(dimension_semantics=("arbitrary",), vmem_limit_bytes=44 << 20,
                                             collective_id=collective_id, has_side_effects=old is not None),
    )(*args)
    return res[:2], res[2:]


def peer_at(d, peers):
    return {"sp": lax.rem(lax.axis_index("sp") + d, peers)}


def meet(peers):
    barrier = pltpu.get_barrier_semaphore()
    for d in range(1, peers):
        pl.semaphore_signal(barrier, inc=1, device_id=peer_at(d, peers), device_id_type=pl.DeviceIdType.MESH)
    pl.semaphore_wait(barrier, peers - 1)


def swap_copies(x_ref, out_ref, send_sem, recv_sem, peers):
    me = lax.axis_index("sp")
    order = [d for near in range(peers // 2) for d in sorted({peers // 2 - near, peers // 2 + near})]
    return [pltpu.make_async_remote_copy(
        src_ref=x_ref.at[lax.rem(me + d, peers)], dst_ref=out_ref.at[me], send_sem=send_sem.at[d - 1], recv_sem=recv_sem.at[d - 1],
        device_id=peer_at(d, peers), device_id_type=pl.DeviceIdType.MESH) for d in order]


def swap_start(x_ref, out_ref, own, send_sem, recv_sem, own_sem, peers):
    me = lax.axis_index("sp")
    for copy in swap_copies(x_ref, out_ref, send_sem, recv_sem, peers):
        copy.start()
    take = pltpu.make_async_copy(x_ref.at[me], own, own_sem)
    take.start()
    take.wait()
    pltpu.make_async_copy(own, out_ref.at[me], own_sem).start()


def swap_wait(x_ref, out_ref, own, send_sem, recv_sem, own_sem, peers):
    pltpu.make_async_copy(own, out_ref.at[lax.axis_index("sp")], own_sem).wait()
    for copy in swap_copies(x_ref, out_ref, send_sem, recv_sem, peers):
        copy.wait()


def swap_scratch(x):
    peers = x.shape[0]
    return [pltpu.VMEM(x.shape[1:], x.dtype), pltpu.SemaphoreType.DMA((peers - 1,)), pltpu.SemaphoreType.DMA((peers - 1,)),
            pltpu.SemaphoreType.DMA]


def tail_body(o_ref, dqkv_ref, o_old, dy_ref, o_new, dqkv_new, full, mine, other, pair, landed, own_o, own_d,
              os_sem, or_sem, oo_sem, ds_sem, dr_sem, do_sem, ps_sem, pr_sem, rs_sem, rr_sem, as_sem, ar_sem, fs_sem, fr_sem, *, peers):
    ring = peers // 2
    me = lax.axis_index("sp")
    z, c = me // 2, me % 2
    half = full.shape[-1] // 2
    cols = (pl.ds(0, half), pl.ds(half, half))
    at = lambda zz, cc: {"sp": 2 * zz + cc}
    turn = lambda k: lax.rem(z + k + 2 * ring, ring)
    step = (1, -1)
    remote = functools.partial(pltpu.make_async_remote_copy, device_id_type=pl.DeviceIdType.MESH)
    meet(peers)
    swap_start(o_ref, o_new, own_o, os_sem, or_sem, oo_sem, peers)
    swap_start(dqkv_ref, dqkv_new, own_d, ds_sem, dr_sem, do_sem, peers)
    swap_wait(o_ref, o_new, own_o, os_sem, or_sem, oo_sem, peers)

    def product(out, side):
        @pl.loop(0, ring)
        def _(k):
            h = 2 * k + side
            out[k] = (jnp.dot(o_old[h], dy_ref[0], preferred_element_type=F32)
                      + jnp.dot(o_new[h], dy_ref[1], preferred_element_type=F32))

    product(other, 1 - c)
    to_pair = remote(src_ref=other, dst_ref=pair, send_sem=ps_sem, recv_sem=pr_sem, device_id=at(z, 1 - c))
    product(mine, c)
    to_pair.start()
    to_pair.wait()

    @pl.loop(0, ring)
    def _(k):
        mine[k] = mine[k] + pair[k]

    def reduce_copy(w, t):
        return remote(src_ref=mine.at[turn(-step[w] * (1 + t)), :, cols[w]], dst_ref=landed.at[w, t],
                      send_sem=rs_sem.at[w, t], recv_sem=rr_sem.at[w, t], device_id=at(turn(step[w]), c))

    def add(w, t, k):
        reduce_copy(w, t).wait_recv()
        mine[k, :, cols[w]] = mine[k, :, cols[w]] + landed[w, t]

    for w in range(2):
        reduce_copy(w, 0).start()

    @pl.loop(1, ring - 1)
    def _(t):
        for w in range(2):
            add(w, t - 1, turn(-step[w] * (1 + t)))
            reduce_copy(w, t).start()

    for w in range(2):
        add(w, ring - 2, z)

    def gather_copy(w, t):
        k = turn(-step[w] * t)
        return remote(src_ref=full.at[k, c, :, cols[w]], dst_ref=full.at[k, c, :, cols[w]],
                      send_sem=as_sem.at[w, t], recv_sem=ar_sem.at[w, t], device_id=at(turn(step[w]), c))

    def over_copy(w, t):
        k = turn(-step[w] * t)
        return remote(src_ref=full.at[k, c, :, cols[w]], dst_ref=full.at[k, c, :, cols[w]],
                      send_sem=fs_sem.at[w, t], recv_sem=fr_sem.at[w, t], device_id=at(z, 1 - c))

    full[z, c] = mine[z]
    for w in range(2):
        gather_copy(w, 0).start()
    for w in range(2):
        over_copy(w, 0).start()

    @pl.loop(1, ring)
    def _(t):
        for w in range(2):
            gather_copy(w, t - 1).wait_recv()

            @pl.when(t < ring - 1)
            def _():
                gather_copy(w, t).start()

            over_copy(w, t).start()

    swap_wait(dqkv_ref, dqkv_new, own_d, ds_sem, dr_sem, do_sem, peers)

    @pl.loop(0, ring - 1)
    def _(t):
        for w in range(2):
            reduce_copy(w, t).wait_send()
            gather_copy(w, t).wait_send()

    @pl.loop(0, ring)
    def _(t):
        for w in range(2):
            over_copy(w, t).wait_send()
            remote(src_ref=full.at[turn(-step[w] * t), 1 - c, :, cols[w]], dst_ref=full.at[turn(-step[w] * t), 1 - c, :, cols[w]],
                   send_sem=fs_sem.at[w, t], recv_sem=fr_sem.at[w, t], device_id=at(z, 1 - c)).wait_recv()


def tail(o, dqkv, o_old, dy, collective_id):
    peers, dim, tok = o.shape
    ring = peers // 2
    hidden = dy.shape[-1]
    hbm, vmem = pl.BlockSpec(memory_space=pltpu.HBM), pl.BlockSpec(memory_space=pltpu.VMEM)
    dma = pltpu.SemaphoreType.DMA
    rows = lambda *lead: pltpu.VMEM(lead + (dim, hidden), F32)
    return pl.pallas_call(
        functools.partial(tail_body, peers=peers),
        name="tail",
        out_shape=[jax.ShapeDtypeStruct(o.shape, BF16), jax.ShapeDtypeStruct(dqkv.shape, BF16),
                   jax.ShapeDtypeStruct((ring, 2, dim, hidden), F32)],
        in_specs=[hbm, hbm, vmem, vmem],
        out_specs=[vmem, hbm, vmem],
        scratch_shapes=[rows(ring), rows(ring), rows(ring), pltpu.VMEM((2, ring - 1, dim, hidden // 2), F32),
                        pltpu.VMEM(o.shape[1:], BF16), pltpu.VMEM(dqkv.shape[1:], BF16),
                        dma((peers - 1,)), dma((peers - 1,)), dma, dma((peers - 1,)), dma((peers - 1,)), dma, dma, dma,
                        dma((2, ring - 1)), dma((2, ring - 1)), dma((2, ring - 1)), dma((2, ring - 1)), dma((2, ring)), dma((2, ring))],
        cost_estimate=pl.CostEstimate(flops=10**11, bytes_accessed=64 << 20, transcendentals=0),
        compiler_params=pltpu.CompilerParams(collective_id=collective_id, has_side_effects=True, vmem_limit_bytes=48 << 20),
    )(o, dqkv, o_old, dy)


def swap_body(*refs, peers, n):
    ins, outs, scratch = refs[:n], refs[n:2 * n], refs[2 * n:]
    meet(peers)
    for k in range(n):
        swap_start(ins[k], outs[k], *scratch[4 * k:4 * k + 4], peers)
    for k in range(n):
        swap_wait(ins[k], outs[k], *scratch[4 * k:4 * k + 4], peers)


def swap(xs, collective_id, name):
    hbm = pl.BlockSpec(memory_space=pltpu.HBM)
    peers = xs[0].shape[0]
    return pl.pallas_call(
        functools.partial(swap_body, peers=peers, n=len(xs)),
        name=name,
        out_shape=[jax.ShapeDtypeStruct(x.shape, x.dtype) for x in xs],
        in_specs=[hbm] * len(xs),
        out_specs=[hbm] * len(xs),
        scratch_shapes=sum((swap_scratch(x) for x in xs), []),
        cost_estimate=pl.CostEstimate(flops=24000 * sum(x.size for x in xs), bytes_accessed=4 * sum(x.size for x in xs), transcendentals=0),
        compiler_params=pltpu.CompilerParams(collective_id=collective_id, has_side_effects=True, vmem_limit_bytes=48 << 20),
    )(*xs)


def exchange_body(x_ref, out_ref, send_sem, recv_sem, *, peers):
    me = lax.axis_index("sp")
    meet(peers)
    copies = [pltpu.make_async_remote_copy(
        src_ref=x_ref, dst_ref=out_ref.at[me], send_sem=send_sem.at[d - 1], recv_sem=recv_sem.at[d - 1],
        device_id=peer_at(d, peers), device_id_type=pl.DeviceIdType.MESH) for d in range(1, peers)]
    for copy in copies:
        copy.start()
    out_ref[me] = x_ref[...]
    for copy in copies:
        copy.wait()


def exchange(x, peers, collective_id, name):
    return pl.pallas_call(
        functools.partial(exchange_body, peers=peers),
        name=name,
        out_shape=jax.ShapeDtypeStruct((peers,) + x.shape, x.dtype),
        in_specs=[pl.BlockSpec(memory_space=pltpu.VMEM)],
        out_specs=pl.BlockSpec(memory_space=pltpu.VMEM),
        scratch_shapes=[pltpu.SemaphoreType.DMA((peers - 1,)), pltpu.SemaphoreType.DMA((peers - 1,))],
        compiler_params=pltpu.CompilerParams(collective_id=collective_id, has_side_effects=True, vmem_limit_bytes=8 << 20),
    )(x)


def copy_body(x_ref, *refs):
    refs[-1][...] = x_ref[...]


def keep_copy(x):
    spec = pl.BlockSpec((x.shape[0] // 8,) + x.shape[1:], lambda i: (i,) + (0,) * (x.ndim - 1))
    return pl.pallas_call(
        copy_body, name="keep_copy", out_shape=jax.ShapeDtypeStruct(x.shape, x.dtype), grid=(8,), in_specs=[spec], out_specs=spec,
        cost_estimate=pl.CostEstimate(flops=10**9, bytes_accessed=8 * x.size, transcendentals=0))(x)


def place(x, into, lanes, first):
    heads, n, dim, hidden = x.shape
    args, in_specs, alias = (x,), [pl.BlockSpec((1, n, dim, hidden), lambda i: (i, 0, 0, 0))], {}
    if into is not None:
        args, in_specs, alias = (x, into), in_specs + [pl.BlockSpec(memory_space=pltpu.HBM)], {1: 0}
    return pl.pallas_call(
        copy_body, name="place", out_shape=jax.ShapeDtypeStruct((heads, lanes, dim, hidden), x.dtype), grid=(heads,),
        in_specs=in_specs, out_specs=pl.BlockSpec((1, n, dim, hidden), lambda i: (i, first // n, 0, 0)), input_output_aliases=alias,
        cost_estimate=pl.CostEstimate(flops=10**9, bytes_accessed=8 * x.size, transcendentals=0))(*args)


def norm_forward(x_blk, ln_gain, ln_bias):
    x_f32 = x_blk.astype(F32)
    centered = x_f32 - jnp.mean(x_f32, axis=-1, keepdims=True)
    inv_std = lax.rsqrt(jnp.mean(centered * centered, axis=-1, keepdims=True) + NORM_EPS)
    x_hat = centered * inv_std
    return x_f32, x_hat, inv_std, (x_hat * ln_gain + ln_bias).astype(BF16)


def solution(mesh):
    peers = mesh.shape["sp"]

    def block_fn(x_blk, pos_blk, keep_blk, ln_gain, ln_bias, w_qkv, b_qkv, w_out, b_out, dy_blk):
        batch, tok, hidden = x_blk.shape
        heads, dim = w_qkv.shape[1], w_qkv.shape[3]
        assert heads == peers
        seq = tok * peers
        blk = 2 * tok
        rank = lax.axis_index("sp")
        x_f32, x_hat, inv_std, x_norm = norm_forward(x_blk, ln_gain, ln_bias)
        xf = [lax.all_gather(x_norm[0], "sp", axis=0, tiled=True)]
        marks = exchange(jnp.concatenate([pos_blk, keep_blk, jnp.zeros((8 - 2 * batch, tok), jnp.int32)]), peers, 0, "marks")
        do_loc = [lax.dot_general(w_out, dy_blk[b], NT, preferred_element_type=F32).astype(BF16).reshape(heads, dim, tok) for b in range(batch)]
        do_t = swap(do_loc, 1, "swap_do")
        for b in range(1, batch):
            xn, _ = lax.optimization_barrier((x_norm[b], xf[-1]))
            xf.append(lax.all_gather(xn, "sp", axis=0, tiled=True))
        w_t = jnp.transpose(w_qkv, (1, 2, 3, 0))
        w_head = lax.dynamic_index_in_dim(w_t, rank, 0, keepdims=False).reshape(3 * dim, hidden)
        b_head = lax.dynamic_index_in_dim(b_qkv, rank, 0, keepdims=False).reshape(3 * dim, 1)
        slope = jnp.exp2(-8.0 * (rank + 1).astype(F32) / heads)
        slope2 = (slope * LOG2E).reshape(1)
        gw = jnp.zeros((3, dim, hidden), F32)
        gb = jnp.zeros((3 * dim,), F32)
        att, got = [], []
        for b in range(batch):
            pos = marks[:, b].reshape(seq).astype(F32)
            keep = marks[:, batch + b].reshape(seq)
            posk = jnp.broadcast_to(jnp.where(keep > 0, pos, MASKED)[:, None], (seq, 128))
            pref = jnp.broadcast_to(pos[::blk][:, None], (seq // blk, 128))
            qkvt = (lax.dot_general(w_head, xf[b], NT, preferred_element_type=F32) + b_head).astype(BF16)
            if b:
                slope2, gw = lax.optimization_barrier((slope2, gw))
                cur, prev = attention(slope2, qkvt, do_t[b], posk, pref, blk=blk, tok=tok, old=att[-1], collective_id=2 + b)
                got.append(prev)
            else:
                cur, _ = attention(slope2, qkvt, do_t[b], posk, pref, blk=blk, tok=tok)
            att.append(cur)
            gw += jnp.einsum("pdt,pth->dh", cur[1].reshape(peers, 3 * dim, tok), xf[b].reshape(peers, tok, hidden), preferred_element_type=F32).reshape(3, dim, hidden)
            gb += jnp.sum(cur[1].astype(F32), axis=(0, 3)).reshape(3 * dim)
        cut = 2
        gw_all = [lax.all_gather(gw[:cut], "sp", axis=0)]
        gw_all.append(lax.all_gather(gw[cut:], "sp", axis=0))
        o_last, dqkv_last, _ = lax.optimization_barrier((*att[-1], gw))
        o_new, dqkv_new, go_all = tail(o_last, dqkv_last, got[0][0], dy_blk, 2)
        got.append((o_new, dqkv_new))
        y, gx, gg, gbias = [], [], 0.0, 0.0
        for b in range(batch):
            o_t = got[b][0].reshape(hidden, tok)
            dqkv_t = got[b][1].reshape(3 * hidden, tok)
            y.append((x_f32[b] + lax.dot_general(o_t, w_out, (((0,), (0,)), ((), ())), preferred_element_type=F32) + b_out).astype(BF16))
            d_norm = lax.dot_general(dqkv_t, w_t.reshape(3 * hidden, hidden), (((0,), (0,)), ((), ())), preferred_element_type=F32)
            gg += jnp.sum(d_norm * x_hat[b], axis=0)
            gbias += jnp.sum(d_norm, axis=0)
            d_hat = d_norm * ln_gain
            d_mean = jnp.mean(d_hat, axis=-1, keepdims=True)
            d_proj = jnp.mean(d_hat * x_hat[b], axis=-1, keepdims=True)
            gx.append((dy_blk[b].astype(F32) + inv_std[b] * (d_hat - d_mean - x_hat[b] * d_proj)).astype(BF16))
        g_out = jnp.sum(dy_blk.astype(F32), axis=(0, 1))
        rows = jnp.stack([gg, gbias, g_out, jnp.pad(gb, (0, hidden - 3 * dim))] + [jnp.zeros((hidden,), F32)] * 4)
        sums = exchange(rows, peers, 4, "sums")
        total = jnp.sum(sums[:, :3], axis=0)
        gb_all = sums[:, 3, :3 * dim].reshape(heads, 3, dim)
        go_all = keep_copy(go_all.reshape(hidden, hidden))
        first, _, _, _ = lax.optimization_barrier((gw_all[0], go_all, y, gx))
        gw_out = place(first, None, 3, 0)
        gw_out = place(gw_all[1], gw_out, 3, cut)
        gw_out = jnp.transpose(gw_out, (3, 0, 1, 2))
        return jnp.stack(y), jnp.stack(gx), gw_out, gb_all, go_all, total[2], total[0], total[1]

    act_spec = P("dp", "sp", None)
    tok_spec = P("dp", "sp")
    in_specs = (act_spec, tok_spec, tok_spec, P(), P(), P(), P(), P(), P(), act_spec)
    out_specs = (act_spec, act_spec, P("dp", None, None, None), P("dp", None, None), P("dp", None), P("dp"), P("dp"), P("dp"))
    return jax.shard_map(block_fn, mesh=mesh, in_specs=in_specs, out_specs=out_specs, check_vma=False)
```

```python
import functools
import jax
import jax.numpy as jnp
from jax import lax
from jax.experimental import pallas as pl
from jax.experimental.pallas import tpu as pltpu
from jax.sharding import PartitionSpec as P

NORM_EPS = 1e-5

LOG2E = 1.4426950408889634
MASKED = -1e30
F32, BF16 = jnp.float32, jnp.bfloat16
NT = (((1,), (1,)), ((), ()))


def attn_body(slope_ref, w_ref, b_ref, x_ref, dot_ref, posk_ref, pref_ref, gw_old, *refs, blk, tok, n_swap):
    peers = dot_ref.shape[0]
    old, (o_ref, dqkv_ref, gw_ref), got = refs[:n_swap], refs[n_swap:n_swap + 3], refs[n_swap + 3:2 * n_swap + 3]
    swaps = [(old[k], got[k]) + refs[len(refs) - 4 * n_swap + 4 * k:][:4] for k in range(n_swap)]
    x_buf, qkvt_ref, k_tok, v_tok, s_buf, q_pad, do_pad, o_acc, dq_acc, dk_acc, dv_acc, x_sem = refs[2 * n_swap + 3:][:12]
    dim = dot_ref.shape[1]
    seq = dot_ref.shape[0] * tok
    pad = k_tok.shape[1] - dim
    nq = blk // tok
    scale = dim ** -0.5
    i = pl.program_id(0)
    half = blk // 2

    def x_copy(k):
        rows = pl.ds(pl.multiple_of(k * blk, blk), blk)
        return pltpu.make_async_copy(x_ref.at[rows], x_buf.at[rows], x_sem.at[k])

    @pl.when(i == 0)
    def _():
        for k in range(seq // blk):
            x_copy(k).start()
        if n_swap:
            meet(peers)
            for one in swaps:
                swap_start(*one, peers)
        dk_acc[...] = jnp.zeros_like(dk_acc)
        dv_acc[...] = jnp.zeros_like(dv_acc)
        q_pad[...] = jnp.zeros_like(q_pad)
        do_pad[...] = jnp.zeros_like(do_pad)

    qcols = pl.ds(pl.multiple_of(i * blk, blk), blk)
    x_copy(i).wait()
    qkvt_ref[:, qcols] = (lax.dot_general(w_ref[...], x_buf[qcols, :], NT, preferred_element_type=F32) + b_ref[...]).astype(BF16)

    @pl.loop(0, blk // 128)
    def _(t):
        cols = pl.ds(pl.multiple_of(i * blk + t * 128, 128), 128)
        for base, dst in ((dim, k_tok), (2 * dim, v_tok)):
            part = qkvt_ref[base:base + dim, cols].astype(F32)
            whole = jnp.concatenate([part, jnp.zeros((pad, 128), F32)], axis=0)
            dst[cols, :] = jnp.transpose(whole).astype(BF16)

    q_pad[0:dim, :] = qkvt_ref[0:dim, qcols]
    for t in range(nq):
        do_pad[0:dim, t * tok:(t + 1) * tok] = dot_ref[i * nq + t]
    slope2 = slope_ref[0]
    ref_pos = pref_ref[pl.ds(i, 1), :]
    c = scale * LOG2E

    def scores(j, m8, diag):
        for sub in range(2):
            rows = pl.ds(pl.multiple_of(j * blk + sub * half, half), half)
            st = jnp.dot(k_tok[rows, :], q_pad[...], preferred_element_type=F32)
            bias = (posk_ref[rows, :] - ref_pos) * slope2
            st = st * c + jnp.concatenate([bias] * (blk // 128), axis=1)
            if diag:
                key = lax.broadcasted_iota(jnp.int32, (half, blk), 0) + sub * half
                qry = lax.broadcasted_iota(jnp.int32, (half, blk), 1)
                st = jnp.where(key <= qry, st, MASKED)
            s_buf[rows, :] = st
            m8 = jnp.maximum(m8, jnp.max(st.reshape(half // 8, 8, blk), axis=0))
        return m8

    m8 = lax.fori_loop(0, i, lambda j, m: scores(j, m, False), jnp.full((8, blk), MASKED, F32))
    m8 = scores(i, m8, True)
    m = jnp.max(m8, axis=0, keepdims=True)

    def exps(j, l8):
        for sub in range(2):
            rows = pl.ds(pl.multiple_of(j * blk + sub * half, half), half)
            e = jnp.exp2(s_buf[rows, :] - m)
            s_buf[rows, :] = e
            l8 = l8 + jnp.sum(e.reshape(half // 8, 8, blk), axis=0)
        return l8

    l8 = lax.fori_loop(0, i + 1, exps, jnp.zeros((8, blk), F32))
    inv = 1.0 / jnp.sum(l8, axis=0, keepdims=True)
    o_acc[...] = jnp.zeros_like(o_acc)
    dq_acc[...] = jnp.zeros_like(dq_acc)

    def values(j, _):
        rows = pl.ds(pl.multiple_of(j * blk, blk), blk)
        p = s_buf[rows, :] * inv
        s_buf[rows, :] = p
        pb = p.astype(BF16)
        o_acc[...] += jnp.dot(qkvt_ref[2 * dim:3 * dim, rows], pb, preferred_element_type=F32)
        dv_acc[:, rows] += lax.dot_general(do_pad[0:dim, :], pb, NT, preferred_element_type=F32)
        return 0

    lax.fori_loop(0, i + 1, values, 0)
    o_lo = o_acc[...].astype(BF16)
    do_f = do_pad[0:dim, :].astype(F32)
    r = jnp.sum(do_f * o_lo.astype(F32), axis=0, keepdims=True)

    def grads(j, _):
        rows = pl.ds(pl.multiple_of(j * blk, blk), blk)
        g = jnp.dot(v_tok[rows, :], do_pad[...], preferred_element_type=F32)
        ds = (s_buf[rows, :] * (g - r)).astype(BF16)
        dq_acc[...] += jnp.dot(qkvt_ref[dim:2 * dim, rows], ds, preferred_element_type=F32)
        dk_acc[:, rows] += lax.dot_general(q_pad[0:dim, :], ds, NT, preferred_element_type=F32)
        return 0

    lax.fori_loop(0, i + 1, grads, 0)
    dq_lo = (dq_acc[...] * scale).astype(BF16)
    for t in range(nq):
        o_ref[i * nq + t] = o_lo[:, t * tok:(t + 1) * tok]
        dqkv_ref[i * nq + t, 0] = dq_lo[:, t * tok:(t + 1) * tok]

    @pl.when(i == pl.num_programs(0) - 1)
    def _():
        @pl.loop(0, seq // tok)
        def _(t):
            cols = pl.ds(pl.multiple_of(t * tok, tok), tok)
            dqkv_ref[t, 1] = (dk_acc[:, cols] * scale).astype(BF16)
            dqkv_ref[t, 2] = dv_acc[:, cols].astype(BF16)

        gw_ref[...] = gw_old[...]

        @pl.loop(0, seq // blk)
        def _(j):
            total = gw_ref[...]
            for t in range(nq):
                rows = pl.ds(pl.multiple_of(j * blk + t * tok, tok), tok)
                total = total + jnp.dot(dqkv_ref[j * nq + t].reshape(3 * dim, tok), x_buf[rows, :], preferred_element_type=F32)
            gw_ref[...] = total

        for one in swaps:
            swap_wait(*one, peers)


def attention(slope2, w_head, b_head, x, dot_, posk, pref, gw, old, *, blk, tok, collective_id):
    blocks, dim, _ = dot_.shape
    seq, hidden = x.shape
    wide = 128 * pl.cdiv(dim, 128)
    hbm = pl.BlockSpec(memory_space=pltpu.HBM)
    full = lambda a: pl.BlockSpec(a.shape, lambda i: (0,) * len(a.shape), pipeline_mode=pl.Buffered(1))
    like = lambda a: jax.ShapeDtypeStruct(a.shape, a.dtype)
    outs = [jax.ShapeDtypeStruct((blocks, dim, tok), BF16), jax.ShapeDtypeStruct((blocks, 3, dim, tok), BF16), like(gw)]
    pairs = (seq // blk) * (seq // blk + 1) // 2
    res = pl.pallas_call(
        functools.partial(attn_body, blk=blk, tok=tok, n_swap=len(old)),
        name="attention",
        out_shape=outs + [like(a) for a in old],
        grid=(seq // blk,),
        in_specs=[pl.BlockSpec(memory_space=pltpu.SMEM), full(w_head), full(b_head), hbm, full(dot_), full(posk), full(pref), full(gw)]
        + [hbm] * len(old),
        out_specs=[full(a) for a in outs] + [hbm] * len(old),
        scratch_shapes=[
            pltpu.VMEM((seq, hidden), BF16), pltpu.VMEM((3 * dim, seq), BF16),
            pltpu.VMEM((seq, wide), BF16), pltpu.VMEM((seq, wide), BF16),
            pltpu.VMEM((seq, blk), F32),
            pltpu.VMEM((wide, blk), BF16), pltpu.VMEM((wide, blk), BF16),
            pltpu.VMEM((dim, blk), F32), pltpu.VMEM((dim, blk), F32),
            pltpu.VMEM((dim, seq), F32), pltpu.VMEM((dim, seq), F32), pltpu.SemaphoreType.DMA((seq // blk,))]
        + sum((swap_scratch(a) for a in old), []),
        cost_estimate=pl.CostEstimate(flops=pairs * 6 * 2 * blk * blk * 256, bytes_accessed=24 << 20, transcendentals=pairs * blk * blk),
        compiler_params=pltpu.CompilerParams(dimension_semantics=("arbitrary",), vmem_limit_bytes=52 << 20,
                                             collective_id=collective_id, has_side_effects=True),
    )(slope2, w_head, b_head, x, dot_, posk, pref, gw, *old)
    return res[:2], res[2], res[3:]


def peer_at(d, peers):
    return {"sp": lax.rem(lax.axis_index("sp") + d, peers)}


def meet(peers):
    barrier = pltpu.get_barrier_semaphore()
    for d in range(1, peers):
        pl.semaphore_signal(barrier, inc=1, device_id=peer_at(d, peers), device_id_type=pl.DeviceIdType.MESH)
    pl.semaphore_wait(barrier, peers - 1)


def swap_copies(x_ref, out_ref, send_sem, recv_sem, peers):
    me = lax.axis_index("sp")
    order = [d for near in range(peers // 2) for d in sorted({peers // 2 - near, peers // 2 + near})]
    return [pltpu.make_async_remote_copy(
        src_ref=x_ref.at[lax.rem(me + d, peers)], dst_ref=out_ref.at[me], send_sem=send_sem.at[d - 1], recv_sem=recv_sem.at[d - 1],
        device_id=peer_at(d, peers), device_id_type=pl.DeviceIdType.MESH) for d in order]


def swap_start(x_ref, out_ref, own, send_sem, recv_sem, own_sem, peers):
    me = lax.axis_index("sp")
    for copy in swap_copies(x_ref, out_ref, send_sem, recv_sem, peers):
        copy.start()
    take = pltpu.make_async_copy(x_ref.at[me], own, own_sem)
    take.start()
    take.wait()
    pltpu.make_async_copy(own, out_ref.at[me], own_sem).start()


def swap_wait(x_ref, out_ref, own, send_sem, recv_sem, own_sem, peers):
    pltpu.make_async_copy(own, out_ref.at[lax.axis_index("sp")], own_sem).wait()
    for copy in swap_copies(x_ref, out_ref, send_sem, recv_sem, peers):
        copy.wait()


def swap_scratch(x):
    peers = x.shape[0]
    return [pltpu.VMEM(x.shape[1:], x.dtype), pltpu.SemaphoreType.DMA((peers - 1,)), pltpu.SemaphoreType.DMA((peers - 1,)),
            pltpu.SemaphoreType.DMA]


def tail_body(o_ref, dqkv_ref, o_old, dy_ref, o_new, dqkv_new, part, mine, other, pair, landed, own_o, own_d,
              os_sem, or_sem, oo_sem, ds_sem, dr_sem, do_sem, ps_sem, pr_sem, rs_sem, rr_sem, *, peers):
    ring = peers // 2
    me = lax.axis_index("sp")
    z, c = me // 2, me % 2
    half = part.shape[-1] // 2
    cols = (pl.ds(0, half), pl.ds(half, half))
    at = lambda zz, cc: {"sp": 2 * zz + cc}
    turn = lambda k: lax.rem(z + k + 2 * ring, ring)
    step = (1, -1)
    remote = functools.partial(pltpu.make_async_remote_copy, device_id_type=pl.DeviceIdType.MESH)
    meet(peers)
    swap_start(o_ref, o_new, own_o, os_sem, or_sem, oo_sem, peers)
    swap_start(dqkv_ref, dqkv_new, own_d, ds_sem, dr_sem, do_sem, peers)
    swap_wait(o_ref, o_new, own_o, os_sem, or_sem, oo_sem, peers)

    def product(out, side):
        @pl.loop(0, ring)
        def _(k):
            h = 2 * k + side
            out[k] = (jnp.dot(o_old[h], dy_ref[0], preferred_element_type=F32)
                      + jnp.dot(o_new[h], dy_ref[1], preferred_element_type=F32))

    product(other, 1 - c)
    to_pair = remote(src_ref=other, dst_ref=pair, send_sem=ps_sem, recv_sem=pr_sem, device_id=at(z, 1 - c))
    product(mine, c)
    to_pair.start()
    to_pair.wait()

    @pl.loop(0, ring)
    def _(k):
        mine[k] = mine[k] + pair[k]

    def reduce_copy(w, t):
        return remote(src_ref=mine.at[turn(-step[w] * (1 + t)), :, cols[w]], dst_ref=landed.at[w, t],
                      send_sem=rs_sem.at[w, t], recv_sem=rr_sem.at[w, t], device_id=at(turn(step[w]), c))

    def add(w, t, k):
        reduce_copy(w, t).wait_recv()
        mine[k, :, cols[w]] = mine[k, :, cols[w]] + landed[w, t]

    for w in range(2):
        reduce_copy(w, 0).start()

    @pl.loop(1, ring - 1)
    def _(t):
        for w in range(2):
            add(w, t - 1, turn(-step[w] * (1 + t)))
            reduce_copy(w, t).start()

    for w in range(2):
        add(w, ring - 2, z)

    part[...] = mine[z]
    swap_wait(dqkv_ref, dqkv_new, own_d, ds_sem, dr_sem, do_sem, peers)

    @pl.loop(0, ring - 1)
    def _(t):
        for w in range(2):
            reduce_copy(w, t).wait_send()


def tail(o, dqkv, o_old, dy, collective_id):
    peers, dim, tok = o.shape
    ring = peers // 2
    hidden = dy.shape[-1]
    hbm, vmem = pl.BlockSpec(memory_space=pltpu.HBM), pl.BlockSpec(memory_space=pltpu.VMEM)
    dma = pltpu.SemaphoreType.DMA
    rows = lambda *lead: pltpu.VMEM(lead + (dim, hidden), F32)
    return pl.pallas_call(
        functools.partial(tail_body, peers=peers),
        name="tail",
        out_shape=[jax.ShapeDtypeStruct(o.shape, BF16), jax.ShapeDtypeStruct(dqkv.shape, BF16),
                   jax.ShapeDtypeStruct((dim, hidden), F32)],
        in_specs=[hbm, hbm, vmem, vmem],
        out_specs=[vmem, hbm, vmem],
        scratch_shapes=[rows(ring), rows(ring), rows(ring), pltpu.VMEM((2, ring - 1, dim, hidden // 2), F32),
                        pltpu.VMEM(o.shape[1:], BF16), pltpu.VMEM(dqkv.shape[1:], BF16),
                        dma((peers - 1,)), dma((peers - 1,)), dma, dma((peers - 1,)), dma((peers - 1,)), dma, dma, dma,
                        dma((2, ring - 1)), dma((2, ring - 1))],
        cost_estimate=pl.CostEstimate(flops=10**11, bytes_accessed=64 << 20, transcendentals=0),
        compiler_params=pltpu.CompilerParams(collective_id=collective_id, has_side_effects=True, vmem_limit_bytes=48 << 20),
    )(o, dqkv, o_old, dy)


def collect_body(part, rows_ref, full, sums, as_sem, ar_sem, fs_sem, fr_sem, xs_sem, xr_sem, *, peers):
    ring = peers // 2
    me = lax.axis_index("sp")
    z, c = me // 2, me % 2
    half = part.shape[-1] // 2
    cols = (pl.ds(0, half), pl.ds(half, half))
    turn = lambda k: lax.rem(z + k + 2 * ring, ring)
    step = (1, -1)
    remote = functools.partial(pltpu.make_async_remote_copy, device_id_type=pl.DeviceIdType.MESH)

    def block_copy(w, t, side, send_sem, recv_sem, to):
        ref = full.at[turn(-step[w] * t), side, :, cols[w]]
        return remote(src_ref=ref, dst_ref=ref, send_sem=send_sem.at[w, t], recv_sem=recv_sem.at[w, t], device_id={"sp": to})

    gather_copy = lambda w, t: block_copy(w, t, c, as_sem, ar_sem, 2 * turn(step[w]) + c)
    over_copy = lambda w, t, side: block_copy(w, t, side, fs_sem, fr_sem, 2 * z + 1 - c)
    full[z, c] = part[...]
    meet(peers)
    small = [remote(src_ref=rows_ref, dst_ref=sums.at[me], send_sem=xs_sem.at[d - 1], recv_sem=xr_sem.at[d - 1],
                    device_id=peer_at(d, peers)) for d in range(1, peers)]
    for copy in small:
        copy.start()
    for w in range(2):
        gather_copy(w, 0).start()
    for w in range(2):
        over_copy(w, 0, c).start()
    sums[me] = rows_ref[...]

    @pl.loop(1, ring)
    def _(t):
        for w in range(2):
            gather_copy(w, t - 1).wait_recv()

            @pl.when(t < ring - 1)
            def _():
                gather_copy(w, t).start()

            over_copy(w, t, c).start()

    for copy in small:
        copy.wait()

    @pl.loop(0, ring - 1)
    def _(t):
        for w in range(2):
            gather_copy(w, t).wait_send()

    @pl.loop(0, ring)
    def _(t):
        for w in range(2):
            over_copy(w, t, c).wait_send()
            over_copy(w, t, 1 - c).wait_recv()


def collect(part, rows, peers, collective_id):
    ring = peers // 2
    vmem = pl.BlockSpec(memory_space=pltpu.VMEM)
    dma = pltpu.SemaphoreType.DMA
    return pl.pallas_call(
        functools.partial(collect_body, peers=peers),
        name="collect",
        out_shape=[jax.ShapeDtypeStruct((ring, 2) + part.shape, F32), jax.ShapeDtypeStruct((peers,) + rows.shape, F32)],
        in_specs=[vmem, vmem],
        out_specs=[vmem, vmem],
        scratch_shapes=[dma((2, ring - 1)), dma((2, ring - 1)), dma((2, ring)), dma((2, ring)), dma((peers - 1,)), dma((peers - 1,))],
        cost_estimate=pl.CostEstimate(flops=5 * 10**10, bytes_accessed=10 << 20, transcendentals=0),
        compiler_params=pltpu.CompilerParams(collective_id=collective_id, has_side_effects=True, vmem_limit_bytes=24 << 20),
    )(part, rows)


def swap_body(*refs, peers, n):
    ins, outs, scratch = refs[:n], refs[n:2 * n], refs[2 * n:]
    meet(peers)
    for k in range(n):
        swap_start(ins[k], outs[k], *scratch[4 * k:4 * k + 4], peers)
    for k in range(n):
        swap_wait(ins[k], outs[k], *scratch[4 * k:4 * k + 4], peers)


def swap(xs, collective_id, name):
    hbm = pl.BlockSpec(memory_space=pltpu.HBM)
    peers = xs[0].shape[0]
    return pl.pallas_call(
        functools.partial(swap_body, peers=peers, n=len(xs)),
        name=name,
        out_shape=[jax.ShapeDtypeStruct(x.shape, x.dtype) for x in xs],
        in_specs=[hbm] * len(xs),
        out_specs=[hbm] * len(xs),
        scratch_shapes=sum((swap_scratch(x) for x in xs), []),
        cost_estimate=pl.CostEstimate(flops=24000 * sum(x.size for x in xs), bytes_accessed=4 * sum(x.size for x in xs), transcendentals=0),
        compiler_params=pltpu.CompilerParams(collective_id=collective_id, has_side_effects=True, vmem_limit_bytes=48 << 20),
    )(*xs)


def exchange_body(x_ref, out_ref, send_sem, recv_sem, *, peers):
    me = lax.axis_index("sp")
    meet(peers)
    copies = [pltpu.make_async_remote_copy(
        src_ref=x_ref, dst_ref=out_ref.at[me], send_sem=send_sem.at[d - 1], recv_sem=recv_sem.at[d - 1],
        device_id=peer_at(d, peers), device_id_type=pl.DeviceIdType.MESH) for d in range(1, peers)]
    for copy in copies:
        copy.start()
    out_ref[me] = x_ref[...]
    for copy in copies:
        copy.wait()


def exchange(x, peers, collective_id, name):
    return pl.pallas_call(
        functools.partial(exchange_body, peers=peers),
        name=name,
        out_shape=jax.ShapeDtypeStruct((peers,) + x.shape, x.dtype),
        in_specs=[pl.BlockSpec(memory_space=pltpu.VMEM)],
        out_specs=pl.BlockSpec(memory_space=pltpu.VMEM),
        scratch_shapes=[pltpu.SemaphoreType.DMA((peers - 1,)), pltpu.SemaphoreType.DMA((peers - 1,))],
        compiler_params=pltpu.CompilerParams(collective_id=collective_id, has_side_effects=True, vmem_limit_bytes=8 << 20),
    )(x)


def place_body(*refs, first):
    x_ref, (out_ref, buf, in_sem, out_sem) = refs[0], refs[-4:]
    heads, n = x_ref.shape[:2]
    reads = [pltpu.make_async_copy(x_ref.at[h], buf.at[h], in_sem.at[h]) for h in range(heads)]
    writes = [pltpu.make_async_copy(buf.at[h], out_ref.at[h, pl.ds(first, n)], out_sem.at[h]) for h in range(heads)]
    for copy in reads:
        copy.start()
    for read, write in zip(reads, writes):
        read.wait()
        write.start()
    for copy in writes:
        copy.wait()


def place(x, into, lanes, first):
    heads, n, dim, hidden = x.shape
    hbm = pl.BlockSpec(memory_space=pltpu.HBM)
    args, alias = ((x,), {}) if into is None else ((x, into), {1: 0})
    dma = pltpu.SemaphoreType.DMA
    return pl.pallas_call(
        functools.partial(place_body, first=first), name="place",
        out_shape=jax.ShapeDtypeStruct((heads, lanes, dim, hidden), x.dtype),
        in_specs=[hbm] * len(args), out_specs=hbm, input_output_aliases=alias,
        scratch_shapes=[pltpu.VMEM(x.shape, x.dtype), dma((heads,)), dma((heads,))],
        cost_estimate=pl.CostEstimate(flops=10**9, bytes_accessed=8 * x.size, transcendentals=0),
        compiler_params=pltpu.CompilerParams(vmem_limit_bytes=60 << 20))(*args)


def lay_body(x_ref, out_ref, sem):
    copies = [pltpu.make_async_copy(x_ref.at[k], out_ref.at[k], sem.at[k]) for k in range(x_ref.shape[0])]
    for copy in copies:
        copy.start()
    for copy in copies:
        copy.wait()


def lay_down(x):
    return pl.pallas_call(
        lay_body, name="lay_down", out_shape=jax.ShapeDtypeStruct(x.shape, x.dtype),
        in_specs=[pl.BlockSpec(memory_space=pltpu.VMEM)], out_specs=pl.BlockSpec(memory_space=pltpu.HBM),
        scratch_shapes=[pltpu.SemaphoreType.DMA((x.shape[0],))],
        cost_estimate=pl.CostEstimate(flops=10**9, bytes_accessed=8 * x.size, transcendentals=0),
        compiler_params=pltpu.CompilerParams(vmem_limit_bytes=24 << 20))(x)


def norm_forward(x_blk, ln_gain, ln_bias):
    x_f32 = x_blk.astype(F32)
    centered = x_f32 - jnp.mean(x_f32, axis=-1, keepdims=True)
    inv_std = lax.rsqrt(jnp.mean(centered * centered, axis=-1, keepdims=True) + NORM_EPS)
    x_hat = centered * inv_std
    return x_f32, x_hat, inv_std, (x_hat * ln_gain + ln_bias).astype(BF16)


def solution(mesh):
    peers = mesh.shape["sp"]

    def block_fn(x_blk, pos_blk, keep_blk, ln_gain, ln_bias, w_qkv, b_qkv, w_out, b_out, dy_blk):
        batch, tok, hidden = x_blk.shape
        heads, dim = w_qkv.shape[1], w_qkv.shape[3]
        assert heads == peers
        seq = tok * peers
        blk = 2 * tok
        rank = lax.axis_index("sp")
        x_f32, x_hat, inv_std, x_norm = norm_forward(x_blk, ln_gain, ln_bias)
        xf = [lax.all_gather(x_norm[0], "sp", axis=0, tiled=True)]
        marks = exchange(jnp.concatenate([pos_blk, keep_blk, jnp.zeros((8 - 2 * batch, tok), jnp.int32)]), peers, 0, "marks")
        do_loc = [lax.dot_general(w_out, dy_blk[b], NT, preferred_element_type=F32).astype(BF16).reshape(heads, dim, tok) for b in range(batch)]
        do_t = list(swap(do_loc[:1], 1, "swap_do"))
        for b in range(1, batch):
            xf.append(lax.all_gather(x_norm[b], "sp", axis=0, tiled=True))
        w_t = jnp.transpose(w_qkv, (1, 2, 3, 0))
        w_head = lax.dynamic_index_in_dim(w_t, rank, 0, keepdims=False).reshape(3 * dim, hidden)
        b_head = lax.dynamic_index_in_dim(b_qkv, rank, 0, keepdims=False).reshape(3 * dim, 1)
        slope = jnp.exp2(-8.0 * (rank + 1).astype(F32) / heads)
        slope2 = (slope * LOG2E).reshape(1)
        gw = jnp.zeros((3 * dim, hidden), F32)
        gb = jnp.zeros((3 * dim,), F32)
        att, got = [], []
        for b in range(batch):
            pos = marks[:, b].reshape(seq).astype(F32)
            keep = marks[:, batch + b].reshape(seq)
            posk = jnp.broadcast_to(jnp.where(keep > 0, pos, MASKED)[:, None], (seq, 128))
            pref = jnp.broadcast_to(pos[::blk][:, None], (seq // blk, 128))
            old = list(do_loc[b + 1:b + 2]) + (list(att[-1]) if b else [])
            cur, gw, swapped = attention(slope2, w_head, b_head, xf[b], do_t[b], posk, pref, gw, old, blk=blk, tok=tok, collective_id=4 + b)
            if b + 1 < batch:
                do_t.append(swapped[0])
            if b:
                got.append(swapped[-2:])
            att.append(cur)
        cut = 2
        gw3 = gw.reshape(3, dim, hidden)
        gw_all = [lax.all_gather(gw3[:cut], "sp", axis=0), lax.all_gather(gw3[cut:], "sp", axis=0)]
        o_last, dqkv_last, _ = lax.optimization_barrier((*att[-1], gw3))
        o_new, dqkv_new, part = tail(o_last, dqkv_last, got[0][0], dy_blk, 2)
        got.append((o_new, dqkv_new))
        late, _ = lax.optimization_barrier(([cur[1] for cur in att], part))
        gb = sum(jnp.sum(one.astype(F32), axis=(0, 3)).reshape(3 * dim) for one in late)
        y, gx, gg, gbias = [], [], 0.0, 0.0
        for b in range(batch):
            o_t = got[b][0].reshape(hidden, tok)
            dqkv_t = got[b][1].reshape(3 * hidden, tok)
            y.append((x_f32[b] + lax.dot_general(o_t, w_out, (((0,), (0,)), ((), ())), preferred_element_type=F32) + b_out).astype(BF16))
            d_norm = lax.dot_general(dqkv_t, w_t.reshape(3 * hidden, hidden), (((0,), (0,)), ((), ())), preferred_element_type=F32)
            gg += jnp.sum(d_norm * x_hat[b], axis=0)
            gbias += jnp.sum(d_norm, axis=0)
            d_hat = d_norm * ln_gain
            d_mean = jnp.mean(d_hat, axis=-1, keepdims=True)
            d_proj = jnp.mean(d_hat * x_hat[b], axis=-1, keepdims=True)
            gx.append((dy_blk[b].astype(F32) + inv_std[b] * (d_hat - d_mean - x_hat[b] * d_proj)).astype(BF16))
        g_out = jnp.sum(dy_blk.astype(F32), axis=(0, 1))
        rows = jnp.stack([gg, gbias, g_out, jnp.pad(gb, (0, hidden - 3 * dim))] + [jnp.zeros((hidden,), F32)] * 4)
        y, gx = jnp.stack(y), jnp.stack(gx)
        first, _, _ = lax.optimization_barrier((gw_all[0], y, gx))
        gw_out = place(first, None, 3, 0)
        rows, gw_out = lax.optimization_barrier((rows, gw_out))
        go_all, sums = collect(part, rows, peers, 3)
        go_all = lay_down(go_all.reshape(heads, dim, hidden)).reshape(hidden, hidden)
        total = jnp.sum(sums[:, :3], axis=0)
        gb_all = sums[:, 3, :3 * dim].reshape(heads, 3, dim)
        second, go_all = lax.optimization_barrier((gw_all[1], go_all))
        gw_out = jnp.transpose(place(second, gw_out, 3, cut), (3, 0, 1, 2))
        return y, gx, gw_out, gb_all, go_all, total[2], total[0], total[1]

    act_spec = P("dp", "sp", None)
    tok_spec = P("dp", "sp")
    in_specs = (act_spec, tok_spec, tok_spec, P(), P(), P(), P(), P(), P(), act_spec)
    out_specs = (act_spec, act_spec, P("dp", None, None, None), P("dp", None, None), P("dp", None), P("dp"), P("dp"), P("dp"))
    return jax.shard_map(block_fn, mesh=mesh, in_specs=in_specs, out_specs=out_specs, check_vma=False)
```

```python
import functools
import jax
import jax.numpy as jnp
from jax import lax
from jax.experimental import pallas as pl
from jax.experimental.pallas import tpu as pltpu
from jax.sharding import PartitionSpec as P

NORM_EPS = 1e-5

LOG2E = 1.4426950408889634
MASKED = -1e30
F32, BF16 = jnp.float32, jnp.bfloat16
NT = (((1,), (1,)), ((), ()))


def attn_body(slope_ref, w_ref, b_ref, x_ref, dot_ref, pos_ref, pref_ref, *refs, blk, tok, n_swap, n_old):
    peers = dot_ref.shape[0]
    gw_old, old, refs = refs[:n_old], refs[n_old:n_old + n_swap], refs[n_old + n_swap:]
    (dqkv_ref, gwa_ref, gwb_ref, o_new), got, refs = refs[:4], refs[4:4 + n_swap], refs[4 + n_swap:]
    x_buf, qkvt_ref, k_tok, v_tok, posk_ref, s_buf, q_pad, do_pad, o_acc, dq_acc, dk_acc, dv_acc, o_ref, x_sem, os_sem, or_sem = refs[:16]
    swaps = [(old[k], got[k]) + refs[16 + 4 * k:20 + 4 * k] for k in range(n_swap)]
    dim = dot_ref.shape[1]
    seq = dot_ref.shape[0] * tok
    pad = k_tok.shape[1] - dim
    nq = blk // tok
    steps = seq // blk
    scale = dim ** -0.5
    me = lax.axis_index("sp")
    step = pl.program_id(0)
    i = lax.rem(me // nq + step, steps)
    half = blk // 2

    def x_copy(k):
        rows = pl.ds(pl.multiple_of(k * blk, blk), blk)
        return pltpu.make_async_copy(x_ref.at[rows], x_buf.at[rows], x_sem.at[k])

    def o_send(to):
        return pltpu.make_async_remote_copy(
            src_ref=o_ref.at[to], dst_ref=o_new.at[me], send_sem=os_sem.at[to], recv_sem=or_sem.at[me],
            device_id={"sp": to}, device_id_type=pl.DeviceIdType.MESH)

    def o_keep():
        return pltpu.make_async_copy(o_ref.at[me], o_new.at[me], os_sem.at[me])

    def o_start(at):
        for t in range(nq):
            to = lax.rem(me // nq + at, steps) * nq + t

            @pl.when(to != me)
            def _():
                o_send(to).start()

            @pl.when(to == me)
            def _():
                o_keep().start()

    @pl.when(step == 0)
    def _():
        for k in range(steps):
            x_copy(k).start()
        meet(peers)
        for one in swaps:
            swap_start(*one, peers)
        dk_acc[...] = jnp.zeros_like(dk_acc)
        dv_acc[...] = jnp.zeros_like(dv_acc)
        q_pad[...] = jnp.zeros_like(q_pad)
        do_pad[...] = jnp.zeros_like(do_pad)

        @pl.loop(0, steps)
        def _(k):
            rows = pl.ds(pl.multiple_of(k * blk, blk), blk)
            x_copy(k).wait()
            qkvt_ref[:, rows] = (lax.dot_general(w_ref[...], x_buf[rows, :], NT, preferred_element_type=F32) + b_ref[...]).astype(BF16)

            @pl.loop(0, blk // 128)
            def _(t):
                cols = pl.ds(pl.multiple_of(k * blk + t * 128, 128), 128)
                for base, dst in ((dim, k_tok), (2 * dim, v_tok)):
                    part = qkvt_ref[base:base + dim, cols].astype(F32)
                    whole = jnp.concatenate([part, jnp.zeros((pad, 128), F32)], axis=0)
                    dst[cols, :] = jnp.transpose(whole).astype(BF16)
                posk_ref[cols, :] = jnp.transpose(jnp.broadcast_to(pos_ref[:, cols], (128, 128)))

    @pl.when(step > 0)
    def _():
        o_start(step - 1)

    qcols = pl.ds(pl.multiple_of(i * blk, blk), blk)
    q_pad[0:dim, :] = qkvt_ref[0:dim, qcols]
    for t in range(nq):
        do_pad[0:dim, t * tok:(t + 1) * tok] = dot_ref[i * nq + t]
    slope2 = slope_ref[0]
    ref_pos = pref_ref[pl.ds(i, 1), :]
    c = scale * LOG2E

    def scores(j, m8, diag):
        for sub in range(2):
            rows = pl.ds(pl.multiple_of(j * blk + sub * half, half), half)
            st = jnp.dot(k_tok[rows, :], q_pad[...], preferred_element_type=F32)
            bias = (posk_ref[rows, :] - ref_pos) * slope2
            st = st * c + jnp.concatenate([bias] * (blk // 128), axis=1)
            if diag:
                key = lax.broadcasted_iota(jnp.int32, (half, blk), 0) + sub * half
                qry = lax.broadcasted_iota(jnp.int32, (half, blk), 1)
                st = jnp.where(key <= qry, st, MASKED)
            s_buf[rows, :] = st
            m8 = jnp.maximum(m8, jnp.max(st.reshape(half // 8, 8, blk), axis=0))
        return m8

    m8 = lax.fori_loop(0, i, lambda j, m: scores(j, m, False), jnp.full((8, blk), MASKED, F32))
    m8 = scores(i, m8, True)
    m = jnp.max(m8, axis=0, keepdims=True)

    def exps(j, l8):
        for sub in range(2):
            rows = pl.ds(pl.multiple_of(j * blk + sub * half, half), half)
            e = jnp.exp2(s_buf[rows, :] - m)
            s_buf[rows, :] = e
            l8 = l8 + jnp.sum(e.reshape(half // 8, 8, blk), axis=0)
        return l8

    l8 = lax.fori_loop(0, i + 1, exps, jnp.zeros((8, blk), F32))
    inv = 1.0 / jnp.sum(l8, axis=0, keepdims=True)
    o_acc[...] = jnp.zeros_like(o_acc)
    dq_acc[...] = jnp.zeros_like(dq_acc)

    def values(j, _):
        rows = pl.ds(pl.multiple_of(j * blk, blk), blk)
        p = s_buf[rows, :] * inv
        s_buf[rows, :] = p
        pb = p.astype(BF16)
        o_acc[...] += jnp.dot(qkvt_ref[2 * dim:3 * dim, rows], pb, preferred_element_type=F32)
        dv_acc[:, rows] += lax.dot_general(do_pad[0:dim, :], pb, NT, preferred_element_type=F32)
        return 0

    lax.fori_loop(0, i + 1, values, 0)
    o_lo = o_acc[...].astype(BF16)
    do_f = do_pad[0:dim, :].astype(F32)
    r = jnp.sum(do_f * o_lo.astype(F32), axis=0, keepdims=True)

    def grads(j, _):
        rows = pl.ds(pl.multiple_of(j * blk, blk), blk)
        g = jnp.dot(v_tok[rows, :], do_pad[...], preferred_element_type=F32)
        ds = (s_buf[rows, :] * (g - r)).astype(BF16)
        dq_acc[...] += jnp.dot(qkvt_ref[dim:2 * dim, rows], ds, preferred_element_type=F32)
        dk_acc[:, rows] += lax.dot_general(q_pad[0:dim, :], ds, NT, preferred_element_type=F32)
        return 0

    lax.fori_loop(0, i + 1, grads, 0)
    dq_lo = (dq_acc[...] * scale).astype(BF16)
    for t in range(nq):
        o_ref[i * nq + t] = o_lo[:, t * tok:(t + 1) * tok]
        dqkv_ref[i * nq + t, 0] = dq_lo[:, t * tok:(t + 1) * tok]

    @pl.when(step == steps - 1)
    def _():
        @pl.loop(0, seq // tok)
        def _(t):
            cols = pl.ds(pl.multiple_of(t * tok, tok), tok)
            dqkv_ref[t, 1] = (dk_acc[:, cols] * scale).astype(BF16)
            dqkv_ref[t, 2] = dv_acc[:, cols].astype(BF16)

        o_start(step)
        if n_old:
            gwa_ref[...] = gw_old[0][...]
            gwb_ref[...] = gw_old[1][...]
        else:
            gwa_ref[...] = jnp.zeros_like(gwa_ref)
            gwb_ref[...] = jnp.zeros_like(gwb_ref)

        @pl.loop(0, steps)
        def _(j):
            rows = pl.ds(pl.multiple_of(j * blk, blk), blk)
            for ref, lo, n in ((gwa_ref, 0, 2), (gwb_ref, 2, 1)):
                lhs = jnp.concatenate([dqkv_ref[j * nq + t, lo:lo + n].reshape(n * dim, tok) for t in range(nq)], axis=1)
                ref[...] += jnp.dot(lhs, x_buf[rows, :], preferred_element_type=F32)

        o_keep().wait()
        for d in range(1, peers):
            o_send(lax.rem(me + d, peers)).wait_send()
            frm = lax.rem(me + d, peers)
            pltpu.make_async_remote_copy(
                src_ref=o_ref.at[frm], dst_ref=o_new.at[frm], send_sem=os_sem.at[frm], recv_sem=or_sem.at[frm],
                device_id={"sp": frm}, device_id_type=pl.DeviceIdType.MESH).wait_recv()
        for one in swaps:
            swap_wait(*one, peers)


def attention(slope2, w_head, b_head, x, dot_, pos, pref, gw, old, *, blk, tok, collective_id):
    blocks, dim, _ = dot_.shape
    seq, hidden = x.shape
    wide = 128 * pl.cdiv(dim, 128)
    hbm = pl.BlockSpec(memory_space=pltpu.HBM)
    full = lambda a: pl.BlockSpec(a.shape, lambda i: (0,) * len(a.shape), pipeline_mode=pl.Buffered(1))
    like = lambda a: jax.ShapeDtypeStruct(a.shape, a.dtype)
    outs = [jax.ShapeDtypeStruct((blocks, 3, dim, tok), BF16), jax.ShapeDtypeStruct((2 * dim, hidden), F32),
            jax.ShapeDtypeStruct((dim, hidden), F32)]
    pairs = (seq // blk) * (seq // blk + 1) // 2
    dma = pltpu.SemaphoreType.DMA
    res = pl.pallas_call(
        functools.partial(attn_body, blk=blk, tok=tok, n_swap=len(old), n_old=len(gw)),
        name="attention",
        out_shape=outs + [like(dot_)] + [like(a) for a in old],
        grid=(seq // blk,),
        in_specs=[pl.BlockSpec(memory_space=pltpu.SMEM), full(w_head), full(b_head), hbm, full(dot_), full(pos), full(pref)]
        + [full(a) for a in gw] + [hbm] * len(old),
        out_specs=[full(a) for a in outs] + [hbm] * (1 + len(old)),
        scratch_shapes=[
            pltpu.VMEM((seq, hidden), BF16), pltpu.VMEM((3 * dim, seq), BF16),
            pltpu.VMEM((seq, wide), BF16), pltpu.VMEM((seq, wide), BF16), pltpu.VMEM((seq, 128), F32),
            pltpu.VMEM((seq, blk), F32),
            pltpu.VMEM((wide, blk), BF16), pltpu.VMEM((wide, blk), BF16),
            pltpu.VMEM((dim, blk), F32), pltpu.VMEM((dim, blk), F32),
            pltpu.VMEM((dim, seq), F32), pltpu.VMEM((dim, seq), F32), pltpu.VMEM(dot_.shape, BF16),
            dma((seq // blk,)), dma((blocks,)), dma((blocks,))]
        + sum((swap_scratch(a) for a in old), []),
        cost_estimate=pl.CostEstimate(flops=pairs * 6 * 2 * blk * blk * 256, bytes_accessed=24 << 20, transcendentals=pairs * blk * blk),
        compiler_params=pltpu.CompilerParams(dimension_semantics=("arbitrary",), vmem_limit_bytes=52 << 20,
                                             collective_id=collective_id, has_side_effects=True),
    )(slope2, w_head, b_head, x, dot_, pos, pref, *gw, *old)
    return res[0], res[1:3], res[3], res[4:]


def peer_at(d, peers):
    return {"sp": lax.rem(lax.axis_index("sp") + d, peers)}


def meet(peers):
    barrier = pltpu.get_barrier_semaphore()
    for d in range(1, peers):
        pl.semaphore_signal(barrier, inc=1, device_id=peer_at(d, peers), device_id_type=pl.DeviceIdType.MESH)
    pl.semaphore_wait(barrier, peers - 1)


def swap_copies(x_ref, out_ref, send_sem, recv_sem, peers):
    me = lax.axis_index("sp")
    order = [d for near in range(peers // 2) for d in sorted({peers // 2 - near, peers // 2 + near})]
    return [pltpu.make_async_remote_copy(
        src_ref=x_ref.at[lax.rem(me + d, peers)], dst_ref=out_ref.at[me], send_sem=send_sem.at[d - 1], recv_sem=recv_sem.at[d - 1],
        device_id=peer_at(d, peers), device_id_type=pl.DeviceIdType.MESH) for d in order]


def swap_start(x_ref, out_ref, own, send_sem, recv_sem, own_sem, peers):
    me = lax.axis_index("sp")
    for copy in swap_copies(x_ref, out_ref, send_sem, recv_sem, peers):
        copy.start()
    take = pltpu.make_async_copy(x_ref.at[me], own, own_sem)
    take.start()
    take.wait()
    pltpu.make_async_copy(own, out_ref.at[me], own_sem).start()


def swap_wait(x_ref, out_ref, own, send_sem, recv_sem, own_sem, peers):
    pltpu.make_async_copy(own, out_ref.at[lax.axis_index("sp")], own_sem).wait()
    for copy in swap_copies(x_ref, out_ref, send_sem, recv_sem, peers):
        copy.wait()


def swap_scratch(x):
    peers = x.shape[0]
    return [pltpu.VMEM(x.shape[1:], x.dtype), pltpu.SemaphoreType.DMA((peers - 1,)), pltpu.SemaphoreType.DMA((peers - 1,)),
            pltpu.SemaphoreType.DMA]


def tail_body(dqkv_ref, o_old, o_new, dy_ref, dqkv_new, part, mine, other, pair, landed, own_d, ds_sem, dr_sem, do_sem, ps_sem, pr_sem, rs_sem, rr_sem, *, peers):
    ring = peers // 2
    me = lax.axis_index("sp")
    z, c = me // 2, me % 2
    half = part.shape[-1] // 2
    cols = (pl.ds(0, half), pl.ds(half, half))
    at = lambda zz, cc: {"sp": 2 * zz + cc}
    turn = lambda k: lax.rem(z + k + 2 * ring, ring)
    step = (1, -1)
    remote = functools.partial(pltpu.make_async_remote_copy, device_id_type=pl.DeviceIdType.MESH)
    meet(peers)
    swap_start(dqkv_ref, dqkv_new, own_d, ds_sem, dr_sem, do_sem, peers)

    def product(out, side):
        @pl.loop(0, ring)
        def _(k):
            h = 2 * k + side
            out[k] = (jnp.dot(o_old[h], dy_ref[0], preferred_element_type=F32)
                      + jnp.dot(o_new[h], dy_ref[1], preferred_element_type=F32))

    product(other, 1 - c)
    to_pair = remote(src_ref=other, dst_ref=pair, send_sem=ps_sem, recv_sem=pr_sem, device_id=at(z, 1 - c))
    product(mine, c)
    to_pair.start()
    to_pair.wait()

    @pl.loop(0, ring)
    def _(k):
        mine[k] = mine[k] + pair[k]

    def reduce_copy(w, t):
        return remote(src_ref=mine.at[turn(-step[w] * (1 + t)), :, cols[w]], dst_ref=landed.at[w, t],
                      send_sem=rs_sem.at[w, t], recv_sem=rr_sem.at[w, t], device_id=at(turn(step[w]), c))

    def add(w, t, k):
        reduce_copy(w, t).wait_recv()
        mine[k, :, cols[w]] = mine[k, :, cols[w]] + landed[w, t]

    for w in range(2):
        reduce_copy(w, 0).start()

    @pl.loop(1, ring - 1)
    def _(t):
        for w in range(2):
            add(w, t - 1, turn(-step[w] * (1 + t)))
            reduce_copy(w, t).start()

    for w in range(2):
        add(w, ring - 2, z)

    part[...] = mine[z]
    swap_wait(dqkv_ref, dqkv_new, own_d, ds_sem, dr_sem, do_sem, peers)

    @pl.loop(0, ring - 1)
    def _(t):
        for w in range(2):
            reduce_copy(w, t).wait_send()


def tail(dqkv, o_old, o_new, dy, collective_id):
    peers, dim, tok = o_old.shape
    ring = peers // 2
    hidden = dy.shape[-1]
    hbm, vmem = pl.BlockSpec(memory_space=pltpu.HBM), pl.BlockSpec(memory_space=pltpu.VMEM)
    dma = pltpu.SemaphoreType.DMA
    rows = lambda *lead: pltpu.VMEM(lead + (dim, hidden), F32)
    return pl.pallas_call(
        functools.partial(tail_body, peers=peers),
        name="tail",
        out_shape=[jax.ShapeDtypeStruct(dqkv.shape, BF16), jax.ShapeDtypeStruct((dim, hidden), F32)],
        in_specs=[hbm, vmem, vmem, vmem],
        out_specs=[hbm, vmem],
        scratch_shapes=[rows(ring), rows(ring), rows(ring), pltpu.VMEM((2, ring - 1, dim, hidden // 2), F32),
                        pltpu.VMEM(dqkv.shape[1:], BF16), dma((peers - 1,)), dma((peers - 1,)), dma, dma, dma,
                        dma((2, ring - 1)), dma((2, ring - 1))],
        cost_estimate=pl.CostEstimate(flops=10**11, bytes_accessed=64 << 20, transcendentals=0),
        compiler_params=pltpu.CompilerParams(collective_id=collective_id, has_side_effects=True, vmem_limit_bytes=48 << 20),
    )(dqkv, o_old, o_new, dy)


def collect_body(part, rows_ref, full, sums, as_sem, ar_sem, fs_sem, fr_sem, xs_sem, xr_sem, *, peers, cuts):
    ring = peers // 2
    me = lax.axis_index("sp")
    z, c = me // 2, me % 2
    half = part.shape[-1] // 2
    few = part.shape[0] // cuts
    turn = lambda k: lax.rem(z + k + 2 * ring, ring)
    step = (1, -1)
    remote = functools.partial(pltpu.make_async_remote_copy, device_id_type=pl.DeviceIdType.MESH)

    def block_copy(w, t, u, side, send_sem, recv_sem, to):
        ref = full.at[turn(-step[w] * t), side, pl.ds(u * few, few), pl.ds(w * half, half)]
        return remote(src_ref=ref, dst_ref=ref, send_sem=send_sem.at[w, t, u], recv_sem=recv_sem.at[w, t, u], device_id={"sp": to})

    gather_copy = lambda w, t, u: block_copy(w, t, u, c, as_sem, ar_sem, 2 * turn(step[w]) + c)
    over_copy = lambda w, t, u, side: block_copy(w, t, u, side, fs_sem, fr_sem, 2 * z + 1 - c)
    parts = [(w, u) for u in range(cuts) for w in range(2)]
    full[z, c] = part[...]
    sums[me] = rows_ref[...]
    meet(peers)
    for w, u in parts:
        gather_copy(w, 0, u).start()
    small = [remote(src_ref=rows_ref, dst_ref=sums.at[me], send_sem=xs_sem.at[d - 1], recv_sem=xr_sem.at[d - 1],
                    device_id=peer_at(d, peers)) for d in range(1, peers)]
    for copy in small:
        copy.start()
    for w, u in parts:
        over_copy(w, 0, u, c).start()

    @pl.loop(1, ring)
    def _(t):
        for w, u in parts:
            gather_copy(w, t - 1, u).wait_recv()

            @pl.when(t < ring - 1)
            def _():
                gather_copy(w, t, u).start()

            over_copy(w, t, u, c).start()

    for copy in small:
        copy.wait()

    @pl.loop(0, ring - 1)
    def _(t):
        for w, u in parts:
            gather_copy(w, t, u).wait_send()

    @pl.loop(0, ring)
    def _(t):
        for w, u in parts:
            over_copy(w, t, u, c).wait_send()
            over_copy(w, t, u, 1 - c).wait_recv()


def collect(part, rows, peers, collective_id, cuts=3):
    ring = peers // 2
    vmem = pl.BlockSpec(memory_space=pltpu.VMEM)
    dma = pltpu.SemaphoreType.DMA
    return pl.pallas_call(
        functools.partial(collect_body, peers=peers, cuts=cuts),
        name="collect",
        out_shape=[jax.ShapeDtypeStruct((ring, 2) + part.shape, F32), jax.ShapeDtypeStruct((peers,) + rows.shape, F32)],
        in_specs=[vmem, vmem],
        out_specs=[vmem, vmem],
        scratch_shapes=[dma((2, ring - 1, cuts)), dma((2, ring - 1, cuts)), dma((2, ring, cuts)), dma((2, ring, cuts)), dma((peers - 1,)), dma((peers - 1,))],
        cost_estimate=pl.CostEstimate(flops=5 * 10**10, bytes_accessed=10 << 20, transcendentals=0),
        compiler_params=pltpu.CompilerParams(collective_id=collective_id, has_side_effects=True, vmem_limit_bytes=24 << 20),
    )(part, rows)


def swap_body(*refs, peers, n):
    ins, outs, scratch = refs[:n], refs[n:2 * n], refs[2 * n:]
    meet(peers)
    for k in range(n):
        swap_start(ins[k], outs[k], *scratch[4 * k:4 * k + 4], peers)
    for k in range(n):
        swap_wait(ins[k], outs[k], *scratch[4 * k:4 * k + 4], peers)


def swap(xs, collective_id, name):
    hbm = pl.BlockSpec(memory_space=pltpu.HBM)
    peers = xs[0].shape[0]
    return pl.pallas_call(
        functools.partial(swap_body, peers=peers, n=len(xs)),
        name=name,
        out_shape=[jax.ShapeDtypeStruct(x.shape, x.dtype) for x in xs],
        in_specs=[hbm] * len(xs),
        out_specs=[hbm] * len(xs),
        scratch_shapes=sum((swap_scratch(x) for x in xs), []),
        cost_estimate=pl.CostEstimate(flops=24000 * sum(x.size for x in xs), bytes_accessed=4 * sum(x.size for x in xs), transcendentals=0),
        compiler_params=pltpu.CompilerParams(collective_id=collective_id, has_side_effects=True, vmem_limit_bytes=48 << 20),
    )(*xs)


def exchange_body(x_ref, out_ref, send_sem, recv_sem, *, peers):
    me = lax.axis_index("sp")
    meet(peers)
    copies = [pltpu.make_async_remote_copy(
        src_ref=x_ref, dst_ref=out_ref.at[me], send_sem=send_sem.at[d - 1], recv_sem=recv_sem.at[d - 1],
        device_id=peer_at(d, peers), device_id_type=pl.DeviceIdType.MESH) for d in range(1, peers)]
    for copy in copies:
        copy.start()
    out_ref[me] = x_ref[...]
    for copy in copies:
        copy.wait()


def exchange(x, peers, collective_id, name):
    return pl.pallas_call(
        functools.partial(exchange_body, peers=peers),
        name=name,
        out_shape=jax.ShapeDtypeStruct((peers,) + x.shape, x.dtype),
        in_specs=[pl.BlockSpec(memory_space=pltpu.VMEM)],
        out_specs=pl.BlockSpec(memory_space=pltpu.VMEM),
        scratch_shapes=[pltpu.SemaphoreType.DMA((peers - 1,)), pltpu.SemaphoreType.DMA((peers - 1,))],
        compiler_params=pltpu.CompilerParams(collective_id=collective_id, has_side_effects=True, vmem_limit_bytes=8 << 20),
    )(x)


def place_body(*refs, first):
    x_ref, (out_ref, buf, in_sem, out_sem) = refs[0], refs[-4:]
    heads, n = x_ref.shape[:2]
    reads = [pltpu.make_async_copy(x_ref.at[h], buf.at[h], in_sem.at[h]) for h in range(heads)]
    writes = [pltpu.make_async_copy(buf.at[h], out_ref.at[h, pl.ds(first, n)], out_sem.at[h]) for h in range(heads)]
    for copy in reads:
        copy.start()
    for read, write in zip(reads, writes):
        read.wait()
        write.start()
    for copy in writes:
        copy.wait()


def place(x, into, lanes, first):
    heads, n, dim, hidden = x.shape
    hbm = pl.BlockSpec(memory_space=pltpu.HBM)
    args, alias = ((x,), {}) if into is None else ((x, into), {1: 0})
    dma = pltpu.SemaphoreType.DMA
    return pl.pallas_call(
        functools.partial(place_body, first=first), name="place",
        out_shape=jax.ShapeDtypeStruct((heads, lanes, dim, hidden), x.dtype),
        in_specs=[hbm] * len(args), out_specs=hbm, input_output_aliases=alias,
        scratch_shapes=[pltpu.VMEM(x.shape, x.dtype), dma((heads,)), dma((heads,))],
        cost_estimate=pl.CostEstimate(flops=10**9, bytes_accessed=8 * x.size, transcendentals=0),
        compiler_params=pltpu.CompilerParams(vmem_limit_bytes=60 << 20))(*args)


def lay_body(x_ref, out_ref, sem):
    copies = [pltpu.make_async_copy(x_ref.at[k], out_ref.at[k], sem.at[k]) for k in range(x_ref.shape[0])]
    for copy in copies:
        copy.start()
    for copy in copies:
        copy.wait()


def lay_down(x):
    return pl.pallas_call(
        lay_body, name="lay_down", out_shape=jax.ShapeDtypeStruct(x.shape, x.dtype),
        in_specs=[pl.BlockSpec(memory_space=pltpu.VMEM)], out_specs=pl.BlockSpec(memory_space=pltpu.HBM),
        scratch_shapes=[pltpu.SemaphoreType.DMA((x.shape[0],))],
        cost_estimate=pl.CostEstimate(flops=10**9, bytes_accessed=8 * x.size, transcendentals=0),
        compiler_params=pltpu.CompilerParams(vmem_limit_bytes=24 << 20))(x)


def norm_forward(x_blk, ln_gain, ln_bias):
    x_f32 = x_blk.astype(F32)
    centered = x_f32 - jnp.mean(x_f32, axis=-1, keepdims=True)
    inv_std = lax.rsqrt(jnp.mean(centered * centered, axis=-1, keepdims=True) + NORM_EPS)
    x_hat = centered * inv_std
    return x_f32, x_hat, inv_std, (x_hat * ln_gain + ln_bias).astype(BF16)


def solution(mesh):
    peers = mesh.shape["sp"]

    def block_fn(x_blk, pos_blk, keep_blk, ln_gain, ln_bias, w_qkv, b_qkv, w_out, b_out, dy_blk):
        batch, tok, hidden = x_blk.shape
        heads, dim = w_qkv.shape[1], w_qkv.shape[3]
        assert heads == peers
        seq = tok * peers
        blk = 2 * tok
        rank = lax.axis_index("sp")
        x_f32, x_hat, inv_std, x_norm = norm_forward(x_blk, ln_gain, ln_bias)
        xf = [lax.all_gather(x_norm[0], "sp", axis=0, tiled=True)]
        marks = exchange(jnp.concatenate([pos_blk, keep_blk, jnp.zeros((8 - 2 * batch, tok), jnp.int32)]), peers, 0, "marks")
        do_loc = [lax.dot_general(w_out, dy_blk[b], NT, preferred_element_type=F32).astype(BF16).reshape(heads, dim, tok) for b in range(batch)]
        do_t = list(swap(do_loc[:1], 1, "swap_do"))
        for b in range(1, batch):
            xf.append(lax.all_gather(x_norm[b], "sp", axis=0, tiled=True))
        w_t = jnp.transpose(w_qkv, (1, 2, 3, 0))
        w_head = lax.dynamic_index_in_dim(w_t, rank, 0, keepdims=False).reshape(3 * dim, hidden)
        b_head = lax.dynamic_index_in_dim(b_qkv, rank, 0, keepdims=False).reshape(3 * dim, 1)
        slope = jnp.exp2(-8.0 * (rank + 1).astype(F32) / heads)
        slope2 = (slope * LOG2E).reshape(1)
        gw, att, o_got, d_got = (), [], [], []
        for b in range(batch):
            pos = marks[:, b].reshape(1, seq).astype(F32)
            keep = marks[:, batch + b].reshape(1, seq)
            pref = jnp.broadcast_to(pos[0, ::blk][:, None], (seq // blk, 128))
            old = list(do_loc[b + 1:b + 2]) + att[b - 1:b]
            cur, gw, o_new, swapped = attention(slope2, w_head, b_head, xf[b], do_t[b], jnp.where(keep > 0, pos, MASKED), pref, gw, old,
                                                blk=blk, tok=tok, collective_id=4 + b)
            if b + 1 < batch:
                do_t.append(swapped[0])
            d_got += swapped[-1:] if b else []
            o_got.append(o_new)
            att.append(cur)
        gw_all = [lax.all_gather(one, "sp", axis=0, tiled=True).reshape(heads, -1, dim, hidden) for one in gw]
        cut = gw_all[0].shape[1]
        dqkv_new, part = tail(att[-1], *o_got, dy_blk, 2)
        d_got.append(dqkv_new)
        late, x_late, _ = lax.optimization_barrier((att, x_blk, part))
        gb = sum(jnp.sum(one.astype(F32), axis=(0, 3)).reshape(3 * dim) for one in late)
        y, gx, gg, gbias = [], [], 0.0, 0.0
        for b in range(batch):
            o_t = o_got[b].reshape(hidden, tok)
            dqkv_t = d_got[b].reshape(3 * hidden, tok)
            y.append((x_late[b].astype(F32) + lax.dot_general(o_t, w_out, (((0,), (0,)), ((), ())), preferred_element_type=F32) + b_out).astype(BF16))
            d_norm = lax.dot_general(dqkv_t, w_t.reshape(3 * hidden, hidden), (((0,), (0,)), ((), ())), preferred_element_type=F32)
            gg += jnp.sum(d_norm * x_hat[b], axis=0)
            gbias += jnp.sum(d_norm, axis=0)
            d_hat = d_norm * ln_gain
            d_mean = jnp.mean(d_hat, axis=-1, keepdims=True)
            d_proj = jnp.mean(d_hat * x_hat[b], axis=-1, keepdims=True)
            gx.append((dy_blk[b].astype(F32) + inv_std[b] * (d_hat - d_mean - x_hat[b] * d_proj)).astype(BF16))
        g_out = jnp.sum(dy_blk.astype(F32), axis=(0, 1))
        rows = jnp.stack([gg, gbias, g_out, jnp.pad(gb, (0, hidden - 3 * dim))] + [jnp.zeros((hidden,), F32)] * 4)
        y, gx = jnp.stack(y), jnp.stack(gx)
        first, _, _ = lax.optimization_barrier((gw_all[0], y, gx))
        gw_out = place(first, None, 3, 0)
        rows, gw_out = lax.optimization_barrier((rows, gw_out))
        go_all, sums = collect(part, rows, peers, 3)
        go_all = lay_down(go_all.reshape(heads, dim, hidden)).reshape(hidden, hidden)
        total = jnp.sum(sums[:, :3], axis=0)
        gb_all = sums[:, 3, :3 * dim].reshape(heads, 3, dim)
        second, go_all = lax.optimization_barrier((gw_all[1], go_all))
        gw_out = jnp.transpose(place(second, gw_out, 3, cut), (3, 0, 1, 2))
        return y, gx, gw_out, gb_all, go_all, total[2], total[0], total[1]

    act_spec = P("dp", "sp", None)
    tok_spec = P("dp", "sp")
    in_specs = (act_spec, tok_spec, tok_spec, P(), P(), P(), P(), P(), P(), act_spec)
    out_specs = (act_spec, act_spec, P("dp", None, None, None), P("dp", None, None), P("dp", None), P("dp"), P("dp"), P("dp"))
    return jax.shard_map(block_fn, mesh=mesh, in_specs=in_specs, out_specs=out_specs, check_vma=False)
```

```python
import functools
import jax
import jax.numpy as jnp
from jax import lax
from jax.experimental import pallas as pl
from jax.experimental.pallas import tpu as pltpu
from jax.sharding import PartitionSpec as P

NORM_EPS = 1e-5

LOG2E = 1.4426950408889634
MASKED = -1e30
F32, BF16 = jnp.float32, jnp.bfloat16
NT = (((1,), (1,)), ((), ()))


def attn_body(slope_ref, w_ref, b_ref, x_ref, dot_ref, pos_ref, pref_ref, *refs, blk, tok, n_swap, n_old, send_o):
    peers = dot_ref.shape[0]
    gw_old, old, refs = refs[:n_old], refs[n_old:n_old + n_swap], refs[n_old + n_swap:]
    (dqkv_ref, gwa_ref, gwb_ref, gb_ref, o_out), got, refs = refs[:5], refs[5:5 + n_swap], refs[5 + n_swap:]
    x_buf, qkvt_ref, k_tok, v_tok, posk_ref, s_buf, q_pad, do_pad, o_acc, dq_acc, dk_acc, dv_acc, x_sem = refs[:13]
    swaps = [(old[k], got[k]) + refs[13 + 4 * k:17 + 4 * k] for k in range(n_swap)]
    if send_o:
        o_ref, os_sem, or_sem = refs[-3:]
        o_new = o_out
    else:
        o_ref = o_out
    dim = dot_ref.shape[1]
    seq = dot_ref.shape[0] * tok
    pad = k_tok.shape[1] - dim
    nq = blk // tok
    steps = seq // blk
    scale = dim ** -0.5
    me = lax.axis_index("sp")
    step = pl.program_id(0)
    i = lax.rem(me // nq + step, steps)
    half = blk // 2

    def x_copy(k):
        rows = pl.ds(pl.multiple_of(k * blk, blk), blk)
        return pltpu.make_async_copy(x_ref.at[rows], x_buf.at[rows], x_sem.at[k])

    def o_send(to):
        return pltpu.make_async_remote_copy(
            src_ref=o_ref.at[to], dst_ref=o_new.at[me], send_sem=os_sem.at[to], recv_sem=or_sem.at[me],
            device_id={"sp": to}, device_id_type=pl.DeviceIdType.MESH)

    def o_keep():
        return pltpu.make_async_copy(o_ref.at[me], o_new.at[me], os_sem.at[me])

    def o_start(at):
        for t in range(nq):
            to = lax.rem(me // nq + at, steps) * nq + t

            @pl.when(to != me)
            def _():
                o_send(to).start()

            @pl.when(to == me)
            def _():
                o_keep().start()

    @pl.when(step == 0)
    def _():
        for k in range(steps):
            x_copy(k).start()
        meet(peers)
        for one in swaps:
            swap_start(*one, peers)
        dk_acc[...] = jnp.zeros_like(dk_acc)
        dv_acc[...] = jnp.zeros_like(dv_acc)
        q_pad[...] = jnp.zeros_like(q_pad)
        do_pad[...] = jnp.zeros_like(do_pad)

        @pl.loop(0, steps)
        def _(k):
            rows = pl.ds(pl.multiple_of(k * blk, blk), blk)
            x_copy(k).wait()
            qkvt_ref[:, rows] = (lax.dot_general(w_ref[...], x_buf[rows, :], NT, preferred_element_type=F32) + b_ref[...]).astype(BF16)

            @pl.loop(0, blk // 128)
            def _(t):
                cols = pl.ds(pl.multiple_of(k * blk + t * 128, 128), 128)
                for base, dst in ((dim, k_tok), (2 * dim, v_tok)):
                    part = qkvt_ref[base:base + dim, cols].astype(F32)
                    whole = jnp.concatenate([part, jnp.zeros((pad, 128), F32)], axis=0)
                    dst[cols, :] = jnp.transpose(whole).astype(BF16)
                posk_ref[cols, :] = jnp.transpose(jnp.broadcast_to(pos_ref[:, cols], (128, 128)))

    if send_o:
        @pl.when(step > 0)
        def _():
            o_start(step - 1)

    qcols = pl.ds(pl.multiple_of(i * blk, blk), blk)
    q_pad[0:dim, :] = qkvt_ref[0:dim, qcols]
    for t in range(nq):
        do_pad[0:dim, t * tok:(t + 1) * tok] = dot_ref[i * nq + t]
    slope2 = slope_ref[0]
    ref_pos = pref_ref[pl.ds(i, 1), :]
    c = scale * LOG2E

    def scores(j, m8, diag):
        for sub in range(2):
            rows = pl.ds(pl.multiple_of(j * blk + sub * half, half), half)
            st = jnp.dot(k_tok[rows, :], q_pad[...], preferred_element_type=F32)
            bias = (posk_ref[rows, :] - ref_pos) * slope2
            st = st * c + jnp.concatenate([bias] * (blk // 128), axis=1)
            if diag:
                key = lax.broadcasted_iota(jnp.int32, (half, blk), 0) + sub * half
                qry = lax.broadcasted_iota(jnp.int32, (half, blk), 1)
                st = jnp.where(key <= qry, st, MASKED)
            s_buf[rows, :] = st
            m8 = jnp.maximum(m8, jnp.max(st.reshape(half // 8, 8, blk), axis=0))
        return m8

    m8 = lax.fori_loop(0, i, lambda j, m: scores(j, m, False), jnp.full((8, blk), MASKED, F32))
    m8 = scores(i, m8, True)
    m = jnp.max(m8, axis=0, keepdims=True)

    def exps(j, l8):
        for sub in range(2):
            rows = pl.ds(pl.multiple_of(j * blk + sub * half, half), half)
            e = jnp.exp2(s_buf[rows, :] - m)
            s_buf[rows, :] = e
            l8 = l8 + jnp.sum(e.reshape(half // 8, 8, blk), axis=0)
        return l8

    l8 = lax.fori_loop(0, i + 1, exps, jnp.zeros((8, blk), F32))
    inv = 1.0 / jnp.sum(l8, axis=0, keepdims=True)
    o_acc[...] = jnp.zeros_like(o_acc)
    dq_acc[...] = jnp.zeros_like(dq_acc)

    def values(j, _):
        rows = pl.ds(pl.multiple_of(j * blk, blk), blk)
        p = s_buf[rows, :] * inv
        s_buf[rows, :] = p
        pb = p.astype(BF16)
        o_acc[...] += jnp.dot(qkvt_ref[2 * dim:3 * dim, rows], pb, preferred_element_type=F32)
        dv_acc[:, rows] += lax.dot_general(do_pad[0:dim, :], pb, NT, preferred_element_type=F32)
        return 0

    lax.fori_loop(0, i + 1, values, 0)
    o_lo = o_acc[...].astype(BF16)
    do_f = do_pad[0:dim, :].astype(F32)
    r = jnp.sum(do_f * o_lo.astype(F32), axis=0, keepdims=True)

    def grads(j, _):
        rows = pl.ds(pl.multiple_of(j * blk, blk), blk)
        g = jnp.dot(v_tok[rows, :], do_pad[...], preferred_element_type=F32)
        ds = (s_buf[rows, :] * (g - r)).astype(BF16)
        dq_acc[...] += jnp.dot(qkvt_ref[dim:2 * dim, rows], ds, preferred_element_type=F32)
        dk_acc[:, rows] += lax.dot_general(q_pad[0:dim, :], ds, NT, preferred_element_type=F32)
        return 0

    lax.fori_loop(0, i + 1, grads, 0)
    dq_lo = (dq_acc[...] * scale).astype(BF16)
    for t in range(nq):
        o_ref[i * nq + t] = o_lo[:, t * tok:(t + 1) * tok]
        dqkv_ref[i * nq + t, 0:dim] = dq_lo[:, t * tok:(t + 1) * tok]

    @pl.when(step == steps - 1)
    def _():
        @pl.loop(0, seq // tok)
        def _(t):
            cols = pl.ds(pl.multiple_of(t * tok, tok), tok)
            dqkv_ref[t, dim:2 * dim] = (dk_acc[:, cols] * scale).astype(BF16)
            dqkv_ref[t, 2 * dim:3 * dim] = dv_acc[:, cols].astype(BF16)

        if send_o:
            o_start(step)
        for k, ref in enumerate((gwa_ref, gwb_ref, gb_ref)):
            ref[...] = gw_old[k][...] if n_old else jnp.zeros_like(ref)
        ones = jnp.ones((blk, 128), BF16)

        @pl.loop(0, steps)
        def _(j):
            rows = pl.ds(pl.multiple_of(j * blk, blk), blk)
            for ref, lo, hi in ((gwa_ref, 0, 2 * dim), (gwb_ref, 2 * dim, 3 * dim)):
                lhs = jnp.concatenate([dqkv_ref[j * nq + t, lo:hi] for t in range(nq)], axis=1)
                ref[...] += jnp.dot(lhs, x_buf[rows, :], preferred_element_type=F32)
                gb_ref[lo:hi, :] += jnp.dot(lhs, ones, preferred_element_type=F32)

        if send_o:
            o_keep().wait()
            for d in range(1, peers):
                frm = lax.rem(me + d, peers)
                o_send(frm).wait_send()
                pltpu.make_async_remote_copy(
                    src_ref=o_ref.at[frm], dst_ref=o_new.at[frm], send_sem=os_sem.at[frm], recv_sem=or_sem.at[frm],
                    device_id={"sp": frm}, device_id_type=pl.DeviceIdType.MESH).wait_recv()
        for one in swaps:
            swap_wait(*one, peers)


def attention(slope2, w_head, b_head, x, dot_, pos, pref, gw, old, *, blk, tok, send_o, collective_id):
    blocks, dim, _ = dot_.shape
    seq, hidden = x.shape
    wide = 128 * pl.cdiv(dim, 128)
    hbm = pl.BlockSpec(memory_space=pltpu.HBM)
    full = lambda a: pl.BlockSpec(a.shape, lambda i: (0,) * len(a.shape), pipeline_mode=pl.Buffered(1))
    like = lambda a: jax.ShapeDtypeStruct(a.shape, a.dtype)
    outs = [jax.ShapeDtypeStruct((blocks, 3 * dim, tok), BF16), jax.ShapeDtypeStruct((2 * dim, hidden), F32),
            jax.ShapeDtypeStruct((dim, hidden), F32), jax.ShapeDtypeStruct((3 * dim, 128), F32)]
    pairs = (seq // blk) * (seq // blk + 1) // 2
    dma = pltpu.SemaphoreType.DMA
    res = pl.pallas_call(
        functools.partial(attn_body, blk=blk, tok=tok, n_swap=len(old), n_old=len(gw), send_o=send_o),
        name="attention",
        out_shape=outs + [like(dot_)] + [like(a) for a in old],
        grid=(seq // blk,),
        in_specs=[pl.BlockSpec(memory_space=pltpu.SMEM), full(w_head), full(b_head), hbm, full(dot_), full(pos), full(pref)]
        + [full(a) for a in gw] + [hbm] * len(old),
        out_specs=[full(a) for a in outs] + [hbm if send_o else full(dot_)] + [hbm] * len(old),
        scratch_shapes=[
            pltpu.VMEM((seq, hidden), BF16), pltpu.VMEM((3 * dim, seq), BF16),
            pltpu.VMEM((seq, wide), BF16), pltpu.VMEM((seq, wide), BF16), pltpu.VMEM((seq, 128), F32),
            pltpu.VMEM((seq, blk), F32),
            pltpu.VMEM((wide, blk), BF16), pltpu.VMEM((wide, blk), BF16),
            pltpu.VMEM((dim, blk), F32), pltpu.VMEM((dim, blk), F32),
            pltpu.VMEM((dim, seq), F32), pltpu.VMEM((dim, seq), F32), dma((seq // blk,))]
        + sum((swap_scratch(a) for a in old), []) + ([pltpu.VMEM(dot_.shape, BF16), dma((blocks,)), dma((blocks,))] if send_o else []),
        cost_estimate=pl.CostEstimate(flops=pairs * 6 * 2 * blk * blk * 256, bytes_accessed=24 << 20, transcendentals=pairs * blk * blk),
        compiler_params=pltpu.CompilerParams(dimension_semantics=("arbitrary",), vmem_limit_bytes=52 << 20,
                                             collective_id=collective_id, has_side_effects=True),
    )(slope2, w_head, b_head, x, dot_, pos, pref, *gw, *old)
    return res[0], res[1:4], res[4], res[5:]


def peer_at(d, peers):
    return {"sp": lax.rem(lax.axis_index("sp") + d, peers)}


def meet(peers):
    barrier = pltpu.get_barrier_semaphore()
    for d in range(1, peers):
        pl.semaphore_signal(barrier, inc=1, device_id=peer_at(d, peers), device_id_type=pl.DeviceIdType.MESH)
    pl.semaphore_wait(barrier, peers - 1)


def swap_copies(x_ref, out_ref, send_sem, recv_sem, peers):
    me = lax.axis_index("sp")
    order = [d for near in range(peers // 2) for d in sorted({peers // 2 - near, peers // 2 + near})]
    return [pltpu.make_async_remote_copy(
        src_ref=x_ref.at[lax.rem(me + d, peers)], dst_ref=out_ref.at[me], send_sem=send_sem.at[d - 1], recv_sem=recv_sem.at[d - 1],
        device_id=peer_at(d, peers), device_id_type=pl.DeviceIdType.MESH) for d in order]


def swap_start(x_ref, out_ref, own, send_sem, recv_sem, own_sem, peers):
    me = lax.axis_index("sp")
    for copy in swap_copies(x_ref, out_ref, send_sem, recv_sem, peers):
        copy.start()
    take = pltpu.make_async_copy(x_ref.at[me], own, own_sem)
    take.start()
    take.wait()
    pltpu.make_async_copy(own, out_ref.at[me], own_sem).start()


def swap_wait(x_ref, out_ref, own, send_sem, recv_sem, own_sem, peers):
    pltpu.make_async_copy(own, out_ref.at[lax.axis_index("sp")], own_sem).wait()
    for copy in swap_copies(x_ref, out_ref, send_sem, recv_sem, peers):
        copy.wait()


def swap_scratch(x):
    peers = x.shape[0]
    return [pltpu.VMEM(x.shape[1:], x.dtype), pltpu.SemaphoreType.DMA((peers - 1,)), pltpu.SemaphoreType.DMA((peers - 1,)),
            pltpu.SemaphoreType.DMA]


def tail_body(dqkv_ref, d_old, o_old, o_new, dy_ref, x_ref, w_hbm, wo_hbm, gain_ref, bo_ref, y_ref, gx_ref, part, rows_ref,
              d_new, w_ref, wo_ref, dn, mine, other, pair, landed, sums, own_d, ds_sem, dr_sem, do_sem, ps_sem, pr_sem, rs_sem, rr_sem,
              w_sem, *, peers):
    ring = peers // 2
    me = lax.axis_index("sp")
    z, c = me // 2, me % 2
    _, tok, hidden = x_ref.shape
    half = hidden // 2
    wide = hidden // 3
    group = 8
    cols = (pl.ds(0, half), pl.ds(half, half))
    at = lambda zz, cc: {"sp": 2 * zz + cc}
    turn = lambda k: lax.rem(z + k + 2 * ring, ring)
    step = (1, -1)
    remote = functools.partial(pltpu.make_async_remote_copy, device_id_type=pl.DeviceIdType.MESH)
    tn = (((0,), (0,)), ((), ()))
    o_refs, d_refs = (o_old, o_new), (d_old, d_new)
    loads = [pltpu.make_async_copy(w_hbm, w_ref, w_sem.at[0]), pltpu.make_async_copy(wo_hbm, wo_ref, w_sem.at[1])]
    for load in loads:
        load.start()
    meet(peers)
    swap_start(dqkv_ref, d_new, own_d, ds_sem, dr_sem, do_sem, peers)

    def product(out, side):
        @pl.loop(0, ring)
        def _(k):
            h = 2 * k + side
            out[k] = (jnp.dot(o_old[h], dy_ref[0], preferred_element_type=F32)
                      + jnp.dot(o_new[h], dy_ref[1], preferred_element_type=F32))

    def forward(b):
        o_t = o_refs[b][...].reshape(hidden, tok)

        @pl.loop(0, 3)
        def _(n):
            at_n = pl.ds(pl.multiple_of(n * wide, wide), wide)
            acc = lax.dot_general(o_t, wo_ref[:, at_n], tn, preferred_element_type=F32)
            y_ref[b, :, at_n] = (x_ref[b, :, at_n].astype(F32) + acc + bo_ref[:, at_n]).astype(BF16)

    def backward(b):
        @pl.loop(0, 3)
        def _(n):
            at_n = pl.ds(pl.multiple_of(n * wide, wide), wide)
            acc = None
            for k in range(0, peers, group):
                lhs = d_refs[b][k:k + group].reshape(-1, tok)
                one = lax.dot_general(lhs, w_ref[k * lhs.shape[0] // group:(k + group) * lhs.shape[0] // group, at_n], tn, preferred_element_type=F32)
                acc = one if acc is None else acc + one
            dn[:, at_n] = acc

        @pl.loop(0, tok // 32)
        def _(k):
            rows = pl.ds(pl.multiple_of(k * 32, 32), 32)
            x = x_ref[b, rows, :].astype(F32)
            dy = dy_ref[b, rows, :].astype(F32)
            d = dn[rows, :]
            cen = x - jnp.mean(x, axis=-1, keepdims=True)
            inv = lax.rsqrt(jnp.mean(cen * cen, axis=-1, keepdims=True) + NORM_EPS)
            hat = cen * inv
            for n, one in enumerate((d * hat, d, dy)):
                sums[n] += jnp.sum(one.reshape(4, 8, hidden), axis=0)
            e = d * gain_ref[...]
            m1 = jnp.mean(e, axis=-1, keepdims=True)
            m2 = jnp.mean(e * hat, axis=-1, keepdims=True)
            gx_ref[b, rows, :] = (dy + inv * (e - m1 - hat * m2)).astype(BF16)

    product(other, 1 - c)
    to_pair = remote(src_ref=other, dst_ref=pair, send_sem=ps_sem, recv_sem=pr_sem, device_id=at(z, 1 - c))
    product(mine, c)
    to_pair.start()
    sums[...] = jnp.zeros_like(sums)
    to_pair.wait()

    @pl.loop(0, ring)
    def _(k):
        mine[k] = mine[k] + pair[k]

    def reduce_copy(w, t):
        return remote(src_ref=mine.at[turn(-step[w] * (1 + t)), :, cols[w]], dst_ref=landed.at[w, t],
                      send_sem=rs_sem.at[w, t], recv_sem=rr_sem.at[w, t], device_id=at(turn(step[w]), c))

    def add(w, t, k):
        reduce_copy(w, t).wait_recv()
        mine[k, :, cols[w]] = mine[k, :, cols[w]] + landed[w, t]

    def hop(t):
        for w in range(2):
            add(w, t - 1, turn(-step[w] * (1 + t)))
            reduce_copy(w, t).start()

    for w in range(2):
        reduce_copy(w, 0).start()
    loads[1].wait()
    forward(0)
    hop(1)
    forward(1)
    hop(2)
    loads[0].wait()
    backward(0)

    @pl.loop(3, ring - 1)
    def _(t):
        hop(t)

    swap_wait(dqkv_ref, d_new, own_d, ds_sem, dr_sem, do_sem, peers)
    backward(1)
    rows_ref[...] = jnp.zeros_like(rows_ref)
    for n in range(3):
        rows_ref[n:n + 1, :] = jnp.sum(sums[n], axis=0, keepdims=True)
    for w in range(2):
        add(w, ring - 2, z)
    part[...] = mine[z]

    @pl.loop(0, ring - 1)
    def _(t):
        for w in range(2):
            reduce_copy(w, t).wait_send()


def tail(dqkv, d_old, o_old, o_new, dy, x, w_flat, w_out, gain, b_out, collective_id):
    peers, dim, tok = o_old.shape
    ring = peers // 2
    hidden = dy.shape[-1]
    hbm, vmem = pl.BlockSpec(memory_space=pltpu.HBM), pl.BlockSpec(memory_space=pltpu.VMEM)
    dma = pltpu.SemaphoreType.DMA
    rows = lambda *lead: pltpu.VMEM(lead + (dim, hidden), F32)
    like = lambda a: jax.ShapeDtypeStruct(a.shape, a.dtype)
    return pl.pallas_call(
        functools.partial(tail_body, peers=peers),
        name="tail",
        out_shape=[like(x), like(x), jax.ShapeDtypeStruct((dim, hidden), F32), jax.ShapeDtypeStruct((8, hidden), F32)],
        in_specs=[hbm, vmem, vmem, vmem, vmem, vmem, hbm, hbm, vmem, vmem],
        out_specs=[vmem] * 4,
        scratch_shapes=[pltpu.VMEM(dqkv.shape, BF16), pltpu.VMEM(w_flat.shape, BF16), pltpu.VMEM(w_out.shape, BF16),
                        pltpu.VMEM((tok, hidden), F32), rows(ring), rows(ring), rows(ring),
                        pltpu.VMEM((2, ring - 1, dim, hidden // 2), F32), pltpu.VMEM((3, 8, hidden), F32),
                        pltpu.VMEM(dqkv.shape[1:], BF16), dma((peers - 1,)), dma((peers - 1,)), dma, dma, dma,
                        dma((2, ring - 1)), dma((2, ring - 1)), dma((2,))],
        cost_estimate=pl.CostEstimate(flops=10**11, bytes_accessed=64 << 20, transcendentals=0),
        compiler_params=pltpu.CompilerParams(collective_id=collective_id, has_side_effects=True, vmem_limit_bytes=47 << 20),
    )(dqkv, d_old, o_old, o_new, dy, x, w_flat, w_out, gain, b_out)


def collect_body(part, rows_ref, gb_ref, full, total, gb_all, stage, as_sem, ar_sem, fs_sem, fr_sem, xs_sem, xr_sem, *, peers, cuts):
    ring = peers // 2
    me = lax.axis_index("sp")
    z, c = me // 2, me % 2
    half = part.shape[-1] // 2
    few = part.shape[0] // cuts
    turn = lambda k: lax.rem(z + k + 2 * ring, ring)
    step = (1, -1)
    remote = functools.partial(pltpu.make_async_remote_copy, device_id_type=pl.DeviceIdType.MESH)

    def block_copy(w, t, u, side, send_sem, recv_sem, to):
        ref = full.at[turn(-step[w] * t), side, pl.ds(u * few, few), pl.ds(w * half, half)]
        return remote(src_ref=ref, dst_ref=ref, send_sem=send_sem.at[w, t, u], recv_sem=recv_sem.at[w, t, u], device_id={"sp": to})

    gather_copy = lambda w, t, u: block_copy(w, t, u, c, as_sem, ar_sem, 2 * turn(step[w]) + c)
    over_copy = lambda w, t, u, side: block_copy(w, t, u, side, fs_sem, fr_sem, 2 * z + 1 - c)
    parts = [(w, u) for u in range(cuts) for w in range(2)]
    owners = rows_ref.shape[1] // 128
    lanes = lambda k: pl.ds(pl.multiple_of(k * 128, 128), 128)
    full[z, c] = part[...]
    gb_all[me] = gb_ref[...]
    meet(peers)
    for w, u in parts:
        gather_copy(w, 0, u).start()

    def small_copy(kind, frm, to):
        src, dst = ((rows_ref.at[:, lanes(to)], stage.at[frm]), (total.at[:, lanes(frm)],) * 2, (gb_ref, gb_all.at[frm]))[kind]
        return remote(src_ref=src, dst_ref=dst, send_sem=xs_sem.at[kind, to], recv_sem=xr_sem.at[kind, frm], device_id={"sp": to})

    def each(act, kind, only_to=False, only_from=False):
        @pl.loop(1, peers)
        def _(d):
            other = lax.rem(me + d, peers)

            def go():
                act(kind, other)

            if only_to:
                pl.when(other < owners)(go)
            elif only_from:
                pl.when(me < owners)(go)
            else:
                go()

    send = lambda kind, other: small_copy(kind, me, other).start()
    sent = lambda kind, other: small_copy(kind, me, other).wait_send()
    came = lambda kind, other: small_copy(kind, other, me).wait_recv()
    each(send, 0, only_to=True)
    each(send, 2)
    for w, u in parts:
        over_copy(w, 0, u, c).start()

    @pl.when(me < owners)
    def _():
        stage[me] = rows_ref[:, lanes(me)]

    each(came, 0, only_from=True)

    @pl.when(me < owners)
    def _():
        total[:, lanes(me)] = jnp.sum(stage[...], axis=0)

    each(send, 1, only_from=True)

    @pl.loop(1, ring)
    def _(t):
        for w, u in parts:
            gather_copy(w, t - 1, u).wait_recv()

            @pl.when(t < ring - 1)
            def _():
                gather_copy(w, t, u).start()

            over_copy(w, t, u, c).start()

    each(came, 1, only_to=True)
    each(came, 2)
    each(sent, 0, only_to=True)
    each(sent, 1, only_from=True)
    each(sent, 2)

    @pl.loop(0, ring - 1)
    def _(t):
        for w, u in parts:
            gather_copy(w, t, u).wait_send()

    @pl.loop(0, ring)
    def _(t):
        for w, u in parts:
            over_copy(w, t, u, c).wait_send()
            over_copy(w, t, u, 1 - c).wait_recv()


def collect(part, rows, gb, peers, collective_id, cuts=3):
    ring = peers // 2
    vmem = pl.BlockSpec(memory_space=pltpu.VMEM)
    dma = pltpu.SemaphoreType.DMA
    return pl.pallas_call(
        functools.partial(collect_body, peers=peers, cuts=cuts),
        name="collect",
        out_shape=[jax.ShapeDtypeStruct((ring, 2) + part.shape, F32), jax.ShapeDtypeStruct(rows.shape, F32),
                   jax.ShapeDtypeStruct((peers,) + gb.shape, F32)],
        in_specs=[vmem] * 3,
        out_specs=[vmem] * 3,
        scratch_shapes=[pltpu.VMEM((peers, rows.shape[0], 128), F32), dma((2, ring - 1, cuts)), dma((2, ring - 1, cuts)),
                        dma((2, ring, cuts)), dma((2, ring, cuts)), dma((3, peers)), dma((3, peers))],
        cost_estimate=pl.CostEstimate(flops=5 * 10**10, bytes_accessed=10 << 20, transcendentals=0),
        compiler_params=pltpu.CompilerParams(collective_id=collective_id, has_side_effects=True, vmem_limit_bytes=24 << 20),
    )(part, rows, gb)


def swap_body(*refs, peers, n):
    ins, outs, scratch = refs[:n], refs[n:2 * n], refs[2 * n:]
    meet(peers)
    for k in range(n):
        swap_start(ins[k], outs[k], *scratch[4 * k:4 * k + 4], peers)
    for k in range(n):
        swap_wait(ins[k], outs[k], *scratch[4 * k:4 * k + 4], peers)


def swap(xs, collective_id, name):
    hbm = pl.BlockSpec(memory_space=pltpu.HBM)
    peers = xs[0].shape[0]
    return pl.pallas_call(
        functools.partial(swap_body, peers=peers, n=len(xs)),
        name=name,
        out_shape=[jax.ShapeDtypeStruct(x.shape, x.dtype) for x in xs],
        in_specs=[hbm] * len(xs),
        out_specs=[hbm] * len(xs),
        scratch_shapes=sum((swap_scratch(x) for x in xs), []),
        cost_estimate=pl.CostEstimate(flops=24000 * sum(x.size for x in xs), bytes_accessed=4 * sum(x.size for x in xs), transcendentals=0),
        compiler_params=pltpu.CompilerParams(collective_id=collective_id, has_side_effects=True, vmem_limit_bytes=48 << 20),
    )(*xs)


def exchange_body(x_ref, out_ref, send_sem, recv_sem, *, peers):
    me = lax.axis_index("sp")
    meet(peers)
    copies = [pltpu.make_async_remote_copy(
        src_ref=x_ref, dst_ref=out_ref.at[me], send_sem=send_sem.at[d - 1], recv_sem=recv_sem.at[d - 1],
        device_id=peer_at(d, peers), device_id_type=pl.DeviceIdType.MESH) for d in range(1, peers)]
    for copy in copies:
        copy.start()
    out_ref[me] = x_ref[...]
    for copy in copies:
        copy.wait()


def exchange(x, peers, collective_id, name):
    return pl.pallas_call(
        functools.partial(exchange_body, peers=peers),
        name=name,
        out_shape=jax.ShapeDtypeStruct((peers,) + x.shape, x.dtype),
        in_specs=[pl.BlockSpec(memory_space=pltpu.VMEM)],
        out_specs=pl.BlockSpec(memory_space=pltpu.VMEM),
        scratch_shapes=[pltpu.SemaphoreType.DMA((peers - 1,)), pltpu.SemaphoreType.DMA((peers - 1,))],
        compiler_params=pltpu.CompilerParams(collective_id=collective_id, has_side_effects=True, vmem_limit_bytes=8 << 20),
    )(x)


def place_body(*refs, first):
    x_ref, (out_ref, buf, in_sem, out_sem) = refs[0], refs[-4:]
    heads, n = x_ref.shape[:2]
    reads = [pltpu.make_async_copy(x_ref.at[h], buf.at[h], in_sem.at[h]) for h in range(heads)]
    writes = [pltpu.make_async_copy(buf.at[h], out_ref.at[h, pl.ds(first, n)], out_sem.at[h]) for h in range(heads)]
    for copy in reads:
        copy.start()
    for read, write in zip(reads, writes):
        read.wait()
        write.start()
    for copy in writes:
        copy.wait()


def place(x, into, lanes, first):
    heads, n, dim, hidden = x.shape
    hbm = pl.BlockSpec(memory_space=pltpu.HBM)
    args, alias = ((x,), {}) if into is None else ((x, into), {1: 0})
    dma = pltpu.SemaphoreType.DMA
    return pl.pallas_call(
        functools.partial(place_body, first=first), name="place",
        out_shape=jax.ShapeDtypeStruct((heads, lanes, dim, hidden), x.dtype),
        in_specs=[hbm] * len(args), out_specs=hbm, input_output_aliases=alias,
        scratch_shapes=[pltpu.VMEM(x.shape, x.dtype), dma((heads,)), dma((heads,))],
        cost_estimate=pl.CostEstimate(flops=10**9, bytes_accessed=8 * x.size, transcendentals=0),
        compiler_params=pltpu.CompilerParams(vmem_limit_bytes=60 << 20))(*args)


def lay_body(x_ref, out_ref, sem):
    copies = [pltpu.make_async_copy(x_ref.at[k], out_ref.at[k], sem.at[k]) for k in range(x_ref.shape[0])]
    for copy in copies:
        copy.start()
    for copy in copies:
        copy.wait()


def lay_down(x):
    return pl.pallas_call(
        lay_body, name="lay_down", out_shape=jax.ShapeDtypeStruct(x.shape, x.dtype),
        in_specs=[pl.BlockSpec(memory_space=pltpu.VMEM)], out_specs=pl.BlockSpec(memory_space=pltpu.HBM),
        scratch_shapes=[pltpu.SemaphoreType.DMA((x.shape[0],))],
        cost_estimate=pl.CostEstimate(flops=10**9, bytes_accessed=8 * x.size, transcendentals=0),
        compiler_params=pltpu.CompilerParams(vmem_limit_bytes=24 << 20))(x)


def norm_body(x_ref, gain_ref, bias_ref, *out_refs):
    for b, out_ref in enumerate(out_refs):
        @pl.loop(0, x_ref.shape[1] // 32)
        def _(k):
            rows = pl.ds(pl.multiple_of(k * 32, 32), 32)
            x = x_ref[b, rows, :].astype(F32)
            cen = x - jnp.mean(x, axis=-1, keepdims=True)
            hat = cen * lax.rsqrt(jnp.mean(cen * cen, axis=-1, keepdims=True) + NORM_EPS)
            out_ref[rows, :] = (hat * gain_ref[...] + bias_ref[...]).astype(BF16)


def norm_forward(x, gain, bias):
    vmem = pl.BlockSpec(memory_space=pltpu.VMEM)
    return pl.pallas_call(
        norm_body, name="norm_forward", out_shape=[jax.ShapeDtypeStruct(x.shape[1:], BF16)] * x.shape[0],
        in_specs=[vmem] * 3, out_specs=[vmem] * x.shape[0],
        cost_estimate=pl.CostEstimate(flops=10**8, bytes_accessed=4 * x.size, transcendentals=0),
        compiler_params=pltpu.CompilerParams(vmem_limit_bytes=8 << 20))(x, gain, bias)


def solution(mesh):
    peers = mesh.shape["sp"]

    def block_fn(x_blk, pos_blk, keep_blk, ln_gain, ln_bias, w_qkv, b_qkv, w_out, b_out, dy_blk):
        batch, tok, hidden = x_blk.shape
        heads, dim = w_qkv.shape[1], w_qkv.shape[3]
        assert heads == peers
        seq = tok * peers
        blk = 2 * tok
        rank = lax.axis_index("sp")
        x_norm = norm_forward(x_blk, ln_gain.reshape(1, hidden), ln_bias.reshape(1, hidden))
        xf = [lax.all_gather(x_norm[0], "sp", axis=0, tiled=True)]
        marks = exchange(jnp.concatenate([pos_blk, keep_blk, jnp.zeros((8 - 2 * batch, tok), jnp.int32)]), peers, 0, "marks")
        do_loc = [lax.dot_general(w_out, dy_blk[b], NT, preferred_element_type=F32).astype(BF16).reshape(heads, dim, tok) for b in range(batch)]
        do_t = list(swap(do_loc[:1], 1, "swap_do"))
        for b in range(1, batch):
            xf.append(lax.all_gather(x_norm[b], "sp", axis=0, tiled=True))
        w_t = jnp.transpose(w_qkv, (1, 2, 3, 0))
        w_head = lax.dynamic_index_in_dim(w_t, rank, 0, keepdims=False).reshape(3 * dim, hidden)
        b_head = lax.dynamic_index_in_dim(b_qkv, rank, 0, keepdims=False).reshape(3 * dim, 1)
        slope = jnp.exp2(-8.0 * (rank + 1).astype(F32) / heads)
        slope2 = (slope * LOG2E).reshape(1)
        gw, att = (), []
        for b in range(batch):
            pos = marks[:, b].reshape(1, seq).astype(F32)
            keep = marks[:, batch + b].reshape(1, seq)
            pref = jnp.broadcast_to(pos[0, ::blk][:, None], (seq // blk, 128))
            old = list(do_loc[b + 1:b + 2]) if b + 1 < batch else list(att)
            att_d, gw, att_o, swapped = attention(slope2, w_head, b_head, xf[b], do_t[b], jnp.where(keep > 0, pos, MASKED), pref, gw, old,
                                                  blk=blk, tok=tok, send_o=b + 1 == batch, collective_id=4 + b)
            if b + 1 < batch:
                do_t.append(swapped[0])
            att = [att_o, att_d]
        o_old, d_old = swapped
        gw_all = [lax.all_gather(one, "sp", axis=0, tiled=True).reshape(heads, -1, dim, hidden) for one in gw[:2]]
        cut = gw_all[0].shape[1]
        y, gx, part, rows = tail(att_d, d_old, o_old, att_o, dy_blk, x_blk, w_t.reshape(3 * hidden, hidden), w_out,
                                 ln_gain.reshape(1, hidden), b_out.reshape(1, hidden), 2)
        gb, _ = lax.optimization_barrier((gw[2], part))
        gb = jnp.pad(gb[:, 0].reshape(3, dim), ((0, 5), (0, 128 - dim)))
        first, _ = lax.optimization_barrier((gw_all[0], part))
        gw_out = place(first, None, 3, 0)
        y, gx = lay_down(y), lay_down(gx)
        rows, gw_out, y, gx = lax.optimization_barrier((rows, gw_out, y, gx))
        go_all, total, gb_all = collect(part, rows, gb, peers, 3)
        go_all = lay_down(go_all.reshape(heads, dim, hidden)).reshape(hidden, hidden)
        second, go_all = lax.optimization_barrier((gw_all[1], go_all))
        gw_out = jnp.transpose(place(second, gw_out, 3, cut), (3, 0, 1, 2))
        return y, gx, gw_out, gb_all[:, :3, :dim], go_all, total[2], total[0], total[1]

    act_spec = P("dp", "sp", None)
    tok_spec = P("dp", "sp")
    in_specs = (act_spec, tok_spec, tok_spec, P(), P(), P(), P(), P(), P(), act_spec)
    out_specs = (act_spec, act_spec, P("dp", None, None, None), P("dp", None, None), P("dp", None), P("dp"), P("dp"), P("dp"))
    return jax.shard_map(block_fn, mesh=mesh, in_specs=in_specs, out_specs=out_specs, check_vma=False)
```

```python
import functools
import jax
import jax.numpy as jnp
from jax import lax
from jax.experimental import pallas as pl
from jax.experimental.pallas import tpu as pltpu
from jax.sharding import PartitionSpec as P

NORM_EPS = 1e-5

LOG2E = 1.4426950408889634
MASKED = -1e30
F32, BF16 = jnp.float32, jnp.bfloat16
NT = (((1,), (1,)), ((), ()))


def attn_body(slope_ref, w_ref, b_ref, dot_ref, pos_ref, pref_ref, *refs, blk, tok, n_swap, n_old, n_x, send_o):
    peers = dot_ref.shape[0]
    x_refs, refs = refs[:n_x], refs[n_x:]
    gw_old, old, refs = refs[:n_old], refs[n_old:n_old + n_swap], refs[n_old + n_swap:]
    (dqkv_ref, gwa_ref, gwb_ref, gb_ref, o_out), got, refs = refs[:5], refs[5:5 + n_swap], refs[5 + n_swap:]
    x_buf, qkvt_ref, k_tok, v_tok, posk_ref, s_buf, q_pad, do_pad, o_acc, dq_acc, dk_acc, dv_acc, x_sem = refs[:13]
    swaps = [(old[k], got[k]) + refs[13 + 4 * k:17 + 4 * k] for k in range(n_swap)]
    if send_o:
        o_ref, os_sem, or_sem = refs[-3:]
        o_new = o_out
    else:
        o_ref = o_out
    dim = dot_ref.shape[1]
    seq = dot_ref.shape[0] * tok
    pad = k_tok.shape[1] - dim
    nq = blk // tok
    steps = seq // blk
    scale = dim ** -0.5
    me = lax.axis_index("sp")
    step = pl.program_id(0)
    i = lax.rem(me // nq + step, steps)
    half = blk // 2

    def x_copies(k):
        rows = pl.ds(pl.multiple_of(k * blk, blk), blk)
        lo = 0
        for n, x_ref in enumerate(x_refs):
            yield pltpu.make_async_copy(x_ref.at[rows], x_buf.at[rows, lo:lo + x_ref.shape[1]], x_sem.at[n, k])
            lo += x_ref.shape[1]

    def o_send(to):
        return pltpu.make_async_remote_copy(
            src_ref=o_ref.at[to], dst_ref=o_new.at[me], send_sem=os_sem.at[to], recv_sem=or_sem.at[me],
            device_id={"sp": to}, device_id_type=pl.DeviceIdType.MESH)

    def o_keep():
        return pltpu.make_async_copy(o_ref.at[me], o_new.at[me], os_sem.at[me])

    def o_start(at):
        for t in range(nq):
            to = lax.rem(me // nq + at, steps) * nq + t

            @pl.when(to != me)
            def _():
                o_send(to).start()

            @pl.when(to == me)
            def _():
                o_keep().start()

    @pl.when(step == 0)
    def _():
        for k in range(steps):
            for copy in x_copies(k):
                copy.start()
        meet(peers)
        for one in swaps:
            swap_start(*one, peers)
        dk_acc[...] = jnp.zeros_like(dk_acc)
        dv_acc[...] = jnp.zeros_like(dv_acc)
        q_pad[...] = jnp.zeros_like(q_pad)
        do_pad[...] = jnp.zeros_like(do_pad)

        @pl.loop(0, steps)
        def _(k):
            rows = pl.ds(pl.multiple_of(k * blk, blk), blk)
            for copy in x_copies(k):
                copy.wait()
            qkvt_ref[:, rows] = (lax.dot_general(w_ref[...], x_buf[rows, :], NT, preferred_element_type=F32) + b_ref[...]).astype(BF16)

            @pl.loop(0, blk // 128)
            def _(t):
                cols = pl.ds(pl.multiple_of(k * blk + t * 128, 128), 128)
                for base, dst in ((dim, k_tok), (2 * dim, v_tok)):
                    part = qkvt_ref[base:base + dim, cols].astype(F32)
                    whole = jnp.concatenate([part, jnp.zeros((pad, 128), F32)], axis=0)
                    dst[cols, :] = jnp.transpose(whole).astype(BF16)
                posk_ref[cols, :] = jnp.transpose(jnp.broadcast_to(pos_ref[:, cols], (128, 128)))

    if send_o:
        @pl.when(step > 0)
        def _():
            o_start(step - 1)

    qcols = pl.ds(pl.multiple_of(i * blk, blk), blk)
    q_pad[0:dim, :] = qkvt_ref[0:dim, qcols]
    for t in range(nq):
        do_pad[0:dim, t * tok:(t + 1) * tok] = dot_ref[i * nq + t]
    slope2 = slope_ref[0]
    ref_pos = pref_ref[pl.ds(i, 1), :]
    c = scale * LOG2E

    def scores(j, m8, diag):
        for sub in range(2):
            rows = pl.ds(pl.multiple_of(j * blk + sub * half, half), half)
            st = jnp.dot(k_tok[rows, :], q_pad[...], preferred_element_type=F32)
            bias = (posk_ref[rows, :] - ref_pos) * slope2
            st = st * c + jnp.concatenate([bias] * (blk // 128), axis=1)
            if diag:
                key = lax.broadcasted_iota(jnp.int32, (half, blk), 0) + sub * half
                qry = lax.broadcasted_iota(jnp.int32, (half, blk), 1)
                st = jnp.where(key <= qry, st, MASKED)
            s_buf[rows, :] = st
            m8 = jnp.maximum(m8, jnp.max(st.reshape(half // 8, 8, blk), axis=0))
        return m8

    m8 = lax.fori_loop(0, i, lambda j, m: scores(j, m, False), jnp.full((8, blk), MASKED, F32))
    m8 = scores(i, m8, True)
    m = jnp.max(m8, axis=0, keepdims=True)

    def exps(j, l8):
        for sub in range(2):
            rows = pl.ds(pl.multiple_of(j * blk + sub * half, half), half)
            e = jnp.exp2(s_buf[rows, :] - m)
            s_buf[rows, :] = e
            l8 = l8 + jnp.sum(e.reshape(half // 8, 8, blk), axis=0)
        return l8

    l8 = lax.fori_loop(0, i + 1, exps, jnp.zeros((8, blk), F32))
    inv = 1.0 / jnp.sum(l8, axis=0, keepdims=True)
    o_acc[...] = jnp.zeros_like(o_acc)
    dq_acc[...] = jnp.zeros_like(dq_acc)

    def values(j, _):
        rows = pl.ds(pl.multiple_of(j * blk, blk), blk)
        p = s_buf[rows, :] * inv
        s_buf[rows, :] = p
        pb = p.astype(BF16)
        o_acc[...] += jnp.dot(qkvt_ref[2 * dim:3 * dim, rows], pb, preferred_element_type=F32)
        dv_acc[:, rows] += lax.dot_general(do_pad[0:dim, :], pb, NT, preferred_element_type=F32)
        return 0

    lax.fori_loop(0, i + 1, values, 0)
    o_lo = o_acc[...].astype(BF16)
    do_f = do_pad[0:dim, :].astype(F32)
    r = jnp.sum(do_f * o_lo.astype(F32), axis=0, keepdims=True)

    def grads(j, _):
        rows = pl.ds(pl.multiple_of(j * blk, blk), blk)
        g = jnp.dot(v_tok[rows, :], do_pad[...], preferred_element_type=F32)
        ds = (s_buf[rows, :] * (g - r)).astype(BF16)
        dq_acc[...] += jnp.dot(qkvt_ref[dim:2 * dim, rows], ds, preferred_element_type=F32)
        dk_acc[:, rows] += lax.dot_general(q_pad[0:dim, :], ds, NT, preferred_element_type=F32)
        return 0

    lax.fori_loop(0, i + 1, grads, 0)
    dq_lo = (dq_acc[...] * scale).astype(BF16)
    for t in range(nq):
        o_ref[i * nq + t] = o_lo[:, t * tok:(t + 1) * tok]
        dqkv_ref[i * nq + t, 0:dim] = dq_lo[:, t * tok:(t + 1) * tok]

    @pl.when(step == steps - 1)
    def _():
        @pl.loop(0, seq // tok)
        def _(t):
            cols = pl.ds(pl.multiple_of(t * tok, tok), tok)
            dqkv_ref[t, dim:2 * dim] = (dk_acc[:, cols] * scale).astype(BF16)
            dqkv_ref[t, 2 * dim:3 * dim] = dv_acc[:, cols].astype(BF16)

        if send_o:
            o_start(step)
        for k, ref in enumerate((gwa_ref, gwb_ref, gb_ref)):
            ref[...] = gw_old[k][...] if n_old else jnp.zeros_like(ref)
        ones = jnp.ones((blk, 128), BF16)

        @pl.loop(0, steps)
        def _(j):
            rows = pl.ds(pl.multiple_of(j * blk, blk), blk)
            for ref, lo, hi in ((gwa_ref, 0, 2 * dim), (gwb_ref, 2 * dim, 3 * dim)):
                lhs = jnp.concatenate([dqkv_ref[j * nq + t, lo:hi] for t in range(nq)], axis=1)
                ref[...] += jnp.dot(lhs, x_buf[rows, :], preferred_element_type=F32)
                gb_ref[lo:hi, :] += jnp.dot(lhs, ones, preferred_element_type=F32)

        if send_o:
            o_keep().wait()
            for d in range(1, peers):
                frm = lax.rem(me + d, peers)
                o_send(frm).wait_send()
                pltpu.make_async_remote_copy(
                    src_ref=o_ref.at[frm], dst_ref=o_new.at[frm], send_sem=os_sem.at[frm], recv_sem=or_sem.at[frm],
                    device_id={"sp": frm}, device_id_type=pl.DeviceIdType.MESH).wait_recv()
        for one in swaps:
            swap_wait(*one, peers)


def attention(slope2, w_head, b_head, xs, dot_, pos, pref, gw, old, *, blk, tok, send_o, collective_id):
    blocks, dim, _ = dot_.shape
    seq, hidden = xs[0].shape[0], w_head.shape[1]
    wide = 128 * pl.cdiv(dim, 128)
    hbm = pl.BlockSpec(memory_space=pltpu.HBM)
    full = lambda a: pl.BlockSpec(a.shape, lambda i: (0,) * len(a.shape), pipeline_mode=pl.Buffered(1))
    like = lambda a: jax.ShapeDtypeStruct(a.shape, a.dtype)
    outs = [jax.ShapeDtypeStruct((blocks, 3 * dim, tok), BF16), jax.ShapeDtypeStruct((2 * dim, hidden), F32),
            jax.ShapeDtypeStruct((dim, hidden), F32), jax.ShapeDtypeStruct((3 * dim, 128), F32)]
    pairs = (seq // blk) * (seq // blk + 1) // 2
    dma = pltpu.SemaphoreType.DMA
    res = pl.pallas_call(
        functools.partial(attn_body, blk=blk, tok=tok, n_swap=len(old), n_old=len(gw), n_x=len(xs), send_o=send_o),
        name="attention",
        out_shape=outs + [like(dot_)] + [like(a) for a in old],
        grid=(seq // blk,),
        in_specs=[pl.BlockSpec(memory_space=pltpu.SMEM), full(w_head), full(b_head), full(dot_), full(pos), full(pref)]
        + [hbm] * len(xs) + [full(a) for a in gw] + [hbm] * len(old),
        out_specs=[full(a) for a in outs] + [hbm if send_o else full(dot_)] + [hbm] * len(old),
        scratch_shapes=[
            pltpu.VMEM((seq, hidden), BF16), pltpu.VMEM((3 * dim, seq), BF16),
            pltpu.VMEM((seq, wide), BF16), pltpu.VMEM((seq, wide), BF16), pltpu.VMEM((seq, 128), F32),
            pltpu.VMEM((seq, blk), F32),
            pltpu.VMEM((wide, blk), BF16), pltpu.VMEM((wide, blk), BF16),
            pltpu.VMEM((dim, blk), F32), pltpu.VMEM((dim, blk), F32),
            pltpu.VMEM((dim, seq), F32), pltpu.VMEM((dim, seq), F32), dma((len(xs), seq // blk))]
        + sum((swap_scratch(a) for a in old), []) + ([pltpu.VMEM(dot_.shape, BF16), dma((blocks,)), dma((blocks,))] if send_o else []),
        cost_estimate=pl.CostEstimate(flops=pairs * 6 * 2 * blk * blk * 256, bytes_accessed=24 << 20, transcendentals=pairs * blk * blk),
        compiler_params=pltpu.CompilerParams(dimension_semantics=("arbitrary",), vmem_limit_bytes=52 << 20,
                                             collective_id=collective_id, has_side_effects=True),
    )(slope2, w_head, b_head, dot_, pos, pref, *xs, *gw, *old)
    return res[0], res[1:4], res[4], res[5:]


def peer_at(d, peers):
    return {"sp": lax.rem(lax.axis_index("sp") + d, peers)}


def meet(peers):
    barrier = pltpu.get_barrier_semaphore()
    for d in range(1, peers):
        pl.semaphore_signal(barrier, inc=1, device_id=peer_at(d, peers), device_id_type=pl.DeviceIdType.MESH)
    pl.semaphore_wait(barrier, peers - 1)


def swap_copies(x_ref, out_ref, send_sem, recv_sem, peers):
    me = lax.axis_index("sp")
    order = [d for near in range(peers // 2) for d in sorted({peers // 2 - near, peers // 2 + near})]
    return [pltpu.make_async_remote_copy(
        src_ref=x_ref.at[lax.rem(me + d, peers)], dst_ref=out_ref.at[me], send_sem=send_sem.at[d - 1], recv_sem=recv_sem.at[d - 1],
        device_id=peer_at(d, peers), device_id_type=pl.DeviceIdType.MESH) for d in order]


def swap_start(x_ref, out_ref, own, send_sem, recv_sem, own_sem, peers):
    me = lax.axis_index("sp")
    for copy in swap_copies(x_ref, out_ref, send_sem, recv_sem, peers):
        copy.start()
    take = pltpu.make_async_copy(x_ref.at[me], own, own_sem)
    take.start()
    take.wait()
    pltpu.make_async_copy(own, out_ref.at[me], own_sem).start()


def swap_wait(x_ref, out_ref, own, send_sem, recv_sem, own_sem, peers):
    pltpu.make_async_copy(own, out_ref.at[lax.axis_index("sp")], own_sem).wait()
    for copy in swap_copies(x_ref, out_ref, send_sem, recv_sem, peers):
        copy.wait()


def swap_scratch(x):
    peers = x.shape[0]
    return [pltpu.VMEM(x.shape[1:], x.dtype), pltpu.SemaphoreType.DMA((peers - 1,)), pltpu.SemaphoreType.DMA((peers - 1,)),
            pltpu.SemaphoreType.DMA]


def ring_gather(block, send_sem, recv_sem, over_sem, came_sem, peers, cuts):
    ring = peers // 2
    me = lax.axis_index("sp")
    z, c = me // 2, me % 2
    turn = lambda k: lax.rem(z + k + 2 * ring, ring)
    step = (1, -1)
    parts = [(w, u) for u in range(cuts) for w in range(2)]

    def copy(w, t, u, side, sems, to):
        ref = block(turn(-step[w] * t), side, w, u)
        return pltpu.make_async_remote_copy(
            src_ref=ref, dst_ref=ref, send_sem=sems[0].at[w, t, u], recv_sem=sems[1].at[w, t, u],
            device_id={"sp": to}, device_id_type=pl.DeviceIdType.MESH)

    along = lambda w, t, u: copy(w, t, u, c, (send_sem, recv_sem), 2 * turn(step[w]) + c)
    across = lambda w, t, u, side: copy(w, t, u, side, (over_sem, came_sem), 2 * z + 1 - c)

    def start():
        for w, u in parts:
            along(w, 0, u).start()
        for w, u in parts:
            across(w, 0, u, c).start()

    def run():
        @pl.loop(1, ring)
        def _(t):
            for w, u in parts:
                along(w, t - 1, u).wait_recv()

                @pl.when(t < ring - 1)
                def _():
                    along(w, t, u).start()

                across(w, t, u, c).start()

    def finish():
        @pl.loop(0, ring - 1)
        def _(t):
            for w, u in parts:
                along(w, t, u).wait_send()

        @pl.loop(0, ring)
        def _(t):
            for w, u in parts:
                across(w, t, u, c).wait_send()
                across(w, t, u, 1 - c).wait_recv()

    return start, run, finish


def ring_scratch(peers, cuts):
    dma = pltpu.SemaphoreType.DMA
    return [dma((2, peers // 2 - 1, cuts)), dma((2, peers // 2 - 1, cuts)), dma((2, peers // 2, cuts)), dma((2, peers // 2, cuts))]


def opening_body(marks_ref, do_ref, xb_ref, marks_all, do_t, x_all, own, ds_sem, dr_sem, do_sem, ms_sem, mr_sem, *ring_sems, peers, cuts):
    me = lax.axis_index("sp")
    rows, few = x_all.shape[1] // 2, x_all.shape[1] // 2 // cuts
    block = lambda k, side, w, u: x_all.at[2 * k + side, pl.ds(w * rows + u * few, few)]
    start, run, finish = ring_gather(block, *ring_sems, peers, cuts)
    x_all[me] = xb_ref[...]
    marks_all[me] = marks_ref[...]
    meet(peers)
    start()
    marks = [pltpu.make_async_remote_copy(
        src_ref=marks_ref, dst_ref=marks_all.at[me], send_sem=ms_sem.at[d - 1], recv_sem=mr_sem.at[d - 1],
        device_id=peer_at(d, peers), device_id_type=pl.DeviceIdType.MESH) for d in range(1, peers)]
    for copy in marks:
        copy.start()
    swap_start(do_ref, do_t, own, ds_sem, dr_sem, do_sem, peers)
    run()
    for copy in marks:
        copy.wait()
    swap_wait(do_ref, do_t, own, ds_sem, dr_sem, do_sem, peers)
    finish()


def opening(marks, do_loc, xb, collective_id, cuts=2):
    peers = do_loc.shape[0]
    hbm, vmem = pl.BlockSpec(memory_space=pltpu.HBM), pl.BlockSpec(memory_space=pltpu.VMEM)
    dma = pltpu.SemaphoreType.DMA
    return pl.pallas_call(
        functools.partial(opening_body, peers=peers, cuts=cuts),
        name="opening",
        out_shape=[jax.ShapeDtypeStruct((peers,) + marks.shape, marks.dtype), jax.ShapeDtypeStruct(do_loc.shape, BF16),
                   jax.ShapeDtypeStruct((peers,) + xb.shape, BF16)],
        in_specs=[vmem, hbm, vmem],
        out_specs=[vmem, hbm, vmem],
        scratch_shapes=swap_scratch(do_loc) + [dma((peers - 1,)), dma((peers - 1,))] + ring_scratch(peers, cuts),
        cost_estimate=pl.CostEstimate(flops=5 * 10**10, bytes_accessed=8 << 20, transcendentals=0),
        compiler_params=pltpu.CompilerParams(collective_id=collective_id, has_side_effects=True, vmem_limit_bytes=24 << 20),
    )(marks, do_loc, xb)


def tail_body(dqkv_ref, d_old, o_old, o_new, dy_ref, x_ref, w_hbm, wo_hbm, gain_ref, bo_ref, gb_ref, y_ref, gx_ref, full, total, gb_all,
              d_new, w_ref, wo_ref, dn, mine, landed, sums, rows_ref, stage, own_d, ds_sem, dr_sem, do_sem, ps_sem, pr_sem, rs_sem, rr_sem,
              w_sem, xs_sem, xr_sem, free_sem, *ring_sems, peers, cuts):
    ring = peers // 2
    me = lax.axis_index("sp")
    z, c = me // 2, me % 2
    _, tok, hidden = x_ref.shape
    half = hidden // 2
    wide = hidden // 3
    group = 8
    cols = (pl.ds(0, half), pl.ds(half, half))
    at = lambda zz, cc: {"sp": 2 * zz + cc}
    turn = lambda k: lax.rem(z + k + 2 * ring, ring)
    step = (1, -1)
    remote = functools.partial(pltpu.make_async_remote_copy, device_id_type=pl.DeviceIdType.MESH)
    tn = (((0,), (0,)), ((), ()))
    o_refs, d_refs = (o_old, o_new), (d_old, d_new)
    loads = [pltpu.make_async_copy(w_hbm, w_ref, w_sem.at[0]), pltpu.make_async_copy(wo_hbm, wo_ref, w_sem.at[1])]
    for load in loads:
        load.start()
    meet(peers)
    swap_start(dqkv_ref, d_new, own_d, ds_sem, dr_sem, do_sem, peers)

    def product(put, side):
        @pl.loop(0, ring)
        def _(k):
            h = 2 * k + side
            put(k, jnp.dot(o_old[h], dy_ref[0], preferred_element_type=F32)
                + jnp.dot(o_new[h], dy_ref[1], preferred_element_type=F32))

    def put_other(k, value):
        full[k, 1 - c] = value

    def put_mine(k, value):
        mine[k] = value

    def forward(b):
        o_t = o_refs[b][...].reshape(hidden, tok)

        @pl.loop(0, 3)
        def _(n):
            at_n = pl.ds(pl.multiple_of(n * wide, wide), wide)
            acc = lax.dot_general(o_t, wo_ref[:, at_n], tn, preferred_element_type=F32)
            y_ref[b, :, at_n] = (x_ref[b, :, at_n].astype(F32) + acc + bo_ref[:, at_n]).astype(BF16)

    def backward(b):
        @pl.loop(0, 3)
        def _(n):
            at_n = pl.ds(pl.multiple_of(n * wide, wide), wide)
            acc = None
            for k in range(0, peers, group):
                lhs = d_refs[b][k:k + group].reshape(-1, tok)
                one = lax.dot_general(lhs, w_ref[k * lhs.shape[0] // group:(k + group) * lhs.shape[0] // group, at_n], tn, preferred_element_type=F32)
                acc = one if acc is None else acc + one
            dn[:, at_n] = acc

        @pl.loop(0, tok // 32)
        def _(k):
            rows = pl.ds(pl.multiple_of(k * 32, 32), 32)
            x = x_ref[b, rows, :].astype(F32)
            dy = dy_ref[b, rows, :].astype(F32)
            d = dn[rows, :]
            cen = x - jnp.mean(x, axis=-1, keepdims=True)
            inv = lax.rsqrt(jnp.mean(cen * cen, axis=-1, keepdims=True) + NORM_EPS)
            hat = cen * inv
            for n, one in enumerate((d * hat, d, dy)):
                sums[n] += jnp.sum(one.reshape(4, 8, hidden), axis=0)
            e = d * gain_ref[...]
            m1 = jnp.mean(e, axis=-1, keepdims=True)
            m2 = jnp.mean(e * hat, axis=-1, keepdims=True)
            gx_ref[b, rows, :] = (dy + inv * (e - m1 - hat * m2)).astype(BF16)

    product(put_other, 1 - c)
    pair_copy = lambda side: remote(src_ref=full.at[:, side], dst_ref=full.at[:, side], send_sem=ps_sem, recv_sem=pr_sem, device_id=at(z, 1 - c))
    product(put_mine, c)
    pair_copy(1 - c).start()
    sums[...] = jnp.zeros_like(sums)
    pair_copy(1 - c).wait_send()
    pl.semaphore_signal(free_sem, inc=1, device_id=at(z, 1 - c), device_id_type=pl.DeviceIdType.MESH)
    pair_copy(c).wait_recv()

    @pl.loop(0, ring)
    def _(k):
        mine[k] = mine[k] + full[k, c]

    def reduce_copy(w, t):
        return remote(src_ref=mine.at[turn(-step[w] * (1 + t)), :, cols[w]], dst_ref=landed.at[w, t],
                      send_sem=rs_sem.at[w, t], recv_sem=rr_sem.at[w, t], device_id=at(turn(step[w]), c))

    def add(w, t, k):
        reduce_copy(w, t).wait_recv()
        mine[k, :, cols[w]] = mine[k, :, cols[w]] + landed[w, t]

    def hop(t):
        for w in range(2):
            add(w, t - 1, turn(-step[w] * (1 + t)))
            reduce_copy(w, t).start()

    for w in range(2):
        reduce_copy(w, 0).start()
    loads[1].wait()
    forward(0)
    hop(1)
    forward(1)
    hop(2)
    loads[0].wait()
    backward(0)

    @pl.loop(3, ring - 1)
    def _(t):
        hop(t)

    owners = hidden // 128
    lanes = lambda k: pl.ds(pl.multiple_of(k * 128, 128), 128)

    def small_copy(kind, frm, to):
        src, dst = ((rows_ref.at[:, lanes(to)], stage.at[frm]), (total.at[:, lanes(frm)],) * 2, (gb_ref, gb_all.at[frm]))[kind]
        return remote(src_ref=src, dst_ref=dst, send_sem=xs_sem.at[kind, to], recv_sem=xr_sem.at[kind, frm], device_id={"sp": to})

    def each(act, kind, only_to=False, only_from=False):
        @pl.loop(1, peers)
        def _(d):
            far = lax.rem(me + d, peers)

            def go():
                act(kind, far)

            if only_to:
                pl.when(far < owners)(go)
            elif only_from:
                pl.when(me < owners)(go)
            else:
                go()

    send = lambda kind, far: small_copy(kind, me, far).start()
    sent = lambda kind, far: small_copy(kind, me, far).wait_send()
    came = lambda kind, far: small_copy(kind, far, me).wait_recv()

    swap_wait(dqkv_ref, d_new, own_d, ds_sem, dr_sem, do_sem, peers)
    backward(1)
    rows_ref[...] = jnp.zeros_like(rows_ref)
    for n in range(3):
        rows_ref[n:n + 1, :] = jnp.sum(sums[n], axis=0, keepdims=True)
    gb_all[me] = gb_ref[...]
    for w in range(2):
        add(w, ring - 2, z)
    full[z, c] = mine[z]
    each(send, 0, only_to=True)
    each(send, 2)
    few = full.shape[2] // cuts
    block = lambda k, side, w, u: full.at[k, side, pl.ds(u * few, few), cols[w]]
    start, run, finish = ring_gather(block, *ring_sems, peers, cuts)
    pl.semaphore_wait(free_sem, 1)
    start()

    @pl.when(me < owners)
    def _():
        stage[me] = rows_ref[:, lanes(me)]

    each(came, 0, only_from=True)

    @pl.when(me < owners)
    def _():
        total[:, lanes(me)] = jnp.sum(stage[...], axis=0)

    each(send, 1, only_from=True)
    run()
    each(came, 1, only_to=True)
    each(came, 2)
    each(sent, 0, only_to=True)
    each(sent, 1, only_from=True)
    each(sent, 2)

    @pl.loop(0, ring - 1)
    def _(t):
        for w in range(2):
            reduce_copy(w, t).wait_send()

    finish()


def tail(dqkv, d_old, o_old, o_new, dy, x, w_flat, w_out, gain, b_out, gb, collective_id, cuts=3):
    peers, dim, tok = o_old.shape
    ring = peers // 2
    hidden = dy.shape[-1]
    hbm, vmem = pl.BlockSpec(memory_space=pltpu.HBM), pl.BlockSpec(memory_space=pltpu.VMEM)
    dma = pltpu.SemaphoreType.DMA
    like = lambda a: jax.ShapeDtypeStruct(a.shape, a.dtype)
    return pl.pallas_call(
        functools.partial(tail_body, peers=peers, cuts=cuts),
        name="tail",
        out_shape=[like(x), like(x), jax.ShapeDtypeStruct((ring, 2, dim, hidden), F32), jax.ShapeDtypeStruct((8, hidden), F32),
                   jax.ShapeDtypeStruct((peers,) + gb.shape, F32)],
        in_specs=[hbm, vmem, vmem, vmem, vmem, vmem, hbm, hbm, vmem, vmem, vmem],
        out_specs=[vmem] * 5,
        scratch_shapes=[pltpu.VMEM(dqkv.shape, BF16), pltpu.VMEM(w_flat.shape, BF16), pltpu.VMEM(w_out.shape, BF16),
                        pltpu.VMEM((tok, hidden), F32), pltpu.VMEM((ring, dim, hidden), F32),
                        pltpu.VMEM((2, ring - 1, dim, hidden // 2), F32), pltpu.VMEM((3, 8, hidden), F32), pltpu.VMEM((8, hidden), F32),
                        pltpu.VMEM((peers, 8, 128), F32), pltpu.VMEM(dqkv.shape[1:], BF16),
                        dma((peers - 1,)), dma((peers - 1,)), dma, dma, dma,
                        dma((2, ring - 1)), dma((2, ring - 1)), dma((2,)), dma((3, peers)), dma((3, peers)), pltpu.SemaphoreType.REGULAR]
        + ring_scratch(peers, cuts),
        cost_estimate=pl.CostEstimate(flops=10**11, bytes_accessed=64 << 20, transcendentals=0),
        compiler_params=pltpu.CompilerParams(collective_id=collective_id, has_side_effects=True, vmem_limit_bytes=44 << 20),
    )(dqkv, d_old, o_old, o_new, dy, x, w_flat, w_out, gain, b_out, gb)


def swap_body(*refs, peers, n):
    ins, outs, scratch = refs[:n], refs[n:2 * n], refs[2 * n:]
    meet(peers)
    for k in range(n):
        swap_start(ins[k], outs[k], *scratch[4 * k:4 * k + 4], peers)
    for k in range(n):
        swap_wait(ins[k], outs[k], *scratch[4 * k:4 * k + 4], peers)


def swap(xs, collective_id, name):
    hbm = pl.BlockSpec(memory_space=pltpu.HBM)
    peers = xs[0].shape[0]
    return pl.pallas_call(
        functools.partial(swap_body, peers=peers, n=len(xs)),
        name=name,
        out_shape=[jax.ShapeDtypeStruct(x.shape, x.dtype) for x in xs],
        in_specs=[hbm] * len(xs),
        out_specs=[hbm] * len(xs),
        scratch_shapes=sum((swap_scratch(x) for x in xs), []),
        cost_estimate=pl.CostEstimate(flops=24000 * sum(x.size for x in xs), bytes_accessed=4 * sum(x.size for x in xs), transcendentals=0),
        compiler_params=pltpu.CompilerParams(collective_id=collective_id, has_side_effects=True, vmem_limit_bytes=48 << 20),
    )(*xs)


def settle_body(*refs, n_in, first, n_plain):
    x_ref, plain, outs = refs[0], refs[1:1 + n_plain], refs[n_in:n_in + 1 + n_plain]
    buf, in_sem, out_sem, plain_sem = refs[n_in + 1 + n_plain:]
    heads, n = x_ref.shape[:2]
    reads = [pltpu.make_async_copy(x_ref.at[h], buf.at[h], in_sem.at[h]) for h in range(heads)]
    writes = [pltpu.make_async_copy(buf.at[h], outs[0].at[h, pl.ds(first, n)], out_sem.at[h]) for h in range(heads)]
    flat = [pltpu.make_async_copy(plain[k], outs[1 + k], plain_sem.at[k]) for k in range(n_plain)]
    for copy in reads + flat:
        copy.start()
    for read, write in zip(reads, writes):
        read.wait()
        write.start()
    for copy in writes + flat:
        copy.wait()


def settle(x, into, plain, lanes, first):
    heads, n, dim, hidden = x.shape
    hbm, vmem = pl.BlockSpec(memory_space=pltpu.HBM), pl.BlockSpec(memory_space=pltpu.VMEM)
    args = (x, *plain) + (() if into is None else (into,))
    dma = pltpu.SemaphoreType.DMA
    return pl.pallas_call(
        functools.partial(settle_body, n_in=len(args), first=first, n_plain=len(plain)), name="settle",
        out_shape=[jax.ShapeDtypeStruct((heads, lanes, dim, hidden), x.dtype)] + [jax.ShapeDtypeStruct(a.shape, a.dtype) for a in plain],
        in_specs=[hbm] + [vmem] * len(plain) + [hbm] * (into is not None), out_specs=[hbm] * (1 + len(plain)),
        input_output_aliases={} if into is None else {len(args) - 1: 0},
        scratch_shapes=[pltpu.VMEM(x.shape, x.dtype), dma((heads,)), dma((heads,)), dma((max(len(plain), 1),))],
        cost_estimate=pl.CostEstimate(flops=10**9, bytes_accessed=8 * x.size, transcendentals=0),
        compiler_params=pltpu.CompilerParams(vmem_limit_bytes=(60 << 20) - 4 * sum(a.size for a in plain)))(*args)


def norm_body(x_ref, gain_ref, bias_ref, *out_refs, pieces):
    for b in range(x_ref.shape[0]):
        @pl.loop(0, x_ref.shape[1] // 32)
        def _(k):
            rows = pl.ds(pl.multiple_of(k * 32, 32), 32)
            x = x_ref[b, rows, :].astype(F32)
            cen = x - jnp.mean(x, axis=-1, keepdims=True)
            hat = cen * lax.rsqrt(jnp.mean(cen * cen, axis=-1, keepdims=True) + NORM_EPS)
            out = (hat * gain_ref[...] + bias_ref[...]).astype(BF16)
            for (of, lo), out_ref in zip(pieces, out_refs):
                if of == b:
                    out_ref[rows, :] = out[:, lo:lo + out_ref.shape[1]]


def norm_forward(x, gain, bias, cut):
    batch, tok, hidden = x.shape
    pieces = [(0, 0), (0, cut)] + [(b, 0) for b in range(1, batch)]
    widths = [cut, hidden - cut] + [hidden] * (batch - 1)
    vmem = pl.BlockSpec(memory_space=pltpu.VMEM)
    return pl.pallas_call(
        functools.partial(norm_body, pieces=pieces), name="norm_forward",
        out_shape=[jax.ShapeDtypeStruct((tok, wide), BF16) for wide in widths],
        in_specs=[vmem] * 3, out_specs=[vmem] * len(widths),
        cost_estimate=pl.CostEstimate(flops=10**8, bytes_accessed=4 * x.size, transcendentals=0),
        compiler_params=pltpu.CompilerParams(vmem_limit_bytes=8 << 20))(x, gain, bias)


def solution(mesh):
    peers = mesh.shape["sp"]

    def block_fn(x_blk, pos_blk, keep_blk, ln_gain, ln_bias, w_qkv, b_qkv, w_out, b_out, dy_blk):
        batch, tok, hidden = x_blk.shape
        heads, dim = w_qkv.shape[1], w_qkv.shape[3]
        assert heads == peers
        seq = tok * peers
        blk = 2 * tok
        rank = lax.axis_index("sp")
        cut = 2 * hidden // 3
        x_lo, x_hi, *x_rest = norm_forward(x_blk, ln_gain.reshape(1, hidden), ln_bias.reshape(1, hidden), cut)
        xf = [lax.all_gather(one, "sp", axis=0, tiled=True) for one in [x_lo] + x_rest]
        do_loc = [lax.dot_general(w_out, dy_blk[b], NT, preferred_element_type=F32).astype(BF16).reshape(heads, dim, tok) for b in range(batch)]
        marks_loc = jnp.concatenate([pos_blk, keep_blk, jnp.zeros((8 - 2 * batch, tok), jnp.int32)])
        marks, do_first, x_hi = opening(marks_loc, do_loc[0], x_hi, 1)
        do_t = [do_first]
        xs = [[xf[0], x_hi.reshape(seq, hidden - cut)]] + [[one] for one in xf[1:]]
        w_t = jnp.transpose(w_qkv, (1, 2, 3, 0))
        w_head = lax.dynamic_index_in_dim(w_t, rank, 0, keepdims=False).reshape(3 * dim, hidden)
        b_head = lax.dynamic_index_in_dim(b_qkv, rank, 0, keepdims=False).reshape(3 * dim, 1)
        slope = jnp.exp2(-8.0 * (rank + 1).astype(F32) / heads)
        slope2 = (slope * LOG2E).reshape(1)
        gw, att = (), []
        for b in range(batch):
            pos = marks[:, b].reshape(1, seq).astype(F32)
            keep = marks[:, batch + b].reshape(1, seq)
            pref = jnp.broadcast_to(pos[0, ::blk][:, None], (seq // blk, 128))
            old = list(do_loc[b + 1:b + 2]) if b + 1 < batch else list(att)
            att_d, gw, att_o, swapped = attention(slope2, w_head, b_head, xs[b], do_t[b], jnp.where(keep > 0, pos, MASKED), pref, gw, old,
                                                  blk=blk, tok=tok, send_o=b + 1 == batch, collective_id=4 + b)
            if b + 1 < batch:
                do_t.append(swapped[0])
            att = [att_o, att_d]
        o_old, d_old = swapped
        gw_all = [lax.all_gather(one, "sp", axis=0, tiled=True).reshape(heads, -1, dim, hidden) for one in gw[:2]]
        lead = gw_all[0].shape[1]
        gb = jnp.pad(gw[2][:, 0].reshape(3, dim), ((0, 5), (0, 128 - dim)))
        y, gx, go_all, total, gb_all = tail(att_d, d_old, o_old, att_o, dy_blk, x_blk, w_t.reshape(3 * hidden, hidden), w_out,
                                            ln_gain.reshape(1, hidden), b_out.reshape(1, hidden), gb, 2)
        first, _ = lax.optimization_barrier((gw_all[0], y))
        gw_out, y, gx, go_all = settle(first, None, (y, gx, go_all.reshape(hidden, hidden)), 3, 0)
        second, gw_out = lax.optimization_barrier((gw_all[1], gw_out))
        gw_out = jnp.transpose(settle(second, gw_out, (), 3, lead)[0], (3, 0, 1, 2))
        return y, gx, gw_out, gb_all[:, :3, :dim], go_all, total[2], total[0], total[1]

    act_spec = P("dp", "sp", None)
    tok_spec = P("dp", "sp")
    in_specs = (act_spec, tok_spec, tok_spec, P(), P(), P(), P(), P(), P(), act_spec)
    out_specs = (act_spec, act_spec, P("dp", None, None, None), P("dp", None, None), P("dp", None), P("dp"), P("dp"), P("dp"))
    return jax.shard_map(block_fn, mesh=mesh, in_specs=in_specs, out_specs=out_specs, check_vma=False)
```

```python
import functools
import jax
import jax.numpy as jnp
from jax import lax
from jax.experimental import pallas as pl
from jax.experimental.pallas import tpu as pltpu
from jax.sharding import PartitionSpec as P

NORM_EPS = 1e-5

LOG2E = 1.4426950408889634
MASKED = -1e30
F32, BF16 = jnp.float32, jnp.bfloat16
NT = (((1,), (1,)), ((), ()))


def attn_body(w_hbm, b_ref, dot_ref, marks_ref, *refs, blk, tok, which, batch, n_swap, n_old, n_x, send_o):
    peers = dot_ref.shape[0]
    x_refs, refs = refs[:n_x], refs[n_x:]
    gw_old, old, refs = refs[:n_old], refs[n_old:n_old + n_swap], refs[n_old + n_swap:]
    (dqkv_ref, gwa_ref, gwb_ref, gb_ref, gbt_ref, o_out), got, refs = refs[:6], refs[6:6 + n_swap], refs[6 + n_swap:]
    w_ref, b_rep, x_buf, qkvt_ref, k_tok, v_tok, posk_ref, s_buf, q_pad, do_pad, o_acc, dq_acc, dk_acc, dv_acc, x_sem, w_sem = refs[:16]
    swaps = [(old[k], got[k]) + refs[16 + 4 * k:20 + 4 * k] for k in range(n_swap)]
    if send_o:
        o_ref, os_sem, or_sem = refs[-3:]
        o_new = o_out
    else:
        o_ref = o_out
    dim = dot_ref.shape[1]
    seq = dot_ref.shape[0] * tok
    pad = k_tok.shape[1] - dim
    nq = blk // tok
    steps = seq // blk
    scale = dim ** -0.5
    me = lax.axis_index("sp")
    step = pl.program_id(0)
    i = lax.rem(me // nq + step, steps)
    half = blk // 2
    sub = tok // 128

    def spread(row):
        return jnp.transpose(jnp.broadcast_to(row, (128, 128)))

    def x_copies(k):
        rows = pl.ds(pl.multiple_of(k * blk, blk), blk)
        lo = 0
        for n, x_ref in enumerate(x_refs):
            yield pltpu.make_async_copy(x_ref.at[rows], x_buf.at[rows, lo:lo + x_ref.shape[1]], x_sem.at[n, k])
            lo += x_ref.shape[1]

    def o_send(to):
        return pltpu.make_async_remote_copy(
            src_ref=o_ref.at[to], dst_ref=o_new.at[me], send_sem=os_sem.at[to], recv_sem=or_sem.at[me],
            device_id={"sp": to}, device_id_type=pl.DeviceIdType.MESH)

    def o_keep():
        return pltpu.make_async_copy(o_ref.at[me], o_new.at[me], os_sem.at[me])

    def o_start(at):
        for t in range(nq):
            to = lax.rem(me // nq + at, steps) * nq + t

            @pl.when(to != me)
            def _():
                o_send(to).start()

            @pl.when(to == me)
            def _():
                o_keep().start()

    @pl.when(step == 0)
    def _():
        w_load = pltpu.make_async_copy(w_hbm.at[me], w_ref, w_sem)
        w_load.start()
        for k in range(steps):
            for copy in x_copies(k):
                copy.start()
        meet(peers)
        for one in swaps:
            swap_start(*one, peers)
        dk_acc[...] = jnp.zeros_like(dk_acc)
        dv_acc[...] = jnp.zeros_like(dv_acc)
        q_pad[...] = jnp.zeros_like(q_pad)
        do_pad[...] = jnp.zeros_like(do_pad)
        for k in range(b_ref.shape[2] // 128):
            b_rep[k * 128:(k + 1) * 128, :] = spread(b_ref[me, :, k * 128:(k + 1) * 128])
        w_load.wait()

        @pl.loop(0, steps)
        def _(k):
            rows = pl.ds(pl.multiple_of(k * blk, blk), blk)
            for copy in x_copies(k):
                copy.wait()
            shift = jnp.concatenate([b_rep[0:3 * dim, :]] * (blk // 128), axis=1)
            qkvt_ref[:, rows] = (lax.dot_general(w_ref[...], x_buf[rows, :], NT, preferred_element_type=F32) + shift).astype(BF16)

            @pl.loop(0, blk // 128)
            def _(t):
                cols = pl.ds(pl.multiple_of(k * blk + t * 128, 128), 128)
                for base, dst in ((dim, k_tok), (2 * dim, v_tok)):
                    part = qkvt_ref[base:base + dim, cols].astype(F32)
                    whole = jnp.concatenate([part, jnp.zeros((pad, 128), F32)], axis=0)
                    dst[cols, :] = jnp.transpose(whole).astype(BF16)
                lanes = pl.ds(pl.multiple_of((t % sub) * 128, 128), 128)
                pos = marks_ref[k * nq + t // sub, which:which + 1, lanes].astype(F32)
                keep = marks_ref[k * nq + t // sub, batch + which:batch + which + 1, lanes]
                posk_ref[cols, :] = spread(jnp.where(keep > 0, pos, MASKED))

    if send_o:
        @pl.when(step > 0)
        def _():
            o_start(step - 1)

    qcols = pl.ds(pl.multiple_of(i * blk, blk), blk)
    q_pad[0:dim, :] = qkvt_ref[0:dim, qcols]
    for t in range(nq):
        do_pad[0:dim, t * tok:(t + 1) * tok] = dot_ref[i * nq + t]
    slope2 = jnp.exp2(jnp.full((1, 128), -8.0 / peers, F32) * (me + 1).astype(F32)) * LOG2E
    ref_pos = jnp.broadcast_to(marks_ref[i * nq, which:which + 1, 0:128][:, 0:1].astype(F32), (1, 128))
    c = scale * LOG2E

    def scores(j, m8, diag):
        for sub in range(2):
            rows = pl.ds(pl.multiple_of(j * blk + sub * half, half), half)
            st = jnp.dot(k_tok[rows, :], q_pad[...], preferred_element_type=F32)
            bias = (posk_ref[rows, :] - ref_pos) * slope2
            st = st * c + jnp.concatenate([bias] * (blk // 128), axis=1)
            if diag:
                key = lax.broadcasted_iota(jnp.int32, (half, blk), 0) + sub * half
                qry = lax.broadcasted_iota(jnp.int32, (half, blk), 1)
                st = jnp.where(key <= qry, st, MASKED)
            s_buf[rows, :] = st
            m8 = jnp.maximum(m8, jnp.max(st.reshape(half // 8, 8, blk), axis=0))
        return m8

    m8 = lax.fori_loop(0, i, lambda j, m: scores(j, m, False), jnp.full((8, blk), MASKED, F32))
    m8 = scores(i, m8, True)
    m = jnp.max(m8, axis=0, keepdims=True)

    def exps(j, l8):
        for sub in range(2):
            rows = pl.ds(pl.multiple_of(j * blk + sub * half, half), half)
            e = jnp.exp2(s_buf[rows, :] - m)
            s_buf[rows, :] = e
            l8 = l8 + jnp.sum(e.reshape(half // 8, 8, blk), axis=0)
        return l8

    l8 = lax.fori_loop(0, i + 1, exps, jnp.zeros((8, blk), F32))
    inv = 1.0 / jnp.sum(l8, axis=0, keepdims=True)
    o_acc[...] = jnp.zeros_like(o_acc)
    dq_acc[...] = jnp.zeros_like(dq_acc)

    def values(j, _):
        rows = pl.ds(pl.multiple_of(j * blk, blk), blk)
        p = s_buf[rows, :] * inv
        s_buf[rows, :] = p
        pb = p.astype(BF16)
        o_acc[...] += jnp.dot(qkvt_ref[2 * dim:3 * dim, rows], pb, preferred_element_type=F32)
        dv_acc[:, rows] += lax.dot_general(do_pad[0:dim, :], pb, NT, preferred_element_type=F32)
        return 0

    lax.fori_loop(0, i + 1, values, 0)
    o_lo = o_acc[...].astype(BF16)
    do_f = do_pad[0:dim, :].astype(F32)
    r = jnp.sum(do_f * o_lo.astype(F32), axis=0, keepdims=True)

    def grads(j, _):
        rows = pl.ds(pl.multiple_of(j * blk, blk), blk)
        g = jnp.dot(v_tok[rows, :], do_pad[...], preferred_element_type=F32)
        ds = (s_buf[rows, :] * (g - r)).astype(BF16)
        dq_acc[...] += jnp.dot(qkvt_ref[dim:2 * dim, rows], ds, preferred_element_type=F32)
        dk_acc[:, rows] += lax.dot_general(q_pad[0:dim, :], ds, NT, preferred_element_type=F32)
        return 0

    lax.fori_loop(0, i + 1, grads, 0)
    dq_lo = (dq_acc[...] * scale).astype(BF16)
    for t in range(nq):
        o_ref[i * nq + t] = o_lo[:, t * tok:(t + 1) * tok]
        dqkv_ref[i * nq + t, 0:dim] = dq_lo[:, t * tok:(t + 1) * tok]

    @pl.when(step == steps - 1)
    def _():
        @pl.loop(0, seq // tok)
        def _(t):
            cols = pl.ds(pl.multiple_of(t * tok, tok), tok)
            dqkv_ref[t, dim:2 * dim] = (dk_acc[:, cols] * scale).astype(BF16)
            dqkv_ref[t, 2 * dim:3 * dim] = dv_acc[:, cols].astype(BF16)

        if send_o:
            o_start(step)
        for k, ref in enumerate((gwa_ref, gwb_ref, gb_ref)):
            ref[...] = gw_old[k][...] if n_old else jnp.zeros_like(ref)
        ones = jnp.ones((blk, 128), BF16)

        @pl.loop(0, steps)
        def _(j):
            rows = pl.ds(pl.multiple_of(j * blk, blk), blk)
            for ref, lo, hi in ((gwa_ref, 0, 2 * dim), (gwb_ref, 2 * dim, 3 * dim)):
                lhs = jnp.concatenate([dqkv_ref[j * nq + t, lo:hi] for t in range(nq)], axis=1)
                ref[...] += jnp.dot(lhs, x_buf[rows, :], preferred_element_type=F32)
                gb_ref[lo:hi, :] += jnp.dot(lhs, ones, preferred_element_type=F32)

        gbt_ref[...] = jnp.zeros_like(gbt_ref)
        for k in range(3):
            part = jnp.concatenate([gb_ref[k * dim:(k + 1) * dim, :], jnp.zeros((pad, 128), F32)], axis=0)
            gbt_ref[k:k + 1, :] = jnp.transpose(part)[0:1, :]

        if send_o:
            o_keep().wait()
            for d in range(1, peers):
                frm = lax.rem(me + d, peers)
                o_send(frm).wait_send()
                pltpu.make_async_remote_copy(
                    src_ref=o_ref.at[frm], dst_ref=o_new.at[frm], send_sem=os_sem.at[frm], recv_sem=or_sem.at[frm],
                    device_id={"sp": frm}, device_id_type=pl.DeviceIdType.MESH).wait_recv()
        for one in swaps:
            swap_wait(*one, peers)


def attention(w_all, b_all, dot_, marks, xs, gw, old, *, blk, tok, which, batch, send_o, collective_id):
    blocks, dim, _ = dot_.shape
    seq, hidden = blocks * tok, w_all.shape[2]
    wide = 128 * pl.cdiv(dim, 128)
    hbm = pl.BlockSpec(memory_space=pltpu.HBM)
    full = lambda a: pl.BlockSpec(a.shape, lambda i: (0,) * len(a.shape), pipeline_mode=pl.Buffered(1))
    like = lambda a: jax.ShapeDtypeStruct(a.shape, a.dtype)
    outs = [jax.ShapeDtypeStruct((blocks, 3 * dim, tok), BF16), jax.ShapeDtypeStruct((2 * dim, hidden), F32),
            jax.ShapeDtypeStruct((dim, hidden), F32), jax.ShapeDtypeStruct((3 * dim, 128), F32), jax.ShapeDtypeStruct((8, 128), F32)]
    pairs = (seq // blk) * (seq // blk + 1) // 2
    dma = pltpu.SemaphoreType.DMA
    res = pl.pallas_call(
        functools.partial(attn_body, blk=blk, tok=tok, which=which, batch=batch, n_swap=len(old), n_old=len(gw), n_x=len(xs), send_o=send_o),
        name="attention",
        out_shape=outs + [like(dot_)] + [like(a) for a in old],
        grid=(seq // blk,),
        in_specs=[hbm, full(b_all), full(dot_), full(marks)] + [hbm] * len(xs) + [full(a) for a in gw] + [hbm] * len(old),
        out_specs=[full(a) for a in outs] + [hbm if send_o else full(dot_)] + [hbm] * len(old),
        scratch_shapes=[
            pltpu.VMEM(w_all.shape[1:], BF16), pltpu.VMEM((b_all.shape[2], 128), F32),
            pltpu.VMEM((seq, hidden), BF16), pltpu.VMEM((3 * dim, seq), BF16),
            pltpu.VMEM((seq, wide), BF16), pltpu.VMEM((seq, wide), BF16), pltpu.VMEM((seq, 128), F32),
            pltpu.VMEM((seq, blk), F32),
            pltpu.VMEM((wide, blk), BF16), pltpu.VMEM((wide, blk), BF16),
            pltpu.VMEM((dim, blk), F32), pltpu.VMEM((dim, blk), F32),
            pltpu.VMEM((dim, seq), F32), pltpu.VMEM((dim, seq), F32), dma((len(xs), seq // blk)), dma]
        + sum((swap_scratch(a) for a in old), []) + ([pltpu.VMEM(dot_.shape, BF16), dma((blocks,)), dma((blocks,))] if send_o else []),
        cost_estimate=pl.CostEstimate(flops=pairs * 6 * 2 * blk * blk * 256, bytes_accessed=24 << 20, transcendentals=pairs * blk * blk),
        compiler_params=pltpu.CompilerParams(dimension_semantics=("arbitrary",), vmem_limit_bytes=52 << 20,
                                             collective_id=collective_id, has_side_effects=True),
    )(w_all, b_all, dot_, marks, *xs, *gw, *old)
    return res[0], res[1:4], res[4], res[5], res[6:]


def peer_at(d, peers):
    return {"sp": lax.rem(lax.axis_index("sp") + d, peers)}


def greet(peers):
    barrier = pltpu.get_barrier_semaphore()
    for d in range(1, peers):
        pl.semaphore_signal(barrier, inc=1, device_id=peer_at(d, peers), device_id_type=pl.DeviceIdType.MESH)
    return lambda: pl.semaphore_wait(barrier, peers - 1)


def meet(peers):
    greet(peers)()


def swap_copies(x_ref, out_ref, send_sem, recv_sem, peers):
    me = lax.axis_index("sp")
    order = [d for near in range(peers // 2) for d in sorted({peers // 2 - near, peers // 2 + near})]
    return [pltpu.make_async_remote_copy(
        src_ref=x_ref.at[lax.rem(me + d, peers)], dst_ref=out_ref.at[me], send_sem=send_sem.at[d - 1], recv_sem=recv_sem.at[d - 1],
        device_id=peer_at(d, peers), device_id_type=pl.DeviceIdType.MESH) for d in order]


def swap_start(x_ref, out_ref, own, send_sem, recv_sem, own_sem, peers):
    me = lax.axis_index("sp")
    for copy in swap_copies(x_ref, out_ref, send_sem, recv_sem, peers):
        copy.start()
    take = pltpu.make_async_copy(x_ref.at[me], own, own_sem)
    take.start()
    take.wait()
    pltpu.make_async_copy(own, out_ref.at[me], own_sem).start()


def swap_wait(x_ref, out_ref, own, send_sem, recv_sem, own_sem, peers):
    pltpu.make_async_copy(own, out_ref.at[lax.axis_index("sp")], own_sem).wait()
    for copy in swap_copies(x_ref, out_ref, send_sem, recv_sem, peers):
        copy.wait()


def swap_scratch(x):
    peers = x.shape[0]
    return [pltpu.VMEM(x.shape[1:], x.dtype), pltpu.SemaphoreType.DMA((peers - 1,)), pltpu.SemaphoreType.DMA((peers - 1,)),
            pltpu.SemaphoreType.DMA]


STEP = (1, -1)


def hops(ring, s, w):
    return ring // 2 - (s != w)


def ring_gather(block, own, sems, peers, cuts):
    ring = peers // 2
    me = lax.axis_index("sp")
    z, c = me // 2, me % 2
    send_sem, recv_sem, over_sem, came_sem = sems
    turn = lambda k: lax.rem(z + k + 2 * ring, ring)
    lots = [(s, w, u) for u in range(cuts) for w in range(2) for s in range(2)]

    def copy(src, dst, one, two, to):
        return pltpu.make_async_remote_copy(src_ref=src, dst_ref=dst, send_sem=one, recv_sem=two, device_id={"sp": to},
                                            device_id_type=pl.DeviceIdType.MESH)

    def along(s, w, t, u):
        ref = block(turn(-STEP[s] * t), c, w, u)
        return copy(own(w, u) if t == 0 else ref, ref, send_sem.at[s, w, t, u], recv_sem.at[s, w, t, u], 2 * turn(STEP[s]) + c)

    def across(s, w, t, u, side):
        ref = block(turn(-STEP[s] * t), side, w, u)
        return copy(own(w, u) if t == 0 and side is c else ref, ref, over_sem.at[s, w, t, u], came_sem.at[s, w, t, u], 2 * z + 1 - c)

    home = [(0, w, 0, u) for u in range(cuts) for w in range(2)]
    moved = [(s, w, t, u) for t in range(1, ring // 2 + 1) for s, w, u in lots if t <= hops(ring, s, w)]

    def start():
        for s, w, u in lots:
            along(s, w, 0, u).start()
        for lot in home:
            across(*lot, c).start()

    def run():
        for s, w, t, u in moved:
            along(s, w, t - 1, u).wait_recv()
            if t < hops(ring, s, w):
                along(s, w, t, u).start()
            across(s, w, t, u, c).start()

    def finish():
        for s, w, t, u in moved:
            along(s, w, t - 1, u).wait_send()
        for lot in home + moved:
            across(*lot, c).wait_send()
            across(*lot, 1 - c).wait_recv()

    return start, run, finish


def ring_scratch(peers, cuts):
    dma = pltpu.SemaphoreType.DMA
    return [dma((2, 2, peers // 4, cuts))] * 2 + [dma((2, 2, peers // 4 + 1, cuts))] * 2


def opening_body(x_ref, dy_ref, wo_hbm, gain_ref, bias_ref, marks_ref, marks_all, do_t, x_all, *refs, peers, batch, cuts):
    x_out, do_out = refs[:batch - 1], refs[batch - 1:2 * batch - 2]
    x_own, do_own, wo_ref, own, ds_sem, dr_sem, do_sem, ms_sem, mr_sem, wo_sem, x_sem = refs[2 * batch - 2:2 * batch + 9]
    ring_sems = refs[2 * batch + 9:]
    me = lax.axis_index("sp")
    tok, dim = x_own.shape[0], do_own.shape[1]
    lot = tok // 2 // cuts
    rows_of = lambda w, u: pl.ds((w * cuts + u) * lot, lot)
    arrived = greet(peers)
    wo_load = pltpu.make_async_copy(wo_hbm, wo_ref, wo_sem)
    wo_load.start()

    def norm(b, out_ref):
        @pl.loop(0, tok // 32)
        def _(k):
            rows = pl.ds(pl.multiple_of(k * 32, 32), 32)
            x = x_ref[b, rows, :].astype(F32)
            cen = x - jnp.mean(x, axis=-1, keepdims=True)
            hat = cen * lax.rsqrt(jnp.mean(cen * cen, axis=-1, keepdims=True) + NORM_EPS)
            out_ref[rows, :] = (hat * gain_ref[...] + bias_ref[...]).astype(BF16)

    def product(b, out_ref):
        @pl.loop(0, peers // 4)
        def _(g):
            rows = pl.ds(pl.multiple_of(g * 4 * dim, 4 * dim), 4 * dim)
            out_ref[pl.ds(g * 4, 4)] = lax.dot_general(wo_ref[rows, :], dy_ref[b], NT, preferred_element_type=F32).astype(BF16).reshape(4, dim, tok)

    norm(0, x_own)
    block = lambda k, side, w, u: x_all.at[2 * k + side, rows_of(w, u)]
    start, run, finish = ring_gather(block, lambda w, u: x_own.at[rows_of(w, u)], ring_sems, peers, cuts)
    arrived()
    start()
    keep = pltpu.make_async_copy(x_own, x_all.at[me], x_sem)
    keep.start()
    marks = [pltpu.make_async_remote_copy(
        src_ref=marks_ref, dst_ref=marks_all.at[me], send_sem=ms_sem.at[d - 1], recv_sem=mr_sem.at[d - 1],
        device_id=peer_at(d, peers), device_id_type=pl.DeviceIdType.MESH) for d in range(1, peers)]
    for copy in marks:
        copy.start()
    marks_all[me] = marks_ref[...]
    wo_load.wait()
    product(0, do_own)
    for b in range(1, batch):
        norm(b, x_out[b - 1])
    swap_start(do_own, do_t, own, ds_sem, dr_sem, do_sem, peers)
    for b in range(1, batch):
        product(b, do_out[b - 1])
    run()
    keep.wait()
    for copy in marks:
        copy.wait()
    swap_wait(do_own, do_t, own, ds_sem, dr_sem, do_sem, peers)
    finish()


def opening(x, dy, w_out, gain, bias, marks, peers, collective_id, cuts=4):
    batch, tok, hidden = x.shape
    dim = hidden // peers
    hbm, vmem = pl.BlockSpec(memory_space=pltpu.HBM), pl.BlockSpec(memory_space=pltpu.VMEM)
    dma = pltpu.SemaphoreType.DMA
    do_shape, x_shape = jax.ShapeDtypeStruct((peers, dim, tok), BF16), jax.ShapeDtypeStruct((tok, hidden), BF16)
    res = pl.pallas_call(
        functools.partial(opening_body, peers=peers, batch=batch, cuts=cuts),
        name="opening",
        out_shape=[jax.ShapeDtypeStruct((peers,) + marks.shape, marks.dtype), do_shape, jax.ShapeDtypeStruct((peers, tok, hidden), BF16)]
        + [x_shape] * (batch - 1) + [do_shape] * (batch - 1),
        in_specs=[vmem, vmem, hbm, vmem, vmem, vmem],
        out_specs=[vmem, hbm, hbm] + [vmem] * (2 * batch - 2),
        scratch_shapes=[pltpu.VMEM(x_shape.shape, BF16), pltpu.VMEM(do_shape.shape, BF16), pltpu.VMEM(w_out.shape, BF16)] + swap_scratch(do_shape)
        + [dma((peers - 1,)), dma((peers - 1,)), dma, dma] + ring_scratch(peers, cuts),
        cost_estimate=pl.CostEstimate(flops=5 * 10**10, bytes_accessed=16 << 20, transcendentals=0),
        compiler_params=pltpu.CompilerParams(collective_id=collective_id, has_side_effects=True, vmem_limit_bytes=32 << 20),
    )(x, dy, w_out, gain, bias, marks)
    return res[0], res[1], res[2], res[3:2 + batch], res[2 + batch:]


def tail_body(dqkv_ref, d_hbm, oo_hbm, on_hbm, dy_hbm, x_hbm, w_hbm, wo_hbm, gain_ref, bo_ref, gb_ref, y_ref, gx_ref, full, total, gb_all,
              d_old, o_old, o_new, dy_ref, x_ref, d_new, w_ref, wo_ref, dn, mine, landed, sums, rows_ref, stage, own_d,
              ds_sem, dr_sem, do_sem, ps_sem, pr_sem, rs_sem, rr_sem, w_sem, xs_sem, xr_sem, free_sem, *ring_sems, peers, cuts):
    ring = peers // 2
    me = lax.axis_index("sp")
    z, c = me // 2, me % 2
    _, tok, hidden = x_ref.shape
    half = hidden // 2
    wide = hidden // 3
    few = full.shape[2] // cuts
    group = 8
    cols = (pl.ds(0, half), pl.ds(half, half))
    at = lambda zz, cc: {"sp": 2 * zz + cc}
    turn = lambda k: lax.rem(z + k + 2 * ring, ring)
    remote = functools.partial(pltpu.make_async_remote_copy, device_id_type=pl.DeviceIdType.MESH)
    tn = (((0,), (0,)), ((), ()))
    o_refs, d_refs = (o_old, o_new), (d_old, d_new)
    pairs = ((oo_hbm, o_old), (on_hbm, o_new), (dy_hbm, dy_ref), (x_hbm, x_ref), (wo_hbm, wo_ref), (d_hbm, d_old), (w_hbm, w_ref))
    loads = [pltpu.make_async_copy(src, dst, w_sem.at[k]) for k, (src, dst) in enumerate(pairs)]
    arrived = greet(peers)
    for load in loads:
        load.start()
    arrived()
    swap_start(dqkv_ref, d_new, own_d, ds_sem, dr_sem, do_sem, peers)
    for load in loads[:3]:
        load.wait()

    def product(put, side):
        @pl.loop(0, ring)
        def _(k):
            h = 2 * k + side
            put(k, jnp.dot(o_old[h], dy_ref[0], preferred_element_type=F32)
                + jnp.dot(o_new[h], dy_ref[1], preferred_element_type=F32))

    def put_other(k, value):
        full[k, 1 - c] = value

    def put_mine(k, value):
        mine[k] = value

    def forward(b):
        o_t = o_refs[b][...].reshape(hidden, tok)

        @pl.loop(0, 3)
        def _(n):
            at_n = pl.ds(pl.multiple_of(n * wide, wide), wide)
            acc = lax.dot_general(o_t, wo_ref[:, at_n], tn, preferred_element_type=F32)
            y_ref[b, :, at_n] = (x_ref[b, :, at_n].astype(F32) + acc + bo_ref[:, at_n]).astype(BF16)

    def backward(b):
        @pl.loop(0, 3)
        def _(n):
            at_n = pl.ds(pl.multiple_of(n * wide, wide), wide)
            acc = None
            for k in range(0, peers, group):
                lhs = d_refs[b][k:k + group].reshape(-1, tok)
                one = lax.dot_general(lhs, w_ref[k * lhs.shape[0] // group:(k + group) * lhs.shape[0] // group, at_n], tn, preferred_element_type=F32)
                acc = one if acc is None else acc + one
            dn[:, at_n] = acc

        @pl.loop(0, tok // 32)
        def _(k):
            rows = pl.ds(pl.multiple_of(k * 32, 32), 32)
            x = x_ref[b, rows, :].astype(F32)
            dy = dy_ref[b, rows, :].astype(F32)
            d = dn[rows, :]
            cen = x - jnp.mean(x, axis=-1, keepdims=True)
            inv = lax.rsqrt(jnp.mean(cen * cen, axis=-1, keepdims=True) + NORM_EPS)
            hat = cen * inv
            for n, one in enumerate((d * hat, d, dy)):
                sums[n] += jnp.sum(one.reshape(4, 8, hidden), axis=0)
            e = d * gain_ref[...]
            m1 = jnp.mean(e, axis=-1, keepdims=True)
            m2 = jnp.mean(e * hat, axis=-1, keepdims=True)
            gx_ref[b, rows, :] = (dy + inv * (e - m1 - hat * m2)).astype(BF16)

    product(put_other, 1 - c)
    pair_copy = lambda side: remote(src_ref=full.at[:, side], dst_ref=full.at[:, side], send_sem=ps_sem, recv_sem=pr_sem, device_id=at(z, 1 - c))
    product(put_mine, c)
    pair_copy(1 - c).start()
    sums[...] = jnp.zeros_like(sums)
    pair_copy(1 - c).wait_send()
    pl.semaphore_signal(free_sem, inc=1, device_id=at(z, 1 - c), device_id_type=pl.DeviceIdType.MESH)
    pair_copy(c).wait_recv()

    @pl.loop(0, ring)
    def _(k):
        mine[k] = mine[k] + full[k, c]

    lots = [(s, w, u) for u in range(cuts) for w in range(2) for s in range(2)]

    def reduce_copy(s, w, t, u):
        return remote(src_ref=mine.at[turn(STEP[s] * (hops(ring, s, w) - t)), pl.ds(u * few, few), cols[w]], dst_ref=landed.at[s, w, t, u],
                      send_sem=rs_sem.at[s, w, t, u], recv_sem=rr_sem.at[s, w, t, u], device_id=at(turn(STEP[s]), c))

    def fold(s, w, t, u):
        reduce_copy(s, w, t, u).wait_recv()
        at_k = (turn(STEP[s] * (hops(ring, s, w) - t - 1)), pl.ds(u * few, few), cols[w])
        mine[at_k] = mine[at_k] + landed[s, w, t, u]

    def hop(t):
        for s, w, u in lots:
            if t < hops(ring, s, w):
                fold(s, w, t - 1, u)
                reduce_copy(s, w, t, u).start()

    for lot in lots:
        reduce_copy(*lot[:2], 0, lot[2]).start()
    loads[3].wait()
    loads[4].wait()
    forward(0)
    for t in range(1, ring // 2):
        hop(t)
        if t == 1:
            forward(1)
        if t == 2:
            loads[5].wait()
            loads[6].wait()
            backward(0)
    for s, w, u in lots:
        fold(s, w, hops(ring, s, w) - 1, u)
    full[z, c] = mine[z]
    block = lambda k, side, w, u: full.at[k, side, pl.ds(u * few, few), cols[w]]
    start, run, finish = ring_gather(block, lambda w, u: block(z, c, w, u), ring_sems, peers, cuts)
    pl.semaphore_wait(free_sem, 1)
    start()
    run()
    owners = hidden // 128
    lanes = lambda k: pl.ds(pl.multiple_of(k * 128, 128), 128)

    def small_copy(kind, frm, to):
        src, dst = ((rows_ref.at[:, lanes(to)], stage.at[frm]), (total.at[:, lanes(frm)],) * 2, (gb_ref, gb_all.at[frm]))[kind]
        return remote(src_ref=src, dst_ref=dst, send_sem=xs_sem.at[kind, to], recv_sem=xr_sem.at[kind, frm], device_id={"sp": to})

    def each(act, kind, only_to=False, only_from=False):
        @pl.loop(1, peers)
        def _(d):
            far = lax.rem(me + d, peers)

            def go():
                act(kind, far)

            if only_to:
                pl.when(far < owners)(go)
            elif only_from:
                pl.when(me < owners)(go)
            else:
                go()

    send = lambda kind, far: small_copy(kind, me, far).start()
    sent = lambda kind, far: small_copy(kind, me, far).wait_send()
    came = lambda kind, far: small_copy(kind, far, me).wait_recv()

    swap_wait(dqkv_ref, d_new, own_d, ds_sem, dr_sem, do_sem, peers)
    backward(1)
    rows_ref[...] = jnp.zeros_like(rows_ref)
    for n in range(3):
        rows_ref[n:n + 1, :] = jnp.sum(sums[n], axis=0, keepdims=True)
    gb_all[me] = gb_ref[...]
    each(send, 2)

    @pl.when(me < owners)
    def _():
        stage[me] = rows_ref[:, lanes(me)]

    each(send, 0, only_to=True)
    each(came, 0, only_from=True)

    @pl.when(me < owners)
    def _():
        total[:, lanes(me)] = jnp.sum(stage[...], axis=0)

    each(send, 1, only_from=True)
    each(came, 1, only_to=True)
    each(came, 2)
    each(sent, 0, only_to=True)
    each(sent, 1, only_from=True)
    each(sent, 2)
    for s, w, u in lots:
        for t in range(hops(ring, s, w)):
            reduce_copy(s, w, t, u).wait_send()
    finish()


def tail(dqkv, d_old, o_old, o_new, dy, x, w_flat, w_out, gain, b_out, gb, collective_id, cuts=2):
    peers, dim, tok = o_old.shape
    ring = peers // 2
    hidden = dy.shape[-1]
    hbm, vmem = pl.BlockSpec(memory_space=pltpu.HBM), pl.BlockSpec(memory_space=pltpu.VMEM)
    dma = pltpu.SemaphoreType.DMA
    like = lambda a: jax.ShapeDtypeStruct(a.shape, a.dtype)
    held = lambda a: pltpu.VMEM(a.shape, a.dtype)
    steps = (2, 2, ring // 2, cuts)
    return pl.pallas_call(
        functools.partial(tail_body, peers=peers, cuts=cuts),
        name="tail",
        out_shape=[like(x), like(x), jax.ShapeDtypeStruct((ring, 2, dim, hidden), F32), jax.ShapeDtypeStruct((8, hidden), F32),
                   jax.ShapeDtypeStruct((peers,) + gb.shape, F32)],
        in_specs=[hbm] * 8 + [vmem] * 3,
        out_specs=[vmem] * 5,
        scratch_shapes=[held(a) for a in (d_old, o_old, o_new, dy, x, dqkv, w_flat, w_out)]
        + [pltpu.VMEM((tok, hidden), F32), pltpu.VMEM((ring, dim, hidden), F32),
           pltpu.VMEM(steps + (dim // cuts, hidden // 2), F32), pltpu.VMEM((3, 8, hidden), F32), pltpu.VMEM((8, hidden), F32),
           pltpu.VMEM((peers, 8, 128), F32), pltpu.VMEM(dqkv.shape[1:], BF16),
           dma((peers - 1,)), dma((peers - 1,)), dma, dma, dma, dma(steps), dma(steps), dma((7,)), dma((3, peers)), dma((3, peers)),
           pltpu.SemaphoreType.REGULAR] + ring_scratch(peers, cuts),
        cost_estimate=pl.CostEstimate(flops=10**11, bytes_accessed=64 << 20, transcendentals=0),
        compiler_params=pltpu.CompilerParams(collective_id=collective_id, has_side_effects=True, vmem_limit_bytes=56 << 20),
    )(dqkv, d_old, o_old, o_new, dy, x, w_flat, w_out, gain, b_out, gb)


def settle_body(*refs, n_in, first, n_plain):
    x_ref, plain, outs = refs[0], refs[1:1 + n_plain], refs[n_in:n_in + 1 + n_plain]
    buf, in_sem, out_sem, plain_sem = refs[n_in + 1 + n_plain:]
    heads, n = x_ref.shape[:2]
    reads = [pltpu.make_async_copy(x_ref.at[h], buf.at[h], in_sem.at[h]) for h in range(heads)]
    writes = [pltpu.make_async_copy(buf.at[h], outs[0].at[h, pl.ds(first, n)], out_sem.at[h]) for h in range(heads)]
    flat = [pltpu.make_async_copy(plain[k], outs[1 + k], plain_sem.at[k]) for k in range(n_plain)]
    for copy in reads + flat:
        copy.start()
    for read, write in zip(reads, writes):
        read.wait()
        write.start()
    for copy in writes + flat:
        copy.wait()


def settle(x, into, plain, lanes, first):
    heads, n, dim, hidden = x.shape
    hbm, vmem = pl.BlockSpec(memory_space=pltpu.HBM), pl.BlockSpec(memory_space=pltpu.VMEM)
    args = (x, *plain) + (() if into is None else (into,))
    dma = pltpu.SemaphoreType.DMA
    return pl.pallas_call(
        functools.partial(settle_body, n_in=len(args), first=first, n_plain=len(plain)), name="settle",
        out_shape=[jax.ShapeDtypeStruct((heads, lanes, dim, hidden), x.dtype)] + [jax.ShapeDtypeStruct(a.shape, a.dtype) for a in plain],
        in_specs=[hbm] + [vmem] * len(plain) + [hbm] * (into is not None), out_specs=[hbm] * (1 + len(plain)),
        input_output_aliases={} if into is None else {len(args) - 1: 0},
        scratch_shapes=[pltpu.VMEM(x.shape, x.dtype), dma((heads,)), dma((heads,)), dma((max(len(plain), 1),))],
        cost_estimate=pl.CostEstimate(flops=10**9, bytes_accessed=8 * x.size, transcendentals=0),
        compiler_params=pltpu.CompilerParams(vmem_limit_bytes=(60 << 20) - 4 * sum(a.size for a in plain)))(*args)


def solution(mesh):
    peers = mesh.shape["sp"]

    def block_fn(x_blk, pos_blk, keep_blk, ln_gain, ln_bias, w_qkv, b_qkv, w_out, b_out, dy_blk):
        batch, tok, hidden = x_blk.shape
        heads, dim = w_qkv.shape[1], w_qkv.shape[3]
        assert heads == peers
        seq = tok * peers
        blk = 2 * tok
        row = lambda v: v.reshape(1, hidden)
        w_all = jnp.transpose(w_qkv, (1, 2, 3, 0)).reshape(heads, 3 * dim, hidden)
        b_all = jnp.pad(b_qkv.reshape(heads, 3 * dim), ((0, 0), (0, -3 * dim % 128)))[:, None]
        marks_loc = jnp.concatenate([pos_blk, keep_blk, jnp.zeros((8 - 2 * batch, tok), jnp.int32)])
        marks, do_first, x_first, x_rest, do_rest = opening(x_blk, dy_blk, w_out, row(ln_gain), row(ln_bias), marks_loc, peers, 1)
        xs = [x_first.reshape(seq, hidden)] + [lax.all_gather(one, "sp", axis=0, tiled=True) for one in x_rest]
        do_t = [do_first]
        gw, att = (), []
        for b in range(batch):
            old = list(do_rest[b:b + 1]) if b + 1 < batch else att
            att_d, gw, gb, att_o, swapped = attention(w_all, b_all, do_t[b], marks, [xs[b]], gw, old, blk=blk, tok=tok, which=b, batch=batch,
                                                      send_o=b + 1 == batch, collective_id=4 + b)
            if b + 1 < batch:
                do_t.append(swapped[0])
            att = [att_o, att_d]
        o_old, d_old = swapped
        gw_all = [lax.all_gather(one, "sp", axis=0, tiled=True).reshape(heads, -1, dim, hidden) for one in gw[:2]]
        lead = gw_all[0].shape[1]
        y, gx, go_all, total, gb_all = tail(att_d, d_old, o_old, att_o, dy_blk, x_blk, w_all.reshape(3 * hidden, hidden), w_out,
                                            row(ln_gain), row(b_out), gb, 2)
        first, _ = lax.optimization_barrier((gw_all[0], y))
        gw_out, y, gx, go_all = settle(first, None, (y, gx, go_all.reshape(hidden, hidden)), 3, 0)
        second, gw_out = lax.optimization_barrier((gw_all[1], gw_out))
        gw_out = jnp.transpose(settle(second, gw_out, (), 3, lead)[0], (3, 0, 1, 2))
        return y, gx, gw_out, gb_all[:, :3, :dim], go_all, total[2], total[0], total[1]

    act_spec = P("dp", "sp", None)
    tok_spec = P("dp", "sp")
    in_specs = (act_spec, tok_spec, tok_spec, P(), P(), P(), P(), P(), P(), act_spec)
    out_specs = (act_spec, act_spec, P("dp", None, None, None), P("dp", None, None), P("dp", None), P("dp"), P("dp"), P("dp"))
    return jax.shard_map(block_fn, mesh=mesh, in_specs=in_specs, out_specs=out_specs, check_vma=False)
```

```python
import functools
import jax
import jax.numpy as jnp
from jax import lax
from jax.experimental import pallas as pl
from jax.experimental.pallas import tpu as pltpu
from jax.sharding import PartitionSpec as P

NORM_EPS = 1e-5

LOG2E = 1.4426950408889634
MASKED = -1e30
VMEM_LIMIT = 62 << 20
F32, BF16 = jnp.float32, jnp.bfloat16
NT = (((1,), (1,)), ((), ()))


def attn_body(w_hbm, b_ref, dot_ref, marks_ref, x_ref, *refs, blk, tok, which, batch, n_swap, n_old, send_o):
    peers = dot_ref.shape[0]
    gw_old, old, refs = refs[:n_old], refs[n_old:n_old + n_swap], refs[n_old + n_swap:]
    (dqkv_ref, gwa_ref, gwb_ref, gb_ref, gbt_ref, o_out), got, refs = refs[:6], refs[6:6 + n_swap], refs[6 + n_swap:]
    x_buf, refs = refs[0], refs[1:]
    w_ref, b_rep, qkvt_ref, k_tok, v_tok, posk_ref, s_buf, q_pad, do_pad, o_acc, dq_acc, dk_acc, dv_acc, x_sem, w_sem = refs[:15]
    swaps = [(old[k], got[k]) + refs[15 + 4 * k:19 + 4 * k] for k in range(n_swap)]
    if send_o:
        o_ref, os_sem, or_sem = refs[-3:]
        o_new = o_out
    else:
        o_ref = o_out
    dim = dot_ref.shape[1]
    seq = dot_ref.shape[0] * tok
    pad = k_tok.shape[1] - dim
    nq = blk // tok
    steps = seq // blk
    scale = dim ** -0.5
    me = lax.axis_index("sp")
    step = pl.program_id(0)
    i = lax.rem(me // nq + step, steps)
    half = blk // 2
    sub = tok // 128

    def spread(row):
        return jnp.transpose(jnp.broadcast_to(row, (128, 128)))

    def x_copy(k):
        rows = pl.ds(pl.multiple_of(k * blk, blk), blk)
        return pltpu.make_async_copy(x_ref.at[rows], x_buf.at[rows], x_sem.at[k])

    def o_send(to):
        return pltpu.make_async_remote_copy(
            src_ref=o_ref.at[to], dst_ref=o_new.at[me], send_sem=os_sem.at[to], recv_sem=or_sem.at[me],
            device_id={"sp": to}, device_id_type=pl.DeviceIdType.MESH)

    def o_keep():
        return pltpu.make_async_copy(o_ref.at[me], o_new.at[me], os_sem.at[me])

    def o_start(at):
        for t in range(nq):
            to = lax.rem(me // nq + at, steps) * nq + t

            @pl.when(to != me)
            def _():
                o_send(to).start()

            @pl.when(to == me)
            def _():
                o_keep().start()

    @pl.when(step == 0)
    def _():
        w_load = pltpu.make_async_copy(w_hbm.at[me], w_ref, w_sem)
        w_load.start()
        for k in range(steps):
            x_copy(k).start()
        meet(peers)
        for one in swaps:
            swap_start(*one, peers)
        dk_acc[...] = jnp.zeros_like(dk_acc)
        dv_acc[...] = jnp.zeros_like(dv_acc)
        q_pad[...] = jnp.zeros_like(q_pad)
        do_pad[...] = jnp.zeros_like(do_pad)
        for k in range(b_ref.shape[2] // 128):
            b_rep[k * 128:(k + 1) * 128, :] = spread(b_ref[me, :, k * 128:(k + 1) * 128])
        w_load.wait()

        @pl.loop(0, steps)
        def _(k):
            rows = pl.ds(pl.multiple_of(k * blk, blk), blk)
            x_copy(k).wait()
            shift = jnp.concatenate([b_rep[0:3 * dim, :]] * (blk // 128), axis=1)
            qkvt_ref[:, rows] = (lax.dot_general(w_ref[...], x_buf[rows, :], NT, preferred_element_type=F32) + shift).astype(BF16)

            @pl.loop(0, blk // 128)
            def _(t):
                cols = pl.ds(pl.multiple_of(k * blk + t * 128, 128), 128)
                for base, dst in ((dim, k_tok), (2 * dim, v_tok)):
                    part = qkvt_ref[base:base + dim, cols].astype(F32)
                    whole = jnp.concatenate([part, jnp.zeros((pad, 128), F32)], axis=0)
                    dst[cols, :] = jnp.transpose(whole).astype(BF16)
                lanes = pl.ds(pl.multiple_of((t % sub) * 128, 128), 128)
                pos = marks_ref[k * nq + t // sub, which:which + 1, lanes].astype(F32)
                keep = marks_ref[k * nq + t // sub, batch + which:batch + which + 1, lanes]
                posk_ref[cols, :] = spread(jnp.where(keep > 0, pos, MASKED))

    if send_o:
        @pl.when(step > 0)
        def _():
            o_start(step - 1)

    qcols = pl.ds(pl.multiple_of(i * blk, blk), blk)
    q_pad[0:dim, :] = qkvt_ref[0:dim, qcols]
    for t in range(nq):
        do_pad[0:dim, t * tok:(t + 1) * tok] = dot_ref[i * nq + t]
    slope2 = jnp.exp2(jnp.full((1, 128), -8.0 / peers, F32) * (me + 1).astype(F32)) * LOG2E
    ref_pos = jnp.broadcast_to(marks_ref[i * nq, which:which + 1, 0:128][:, 0:1].astype(F32), (1, 128))
    c = scale * LOG2E

    def scores(j, m8, diag):
        for sub in range(2):
            rows = pl.ds(pl.multiple_of(j * blk + sub * half, half), half)
            st = jnp.dot(k_tok[rows, :], q_pad[...], preferred_element_type=F32)
            bias = (posk_ref[rows, :] - ref_pos) * slope2
            st = st * c + jnp.concatenate([bias] * (blk // 128), axis=1)
            if diag:
                key = lax.broadcasted_iota(jnp.int32, (half, blk), 0) + sub * half
                qry = lax.broadcasted_iota(jnp.int32, (half, blk), 1)
                st = jnp.where(key <= qry, st, MASKED)
            s_buf[rows, :] = st
            m8 = jnp.maximum(m8, jnp.max(st.reshape(half // 8, 8, blk), axis=0))
        return m8

    m8 = lax.fori_loop(0, i, lambda j, m: scores(j, m, False), jnp.full((8, blk), MASKED, F32))
    m8 = scores(i, m8, True)
    m = jnp.max(m8, axis=0, keepdims=True)

    def exps(j, l8):
        for sub in range(2):
            rows = pl.ds(pl.multiple_of(j * blk + sub * half, half), half)
            e = jnp.exp2(s_buf[rows, :] - m)
            s_buf[rows, :] = e
            l8 = l8 + jnp.sum(e.reshape(half // 8, 8, blk), axis=0)
        return l8

    l8 = lax.fori_loop(0, i + 1, exps, jnp.zeros((8, blk), F32))
    inv = 1.0 / jnp.sum(l8, axis=0, keepdims=True)
    o_acc[...] = jnp.zeros_like(o_acc)
    dq_acc[...] = jnp.zeros_like(dq_acc)

    def values(j, _):
        rows = pl.ds(pl.multiple_of(j * blk, blk), blk)
        p = s_buf[rows, :] * inv
        s_buf[rows, :] = p
        pb = p.astype(BF16)
        o_acc[...] += jnp.dot(qkvt_ref[2 * dim:3 * dim, rows], pb, preferred_element_type=F32)
        dv_acc[:, rows] += lax.dot_general(do_pad[0:dim, :], pb, NT, preferred_element_type=F32)
        return 0

    lax.fori_loop(0, i + 1, values, 0)
    o_lo = o_acc[...].astype(BF16)
    do_f = do_pad[0:dim, :].astype(F32)
    r = jnp.sum(do_f * o_lo.astype(F32), axis=0, keepdims=True)

    def grads(j, _):
        rows = pl.ds(pl.multiple_of(j * blk, blk), blk)
        g = jnp.dot(v_tok[rows, :], do_pad[...], preferred_element_type=F32)
        ds = (s_buf[rows, :] * (g - r)).astype(BF16)
        dq_acc[...] += jnp.dot(qkvt_ref[dim:2 * dim, rows], ds, preferred_element_type=F32)
        dk_acc[:, rows] += lax.dot_general(q_pad[0:dim, :], ds, NT, preferred_element_type=F32)
        return 0

    lax.fori_loop(0, i + 1, grads, 0)
    dq_lo = (dq_acc[...] * scale).astype(BF16)
    for t in range(nq):
        o_ref[i * nq + t] = o_lo[:, t * tok:(t + 1) * tok]
        dqkv_ref[i * nq + t, 0:dim] = dq_lo[:, t * tok:(t + 1) * tok]

    @pl.when(step == steps - 1)
    def _():
        @pl.loop(0, seq // tok)
        def _(t):
            cols = pl.ds(pl.multiple_of(t * tok, tok), tok)
            dqkv_ref[t, dim:2 * dim] = (dk_acc[:, cols] * scale).astype(BF16)
            dqkv_ref[t, 2 * dim:3 * dim] = dv_acc[:, cols].astype(BF16)

        if send_o:
            o_start(step)
        for k, ref in enumerate((gwa_ref, gwb_ref, gb_ref)):
            ref[...] = gw_old[k][...] if n_old else jnp.zeros_like(ref)
        ones = jnp.ones((blk, 128), BF16)

        @pl.loop(0, steps)
        def _(j):
            rows = pl.ds(pl.multiple_of(j * blk, blk), blk)
            for ref, lo, hi in ((gwa_ref, 0, 2 * dim), (gwb_ref, 2 * dim, 3 * dim)):
                lhs = jnp.concatenate([dqkv_ref[j * nq + t, lo:hi] for t in range(nq)], axis=1)
                ref[...] += jnp.dot(lhs, x_buf[rows, :], preferred_element_type=F32)
                gb_ref[lo:hi, :] += jnp.dot(lhs, ones, preferred_element_type=F32)

        gbt_ref[...] = jnp.zeros_like(gbt_ref)
        for k in range(3):
            part = jnp.concatenate([gb_ref[k * dim:(k + 1) * dim, :], jnp.zeros((pad, 128), F32)], axis=0)
            gbt_ref[k:k + 1, :] = jnp.transpose(part)[0:1, :]

        if send_o:
            o_keep().wait()
            for d in range(1, peers):
                frm = lax.rem(me + d, peers)
                o_send(frm).wait_send()
                pltpu.make_async_remote_copy(
                    src_ref=o_ref.at[frm], dst_ref=o_new.at[frm], send_sem=os_sem.at[frm], recv_sem=or_sem.at[frm],
                    device_id={"sp": frm}, device_id_type=pl.DeviceIdType.MESH).wait_recv()
        for one in swaps:
            swap_wait(*one, peers)


def attention(w_all, b_all, dot_, marks, x, gw, old, *, blk, tok, which, batch, send_o, collective_id):
    blocks, dim, _ = dot_.shape
    seq, hidden = blocks * tok, w_all.shape[2]
    wide = 128 * pl.cdiv(dim, 128)
    hbm = pl.BlockSpec(memory_space=pltpu.HBM)
    full = lambda a: pl.BlockSpec(a.shape, lambda i: (0,) * len(a.shape), pipeline_mode=pl.Buffered(1))
    like = lambda a: jax.ShapeDtypeStruct(a.shape, a.dtype)
    outs = [jax.ShapeDtypeStruct((blocks, 3 * dim, tok), BF16), jax.ShapeDtypeStruct((2 * dim, hidden), F32),
            jax.ShapeDtypeStruct((dim, hidden), F32), jax.ShapeDtypeStruct((3 * dim, 128), F32), jax.ShapeDtypeStruct((8, 128), F32)]
    pairs = (seq // blk) * (seq // blk + 1) // 2
    dma = pltpu.SemaphoreType.DMA
    res = pl.pallas_call(
        functools.partial(attn_body, blk=blk, tok=tok, which=which, batch=batch, n_swap=len(old), n_old=len(gw), send_o=send_o),
        name="attention",
        out_shape=outs + [like(dot_)] + [like(a) for a in old],
        grid=(seq // blk,),
        in_specs=[hbm, full(b_all), full(dot_), full(marks), hbm] + [full(a) for a in gw] + [hbm] * len(old),
        out_specs=[full(a) for a in outs] + [hbm if send_o else full(dot_)] + [hbm] * len(old),
        scratch_shapes=[
            pltpu.VMEM((seq, hidden), BF16),
            pltpu.VMEM(w_all.shape[1:], BF16), pltpu.VMEM((b_all.shape[2], 128), F32), pltpu.VMEM((3 * dim, seq), BF16),
            pltpu.VMEM((seq, wide), BF16), pltpu.VMEM((seq, wide), BF16), pltpu.VMEM((seq, 128), F32),
            pltpu.VMEM((seq, blk), F32),
            pltpu.VMEM((wide, blk), BF16), pltpu.VMEM((wide, blk), BF16),
            pltpu.VMEM((dim, blk), F32), pltpu.VMEM((dim, blk), F32),
            pltpu.VMEM((dim, seq), F32), pltpu.VMEM((dim, seq), F32), dma((seq // blk,)), dma]
        + sum((swap_scratch(a) for a in old), []) + ([pltpu.VMEM(dot_.shape, BF16), dma((blocks,)), dma((blocks,))] if send_o else []),
        cost_estimate=pl.CostEstimate(flops=pairs * 6 * 2 * blk * blk * 256, bytes_accessed=24 << 20, transcendentals=pairs * blk * blk),
        compiler_params=pltpu.CompilerParams(dimension_semantics=("arbitrary",), vmem_limit_bytes=VMEM_LIMIT,
                                             collective_id=collective_id, has_side_effects=True),
    )(w_all, b_all, dot_, marks, x, *gw, *old)
    return res[0], res[1:4], res[4], res[5], res[6:]


def peer_at(d, peers):
    return {"sp": lax.rem(lax.axis_index("sp") + d, peers)}


def greet(peers):
    barrier = pltpu.get_barrier_semaphore()
    for d in range(1, peers):
        pl.semaphore_signal(barrier, inc=1, device_id=peer_at(d, peers), device_id_type=pl.DeviceIdType.MESH)
    return lambda: pl.semaphore_wait(barrier, peers - 1)


def meet(peers):
    greet(peers)()


def swap_copies(x_ref, out_ref, send_sem, recv_sem, peers):
    me = lax.axis_index("sp")
    order = [d for near in range(peers // 2) for d in sorted({peers // 2 - near, peers // 2 + near})]
    return [pltpu.make_async_remote_copy(
        src_ref=x_ref.at[lax.rem(me + d, peers)], dst_ref=out_ref.at[me], send_sem=send_sem.at[d - 1], recv_sem=recv_sem.at[d - 1],
        device_id=peer_at(d, peers), device_id_type=pl.DeviceIdType.MESH) for d in order]


def swap_start(x_ref, out_ref, own, send_sem, recv_sem, own_sem, peers):
    me = lax.axis_index("sp")
    for copy in swap_copies(x_ref, out_ref, send_sem, recv_sem, peers):
        copy.start()
    take = pltpu.make_async_copy(x_ref.at[me], own, own_sem)
    take.start()
    take.wait()
    pltpu.make_async_copy(own, out_ref.at[me], own_sem).start()


def swap_wait(x_ref, out_ref, own, send_sem, recv_sem, own_sem, peers):
    pltpu.make_async_copy(own, out_ref.at[lax.axis_index("sp")], own_sem).wait()
    for copy in swap_copies(x_ref, out_ref, send_sem, recv_sem, peers):
        copy.wait()


def swap_scratch(x):
    peers = x.shape[0]
    return [pltpu.VMEM(x.shape[1:], x.dtype), pltpu.SemaphoreType.DMA((peers - 1,)), pltpu.SemaphoreType.DMA((peers - 1,)),
            pltpu.SemaphoreType.DMA]


STEP = (1, -1)


def hops(ring, s, w):
    return ring // 2 - (s != w)


def ring_gather(block, own, sems, peers, cuts):
    ring = peers // 2
    me = lax.axis_index("sp")
    z, c = me // 2, me % 2
    send_sem, recv_sem, over_sem, came_sem = sems
    turn = lambda k: lax.rem(z + k + 2 * ring, ring)
    lots = [(s, w, u) for u in range(cuts) for w in range(2) for s in range(2)]

    def copy(src, dst, one, two, to):
        return pltpu.make_async_remote_copy(src_ref=src, dst_ref=dst, send_sem=one, recv_sem=two, device_id={"sp": to},
                                            device_id_type=pl.DeviceIdType.MESH)

    def along(s, w, t, u):
        ref = block(turn(-STEP[s] * t), c, w, u)
        return copy(own(w, u) if t == 0 else ref, ref, send_sem.at[s, w, t, u], recv_sem.at[s, w, t, u], 2 * turn(STEP[s]) + c)

    def across(s, w, t, u, side):
        ref = block(turn(-STEP[s] * t), side, w, u)
        return copy(own(w, u) if t == 0 and side is c else ref, ref, over_sem.at[s, w, t, u], came_sem.at[s, w, t, u], 2 * z + 1 - c)

    home = [(0, w, 0, u) for u in range(cuts) for w in range(2)]
    moved = [(s, w, t, u) for t in range(1, ring // 2 + 1) for s, w, u in lots if t <= hops(ring, s, w)]

    def start():
        for s, w, u in lots:
            along(s, w, 0, u).start()
        for lot in home:
            across(*lot, c).start()

    def run(lo=1, hi=ring):
        for s, w, t, u in moved:
            if lo <= t < hi:
                along(s, w, t - 1, u).wait_recv()
                if t < hops(ring, s, w):
                    along(s, w, t, u).start()
                across(s, w, t, u, c).start()

    def finish():
        for s, w, t, u in moved:
            along(s, w, t - 1, u).wait_send()
        for lot in home + moved:
            across(*lot, c).wait_send()
            across(*lot, 1 - c).wait_recv()

    return start, run, finish


def ring_scratch(peers, cuts):
    dma = pltpu.SemaphoreType.DMA
    return [dma((2, 2, peers // 4, cuts))] * 2 + [dma((2, 2, peers // 4 + 1, cuts))] * 2


def opening_body(x_hbm, dy_hbm, wo_hbm, vec_ref, marks_ref, marks_all, do_t, x_all, *refs, peers, batch, cuts):
    x_out, do_out = refs[:batch - 1], refs[batch - 1:2 * batch - 2]
    x_ref, dy_ref, x_own, do_own, wo_ref, own, ds_sem, dr_sem, do_sem, ms_sem, mr_sem, in_sem = refs[2 * batch - 2:2 * batch + 10]
    ring_sems = refs[2 * batch + 10:]
    me = lax.axis_index("sp")
    tok, dim = x_own.shape[0], do_own.shape[1]
    lot = tok // 2 // cuts
    rows_of = lambda w, u: pl.ds((w * cuts + u) * lot, lot)
    arrived = greet(peers)
    loads = [pltpu.make_async_copy(x_hbm.at[b], x_ref.at[b], in_sem.at[b]) for b in range(batch)]
    loads += [pltpu.make_async_copy(dy_hbm, dy_ref, in_sem.at[batch]), pltpu.make_async_copy(wo_hbm, wo_ref, in_sem.at[batch + 1])]
    for load in loads:
        load.start()

    def norm(b, out_ref):
        loads[b].wait()

        @pl.loop(0, tok // 32)
        def _(k):
            rows = pl.ds(pl.multiple_of(k * 32, 32), 32)
            x = x_ref[b, rows, :].astype(F32)
            cen = x - jnp.mean(x, axis=-1, keepdims=True)
            hat = cen * lax.rsqrt(jnp.mean(cen * cen, axis=-1, keepdims=True) + NORM_EPS)
            out_ref[rows, :] = (hat * vec_ref[0:1, :] + vec_ref[1:2, :]).astype(BF16)

    def product(b, out_ref):
        @pl.loop(0, peers // 4)
        def _(g):
            rows = pl.ds(pl.multiple_of(g * 4 * dim, 4 * dim), 4 * dim)
            out_ref[pl.ds(g * 4, 4)] = lax.dot_general(wo_ref[rows, :], dy_ref[b], NT, preferred_element_type=F32).astype(BF16).reshape(4, dim, tok)

    norm(0, x_own)
    block = lambda k, side, w, u: x_all.at[2 * k + side, rows_of(w, u)]
    start, run, finish = ring_gather(block, lambda w, u: x_own.at[rows_of(w, u)], ring_sems, peers, cuts)
    arrived()
    start()
    keep = pltpu.make_async_copy(x_own, x_all.at[me], in_sem.at[batch + 2])
    keep.start()
    marks = [pltpu.make_async_remote_copy(
        src_ref=marks_ref, dst_ref=marks_all.at[me], send_sem=ms_sem.at[d - 1], recv_sem=mr_sem.at[d - 1],
        device_id=peer_at(d, peers), device_id_type=pl.DeviceIdType.MESH) for d in range(1, peers)]
    for copy in marks:
        copy.start()
    marks_all[me] = marks_ref[...]
    loads[-2].wait()
    loads[-1].wait()
    product(0, do_own)
    for b in range(1, batch):
        norm(b, x_out[b - 1])
    swap_start(do_own, do_t, own, ds_sem, dr_sem, do_sem, peers)
    for b in range(1, batch):
        product(b, do_out[b - 1])
    run()
    keep.wait()
    for copy in marks:
        copy.wait()
    swap_wait(do_own, do_t, own, ds_sem, dr_sem, do_sem, peers)
    finish()


def opening(x, dy, w_out, vecs, marks, peers, collective_id, cuts=4):
    batch, tok, hidden = x.shape
    dim = hidden // peers
    hbm, vmem = pl.BlockSpec(memory_space=pltpu.HBM), pl.BlockSpec(memory_space=pltpu.VMEM)
    dma = pltpu.SemaphoreType.DMA
    do_shape, x_shape = jax.ShapeDtypeStruct((peers, dim, tok), BF16), jax.ShapeDtypeStruct((tok, hidden), BF16)
    res = pl.pallas_call(
        functools.partial(opening_body, peers=peers, batch=batch, cuts=cuts),
        name="opening",
        out_shape=[jax.ShapeDtypeStruct((peers,) + marks.shape, marks.dtype), do_shape, jax.ShapeDtypeStruct((peers, tok, hidden), BF16)]
        + [x_shape] * (batch - 1) + [do_shape] * (batch - 1),
        in_specs=[hbm, hbm, hbm, vmem, vmem],
        out_specs=[vmem, hbm, hbm] + [vmem] * (2 * batch - 2),
        scratch_shapes=[pltpu.VMEM(x.shape, BF16), pltpu.VMEM(dy.shape, BF16), pltpu.VMEM(x_shape.shape, BF16), pltpu.VMEM(do_shape.shape, BF16),
                        pltpu.VMEM(w_out.shape, BF16)] + swap_scratch(do_shape)
        + [dma((peers - 1,)), dma((peers - 1,)), dma((batch + 3,))] + ring_scratch(peers, cuts),
        cost_estimate=pl.CostEstimate(flops=5 * 10**10, bytes_accessed=16 << 20, transcendentals=0),
        compiler_params=pltpu.CompilerParams(collective_id=collective_id, has_side_effects=True, vmem_limit_bytes=VMEM_LIMIT),
    )(x, dy, w_out, vecs, marks)
    return res[0], res[1], res[2], res[3:2 + batch], res[2 + batch:]


TN = (((0,), (0,)), ((), ()))


def tail_a_body(dqkv_ref, oo_hbm, on_hbm, dy_hbm, x_hbm, wo_hbm, vec_ref, y_ref, part, d_out,
                o_old, o_new, dy_ref, x_ref, wo_ref, both, mine, landed, own_d, ds_sem, dr_sem, do_sem, ps_sem, pr_sem, rs_sem, rr_sem,
                w_sem, *, peers, cuts, sent):
    ring = peers // 2
    me = lax.axis_index("sp")
    z, c = me // 2, me % 2
    _, tok, hidden = x_ref.shape
    half, wide, few = hidden // 2, hidden // 3, part.shape[0] // cuts
    cols = (pl.ds(0, half), pl.ds(half, half))
    at = lambda zz, cc: {"sp": 2 * zz + cc}
    turn = lambda k: lax.rem(z + k + 2 * ring, ring)
    remote = functools.partial(pltpu.make_async_remote_copy, device_id_type=pl.DeviceIdType.MESH)
    pairs = ((oo_hbm, o_old), (on_hbm, o_new), (dy_hbm, dy_ref), (x_hbm, x_ref), (wo_hbm, wo_ref))
    loads = [pltpu.make_async_copy(src, dst, w_sem.at[k]) for k, (src, dst) in enumerate(pairs)]
    swap = (dqkv_ref.at[:, pl.ds(0, sent)], d_out, own_d, ds_sem, dr_sem, do_sem, peers)
    arrived = greet(peers)
    for load in loads:
        load.start()
    arrived()
    swap_start(*swap)
    for load in loads[:3]:
        load.wait()

    def product(put, side):
        @pl.loop(0, ring)
        def _(k):
            h = 2 * k + side
            put(k, jnp.dot(o_old[h], dy_ref[0], preferred_element_type=F32)
                + jnp.dot(o_new[h], dy_ref[1], preferred_element_type=F32))

    def put_other(k, value):
        both[k, 1 - c] = value

    def put_mine(k, value):
        mine[k] = value

    def forward(b, o_ref):
        o_t = o_ref[...].reshape(hidden, tok)

        @pl.loop(0, 3)
        def _(n):
            at_n = pl.ds(pl.multiple_of(n * wide, wide), wide)
            acc = lax.dot_general(o_t, wo_ref[:, at_n], TN, preferred_element_type=F32)
            y_ref[b, :, at_n] = (x_ref[b, :, at_n].astype(F32) + acc + vec_ref[2:3, at_n]).astype(BF16)

    product(put_other, 1 - c)
    pair_copy = lambda side: remote(src_ref=both.at[:, side], dst_ref=both.at[:, side], send_sem=ps_sem, recv_sem=pr_sem, device_id=at(z, 1 - c))
    product(put_mine, c)
    pair_copy(1 - c).start()
    pair_copy(1 - c).wait_send()
    pair_copy(c).wait_recv()

    @pl.loop(0, ring)
    def _(k):
        mine[k] = mine[k] + both[k, c]

    lots = [(s, w, u) for u in range(cuts) for w in range(2) for s in range(2)]

    def reduce_copy(s, w, t, u):
        return remote(src_ref=mine.at[turn(STEP[s] * (hops(ring, s, w) - t)), pl.ds(u * few, few), cols[w]], dst_ref=landed.at[s, w, t, u],
                      send_sem=rs_sem.at[s, w, t, u], recv_sem=rr_sem.at[s, w, t, u], device_id=at(turn(STEP[s]), c))

    def fold(s, w, t, u):
        reduce_copy(s, w, t, u).wait_recv()
        at_k = (turn(STEP[s] * (hops(ring, s, w) - t - 1)), pl.ds(u * few, few), cols[w])
        mine[at_k] = mine[at_k] + landed[s, w, t, u]

    def hop(t):
        for s, w, u in lots:
            if t < hops(ring, s, w):
                fold(s, w, t - 1, u)
                reduce_copy(s, w, t, u).start()

    for s, w, u in lots:
        reduce_copy(s, w, 0, u).start()
    loads[3].wait()
    loads[4].wait()
    forward(0, o_old)
    hop(1)
    forward(1, o_new)
    for t in range(2, ring // 2):
        hop(t)
    for s, w, u in lots:
        fold(s, w, hops(ring, s, w) - 1, u)
    part[...] = mine[z]
    swap_wait(*swap)
    for s, w, u in lots:
        for t in range(hops(ring, s, w)):
            reduce_copy(s, w, t, u).wait_send()


def tail_a(dqkv, o_old, o_new, dy, x, w_out, vecs, sent, collective_id, cuts=2):
    peers, dim, tok = o_old.shape
    ring = peers // 2
    hidden = dy.shape[-1]
    hbm, vmem = pl.BlockSpec(memory_space=pltpu.HBM), pl.BlockSpec(memory_space=pltpu.VMEM)
    dma = pltpu.SemaphoreType.DMA
    held = lambda a: pltpu.VMEM(a.shape, a.dtype)
    steps = (2, 2, ring // 2, cuts)
    return pl.pallas_call(
        functools.partial(tail_a_body, peers=peers, cuts=cuts, sent=sent),
        name="tail_a",
        out_shape=[jax.ShapeDtypeStruct(x.shape, BF16), jax.ShapeDtypeStruct((dim, hidden), F32),
                   jax.ShapeDtypeStruct((peers, sent, tok), BF16)],
        in_specs=[hbm] * 6 + [vmem],
        out_specs=[vmem, vmem, hbm],
        scratch_shapes=[held(a) for a in (o_old, o_new, dy, x, w_out)]
        + [pltpu.VMEM((ring, 2, dim, hidden), F32), pltpu.VMEM((ring, dim, hidden), F32), pltpu.VMEM(steps + (dim // cuts, hidden // 2), F32),
           pltpu.VMEM((sent, tok), BF16), dma((peers - 1,)), dma((peers - 1,)), dma, dma, dma, dma(steps), dma(steps), dma((5,))],
        cost_estimate=pl.CostEstimate(flops=10**11, bytes_accessed=64 << 20, transcendentals=0),
        compiler_params=pltpu.CompilerParams(collective_id=collective_id, has_side_effects=True, vmem_limit_bytes=VMEM_LIMIT),
    )(dqkv, o_old, o_new, dy, x, w_out, vecs)


def tail_b_body(dqkv_ref, da_hbm, d_hbm, dy_hbm, x_hbm, w_hbm, part, vec_ref, gb_ref, gx_ref, full, total, gb_all,
                d_old, d_new, dy_ref, x_ref, w_ref, dn, sums, rows_ref, stage, own_d, ds_sem, dr_sem, do_sem, w_sem, xs_sem, xr_sem,
                *ring_sems, peers, cuts):
    ring = peers // 2
    me = lax.axis_index("sp")
    z, c = me // 2, me % 2
    _, tok, hidden = x_ref.shape
    half, wide, few = hidden // 2, hidden // 3, full.shape[2] // cuts
    sent, span = da_hbm.shape[1], d_old.shape[1]
    rest = pl.ds(sent, span - sent)
    group = 8
    cols = (pl.ds(0, half), pl.ds(half, half))
    remote = functools.partial(pltpu.make_async_remote_copy, device_id_type=pl.DeviceIdType.MESH)
    pairs = ((w_hbm, w_ref), (d_hbm, d_old), (dy_hbm, dy_ref), (x_hbm, x_ref), (da_hbm, d_new.at[:, pl.ds(0, sent)]))
    loads = [pltpu.make_async_copy(src, dst, w_sem.at[k]) for k, (src, dst) in enumerate(pairs)]
    swap = (dqkv_ref.at[:, rest], d_new.at[:, rest], own_d, ds_sem, dr_sem, do_sem, peers)
    arrived = greet(peers)
    for load in loads:
        load.start()
    full[z, c] = part[...]
    gb_all[me] = gb_ref[...]
    sums[...] = jnp.zeros_like(sums)
    block = lambda k, side, w, u: full.at[k, side, pl.ds(u * few, few), cols[w]]
    start, run, finish = ring_gather(block, lambda w, u: block(z, c, w, u), ring_sems, peers, cuts)

    def backward(b, d_ref):
        @pl.loop(0, 3)
        def _(n):
            at_n = pl.ds(pl.multiple_of(n * wide, wide), wide)
            acc = None
            for k in range(0, peers, group):
                lhs = d_ref[k:k + group].reshape(-1, tok)
                one = lax.dot_general(lhs, w_ref[k * span:(k + group) * span, at_n], TN, preferred_element_type=F32)
                acc = one if acc is None else acc + one
            dn[:, at_n] = acc

        @pl.loop(0, tok // 32)
        def _(k):
            rows = pl.ds(pl.multiple_of(k * 32, 32), 32)
            x = x_ref[b, rows, :].astype(F32)
            dy = dy_ref[b, rows, :].astype(F32)
            d = dn[rows, :]
            cen = x - jnp.mean(x, axis=-1, keepdims=True)
            inv = lax.rsqrt(jnp.mean(cen * cen, axis=-1, keepdims=True) + NORM_EPS)
            hat = cen * inv
            for n, one in enumerate((d * hat, d, dy)):
                sums[n] += jnp.sum(one.reshape(4, 8, hidden), axis=0)
            e = d * vec_ref[0:1, :]
            m1 = jnp.mean(e, axis=-1, keepdims=True)
            m2 = jnp.mean(e * hat, axis=-1, keepdims=True)
            gx_ref[b, rows, :] = (dy + inv * (e - m1 - hat * m2)).astype(BF16)

    owners = hidden // 128
    lanes = lambda k: pl.ds(pl.multiple_of(k * 128, 128), 128)

    def small_copy(kind, frm, to):
        src, dst = ((rows_ref.at[:, lanes(to)], stage.at[frm]), (total.at[:, lanes(frm)],) * 2, (gb_ref, gb_all.at[frm]))[kind]
        return remote(src_ref=src, dst_ref=dst, send_sem=xs_sem.at[kind, to], recv_sem=xr_sem.at[kind, frm], device_id={"sp": to})

    def each(act, kind, only_to=False, only_from=False):
        @pl.loop(1, peers)
        def _(d):
            far = lax.rem(me + d, peers)

            def go():
                act(kind, far)

            if only_to:
                pl.when(far < owners)(go)
            elif only_from:
                pl.when(me < owners)(go)
            else:
                go()

    send = lambda kind, far: small_copy(kind, me, far).start()
    over = lambda kind, far: small_copy(kind, me, far).wait_send()
    came = lambda kind, far: small_copy(kind, far, me).wait_recv()

    arrived()
    start()
    swap_start(*swap)
    each(send, 2)
    run(1, 2)
    for load in loads[:4]:
        load.wait()
    backward(0, d_old)
    run(2)
    loads[4].wait()
    swap_wait(*swap)
    backward(1, d_new)
    rows_ref[...] = jnp.zeros_like(rows_ref)
    for n in range(3):
        rows_ref[n:n + 1, :] = jnp.sum(sums[n], axis=0, keepdims=True)

    @pl.when(me < owners)
    def _():
        stage[me] = rows_ref[:, lanes(me)]

    each(send, 0, only_to=True)
    each(came, 0, only_from=True)

    @pl.when(me < owners)
    def _():
        total[:, lanes(me)] = jnp.sum(stage[...], axis=0)

    each(send, 1, only_from=True)
    each(came, 1, only_to=True)
    each(came, 2)
    each(over, 0, only_to=True)
    each(over, 1, only_from=True)
    each(over, 2)
    finish()


def tail_b(dqkv, d_part, d_old, dy, x, w_flat, part, vecs, gb, peers, collective_id, cuts=2):
    ring = peers // 2
    tok, hidden = x.shape[1:]
    hbm, vmem = pl.BlockSpec(memory_space=pltpu.HBM), pl.BlockSpec(memory_space=pltpu.VMEM)
    dma = pltpu.SemaphoreType.DMA
    held = lambda a: pltpu.VMEM(a.shape, a.dtype)
    return pl.pallas_call(
        functools.partial(tail_b_body, peers=peers, cuts=cuts),
        name="tail_b",
        out_shape=[jax.ShapeDtypeStruct(x.shape, BF16), jax.ShapeDtypeStruct((ring, 2) + part.shape, F32),
                   jax.ShapeDtypeStruct((8, hidden), F32), jax.ShapeDtypeStruct((peers,) + gb.shape, F32)],
        in_specs=[hbm] * 6 + [vmem] * 3,
        out_specs=[vmem] * 4,
        scratch_shapes=[held(a) for a in (d_old, d_old, dy, x, w_flat)]
        + [pltpu.VMEM((tok, hidden), F32), pltpu.VMEM((3, 8, hidden), F32), pltpu.VMEM((8, hidden), F32), pltpu.VMEM((peers, 8, 128), F32),
           pltpu.VMEM((d_old.shape[1] - d_part.shape[1], tok), BF16), dma((peers - 1,)), dma((peers - 1,)), dma, dma((5,)),
           dma((3, peers)), dma((3, peers))] + ring_scratch(peers, cuts),
        cost_estimate=pl.CostEstimate(flops=10**11, bytes_accessed=64 << 20, transcendentals=0),
        compiler_params=pltpu.CompilerParams(collective_id=collective_id, has_side_effects=True, vmem_limit_bytes=VMEM_LIMIT),
    )(dqkv, d_part, d_old, dy, x, w_flat, part, vecs, gb)


def settle_body(*refs, n_in, first, n_plain):
    x_ref, plain, outs = refs[0], refs[1:1 + n_plain], refs[n_in:n_in + 1 + n_plain]
    buf, in_sem, out_sem, plain_sem = refs[n_in + 1 + n_plain:]
    heads, n = x_ref.shape[:2]
    reads = [pltpu.make_async_copy(x_ref.at[h], buf.at[h], in_sem.at[h]) for h in range(heads)]
    writes = [pltpu.make_async_copy(buf.at[h], outs[0].at[h, pl.ds(first, n)], out_sem.at[h]) for h in range(heads)]
    flat = [pltpu.make_async_copy(plain[k], outs[1 + k], plain_sem.at[k]) for k in range(n_plain)]
    for copy in reads + flat:
        copy.start()
    for read, write in zip(reads, writes):
        read.wait()
        write.start()
    for copy in writes + flat:
        copy.wait()


def settle(x, into, plain, lanes, first):
    heads, n, dim, hidden = x.shape
    hbm, vmem = pl.BlockSpec(memory_space=pltpu.HBM), pl.BlockSpec(memory_space=pltpu.VMEM)
    args = (x, *plain) + (() if into is None else (into,))
    dma = pltpu.SemaphoreType.DMA
    return pl.pallas_call(
        functools.partial(settle_body, n_in=len(args), first=first, n_plain=len(plain)), name="settle",
        out_shape=[jax.ShapeDtypeStruct((heads, lanes, dim, hidden), x.dtype)] + [jax.ShapeDtypeStruct(a.shape, a.dtype) for a in plain],
        in_specs=[hbm] + [vmem] * len(plain) + [hbm] * (into is not None), out_specs=[hbm] * (1 + len(plain)),
        input_output_aliases={} if into is None else {len(args) - 1: 0},
        scratch_shapes=[pltpu.VMEM(x.shape, x.dtype), dma((heads,)), dma((heads,)), dma((max(len(plain), 1),))],
        cost_estimate=pl.CostEstimate(flops=10**9, bytes_accessed=8 * x.size, transcendentals=0),
        compiler_params=pltpu.CompilerParams(vmem_limit_bytes=(60 << 20) - 4 * sum(a.size for a in plain)))(*args)


def solution(mesh):
    peers = mesh.shape["sp"]

    def block_fn(x_blk, pos_blk, keep_blk, ln_gain, ln_bias, w_qkv, b_qkv, w_out, b_out, dy_blk):
        batch, tok, hidden = x_blk.shape
        heads, dim = w_qkv.shape[1], w_qkv.shape[3]
        assert heads == peers
        seq = tok * peers
        blk = 2 * tok
        vecs = jnp.stack([ln_gain, ln_bias, b_out] + [jnp.zeros_like(b_out)] * 5)
        w_all = jnp.transpose(w_qkv, (1, 2, 3, 0)).reshape(heads, 3 * dim, hidden)
        b_all = jnp.pad(b_qkv.reshape(heads, 3 * dim), ((0, 0), (0, -3 * dim % 128)))[:, None]
        marks_loc = jnp.concatenate([pos_blk, keep_blk, jnp.zeros((8 - 2 * batch, tok), jnp.int32)])
        marks, do_first, x_first, x_rest, do_rest = opening(x_blk, dy_blk, w_out, vecs, marks_loc, peers, 1)
        xs = [x_first.reshape(seq, hidden)] + [lax.all_gather(one, "sp", axis=0, tiled=True) for one in x_rest]
        do_t = [do_first]
        gw, att = (), []
        for b in range(batch):
            old = list(do_rest[b:b + 1]) if b + 1 < batch else att
            att_d, gw, gb, att_o, swapped = attention(w_all, b_all, do_t[b], marks, xs[b], gw, old, blk=blk, tok=tok, which=b, batch=batch,
                                                      send_o=b + 1 == batch, collective_id=4 + b)
            if b + 1 < batch:
                do_t.append(swapped[0])
            att = [att_o, att_d]
        o_old, d_old = swapped
        gw_all = [lax.all_gather(one, "sp", axis=0, tiled=True).reshape(heads, -1, dim, hidden) for one in gw[:2]]
        lead = gw_all[0].shape[1]
        y, part, d_part = tail_a(att_d, o_old, att_o, dy_blk, x_blk, w_out, vecs, 2 * dim, 2)
        first, _ = lax.optimization_barrier((gw_all[0], y))
        gw_out, y = settle(first, None, (y,), 3, 0)
        part, gw_out, y = lax.optimization_barrier((part, gw_out, y))
        gx, go_all, total, gb_all = tail_b(att_d, d_part, d_old, dy_blk, x_blk, w_all.reshape(3 * hidden, hidden), part, vecs, gb, peers, 3)
        second, gw_out, gx = lax.optimization_barrier((gw_all[1], gw_out, gx))
        gw_out, gx, go_all = settle(second, gw_out, (gx, go_all.reshape(hidden, hidden)), 3, lead)
        gw_out = jnp.transpose(gw_out, (3, 0, 1, 2))
        return y, gx, gw_out, gb_all[:, :3, :dim], go_all, total[2], total[0], total[1]

    act_spec = P("dp", "sp", None)
    tok_spec = P("dp", "sp")
    in_specs = (act_spec, tok_spec, tok_spec, P(), P(), P(), P(), P(), P(), act_spec)
    out_specs = (act_spec, act_spec, P("dp", None, None, None), P("dp", None, None), P("dp", None), P("dp"), P("dp"), P("dp"))
    return jax.shard_map(block_fn, mesh=mesh, in_specs=in_specs, out_specs=out_specs, check_vma=False)
```

```python
import functools
import jax
import jax.numpy as jnp
from jax import lax
from jax.experimental import pallas as pl
from jax.experimental.pallas import tpu as pltpu
from jax.sharding import PartitionSpec as P

NORM_EPS = 1e-5

LOG2E = 1.4426950408889634
MASKED = -1e30
VMEM_LIMIT = 62 << 20
F32, BF16 = jnp.float32, jnp.bfloat16
NT = (((1,), (1,)), ((), ()))


def attn_body(w_hbm, b_ref, dot_ref, marks_ref, x_ref, *refs, blk, tok, which, batch, n_swap, n_old, send_o):
    peers = dot_ref.shape[0]
    gw_old, old, refs = refs[:n_old], refs[n_old:n_old + n_swap], refs[n_old + n_swap:]
    (dqkv_ref, gwa_ref, gwb_ref, gb_ref, gbt_ref, o_out), got, refs = refs[:6], refs[6:6 + n_swap], refs[6 + n_swap:]
    x_buf, refs = refs[0], refs[1:]
    w_ref, b_rep, qkvt_ref, k_tok, v_tok, posk_ref, s_buf, q_pad, do_pad, o_acc, dq_acc, dk_acc, dv_acc, x_sem, w_sem = refs[:15]
    swaps = [(old[k], got[k]) + refs[15 + 4 * k:19 + 4 * k] for k in range(n_swap)]
    if send_o:
        o_ref, os_sem, or_sem = refs[-3:]
        o_new = o_out
    else:
        o_ref = o_out
    dim = dot_ref.shape[1]
    seq = dot_ref.shape[0] * tok
    pad = k_tok.shape[1] - dim
    nq = blk // tok
    steps = seq // blk
    scale = dim ** -0.5
    me = lax.axis_index("sp")
    step = pl.program_id(0)
    i = lax.rem(me // nq + step, steps)
    half = blk // 2
    sub = tok // 128

    def spread(row):
        return jnp.transpose(jnp.broadcast_to(row, (128, 128)))

    def x_copy(k):
        rows = pl.ds(pl.multiple_of(k * blk, blk), blk)
        return pltpu.make_async_copy(x_ref.at[rows], x_buf.at[rows], x_sem.at[k])

    def o_send(to):
        return pltpu.make_async_remote_copy(
            src_ref=o_ref.at[to], dst_ref=o_new.at[me], send_sem=os_sem.at[to], recv_sem=or_sem.at[me],
            device_id={"sp": to}, device_id_type=pl.DeviceIdType.MESH)

    def o_keep():
        return pltpu.make_async_copy(o_ref.at[me], o_new.at[me], os_sem.at[me])

    def o_start(at):
        for t in range(nq):
            to = lax.rem(me // nq + at, steps) * nq + t

            @pl.when(to != me)
            def _():
                o_send(to).start()

            @pl.when(to == me)
            def _():
                o_keep().start()

    @pl.when(step == 0)
    def _():
        w_load = pltpu.make_async_copy(w_hbm.at[me], w_ref, w_sem)
        w_load.start()
        for k in range(steps):
            x_copy(k).start()
        meet(peers)
        for one in swaps:
            swap_start(*one, peers)
        dk_acc[...] = jnp.zeros_like(dk_acc)
        dv_acc[...] = jnp.zeros_like(dv_acc)
        q_pad[...] = jnp.zeros_like(q_pad)
        do_pad[...] = jnp.zeros_like(do_pad)
        mine = lax.broadcasted_iota(jnp.int32, (peers, dim), 0) == me
        for k in range(3):
            row = jnp.sum(jnp.where(mine, b_ref[k], 0.0), axis=0, keepdims=True)
            b_rep[k * dim:(k + 1) * dim, :] = spread(jnp.concatenate([row, jnp.zeros((1, pad), F32)], axis=1))[0:dim]
        w_load.wait()

        @pl.loop(0, steps)
        def _(k):
            rows = pl.ds(pl.multiple_of(k * blk, blk), blk)
            x_copy(k).wait()
            shift = jnp.concatenate([b_rep[...]] * (blk // 128), axis=1)
            qkvt_ref[:, rows] = (lax.dot_general(w_ref[...], x_buf[rows, :], NT, preferred_element_type=F32) + shift).astype(BF16)

            @pl.loop(0, blk // 128)
            def _(t):
                cols = pl.ds(pl.multiple_of(k * blk + t * 128, 128), 128)
                for base, dst in ((dim, k_tok), (2 * dim, v_tok)):
                    part = qkvt_ref[base:base + dim, cols].astype(F32)
                    whole = jnp.concatenate([part, jnp.zeros((pad, 128), F32)], axis=0)
                    dst[cols, :] = jnp.transpose(whole).astype(BF16)
                lanes = pl.ds(pl.multiple_of((t % sub) * 128, 128), 128)
                pos = marks_ref[k * nq + t // sub, which:which + 1, lanes].astype(F32)
                keep = marks_ref[k * nq + t // sub, batch + which:batch + which + 1, lanes]
                posk_ref[cols, :] = spread(jnp.where(keep > 0, pos, MASKED))

    if send_o:
        @pl.when(step > 0)
        def _():
            o_start(step - 1)

    qcols = pl.ds(pl.multiple_of(i * blk, blk), blk)
    q_pad[0:dim, :] = qkvt_ref[0:dim, qcols]
    for t in range(nq):
        do_pad[0:dim, t * tok:(t + 1) * tok] = dot_ref[i * nq + t]
    slope2 = jnp.exp2(jnp.full((1, 128), -8.0 / peers, F32) * (me + 1).astype(F32)) * LOG2E
    ref_pos = jnp.broadcast_to(marks_ref[i * nq, which:which + 1, 0:128][:, 0:1].astype(F32), (1, 128))
    c = scale * LOG2E

    def scores(j, m8, diag):
        for sub in range(2):
            rows = pl.ds(pl.multiple_of(j * blk + sub * half, half), half)
            st = jnp.dot(k_tok[rows, :], q_pad[...], preferred_element_type=F32)
            bias = (posk_ref[rows, :] - ref_pos) * slope2
            st = st * c + jnp.concatenate([bias] * (blk // 128), axis=1)
            if diag:
                key = lax.broadcasted_iota(jnp.int32, (half, blk), 0) + sub * half
                qry = lax.broadcasted_iota(jnp.int32, (half, blk), 1)
                st = jnp.where(key <= qry, st, MASKED)
            s_buf[rows, :] = st
            m8 = jnp.maximum(m8, jnp.max(st.reshape(half // 8, 8, blk), axis=0))
        return m8

    m8 = lax.fori_loop(0, i, lambda j, m: scores(j, m, False), jnp.full((8, blk), MASKED, F32))
    m8 = scores(i, m8, True)
    m = jnp.max(m8, axis=0, keepdims=True)

    def exps(j, l8):
        for sub in range(2):
            rows = pl.ds(pl.multiple_of(j * blk + sub * half, half), half)
            e = jnp.exp2(s_buf[rows, :] - m)
            s_buf[rows, :] = e
            l8 = l8 + jnp.sum(e.reshape(half // 8, 8, blk), axis=0)
        return l8

    l8 = lax.fori_loop(0, i + 1, exps, jnp.zeros((8, blk), F32))
    inv = 1.0 / jnp.sum(l8, axis=0, keepdims=True)
    o_acc[...] = jnp.zeros_like(o_acc)
    dq_acc[...] = jnp.zeros_like(dq_acc)

    def values(j, _):
        rows = pl.ds(pl.multiple_of(j * blk, blk), blk)
        p = s_buf[rows, :] * inv
        s_buf[rows, :] = p
        pb = p.astype(BF16)
        o_acc[...] += jnp.dot(qkvt_ref[2 * dim:3 * dim, rows], pb, preferred_element_type=F32)
        dv_acc[:, rows] += lax.dot_general(do_pad[0:dim, :], pb, NT, preferred_element_type=F32)
        return 0

    lax.fori_loop(0, i + 1, values, 0)
    o_lo = o_acc[...].astype(BF16)
    do_f = do_pad[0:dim, :].astype(F32)
    r = jnp.sum(do_f * o_lo.astype(F32), axis=0, keepdims=True)

    def grads(j, _):
        rows = pl.ds(pl.multiple_of(j * blk, blk), blk)
        g = jnp.dot(v_tok[rows, :], do_pad[...], preferred_element_type=F32)
        ds = (s_buf[rows, :] * (g - r)).astype(BF16)
        dq_acc[...] += jnp.dot(qkvt_ref[dim:2 * dim, rows], ds, preferred_element_type=F32)
        dk_acc[:, rows] += lax.dot_general(q_pad[0:dim, :], ds, NT, preferred_element_type=F32)
        return 0

    lax.fori_loop(0, i + 1, grads, 0)
    dq_lo = (dq_acc[...] * scale).astype(BF16)
    for t in range(nq):
        o_ref[i * nq + t] = o_lo[:, t * tok:(t + 1) * tok]
        dqkv_ref[i * nq + t, 0:dim] = dq_lo[:, t * tok:(t + 1) * tok]

    @pl.when(step == steps - 1)
    def _():
        @pl.loop(0, seq // tok)
        def _(t):
            cols = pl.ds(pl.multiple_of(t * tok, tok), tok)
            dqkv_ref[t, dim:2 * dim] = (dk_acc[:, cols] * scale).astype(BF16)
            dqkv_ref[t, 2 * dim:3 * dim] = dv_acc[:, cols].astype(BF16)

        if send_o:
            o_start(step)
        for k, ref in enumerate((gwa_ref, gwb_ref, gb_ref)):
            ref[...] = gw_old[k][...] if n_old else jnp.zeros_like(ref)
        ones = jnp.ones((blk, 128), BF16)

        @pl.loop(0, steps)
        def _(j):
            rows = pl.ds(pl.multiple_of(j * blk, blk), blk)
            for ref, lo, hi in ((gwa_ref, 0, 2 * dim), (gwb_ref, 2 * dim, 3 * dim)):
                lhs = jnp.concatenate([dqkv_ref[j * nq + t, lo:hi] for t in range(nq)], axis=1)
                ref[...] += jnp.dot(lhs, x_buf[rows, :], preferred_element_type=F32)
                gb_ref[lo:hi, :] += jnp.dot(lhs, ones, preferred_element_type=F32)

        gbt_ref[...] = jnp.zeros_like(gbt_ref)
        for k in range(3):
            part = jnp.concatenate([gb_ref[k * dim:(k + 1) * dim, :], jnp.zeros((pad, 128), F32)], axis=0)
            gbt_ref[k:k + 1, :] = jnp.transpose(part)[0:1, :]

        if send_o:
            o_keep().wait()
            for d in range(1, peers):
                frm = lax.rem(me + d, peers)
                o_send(frm).wait_send()
                pltpu.make_async_remote_copy(
                    src_ref=o_ref.at[frm], dst_ref=o_new.at[frm], send_sem=os_sem.at[frm], recv_sem=or_sem.at[frm],
                    device_id={"sp": frm}, device_id_type=pl.DeviceIdType.MESH).wait_recv()
        for one in swaps:
            swap_wait(*one, peers)


def attention(w_all, b_all, dot_, marks, x, gw, old, *, blk, tok, which, batch, send_o, collective_id):
    blocks, dim, _ = dot_.shape
    seq, hidden = blocks * tok, w_all.shape[2]
    wide = 128 * pl.cdiv(dim, 128)
    hbm = pl.BlockSpec(memory_space=pltpu.HBM)
    full = lambda a: pl.BlockSpec(a.shape, lambda i: (0,) * len(a.shape), pipeline_mode=pl.Buffered(1))
    like = lambda a: jax.ShapeDtypeStruct(a.shape, a.dtype)
    outs = [jax.ShapeDtypeStruct((blocks, 3 * dim, tok), BF16), jax.ShapeDtypeStruct((2 * dim, hidden), F32),
            jax.ShapeDtypeStruct((dim, hidden), F32), jax.ShapeDtypeStruct((3 * dim, 128), F32), jax.ShapeDtypeStruct((8, 128), F32)]
    pairs = (seq // blk) * (seq // blk + 1) // 2
    dma = pltpu.SemaphoreType.DMA
    res = pl.pallas_call(
        functools.partial(attn_body, blk=blk, tok=tok, which=which, batch=batch, n_swap=len(old), n_old=len(gw), send_o=send_o),
        name="attention",
        out_shape=outs + [like(dot_)] + [like(a) for a in old],
        grid=(seq // blk,),
        in_specs=[hbm, full(b_all), full(dot_), full(marks), hbm] + [full(a) for a in gw] + [hbm] * len(old),
        out_specs=[full(a) for a in outs] + [hbm if send_o else full(dot_)] + [hbm] * len(old),
        scratch_shapes=[
            pltpu.VMEM((seq, hidden), BF16),
            pltpu.VMEM(w_all.shape[1:], BF16), pltpu.VMEM((3 * dim, 128), F32), pltpu.VMEM((3 * dim, seq), BF16),
            pltpu.VMEM((seq, wide), BF16), pltpu.VMEM((seq, wide), BF16), pltpu.VMEM((seq, 128), F32),
            pltpu.VMEM((seq, blk), F32),
            pltpu.VMEM((wide, blk), BF16), pltpu.VMEM((wide, blk), BF16),
            pltpu.VMEM((dim, blk), F32), pltpu.VMEM((dim, blk), F32),
            pltpu.VMEM((dim, seq), F32), pltpu.VMEM((dim, seq), F32), dma((seq // blk,)), dma]
        + sum((swap_scratch(a) for a in old), []) + ([pltpu.VMEM(dot_.shape, BF16), dma((blocks,)), dma((blocks,))] if send_o else []),
        cost_estimate=pl.CostEstimate(flops=pairs * 6 * 2 * blk * blk * 256, bytes_accessed=24 << 20, transcendentals=pairs * blk * blk),
        compiler_params=pltpu.CompilerParams(dimension_semantics=("arbitrary",), vmem_limit_bytes=VMEM_LIMIT,
                                             collective_id=collective_id, has_side_effects=True),
    )(w_all, b_all, dot_, marks, x, *gw, *old)
    return res[0], res[1:4], res[4], res[5], res[6:]


def peer_at(d, peers):
    return {"sp": lax.rem(lax.axis_index("sp") + d, peers)}


def greet(peers):
    barrier = pltpu.get_barrier_semaphore()
    for d in range(1, peers):
        pl.semaphore_signal(barrier, inc=1, device_id=peer_at(d, peers), device_id_type=pl.DeviceIdType.MESH)
    return lambda: pl.semaphore_wait(barrier, peers - 1)


def meet(peers):
    greet(peers)()


def swap_copies(x_ref, out_ref, send_sem, recv_sem, peers):
    me = lax.axis_index("sp")
    order = [d for near in range(peers // 2) for d in sorted({peers // 2 - near, peers // 2 + near})]
    return [pltpu.make_async_remote_copy(
        src_ref=x_ref.at[lax.rem(me + d, peers)], dst_ref=out_ref.at[me], send_sem=send_sem.at[d - 1], recv_sem=recv_sem.at[d - 1],
        device_id=peer_at(d, peers), device_id_type=pl.DeviceIdType.MESH) for d in order]


def swap_start(x_ref, out_ref, own, send_sem, recv_sem, own_sem, peers):
    me = lax.axis_index("sp")
    for copy in swap_copies(x_ref, out_ref, send_sem, recv_sem, peers):
        copy.start()
    take = pltpu.make_async_copy(x_ref.at[me], own, own_sem)
    take.start()
    take.wait()
    pltpu.make_async_copy(own, out_ref.at[me], own_sem).start()


def swap_wait(x_ref, out_ref, own, send_sem, recv_sem, own_sem, peers):
    pltpu.make_async_copy(own, out_ref.at[lax.axis_index("sp")], own_sem).wait()
    for copy in swap_copies(x_ref, out_ref, send_sem, recv_sem, peers):
        copy.wait()


def swap_scratch(x):
    peers = x.shape[0]
    return [pltpu.VMEM(x.shape[1:], x.dtype), pltpu.SemaphoreType.DMA((peers - 1,)), pltpu.SemaphoreType.DMA((peers - 1,)),
            pltpu.SemaphoreType.DMA]


STEP = (1, -1)


def hops(ring, s, w):
    return ring // 2 - (s != w)


def ring_gather(block, own, sems, peers, cuts):
    ring = peers // 2
    me = lax.axis_index("sp")
    z, c = me // 2, me % 2
    send_sem, recv_sem, over_sem, came_sem = sems
    turn = lambda k: lax.rem(z + k + 2 * ring, ring)
    lots = [(s, w, u) for u in range(cuts) for w in range(2) for s in range(2)]

    def copy(src, dst, one, two, to):
        return pltpu.make_async_remote_copy(src_ref=src, dst_ref=dst, send_sem=one, recv_sem=two, device_id={"sp": to},
                                            device_id_type=pl.DeviceIdType.MESH)

    def along(s, w, t, u):
        ref = block(turn(-STEP[s] * t), c, w, u)
        return copy(own(w, u) if t == 0 else ref, ref, send_sem.at[s, w, t, u], recv_sem.at[s, w, t, u], 2 * turn(STEP[s]) + c)

    def across(s, w, t, u, side):
        ref = block(turn(-STEP[s] * t), side, w, u)
        return copy(own(w, u) if t == 0 and side is c else ref, ref, over_sem.at[s, w, t, u], came_sem.at[s, w, t, u], 2 * z + 1 - c)

    home = [(0, w, 0, u) for u in range(cuts) for w in range(2)]
    moved = [(s, w, t, u) for t in range(1, ring // 2 + 1) for s, w, u in lots if t <= hops(ring, s, w)]

    def start():
        for s, w, u in lots:
            along(s, w, 0, u).start()
        for lot in home:
            across(*lot, c).start()

    def run(lo=1, hi=ring):
        for s, w, t, u in moved:
            if lo <= t < hi:
                along(s, w, t - 1, u).wait_recv()
                if t < hops(ring, s, w):
                    along(s, w, t, u).start()
                across(s, w, t, u, c).start()

    def finish():
        for s, w, t, u in moved:
            along(s, w, t - 1, u).wait_send()
        for lot in home + moved:
            across(*lot, c).wait_send()
            across(*lot, 1 - c).wait_recv()

    return start, run, finish


def ring_scratch(peers, cuts):
    dma = pltpu.SemaphoreType.DMA
    return [dma((2, 2, peers // 4, cuts))] * 2 + [dma((2, 2, peers // 4 + 1, cuts))] * 2


def opening_body(x_hbm, dy_hbm, wo_hbm, gain_ref, bias_ref, pos_ref, keep_ref, marks_all, do_t, x_all, *refs, peers, batch, cuts):
    x_out, do_out = refs[:batch - 1], refs[batch - 1:2 * batch - 2]
    x_ref, dy_ref, x_own, do_own, wo_ref, marks_ref, own, ds_sem, dr_sem, do_sem, ms_sem, mr_sem, in_sem = refs[2 * batch - 2:2 * batch + 11]
    ring_sems = refs[2 * batch + 11:]
    gain, bias = gain_ref[...].reshape(1, -1), bias_ref[...].reshape(1, -1)
    me = lax.axis_index("sp")
    tok, dim = x_own.shape[0], do_own.shape[1]
    lot = tok // 2 // cuts
    rows_of = lambda w, u: pl.ds((w * cuts + u) * lot, lot)
    arrived = greet(peers)
    loads = [pltpu.make_async_copy(x_hbm.at[b], x_ref.at[b], in_sem.at[b]) for b in range(batch)]
    loads += [pltpu.make_async_copy(dy_hbm, dy_ref, in_sem.at[batch]), pltpu.make_async_copy(wo_hbm, wo_ref, in_sem.at[batch + 1])]
    for load in loads:
        load.start()

    def norm(b, out_ref):
        loads[b].wait()

        @pl.loop(0, tok // 32)
        def _(k):
            rows = pl.ds(pl.multiple_of(k * 32, 32), 32)
            x = x_ref[b, rows, :].astype(F32)
            cen = x - jnp.mean(x, axis=-1, keepdims=True)
            hat = cen * lax.rsqrt(jnp.mean(cen * cen, axis=-1, keepdims=True) + NORM_EPS)
            out_ref[rows, :] = (hat * gain + bias).astype(BF16)

    def product(b, out_ref):
        @pl.loop(0, peers // 4)
        def _(g):
            rows = pl.ds(pl.multiple_of(g * 4 * dim, 4 * dim), 4 * dim)
            out_ref[pl.ds(g * 4, 4)] = lax.dot_general(wo_ref[rows, :], dy_ref[b], NT, preferred_element_type=F32).astype(BF16).reshape(4, dim, tok)

    marks_ref[...] = jnp.zeros_like(marks_ref)
    marks_ref[0:batch, :] = pos_ref[...]
    marks_ref[batch:2 * batch, :] = keep_ref[...]
    norm(0, x_own)
    block = lambda k, side, w, u: x_all.at[2 * k + side, rows_of(w, u)]
    start, run, finish = ring_gather(block, lambda w, u: x_own.at[rows_of(w, u)], ring_sems, peers, cuts)
    arrived()
    start()
    keep = pltpu.make_async_copy(x_own, x_all.at[me], in_sem.at[batch + 2])
    keep.start()
    marks = [pltpu.make_async_remote_copy(
        src_ref=marks_ref, dst_ref=marks_all.at[me], send_sem=ms_sem.at[d - 1], recv_sem=mr_sem.at[d - 1],
        device_id=peer_at(d, peers), device_id_type=pl.DeviceIdType.MESH) for d in range(1, peers)]
    for copy in marks:
        copy.start()
    marks_all[me] = marks_ref[...]
    loads[-2].wait()
    loads[-1].wait()
    product(0, do_own)
    for b in range(1, batch):
        norm(b, x_out[b - 1])
    swap_start(do_own, do_t, own, ds_sem, dr_sem, do_sem, peers)
    for b in range(1, batch):
        product(b, do_out[b - 1])
    run()
    keep.wait()
    for copy in marks:
        copy.wait()
    swap_wait(do_own, do_t, own, ds_sem, dr_sem, do_sem, peers)
    finish()


def opening(x, dy, w_out, gain, bias, pos, keep, peers, collective_id, cuts=4):
    batch, tok, hidden = x.shape
    dim = hidden // peers
    hbm, vmem = pl.BlockSpec(memory_space=pltpu.HBM), pl.BlockSpec(memory_space=pltpu.VMEM)
    dma = pltpu.SemaphoreType.DMA
    do_shape, x_shape = jax.ShapeDtypeStruct((peers, dim, tok), BF16), jax.ShapeDtypeStruct((tok, hidden), BF16)
    res = pl.pallas_call(
        functools.partial(opening_body, peers=peers, batch=batch, cuts=cuts),
        name="opening",
        out_shape=[jax.ShapeDtypeStruct((peers, 8, tok), pos.dtype), do_shape, jax.ShapeDtypeStruct((peers, tok, hidden), BF16)]
        + [x_shape] * (batch - 1) + [do_shape] * (batch - 1),
        in_specs=[hbm, hbm, hbm, vmem, vmem, vmem, vmem],
        out_specs=[vmem, hbm, hbm] + [vmem] * (2 * batch - 2),
        scratch_shapes=[pltpu.VMEM(x.shape, BF16), pltpu.VMEM(dy.shape, BF16), pltpu.VMEM(x_shape.shape, BF16), pltpu.VMEM(do_shape.shape, BF16),
                        pltpu.VMEM(w_out.shape, BF16), pltpu.VMEM((8, tok), pos.dtype)] + swap_scratch(do_shape)
        + [dma((peers - 1,)), dma((peers - 1,)), dma((batch + 3,))] + ring_scratch(peers, cuts),
        cost_estimate=pl.CostEstimate(flops=5 * 10**10, bytes_accessed=16 << 20, transcendentals=0),
        compiler_params=pltpu.CompilerParams(collective_id=collective_id, has_side_effects=True, vmem_limit_bytes=VMEM_LIMIT),
    )(x, dy, w_out, gain, bias, pos, keep)
    return res[0], res[1], res[2], res[3:2 + batch], res[2 + batch:]


TN = (((0,), (0,)), ((), ()))


def tail_a_body(dqkv_ref, oo_hbm, on_hbm, dy_hbm, x_hbm, wo_hbm, d_hbm, w_hbm, gain_ref, bo_ref, y_ref, gx_ref, part, rows_ref,
                o_old, o_new, dy_ref, x_ref, wo_ref, d_old, w_ref, d_new, dn, sums, bo_rep, both, mine, landed, own_d,
                ds_sem, dr_sem, do_sem, ps_sem, pr_sem, rs_sem, rr_sem, w_sem, *, peers, cuts):
    ring = peers // 2
    me = lax.axis_index("sp")
    z, c = me // 2, me % 2
    _, tok, hidden = x_ref.shape
    half, wide, few = hidden // 2, hidden // 3, part.shape[0] // cuts
    cols = (pl.ds(0, half), pl.ds(half, half))
    at = lambda zz, cc: {"sp": 2 * zz + cc}
    turn = lambda k: lax.rem(z + k + 2 * ring, ring)
    remote = functools.partial(pltpu.make_async_remote_copy, device_id_type=pl.DeviceIdType.MESH)
    span, group = d_old.shape[1], 8
    gain, b_out = gain_ref[...].reshape(1, hidden), bo_ref[...].reshape(1, hidden)
    pairs = ((oo_hbm, o_old), (on_hbm, o_new), (dy_hbm, dy_ref), (x_hbm, x_ref), (wo_hbm, wo_ref), (d_hbm, d_old), (w_hbm, w_ref))
    loads = [pltpu.make_async_copy(src, dst, w_sem.at[k]) for k, (src, dst) in enumerate(pairs)]
    swap = (dqkv_ref, d_new, own_d, ds_sem, dr_sem, do_sem, peers)
    arrived = greet(peers)
    for load in loads:
        load.start()
    arrived()
    swap_start(*swap)
    for load in loads[:3]:
        load.wait()

    def product(put, side):
        @pl.loop(0, ring)
        def _(k):
            h = 2 * k + side
            put(k, jnp.dot(o_old[h], dy_ref[0], preferred_element_type=F32)
                + jnp.dot(o_new[h], dy_ref[1], preferred_element_type=F32))

    def put_other(k, value):
        both[k, 1 - c] = value

    def put_mine(k, value):
        mine[k] = value

    def forward(b, o_ref):
        o_t = o_ref[...].reshape(hidden, tok)

        @pl.loop(0, 3)
        def _(n):
            at_n = pl.ds(pl.multiple_of(n * wide, wide), wide)
            acc = lax.dot_general(o_t, wo_ref[:, at_n], TN, preferred_element_type=F32)
            y_ref[b, :, at_n] = (x_ref[b, :, at_n].astype(F32) + acc + bo_rep[0:1, at_n]).astype(BF16)

    def backward(b, d_ref):
        @pl.loop(0, 3)
        def _(n):
            at_n = pl.ds(pl.multiple_of(n * wide, wide), wide)
            acc = None
            for k in range(0, peers, group):
                lhs = d_ref[k:k + group].reshape(-1, tok)
                one = lax.dot_general(lhs, w_ref[k * span:(k + group) * span, at_n], TN, preferred_element_type=F32)
                acc = one if acc is None else acc + one
            dn[:, at_n] = acc

        @pl.loop(0, tok // 32)
        def _(k):
            rows = pl.ds(pl.multiple_of(k * 32, 32), 32)
            x = x_ref[b, rows, :].astype(F32)
            dy = dy_ref[b, rows, :].astype(F32)
            d = dn[rows, :]
            cen = x - jnp.mean(x, axis=-1, keepdims=True)
            inv = lax.rsqrt(jnp.mean(cen * cen, axis=-1, keepdims=True) + NORM_EPS)
            hat = cen * inv
            for n, one in enumerate((d * hat, d, dy)):
                sums[n] += jnp.sum(one.reshape(4, 8, hidden), axis=0)
            e = d * gain
            m1 = jnp.mean(e, axis=-1, keepdims=True)
            m2 = jnp.mean(e * hat, axis=-1, keepdims=True)
            gx_ref[b, rows, :] = (dy + inv * (e - m1 - hat * m2)).astype(BF16)

    bo_rep[...] = jnp.broadcast_to(b_out, bo_rep.shape)
    sums[...] = jnp.zeros_like(sums)
    product(put_other, 1 - c)
    pair_copy = lambda side: remote(src_ref=both.at[:, side], dst_ref=both.at[:, side], send_sem=ps_sem, recv_sem=pr_sem, device_id=at(z, 1 - c))
    product(put_mine, c)
    pair_copy(1 - c).start()
    pair_copy(1 - c).wait_send()
    pair_copy(c).wait_recv()

    @pl.loop(0, ring)
    def _(k):
        mine[k] = mine[k] + both[k, c]

    lots = [(s, w, u) for u in range(cuts) for w in range(2) for s in range(2)]

    def reduce_copy(s, w, t, u):
        return remote(src_ref=mine.at[turn(STEP[s] * (hops(ring, s, w) - t)), pl.ds(u * few, few), cols[w]], dst_ref=landed.at[s, w, t, u],
                      send_sem=rs_sem.at[s, w, t, u], recv_sem=rr_sem.at[s, w, t, u], device_id=at(turn(STEP[s]), c))

    def fold(s, w, t, u):
        reduce_copy(s, w, t, u).wait_recv()
        at_k = (turn(STEP[s] * (hops(ring, s, w) - t - 1)), pl.ds(u * few, few), cols[w])
        mine[at_k] = mine[at_k] + landed[s, w, t, u]

    def hop(t):
        for s, w, u in lots:
            if t < hops(ring, s, w):
                fold(s, w, t - 1, u)
                reduce_copy(s, w, t, u).start()

    for s, w, u in lots:
        reduce_copy(s, w, 0, u).start()
    for load in loads[3:5]:
        load.wait()
    forward(0, o_old)
    forward(1, o_new)
    for load in loads[5:]:
        load.wait()
    backward(0, d_old)
    for t in range(1, ring // 2 - 1):
        hop(t)
    swap_wait(*swap)
    backward(1, d_new)
    hop(ring // 2 - 1)
    rows_ref[...] = jnp.zeros_like(rows_ref)
    for n in range(3):
        rows_ref[n:n + 1, :] = jnp.sum(sums[n], axis=0, keepdims=True)
    for s, w, u in lots:
        fold(s, w, hops(ring, s, w) - 1, u)
    part[...] = mine[z]
    for s, w, u in lots:
        for t in range(hops(ring, s, w)):
            reduce_copy(s, w, t, u).wait_send()


def tail_a(dqkv, d_old, o_old, o_new, dy, x, w_flat, w_out, gain, b_out, collective_id, cuts=2):
    peers, dim, tok = o_old.shape
    ring = peers // 2
    hidden = dy.shape[-1]
    hbm, vmem = pl.BlockSpec(memory_space=pltpu.HBM), pl.BlockSpec(memory_space=pltpu.VMEM)
    dma = pltpu.SemaphoreType.DMA
    held = lambda a: pltpu.VMEM(a.shape, a.dtype)
    steps = (2, 2, ring // 2, cuts)
    return pl.pallas_call(
        functools.partial(tail_a_body, peers=peers, cuts=cuts),
        name="tail_a",
        out_shape=[jax.ShapeDtypeStruct(x.shape, BF16), jax.ShapeDtypeStruct(x.shape, BF16), jax.ShapeDtypeStruct((dim, hidden), F32),
                   jax.ShapeDtypeStruct((8, hidden), F32)],
        in_specs=[hbm] * 8 + [vmem] * 2,
        out_specs=[vmem] * 4,
        scratch_shapes=[held(a) for a in (o_old, o_new, dy, x, w_out, d_old, w_flat, dqkv)]
        + [pltpu.VMEM((tok, hidden), F32), pltpu.VMEM((3, 8, hidden), F32), pltpu.VMEM((8, hidden), F32),
           pltpu.VMEM((ring, 2, dim, hidden), F32), pltpu.VMEM((ring, dim, hidden), F32), pltpu.VMEM(steps + (dim // cuts, hidden // 2), F32),
           pltpu.VMEM(dqkv.shape[1:], BF16), dma((peers - 1,)), dma((peers - 1,)), dma, dma, dma, dma(steps), dma(steps), dma((7,))],
        cost_estimate=pl.CostEstimate(flops=10**11, bytes_accessed=64 << 20, transcendentals=0),
        compiler_params=pltpu.CompilerParams(collective_id=collective_id, has_side_effects=True, vmem_limit_bytes=VMEM_LIMIT),
    )(dqkv, o_old, o_new, dy, x, w_out, d_old, w_flat, gain, b_out)


def tail_b_body(part, rows_ref, gb_ref, full, total, gb_all, stage, xs_sem, xr_sem, *ring_sems, peers, cuts):
    ring = peers // 2
    me = lax.axis_index("sp")
    z, c = me // 2, me % 2
    hidden = part.shape[1]
    half, few = hidden // 2, part.shape[0] // cuts
    cols = (pl.ds(0, half), pl.ds(half, half))
    remote = functools.partial(pltpu.make_async_remote_copy, device_id_type=pl.DeviceIdType.MESH)
    arrived = greet(peers)
    full[z, c] = part[...]
    gb_all[me] = gb_ref[...]
    block = lambda k, side, w, u: full.at[k, side, pl.ds(u * few, few), cols[w]]
    start, run, finish = ring_gather(block, lambda w, u: block(z, c, w, u), ring_sems, peers, cuts)
    owners = hidden // 128
    lanes = lambda k: pl.ds(pl.multiple_of(k * 128, 128), 128)

    def small_copy(kind, frm, to):
        src, dst = ((rows_ref.at[:, lanes(to)], stage.at[frm]), (total.at[:, lanes(frm)],) * 2, (gb_ref, gb_all.at[frm]))[kind]
        return remote(src_ref=src, dst_ref=dst, send_sem=xs_sem.at[kind, to], recv_sem=xr_sem.at[kind, frm], device_id={"sp": to})

    def each(act, kind, only_to=False, only_from=False):
        @pl.loop(1, peers)
        def _(d):
            far = lax.rem(me + d, peers)

            def go():
                act(kind, far)

            if only_to:
                pl.when(far < owners)(go)
            elif only_from:
                pl.when(me < owners)(go)
            else:
                go()

    send = lambda kind, far: small_copy(kind, me, far).start()
    over = lambda kind, far: small_copy(kind, me, far).wait_send()
    came = lambda kind, far: small_copy(kind, far, me).wait_recv()

    @pl.when(me < owners)
    def _():
        stage[me] = rows_ref[:, lanes(me)]

    arrived()
    start()
    each(send, 0, only_to=True)
    each(send, 2)
    run(1, 2)
    each(came, 0, only_from=True)

    @pl.when(me < owners)
    def _():
        total[:, lanes(me)] = jnp.sum(stage[...], axis=0)

    each(send, 1, only_from=True)
    run(2)
    each(came, 1, only_to=True)
    each(came, 2)
    each(over, 0, only_to=True)
    each(over, 1, only_from=True)
    each(over, 2)
    finish()


def tail_b(part, rows, gb, peers, collective_id, cuts=2):
    ring = peers // 2
    vmem = pl.BlockSpec(memory_space=pltpu.VMEM)
    dma = pltpu.SemaphoreType.DMA
    return pl.pallas_call(
        functools.partial(tail_b_body, peers=peers, cuts=cuts),
        name="tail_b",
        out_shape=[jax.ShapeDtypeStruct((ring, 2) + part.shape, F32), jax.ShapeDtypeStruct(rows.shape, F32),
                   jax.ShapeDtypeStruct((peers,) + gb.shape, F32)],
        in_specs=[vmem] * 3,
        out_specs=[vmem] * 3,
        scratch_shapes=[pltpu.VMEM((peers, 8, 128), F32), dma((3, peers)), dma((3, peers))] + ring_scratch(peers, cuts),
        cost_estimate=pl.CostEstimate(flops=5 * 10**10, bytes_accessed=10 << 20, transcendentals=0),
        compiler_params=pltpu.CompilerParams(collective_id=collective_id, has_side_effects=True, vmem_limit_bytes=32 << 20),
    )(part, rows, gb)


def settle_body(*refs, n_in, first, n_plain):
    x_ref, plain = refs[0], refs[1:1 + n_plain]
    outs, (buf, in_sem, out_sem, plain_sem) = refs[n_in:-4], refs[-4:]
    heads, n = x_ref.shape[:2]
    reads = [pltpu.make_async_copy(x_ref.at[h], buf.at[h], in_sem.at[h]) for h in range(heads)]
    writes = [pltpu.make_async_copy(buf.at[h], outs[0].at[h, pl.ds(first, n)], out_sem.at[h]) for h in range(heads)]
    flat = [pltpu.make_async_copy(plain[k], outs[1 + k], plain_sem.at[k]) for k in range(n_plain)]
    for copy in reads + flat:
        copy.start()
    for read, write in zip(reads, writes):
        read.wait()
        write.start()
    for copy in writes + flat:
        copy.wait()


def settle(x, into, plain, lanes, first):
    heads, n, dim, hidden = x.shape
    hbm, vmem = pl.BlockSpec(memory_space=pltpu.HBM), pl.BlockSpec(memory_space=pltpu.VMEM)
    args = (pltpu.with_memory_space_constraint(x, pltpu.HBM), *plain) + (() if into is None else (into,))
    dma = pltpu.SemaphoreType.DMA
    return pl.pallas_call(
        functools.partial(settle_body, n_in=len(args), first=first, n_plain=len(plain)), name="settle",
        out_shape=[jax.ShapeDtypeStruct((heads, lanes, dim, hidden), x.dtype)] + [jax.ShapeDtypeStruct(a.shape, a.dtype) for a in plain],
        in_specs=[hbm] + [vmem] * len(plain) + [hbm] * (into is not None), out_specs=[hbm] * (1 + len(plain)),
        input_output_aliases={} if into is None else {len(args) - 1: 0},
        scratch_shapes=[pltpu.VMEM(x.shape, x.dtype), dma((heads,)), dma((heads,)), dma((max(len(plain), 1),))],
        cost_estimate=pl.CostEstimate(flops=10**9, bytes_accessed=8 * x.size, transcendentals=0),
        compiler_params=pltpu.CompilerParams(vmem_limit_bytes=24 << 20))(*args)


def lay_body(go_ref, total, gb_all, go_out, gb_out, *refs):
    vectors, sem = refs[:-1], refs[-1]
    copies = [pltpu.make_async_copy(go_ref.at[k], go_out.at[k], sem.at[k]) for k in range(go_ref.shape[0])]
    for copy in copies:
        copy.start()
    for k in range(3):
        gb_out[k] = gb_all[:, k, 0:gb_out.shape[2]]
        vectors[k][...] = total[k]
    for copy in copies:
        copy.wait()


def lay_down(go, total, gb_all):
    hbm, vmem = pl.BlockSpec(memory_space=pltpu.HBM), pl.BlockSpec(memory_space=pltpu.VMEM)
    ring, _, dim, hidden = go.shape
    return pl.pallas_call(
        lay_body, name="lay_down",
        out_shape=[jax.ShapeDtypeStruct(go.shape, F32), jax.ShapeDtypeStruct((3, 2 * ring, dim), F32)] + [jax.ShapeDtypeStruct((hidden,), F32)] * 3,
        in_specs=[vmem] * 3, out_specs=[hbm] + [vmem] * 4,
        scratch_shapes=[pltpu.SemaphoreType.DMA((ring,))],
        cost_estimate=pl.CostEstimate(flops=10**9, bytes_accessed=8 * go.size, transcendentals=0),
        compiler_params=pltpu.CompilerParams(vmem_limit_bytes=24 << 20))(go, total, gb_all)


def solution(mesh):
    peers = mesh.shape["sp"]

    def block_fn(x_blk, pos_blk, keep_blk, ln_gain, ln_bias, w_qkv, b_qkv, w_out, b_out, dy_blk):
        batch, tok, hidden = x_blk.shape
        heads, dim = w_qkv.shape[1], w_qkv.shape[3]
        assert heads == peers
        seq = tok * peers
        blk = 2 * tok
        w_all = jnp.transpose(w_qkv, (1, 2, 3, 0)).reshape(heads, 3 * dim, hidden)
        b_all = jnp.transpose(b_qkv, (1, 0, 2))
        marks, do_first, x_first, x_rest, do_rest = opening(x_blk, dy_blk, w_out, ln_gain, ln_bias, pos_blk, keep_blk, peers, 1)
        xs = [x_first.reshape(seq, hidden)] + [lax.all_gather(one, "sp", axis=0, tiled=True) for one in x_rest]
        do_t = [do_first]
        gw, att = (), []
        for b in range(batch):
            old = list(do_rest[b:b + 1]) if b + 1 < batch else att
            att_d, gw, gb, att_o, swapped = attention(w_all, b_all, do_t[b], marks, xs[b], gw, old, blk=blk, tok=tok, which=b, batch=batch,
                                                      send_o=b + 1 == batch, collective_id=4 + b)
            if b + 1 < batch:
                do_t.append(swapped[0])
            att = [att_o, att_d]
        o_old, d_old = swapped
        gw_all = [lax.all_gather(one, "sp", axis=0, tiled=True).reshape(heads, -1, dim, hidden) for one in gw[:2]]
        lead = gw_all[0].shape[1]
        y, gx, part, rows = tail_a(att_d, d_old, o_old, att_o, dy_blk, x_blk, w_all.reshape(3 * hidden, hidden), w_out, ln_gain, b_out, 2)
        first, _ = lax.optimization_barrier((gw_all[0], y))
        gw_out, y, gx = settle(first, None, (y, gx), 3, 0)
        part, gw_out, y, gx = lax.optimization_barrier((part, gw_out, y, gx))
        go_all, gb_all, g_gain, g_bias, g_out = lay_down(*tail_b(part, rows, gb, peers, 3))
        second, gw_out, go_all = lax.optimization_barrier((gw_all[1], gw_out, go_all))
        gw_out, = settle(second, gw_out, (), 3, lead)
        return (y, gx, jnp.transpose(gw_out, (3, 0, 1, 2)), jnp.transpose(gb_all, (1, 0, 2)), go_all.reshape(hidden, hidden),
                g_out, g_gain, g_bias)

    act_spec = P("dp", "sp", None)
    tok_spec = P("dp", "sp")
    in_specs = (act_spec, tok_spec, tok_spec, P(), P(), P(), P(), P(), P(), act_spec)
    out_specs = (act_spec, act_spec, P("dp", None, None, None), P("dp", None, None), P("dp", None), P("dp"), P("dp"), P("dp"))
    return jax.shard_map(block_fn, mesh=mesh, in_specs=in_specs, out_specs=out_specs, check_vma=False)
```

```python
import functools
import jax
import jax.numpy as jnp
from jax import lax
from jax.experimental import pallas as pl
from jax.experimental.pallas import tpu as pltpu
from jax.sharding import PartitionSpec as P

NORM_EPS = 1e-5

LOG2E = 1.4426950408889634
MASKED = -1e30
VMEM_LIMIT = 62 << 20
F32, BF16 = jnp.float32, jnp.bfloat16
NT = (((1,), (1,)), ((), ()))


def attn_body(w_hbm, b_ref, dot_ref, marks_ref, x_ref, *refs, blk, tok, which, batch, n_swap, n_old, send_o):
    peers = dot_ref.shape[0]
    gw_old, old, refs = refs[:n_old], refs[n_old:n_old + n_swap], refs[n_old + n_swap:]
    (dqkv_ref, gwa_ref, gwb_ref, gb_ref, gbt_ref, o_out), got, refs = refs[:6], refs[6:6 + n_swap], refs[6 + n_swap:]
    x_buf, refs = refs[0], refs[1:]
    w_ref, b_rep, qkvt_ref, k_tok, v_tok, posk_ref, s_buf, m_buf, q_pad, do_pad, o_acc, dq_acc, dk_acc, dv_acc, x_sem, w_sem = refs[:16]
    swaps = [(old[k], got[k]) + refs[16 + 4 * k:20 + 4 * k] for k in range(n_swap)]
    if send_o:
        o_ref, os_sem, or_sem = refs[-3:]
        o_new = o_out
    else:
        o_ref = o_out
    dim, lead = dot_ref.shape[1], gwa_ref.shape[0]
    seq = dot_ref.shape[0] * tok
    pad = k_tok.shape[1] - dim
    nq = blk // tok
    steps = seq // blk
    scale = dim ** -0.5
    me = lax.axis_index("sp")
    step = pl.program_id(0)
    i = lax.rem(me // nq + step, steps)
    half = blk // 2
    sub = tok // 128

    def spread(row):
        return jnp.transpose(jnp.broadcast_to(row, (128, 128)))

    def x_copy(k):
        rows = pl.ds(pl.multiple_of(k * blk, blk), blk)
        return pltpu.make_async_copy(x_ref.at[rows], x_buf.at[rows], x_sem.at[k])

    def o_send(to):
        return pltpu.make_async_remote_copy(
            src_ref=o_ref.at[to], dst_ref=o_new.at[me], send_sem=os_sem.at[to], recv_sem=or_sem.at[me],
            device_id={"sp": to}, device_id_type=pl.DeviceIdType.MESH)

    def o_keep():
        return pltpu.make_async_copy(o_ref.at[me], o_new.at[me], os_sem.at[me])

    def o_start(at):
        for t in range(nq):
            to = lax.rem(me // nq + at, steps) * nq + t

            @pl.when(to != me)
            def _():
                o_send(to).start()

            @pl.when(to == me)
            def _():
                o_keep().start()

    @pl.when(step == 0)
    def _():
        w_load = pltpu.make_async_copy(w_hbm.at[me], w_ref, w_sem)
        w_load.start()
        for k in range(steps):
            x_copy(k).start()
        meet(peers)
        for one in swaps:
            swap_start(*one, peers)
        dk_acc[...] = jnp.zeros_like(dk_acc)
        dv_acc[...] = jnp.zeros_like(dv_acc)
        q_pad[...] = jnp.zeros_like(q_pad)
        do_pad[...] = jnp.zeros_like(do_pad)
        mine = lax.broadcasted_iota(jnp.int32, (peers, dim), 0) == me
        for k in range(3):
            row = jnp.sum(jnp.where(mine, b_ref[k], 0.0), axis=0, keepdims=True)
            b_rep[k * dim:(k + 1) * dim, :] = spread(jnp.concatenate([row, jnp.zeros((1, pad), F32)], axis=1))[0:dim]
        w_load.wait()

        @pl.loop(0, steps)
        def _(k):
            rows = pl.ds(pl.multiple_of(k * blk, blk), blk)
            x_copy(k).wait()
            shift = jnp.concatenate([b_rep[...]] * (blk // 128), axis=1)
            qkvt_ref[:, rows] = (lax.dot_general(w_ref[...], x_buf[rows, :], NT, preferred_element_type=F32) + shift).astype(BF16)

            @pl.loop(0, blk // 128)
            def _(t):
                cols = pl.ds(pl.multiple_of(k * blk + t * 128, 128), 128)
                for base, dst in ((dim, k_tok), (2 * dim, v_tok)):
                    part = qkvt_ref[base:base + dim, cols].astype(F32)
                    whole = jnp.concatenate([part, jnp.zeros((pad, 128), F32)], axis=0)
                    dst[cols, :] = jnp.transpose(whole).astype(BF16)
                lanes = pl.ds(pl.multiple_of((t % sub) * 128, 128), 128)
                pos = marks_ref[k * nq + t // sub, which:which + 1, lanes].astype(F32)
                keep = marks_ref[k * nq + t // sub, batch + which:batch + which + 1, lanes]
                posk_ref[cols, :] = spread(jnp.where(keep > 0, pos, MASKED))

    if send_o:
        @pl.when(step > 0)
        def _():
            o_start(step - 1)

    qcols = pl.ds(pl.multiple_of(i * blk, blk), blk)
    q_pad[0:dim, :] = qkvt_ref[0:dim, qcols]
    for t in range(nq):
        do_pad[0:dim, t * tok:(t + 1) * tok] = dot_ref[i * nq + t]
    slope2 = jnp.exp2(jnp.full((1, 128), -8.0 / peers, F32) * (me + 1).astype(F32)) * LOG2E
    ref_pos = jnp.broadcast_to(marks_ref[i * nq, which:which + 1, 0:128][:, 0:1].astype(F32), (1, 128))
    c = scale * LOG2E

    def scores(j, carry, diag):
        m, l8 = carry
        for sub in range(2):
            rows = pl.ds(pl.multiple_of(j * blk + sub * half, half), half)
            st = jnp.dot(k_tok[rows, :], q_pad[...], preferred_element_type=F32)
            bias = (posk_ref[rows, :] - ref_pos) * slope2
            st = st * c + jnp.concatenate([bias] * (blk // 128), axis=1)
            if diag:
                key = lax.broadcasted_iota(jnp.int32, (half, blk), 0) + sub * half
                qry = lax.broadcasted_iota(jnp.int32, (half, blk), 1)
                st = jnp.where(key <= qry, st, MASKED)
            m_new = jnp.maximum(m, jnp.max(st, axis=0, keepdims=True))
            e = jnp.exp2(st - m_new)
            s_buf[rows, :] = e
            m_buf[2 * j + sub] = jnp.broadcast_to(m_new, (8, blk))
            l8 = l8 * jnp.exp2(m - m_new) + jnp.sum(e.reshape(half // 8, 8, blk), axis=0)
            m = m_new
        return m, l8

    start = (jnp.full((1, blk), MASKED, F32), jnp.zeros((8, blk), F32))
    m, l8 = scores(i, lax.fori_loop(0, i, lambda j, carry: scores(j, carry, False), start), True)
    inv = 1.0 / jnp.sum(l8, axis=0, keepdims=True)
    o_acc[...] = jnp.zeros_like(o_acc)
    dq_acc[...] = jnp.zeros_like(dq_acc)

    def values(j, _):
        rows = pl.ds(pl.multiple_of(j * blk, blk), blk)
        pbs = []
        for sub in range(2):
            part = pl.ds(pl.multiple_of(j * blk + sub * half, half), half)
            p = s_buf[part, :] * (jnp.exp2(m_buf[2 * j + sub][0:1, :] - m) * inv)
            s_buf[part, :] = p
            pbs.append(p.astype(BF16))
        pb = jnp.concatenate(pbs, axis=0)
        o_acc[...] += jnp.dot(qkvt_ref[2 * dim:3 * dim, rows], pb, preferred_element_type=F32)
        dv_acc[:, rows] += lax.dot_general(do_pad[0:dim, :], pb, NT, preferred_element_type=F32)
        return 0

    lax.fori_loop(0, i + 1, values, 0)
    o_lo = o_acc[...].astype(BF16)
    do_f = do_pad[0:dim, :].astype(F32)
    r = jnp.sum(do_f * o_lo.astype(F32), axis=0, keepdims=True)

    def grads(j, _):
        rows = pl.ds(pl.multiple_of(j * blk, blk), blk)
        g = jnp.dot(v_tok[rows, :], do_pad[...], preferred_element_type=F32)
        ds = (s_buf[rows, :] * (g - r)).astype(BF16)
        dq_acc[...] += jnp.dot(qkvt_ref[dim:2 * dim, rows], ds, preferred_element_type=F32)
        dk_acc[:, rows] += lax.dot_general(q_pad[0:dim, :], ds, NT, preferred_element_type=F32)
        return 0

    lax.fori_loop(0, i + 1, grads, 0)
    dq_lo = (dq_acc[...] * scale).astype(BF16)
    for t in range(nq):
        o_ref[i * nq + t] = o_lo[:, t * tok:(t + 1) * tok]
        dqkv_ref[i * nq + t, 0:dim] = dq_lo[:, t * tok:(t + 1) * tok]

    @pl.when(step == steps - 1)
    def _():
        @pl.loop(0, seq // tok)
        def _(t):
            cols = pl.ds(pl.multiple_of(t * tok, tok), tok)
            dqkv_ref[t, dim:2 * dim] = (dk_acc[:, cols] * scale).astype(BF16)
            dqkv_ref[t, 2 * dim:3 * dim] = dv_acc[:, cols].astype(BF16)

        if send_o:
            o_start(step)
        for k, ref in enumerate((gwa_ref, gwb_ref, gb_ref)):
            ref[...] = gw_old[k][...] if n_old else jnp.zeros_like(ref)
        ones = jnp.ones((blk, 128), BF16)

        @pl.loop(0, steps)
        def _(j):
            rows = pl.ds(pl.multiple_of(j * blk, blk), blk)
            for ref, lo, hi in ((gwa_ref, 0, lead), (gwb_ref, lead, 3 * dim)):
                lhs = jnp.concatenate([dqkv_ref[j * nq + t, lo:hi] for t in range(nq)], axis=1)
                ref[...] += jnp.dot(lhs, x_buf[rows, :], preferred_element_type=F32)
                gb_ref[lo:hi, :] += jnp.dot(lhs, ones, preferred_element_type=F32)

        gbt_ref[...] = jnp.zeros_like(gbt_ref)
        for k in range(3):
            part = jnp.concatenate([gb_ref[k * dim:(k + 1) * dim, :], jnp.zeros((pad, 128), F32)], axis=0)
            gbt_ref[k:k + 1, :] = jnp.transpose(part)[0:1, :]

        if send_o:
            o_keep().wait()
            for d in range(1, peers):
                frm = lax.rem(me + d, peers)
                o_send(frm).wait_send()
                pltpu.make_async_remote_copy(
                    src_ref=o_ref.at[frm], dst_ref=o_new.at[frm], send_sem=os_sem.at[frm], recv_sem=or_sem.at[frm],
                    device_id={"sp": frm}, device_id_type=pl.DeviceIdType.MESH).wait_recv()
        for one in swaps:
            swap_wait(*one, peers)


def attention(w_all, b_all, dot_, marks, x, gw, old, *, blk, tok, which, batch, lead, send_o, collective_id):
    blocks, dim, _ = dot_.shape
    seq, hidden = blocks * tok, w_all.shape[2]
    wide = 128 * pl.cdiv(dim, 128)
    hbm = pl.BlockSpec(memory_space=pltpu.HBM)
    full = lambda a: pl.BlockSpec(a.shape, lambda i: (0,) * len(a.shape), pipeline_mode=pl.Buffered(1))
    like = lambda a: jax.ShapeDtypeStruct(a.shape, a.dtype)
    outs = [jax.ShapeDtypeStruct((blocks, 3 * dim, tok), BF16), jax.ShapeDtypeStruct((lead, hidden), F32),
            jax.ShapeDtypeStruct((3 * dim - lead, hidden), F32), jax.ShapeDtypeStruct((3 * dim, 128), F32), jax.ShapeDtypeStruct((8, 128), F32)]
    pairs = (seq // blk) * (seq // blk + 1) // 2
    dma = pltpu.SemaphoreType.DMA
    res = pl.pallas_call(
        functools.partial(attn_body, blk=blk, tok=tok, which=which, batch=batch, n_swap=len(old), n_old=len(gw), send_o=send_o),
        name="attention",
        out_shape=outs + [like(dot_)] + [like(a) for a in old],
        grid=(seq // blk,),
        in_specs=[hbm, full(b_all), full(dot_), full(marks), hbm] + [full(a) for a in gw] + [hbm] * len(old),
        out_specs=[full(a) for a in outs] + [hbm if send_o else full(dot_)] + [hbm] * len(old),
        scratch_shapes=[
            pltpu.VMEM((seq, hidden), BF16),
            pltpu.VMEM(w_all.shape[1:], BF16), pltpu.VMEM((3 * dim, 128), F32), pltpu.VMEM((3 * dim, seq), BF16),
            pltpu.VMEM((seq, wide), BF16), pltpu.VMEM((seq, wide), BF16), pltpu.VMEM((seq, 128), F32),
            pltpu.VMEM((seq, blk), F32), pltpu.VMEM((2 * seq // blk, 8, blk), F32),
            pltpu.VMEM((wide, blk), BF16), pltpu.VMEM((wide, blk), BF16),
            pltpu.VMEM((dim, blk), F32), pltpu.VMEM((dim, blk), F32),
            pltpu.VMEM((dim, seq), F32), pltpu.VMEM((dim, seq), F32), dma((seq // blk,)), dma]
        + sum((swap_scratch(a) for a in old), []) + ([pltpu.VMEM(dot_.shape, BF16), dma((blocks,)), dma((blocks,))] if send_o else []),
        cost_estimate=pl.CostEstimate(flops=pairs * 6 * 2 * blk * blk * 256, bytes_accessed=24 << 20, transcendentals=pairs * blk * blk),
        compiler_params=pltpu.CompilerParams(dimension_semantics=("arbitrary",), vmem_limit_bytes=VMEM_LIMIT,
                                             collective_id=collective_id, has_side_effects=True),
    )(w_all, b_all, dot_, marks, x, *gw, *old)
    return res[0], res[1:4], res[4], res[5], res[6:]


def peer_at(d, peers):
    return {"sp": lax.rem(lax.axis_index("sp") + d, peers)}


def greet(peers):
    barrier = pltpu.get_barrier_semaphore()
    for d in range(1, peers):
        pl.semaphore_signal(barrier, inc=1, device_id=peer_at(d, peers), device_id_type=pl.DeviceIdType.MESH)
    return lambda: pl.semaphore_wait(barrier, peers - 1)


def meet(peers):
    greet(peers)()


def swap_copies(x_ref, out_ref, send_sem, recv_sem, peers):
    me = lax.axis_index("sp")
    order = [d for near in range(peers // 2) for d in sorted({peers // 2 - near, peers // 2 + near})]
    return [pltpu.make_async_remote_copy(
        src_ref=x_ref.at[lax.rem(me + d, peers)], dst_ref=out_ref.at[me], send_sem=send_sem.at[d - 1], recv_sem=recv_sem.at[d - 1],
        device_id=peer_at(d, peers), device_id_type=pl.DeviceIdType.MESH) for d in order]


def swap_start(x_ref, out_ref, own, send_sem, recv_sem, own_sem, peers):
    me = lax.axis_index("sp")
    for copy in swap_copies(x_ref, out_ref, send_sem, recv_sem, peers):
        copy.start()
    take = pltpu.make_async_copy(x_ref.at[me], own, own_sem)
    take.start()
    take.wait()
    pltpu.make_async_copy(own, out_ref.at[me], own_sem).start()


def swap_wait(x_ref, out_ref, own, send_sem, recv_sem, own_sem, peers):
    pltpu.make_async_copy(own, out_ref.at[lax.axis_index("sp")], own_sem).wait()
    for copy in swap_copies(x_ref, out_ref, send_sem, recv_sem, peers):
        copy.wait()


def swap_scratch(x):
    peers = x.shape[0]
    return [pltpu.VMEM(x.shape[1:], x.dtype), pltpu.SemaphoreType.DMA((peers - 1,)), pltpu.SemaphoreType.DMA((peers - 1,)),
            pltpu.SemaphoreType.DMA]


STEP = (1, -1)


def hops(ring, s, w):
    return ring // 2 - (s != w)


def ring_gather(block, own, sems, peers, cuts):
    ring = peers // 2
    me = lax.axis_index("sp")
    z, c = me // 2, me % 2
    send_sem, recv_sem, over_sem, came_sem = sems
    turn = lambda k: lax.rem(z + k + 2 * ring, ring)
    lots = [(s, w, u) for u in range(cuts) for w in range(2) for s in range(2)]

    def copy(src, dst, one, two, to):
        return pltpu.make_async_remote_copy(src_ref=src, dst_ref=dst, send_sem=one, recv_sem=two, device_id={"sp": to},
                                            device_id_type=pl.DeviceIdType.MESH)

    def along(s, w, t, u):
        ref = block(turn(-STEP[s] * t), c, w, u)
        return copy(own(w, u) if t == 0 else ref, ref, send_sem.at[s, w, t, u], recv_sem.at[s, w, t, u], 2 * turn(STEP[s]) + c)

    def across(s, w, t, u, side):
        ref = block(turn(-STEP[s] * t), side, w, u)
        return copy(own(w, u) if t == 0 and side is c else ref, ref, over_sem.at[s, w, t, u], came_sem.at[s, w, t, u], 2 * z + 1 - c)

    home = [(0, w, 0, u) for u in range(cuts) for w in range(2)]
    moved = [(s, w, t, u) for t in range(1, ring // 2 + 1) for s, w, u in lots if t <= hops(ring, s, w)]

    def start(only=None):
        for s, w, u in lots:
            if only in (None, (w, u)):
                along(s, w, 0, u).start()
        for lot in home:
            if only in (None, (lot[1], lot[3])):
                across(*lot, c).start()

    def run(lo=1, hi=ring):
        for s, w, t, u in moved:
            if lo <= t < hi:
                along(s, w, t - 1, u).wait_recv()
                if t < hops(ring, s, w):
                    along(s, w, t, u).start()
                across(s, w, t, u, c).start()

    def finish():
        for s, w, t, u in moved:
            along(s, w, t - 1, u).wait_send()
        for lot in home + moved:
            across(*lot, c).wait_send()
            across(*lot, 1 - c).wait_recv()

    return start, run, finish


def ring_scratch(peers, cuts):
    dma = pltpu.SemaphoreType.DMA
    return [dma((2, 2, peers // 4, cuts))] * 2 + [dma((2, 2, peers // 4 + 1, cuts))] * 2


def opening_body(x_hbm, dy_hbm, wo_hbm, gain_ref, bias_ref, pos_ref, keep_ref, marks_all, do_t, x_all, *refs, peers, batch, cuts):
    x_out, do_out = refs[:batch - 1], refs[batch - 1:2 * batch - 2]
    x_ref, dy_ref, x_own, do_own, wo_ref, marks_ref, own, ds_sem, dr_sem, do_sem, ms_sem, mr_sem, in_sem = refs[2 * batch - 2:2 * batch + 11]
    ring_sems = refs[2 * batch + 11:]
    gain, bias = gain_ref[...].reshape(1, -1), bias_ref[...].reshape(1, -1)
    me = lax.axis_index("sp")
    tok, dim = x_own.shape[0], do_own.shape[1]
    lot = tok // 2 // cuts
    rows_of = lambda w, u: pl.ds((w * cuts + u) * lot, lot)
    arrived = greet(peers)
    loads = [pltpu.make_async_copy(x_hbm.at[b], x_ref.at[b], in_sem.at[b]) for b in range(batch)]
    loads += [pltpu.make_async_copy(dy_hbm, dy_ref, in_sem.at[batch]), pltpu.make_async_copy(wo_hbm, wo_ref, in_sem.at[batch + 1])]
    for load in loads:
        load.start()

    def norm_rows(b, out_ref, rows):
        x = x_ref[b, rows, :].astype(F32)
        cen = x - jnp.mean(x, axis=-1, keepdims=True)
        hat = cen * lax.rsqrt(jnp.mean(cen * cen, axis=-1, keepdims=True) + NORM_EPS)
        out_ref[rows, :] = (hat * gain + bias).astype(BF16)

    def norm(b, out_ref):
        loads[b].wait()

        @pl.loop(0, tok // 32)
        def _(k):
            norm_rows(b, out_ref, pl.ds(pl.multiple_of(k * 32, 32), 32))

    def product(b, out_ref):
        @pl.loop(0, peers // 4)
        def _(g):
            rows = pl.ds(pl.multiple_of(g * 4 * dim, 4 * dim), 4 * dim)
            out_ref[pl.ds(g * 4, 4)] = lax.dot_general(wo_ref[rows, :], dy_ref[b], NT, preferred_element_type=F32).astype(BF16).reshape(4, dim, tok)

    marks_ref[...] = jnp.zeros_like(marks_ref)
    marks_ref[0:batch, :] = pos_ref[...]
    marks_ref[batch:2 * batch, :] = keep_ref[...]
    block = lambda k, side, w, u: x_all.at[2 * k + side, rows_of(w, u)]
    start, run, finish = ring_gather(block, lambda w, u: x_own.at[rows_of(w, u)], ring_sems, peers, cuts)
    loads[0].wait()
    pieces = [(w, u) for u in range(cuts) for w in range(2)]
    for k, piece in enumerate(pieces):
        norm_rows(0, x_own, rows_of(*piece))
        if k == 1:
            arrived()
        if k:
            start(pieces[k - 1])
    start(pieces[-1])
    keep = pltpu.make_async_copy(x_own, x_all.at[me], in_sem.at[batch + 2])
    keep.start()
    marks = [pltpu.make_async_remote_copy(
        src_ref=marks_ref, dst_ref=marks_all.at[me], send_sem=ms_sem.at[d - 1], recv_sem=mr_sem.at[d - 1],
        device_id=peer_at(d, peers), device_id_type=pl.DeviceIdType.MESH) for d in range(1, peers)]
    for copy in marks:
        copy.start()
    marks_all[me] = marks_ref[...]
    loads[-2].wait()
    loads[-1].wait()
    product(0, do_own)
    for b in range(1, batch):
        norm(b, x_out[b - 1])
    swap_start(do_own, do_t, own, ds_sem, dr_sem, do_sem, peers)
    for b in range(1, batch):
        product(b, do_out[b - 1])
    run()
    keep.wait()
    for copy in marks:
        copy.wait()
    swap_wait(do_own, do_t, own, ds_sem, dr_sem, do_sem, peers)
    finish()


def opening(x, dy, w_out, gain, bias, pos, keep, peers, collective_id, cuts=4):
    batch, tok, hidden = x.shape
    dim = hidden // peers
    hbm, vmem = pl.BlockSpec(memory_space=pltpu.HBM), pl.BlockSpec(memory_space=pltpu.VMEM)
    dma = pltpu.SemaphoreType.DMA
    do_shape, x_shape = jax.ShapeDtypeStruct((peers, dim, tok), BF16), jax.ShapeDtypeStruct((tok, hidden), BF16)
    res = pl.pallas_call(
        functools.partial(opening_body, peers=peers, batch=batch, cuts=cuts),
        name="opening",
        out_shape=[jax.ShapeDtypeStruct((peers, 8, tok), pos.dtype), do_shape, jax.ShapeDtypeStruct((peers, tok, hidden), BF16)]
        + [x_shape] * (batch - 1) + [do_shape] * (batch - 1),
        in_specs=[hbm, hbm, hbm, vmem, vmem, vmem, vmem],
        out_specs=[vmem, hbm, hbm] + [vmem] * (2 * batch - 2),
        scratch_shapes=[pltpu.VMEM(x.shape, BF16), pltpu.VMEM(dy.shape, BF16), pltpu.VMEM(x_shape.shape, BF16), pltpu.VMEM(do_shape.shape, BF16),
                        pltpu.VMEM(w_out.shape, BF16), pltpu.VMEM((8, tok), pos.dtype)] + swap_scratch(do_shape)
        + [dma((peers - 1,)), dma((peers - 1,)), dma((batch + 3,))] + ring_scratch(peers, cuts),
        cost_estimate=pl.CostEstimate(flops=5 * 10**10, bytes_accessed=16 << 20, transcendentals=0),
        compiler_params=pltpu.CompilerParams(collective_id=collective_id, has_side_effects=True, vmem_limit_bytes=VMEM_LIMIT),
    )(x, dy, w_out, gain, bias, pos, keep)
    return res[0], res[1], res[2], res[3:2 + batch], res[2 + batch:]


TN = (((0,), (0,)), ((), ()))


def tail_a_body(dqkv_ref, oo_hbm, on_hbm, dy_hbm, x_hbm, wo_hbm, d_hbm, w_hbm, gain_ref, bo_ref, y_ref, gx_ref, part, rows_ref,
                o_old, o_new, dy_ref, x_ref, wo_ref, d_old, w_ref, d_new, dn, sums, bo_rep, both, mine, landed, own_d,
                ds_sem, dr_sem, do_sem, ps_sem, pr_sem, rs_sem, rr_sem, w_sem, *, peers, cuts):
    ring = peers // 2
    me = lax.axis_index("sp")
    z, c = me // 2, me % 2
    _, tok, hidden = x_ref.shape
    half, wide, few = hidden // 2, hidden // 3, part.shape[0] // cuts
    cols = (pl.ds(0, half), pl.ds(half, half))
    at = lambda zz, cc: {"sp": 2 * zz + cc}
    turn = lambda k: lax.rem(z + k + 2 * ring, ring)
    remote = functools.partial(pltpu.make_async_remote_copy, device_id_type=pl.DeviceIdType.MESH)
    span, group = d_old.shape[1], 8
    gain, b_out = gain_ref[...].reshape(1, hidden), bo_ref[...].reshape(1, hidden)
    pairs = ((oo_hbm, o_old), (on_hbm, o_new), (dy_hbm, dy_ref), (x_hbm, x_ref), (wo_hbm, wo_ref), (d_hbm, d_old), (w_hbm, w_ref))
    loads = [pltpu.make_async_copy(src, dst, w_sem.at[k]) for k, (src, dst) in enumerate(pairs)]
    swap = (dqkv_ref, d_new, own_d, ds_sem, dr_sem, do_sem, peers)
    arrived = greet(peers)
    for load in loads:
        load.start()
    arrived()
    swap_start(*swap)
    for load in loads[:3]:
        load.wait()

    def product(put, side):
        @pl.loop(0, ring)
        def _(k):
            h = 2 * k + side
            put(k, jnp.dot(o_old[h], dy_ref[0], preferred_element_type=F32)
                + jnp.dot(o_new[h], dy_ref[1], preferred_element_type=F32))

    def put_other(k, value):
        both[k, 1 - c] = value

    def put_mine(k, value):
        mine[k] = value

    def forward(b, o_ref):
        o_t = o_ref[...].reshape(hidden, tok)

        @pl.loop(0, 3)
        def _(n):
            at_n = pl.ds(pl.multiple_of(n * wide, wide), wide)
            acc = lax.dot_general(o_t, wo_ref[:, at_n], TN, preferred_element_type=F32)
            y_ref[b, :, at_n] = (x_ref[b, :, at_n].astype(F32) + acc + bo_rep[0:1, at_n]).astype(BF16)

    def backward(b, d_ref):
        @pl.loop(0, 3)
        def _(n):
            at_n = pl.ds(pl.multiple_of(n * wide, wide), wide)
            acc = None
            for k in range(0, peers, group):
                lhs = d_ref[k:k + group].reshape(-1, tok)
                one = lax.dot_general(lhs, w_ref[k * span:(k + group) * span, at_n], TN, preferred_element_type=F32)
                acc = one if acc is None else acc + one
            dn[:, at_n] = acc

        @pl.loop(0, tok // 32)
        def _(k):
            rows = pl.ds(pl.multiple_of(k * 32, 32), 32)
            x = x_ref[b, rows, :].astype(F32)
            dy = dy_ref[b, rows, :].astype(F32)
            d = dn[rows, :]
            cen = x - jnp.mean(x, axis=-1, keepdims=True)
            inv = lax.rsqrt(jnp.mean(cen * cen, axis=-1, keepdims=True) + NORM_EPS)
            hat = cen * inv
            for n, one in enumerate((d * hat, d, dy)):
                sums[n] += jnp.sum(one.reshape(4, 8, hidden), axis=0)
            e = d * gain
            m1 = jnp.mean(e, axis=-1, keepdims=True)
            m2 = jnp.mean(e * hat, axis=-1, keepdims=True)
            gx_ref[b, rows, :] = (dy + inv * (e - m1 - hat * m2)).astype(BF16)

    bo_rep[...] = jnp.broadcast_to(b_out, bo_rep.shape)
    sums[...] = jnp.zeros_like(sums)
    product(put_other, 1 - c)
    pair_copy = lambda side: remote(src_ref=both.at[:, side], dst_ref=both.at[:, side], send_sem=ps_sem, recv_sem=pr_sem, device_id=at(z, 1 - c))
    product(put_mine, c)
    pair_copy(1 - c).start()
    pair_copy(1 - c).wait_send()
    pair_copy(c).wait_recv()

    @pl.loop(0, ring)
    def _(k):
        mine[k] = mine[k] + both[k, c]

    lots = [(s, w, u) for u in range(cuts) for w in range(2) for s in range(2)]

    def reduce_copy(s, w, t, u):
        return remote(src_ref=mine.at[turn(STEP[s] * (hops(ring, s, w) - t)), pl.ds(u * few, few), cols[w]], dst_ref=landed.at[s, w, t, u],
                      send_sem=rs_sem.at[s, w, t, u], recv_sem=rr_sem.at[s, w, t, u], device_id=at(turn(STEP[s]), c))

    def fold(s, w, t, u):
        reduce_copy(s, w, t, u).wait_recv()
        at_k = (turn(STEP[s] * (hops(ring, s, w) - t - 1)), pl.ds(u * few, few), cols[w])
        mine[at_k] = mine[at_k] + landed[s, w, t, u]

    def hop(t):
        for s, w, u in lots:
            if t < hops(ring, s, w):
                fold(s, w, t - 1, u)
                reduce_copy(s, w, t, u).start()

    for s, w, u in lots:
        reduce_copy(s, w, 0, u).start()
    for load in loads[3:5]:
        load.wait()
    forward(0, o_old)
    forward(1, o_new)
    for load in loads[5:]:
        load.wait()
    backward(0, d_old)
    for t in range(1, ring // 2 - 1):
        hop(t)
    swap_wait(*swap)
    backward(1, d_new)
    hop(ring // 2 - 1)
    rows_ref[...] = jnp.zeros_like(rows_ref)
    for n in range(3):
        rows_ref[n:n + 1, :] = jnp.sum(sums[n], axis=0, keepdims=True)
    for s, w, u in lots:
        fold(s, w, hops(ring, s, w) - 1, u)
    part[...] = mine[z]
    for s, w, u in lots:
        for t in range(hops(ring, s, w)):
            reduce_copy(s, w, t, u).wait_send()


def tail_a(dqkv, d_old, o_old, o_new, dy, x, w_flat, w_out, gain, b_out, collective_id, cuts=2):
    peers, dim, tok = o_old.shape
    ring = peers // 2
    hidden = dy.shape[-1]
    hbm, vmem = pl.BlockSpec(memory_space=pltpu.HBM), pl.BlockSpec(memory_space=pltpu.VMEM)
    dma = pltpu.SemaphoreType.DMA
    held = lambda a: pltpu.VMEM(a.shape, a.dtype)
    steps = (2, 2, ring // 2, cuts)
    return pl.pallas_call(
        functools.partial(tail_a_body, peers=peers, cuts=cuts),
        name="tail_a",
        out_shape=[jax.ShapeDtypeStruct(x.shape, BF16), jax.ShapeDtypeStruct(x.shape, BF16), jax.ShapeDtypeStruct((dim, hidden), F32),
                   jax.ShapeDtypeStruct((8, hidden), F32)],
        in_specs=[hbm] * 8 + [vmem] * 2,
        out_specs=[vmem] * 4,
        scratch_shapes=[held(a) for a in (o_old, o_new, dy, x, w_out, d_old, w_flat, dqkv)]
        + [pltpu.VMEM((tok, hidden), F32), pltpu.VMEM((3, 8, hidden), F32), pltpu.VMEM((8, hidden), F32),
           pltpu.VMEM((ring, 2, dim, hidden), F32), pltpu.VMEM((ring, dim, hidden), F32), pltpu.VMEM(steps + (dim // cuts, hidden // 2), F32),
           pltpu.VMEM(dqkv.shape[1:], BF16), dma((peers - 1,)), dma((peers - 1,)), dma, dma, dma, dma(steps), dma(steps), dma((7,))],
        cost_estimate=pl.CostEstimate(flops=10**11, bytes_accessed=64 << 20, transcendentals=0),
        compiler_params=pltpu.CompilerParams(collective_id=collective_id, has_side_effects=True, vmem_limit_bytes=VMEM_LIMIT),
    )(dqkv, o_old, o_new, dy, x, w_out, d_old, w_flat, gain, b_out)


def tail_b_body(part, rows_ref, gb_ref, full, total, gb_all, stage, xs_sem, xr_sem, *ring_sems, peers, cuts):
    ring = peers // 2
    me = lax.axis_index("sp")
    z, c = me // 2, me % 2
    hidden = part.shape[1]
    half, few = hidden // 2, part.shape[0] // cuts
    cols = (pl.ds(0, half), pl.ds(half, half))
    remote = functools.partial(pltpu.make_async_remote_copy, device_id_type=pl.DeviceIdType.MESH)
    arrived = greet(peers)
    full[z, c] = part[...]
    gb_all[me] = gb_ref[...]
    block = lambda k, side, w, u: full.at[k, side, pl.ds(u * few, few), cols[w]]
    start, run, finish = ring_gather(block, lambda w, u: block(z, c, w, u), ring_sems, peers, cuts)
    owners = hidden // 128
    lanes = lambda k: pl.ds(pl.multiple_of(k * 128, 128), 128)

    def small_copy(kind, frm, to):
        src, dst = ((rows_ref.at[:, lanes(to)], stage.at[frm]), (total.at[:, lanes(frm)],) * 2, (gb_ref, gb_all.at[frm]))[kind]
        return remote(src_ref=src, dst_ref=dst, send_sem=xs_sem.at[kind, to], recv_sem=xr_sem.at[kind, frm], device_id={"sp": to})

    def each(act, kind, only_to=False, only_from=False):
        @pl.loop(1, peers)
        def _(d):
            far = lax.rem(me + d, peers)

            def go():
                act(kind, far)

            if only_to:
                pl.when(far < owners)(go)
            elif only_from:
                pl.when(me < owners)(go)
            else:
                go()

    send = lambda kind, far: small_copy(kind, me, far).start()
    over = lambda kind, far: small_copy(kind, me, far).wait_send()
    came = lambda kind, far: small_copy(kind, far, me).wait_recv()

    @pl.when(me < owners)
    def _():
        stage[me] = rows_ref[:, lanes(me)]

    arrived()
    start()
    each(send, 0, only_to=True)
    each(send, 2)
    run(1, 2)
    each(came, 0, only_from=True)

    @pl.when(me < owners)
    def _():
        total[:, lanes(me)] = jnp.sum(stage[...], axis=0)

    each(send, 1, only_from=True)
    run(2)
    each(came, 1, only_to=True)
    each(came, 2)
    each(over, 0, only_to=True)
    each(over, 1, only_from=True)
    each(over, 2)
    finish()


def tail_b(part, rows, gb, peers, collective_id, cuts=2):
    ring = peers // 2
    vmem = pl.BlockSpec(memory_space=pltpu.VMEM)
    dma = pltpu.SemaphoreType.DMA
    return pl.pallas_call(
        functools.partial(tail_b_body, peers=peers, cuts=cuts),
        name="tail_b",
        out_shape=[jax.ShapeDtypeStruct((ring, 2) + part.shape, F32), jax.ShapeDtypeStruct(rows.shape, F32),
                   jax.ShapeDtypeStruct((peers,) + gb.shape, F32)],
        in_specs=[vmem] * 3,
        out_specs=[vmem] * 3,
        scratch_shapes=[pltpu.VMEM((peers, 8, 128), F32), dma((3, peers)), dma((3, peers))] + ring_scratch(peers, cuts),
        cost_estimate=pl.CostEstimate(flops=5 * 10**10, bytes_accessed=10 << 20, transcendentals=0),
        compiler_params=pltpu.CompilerParams(collective_id=collective_id, has_side_effects=True, vmem_limit_bytes=32 << 20),
    )(part, rows, gb)


def settle_body(*refs, n_in, first, n_plain, n_held):
    x_ref, plain, held = refs[0], refs[1:1 + n_plain], refs[1 + n_plain:1 + n_plain + n_held]
    outs = refs[n_in:n_in + 1 + n_plain + n_held]
    buf, in_sem, out_sem, in_plain, out_plain, *rooms = refs[n_in + 1 + n_plain + n_held:]
    heads, n = x_ref.shape[:2]
    copy = pltpu.make_async_copy
    reads = [copy(x_ref.at[h], buf.at[h], in_sem.at[h]) for h in range(heads)]
    writes = [copy(buf.at[h], outs[0].at[h, pl.ds(first, n)], out_sem.at[h]) for h in range(heads)]
    reads += [copy(plain[k], rooms[k], in_plain.at[k]) for k in range(n_plain)]
    writes += [copy(rooms[k], outs[1 + k], out_plain.at[k]) for k in range(n_plain)]
    flat = [copy(held[k], outs[1 + n_plain + k], out_plain.at[n_plain + k]) for k in range(n_held)]
    for one in reads + flat:
        one.start()
    for read, write in zip(reads, writes):
        read.wait()
        write.start()
    for one in writes + flat:
        one.wait()


def settle(x, into, plain, held, span, first):
    heads, n, hidden = x.shape
    hbm, vmem = pl.BlockSpec(memory_space=pltpu.HBM), pl.BlockSpec(memory_space=pltpu.VMEM)
    pin = lambda a: pltpu.with_memory_space_constraint(a, pltpu.HBM)
    args = (pin(x), *[pin(a) for a in plain], *held) + (() if into is None else (into,))
    dma = pltpu.SemaphoreType.DMA
    extra = max(len(plain) + len(held), 1)
    return pl.pallas_call(
        functools.partial(settle_body, n_in=len(args), first=first, n_plain=len(plain), n_held=len(held)), name="settle",
        out_shape=[jax.ShapeDtypeStruct((heads, span, hidden), x.dtype)] + [jax.ShapeDtypeStruct(a.shape, a.dtype) for a in (*plain, *held)],
        in_specs=[hbm] * (1 + len(plain)) + [vmem] * len(held) + [hbm] * (into is not None),
        out_specs=[hbm] * (1 + len(plain) + len(held)),
        input_output_aliases={} if into is None else {len(args) - 1: 0},
        scratch_shapes=[pltpu.VMEM(x.shape, x.dtype), dma((heads,)), dma((heads,)), dma((extra,)), dma((extra,))]
        + [pltpu.VMEM(a.shape, a.dtype) for a in plain],
        cost_estimate=pl.CostEstimate(flops=10**9, bytes_accessed=8 * x.size, transcendentals=0),
        compiler_params=pltpu.CompilerParams(vmem_limit_bytes=24 << 20))(*args)


def lay_body(go_ref, total, gb_all, go_out, gb_out, *refs):
    vectors, sem = refs[:-1], refs[-1]
    copies = [pltpu.make_async_copy(go_ref.at[k], go_out.at[k], sem.at[k]) for k in range(go_ref.shape[0])]
    for copy in copies:
        copy.start()
    for k in range(3):
        gb_out[k] = gb_all[:, k, 0:gb_out.shape[2]]
        vectors[k][...] = total[k]
    for copy in copies:
        copy.wait()


def lay_down(go, total, gb_all):
    hbm, vmem = pl.BlockSpec(memory_space=pltpu.HBM), pl.BlockSpec(memory_space=pltpu.VMEM)
    ring, _, dim, hidden = go.shape
    return pl.pallas_call(
        lay_body, name="lay_down",
        out_shape=[jax.ShapeDtypeStruct(go.shape, F32), jax.ShapeDtypeStruct((3, 2 * ring, dim), F32)] + [jax.ShapeDtypeStruct((hidden,), F32)] * 3,
        in_specs=[vmem] * 3, out_specs=[hbm] + [vmem] * 4,
        scratch_shapes=[pltpu.SemaphoreType.DMA((ring,))],
        cost_estimate=pl.CostEstimate(flops=10**9, bytes_accessed=8 * go.size, transcendentals=0),
        compiler_params=pltpu.CompilerParams(vmem_limit_bytes=24 << 20))(go, total, gb_all)


def solution(mesh):
    peers = mesh.shape["sp"]

    def block_fn(x_blk, pos_blk, keep_blk, ln_gain, ln_bias, w_qkv, b_qkv, w_out, b_out, dy_blk):
        batch, tok, hidden = x_blk.shape
        heads, dim = w_qkv.shape[1], w_qkv.shape[3]
        assert heads == peers
        seq = tok * peers
        blk = 2 * tok
        w_all = jnp.transpose(w_qkv, (1, 2, 3, 0)).reshape(heads, 3 * dim, hidden)
        b_all = jnp.transpose(b_qkv, (1, 0, 2))
        marks, do_first, x_first, x_rest, do_rest = opening(x_blk, dy_blk, w_out, ln_gain, ln_bias, pos_blk, keep_blk, peers, 1)
        xs = [x_first.reshape(seq, hidden)] + [lax.all_gather(one, "sp", axis=0, tiled=True) for one in x_rest]
        do_t = [do_first]
        lead = 5 * dim // 3
        gw, att = (), []
        for b in range(batch):
            old = list(do_rest[b:b + 1]) if b + 1 < batch else att
            att_d, gw, gb, att_o, swapped = attention(w_all, b_all, do_t[b], marks, xs[b], gw, old, blk=blk, tok=tok, which=b, batch=batch, lead=lead,
                                                      send_o=b + 1 == batch, collective_id=4 + b)
            if b + 1 < batch:
                do_t.append(swapped[0])
            att = [att_o, att_d]
        o_old, d_old = swapped
        gw_all = [lax.all_gather(one, "sp", axis=0, tiled=True).reshape(heads, -1, hidden) for one in gw[:2]]
        y, gx, part, rows = tail_a(att_d, d_old, o_old, att_o, dy_blk, x_blk, w_all.reshape(3 * hidden, hidden), w_out, ln_gain, b_out, 2)
        first, _ = lax.optimization_barrier((gw_all[0], y))
        gw_out, y, gx = settle(first, None, (y, gx), (), 3 * dim, 0)
        part, gw_out, y, gx = lax.optimization_barrier((part, gw_out, y, gx))
        go_all, gb_all, g_gain, g_bias, g_out = lay_down(*tail_b(part, rows, gb, peers, 3))
        second, gw_out, go_all = lax.optimization_barrier((gw_all[1], gw_out, go_all))
        gw_out, = settle(second, gw_out, (), (), 3 * dim, lead)
        gw_out = jnp.transpose(gw_out.reshape(heads, 3, dim, hidden), (3, 0, 1, 2))
        return y, gx, gw_out, jnp.transpose(gb_all, (1, 0, 2)), go_all.reshape(hidden, hidden), g_out, g_gain, g_bias

    act_spec = P("dp", "sp", None)
    tok_spec = P("dp", "sp")
    in_specs = (act_spec, tok_spec, tok_spec, P(), P(), P(), P(), P(), P(), act_spec)
    out_specs = (act_spec, act_spec, P("dp", None, None, None), P("dp", None, None), P("dp", None), P("dp"), P("dp"), P("dp"))
    return jax.shard_map(block_fn, mesh=mesh, in_specs=in_specs, out_specs=out_specs, check_vma=False)
```

```python
import functools
import jax
import jax.numpy as jnp
from jax import lax
from jax.experimental import pallas as pl
from jax.experimental.pallas import tpu as pltpu
from jax.sharding import PartitionSpec as P

NORM_EPS = 1e-5

LOG2E = 1.4426950408889634
MASKED = -1e30
VMEM_LIMIT = 62 << 20
F32, BF16 = jnp.float32, jnp.bfloat16
NT = (((1,), (1,)), ((), ()))


def attn_body(w_hbm, b_ref, dot_ref, marks_ref, x_ref, *refs, blk, tok, which, batch, n_swap, n_old, send_o):
    peers = dot_ref.shape[0]
    gw_old, old, refs = refs[:n_old], refs[n_old:n_old + n_swap], refs[n_old + n_swap:]
    (dqkv_ref, gwa_ref, gwb_ref, gb_ref, gbt_ref, o_out), got, refs = refs[:6], refs[6:6 + n_swap], refs[6 + n_swap:]
    x_buf, refs = refs[0], refs[1:]
    w_ref, b_rep, qkvt_ref, k_tok, v_tok, posk_ref, s_buf, m_buf, q_pad, do_pad, o_acc, dq_acc, dk_acc, dv_acc, x_sem, w_sem = refs[:16]
    swaps = [(old[k], got[k]) + refs[16 + 4 * k:20 + 4 * k] for k in range(n_swap)]
    if send_o:
        o_ref, os_sem, or_sem = refs[-3:]
        o_new = o_out
    else:
        o_ref = o_out
    dim, lead = dot_ref.shape[1], gwa_ref.shape[0]
    seq = dot_ref.shape[0] * tok
    pad = k_tok.shape[1] - dim
    nq = blk // tok
    steps = seq // blk
    scale = dim ** -0.5
    me = lax.axis_index("sp")
    step = pl.program_id(0)
    i = lax.rem(me // nq + step, steps)
    half = blk // 2
    sub = tok // 128

    def spread(row):
        return jnp.transpose(jnp.broadcast_to(row, (128, 128)))

    def x_copy(k):
        rows = pl.ds(pl.multiple_of(k * blk, blk), blk)
        return pltpu.make_async_copy(x_ref.at[rows], x_buf.at[rows], x_sem.at[k])

    def o_send(to):
        return pltpu.make_async_remote_copy(
            src_ref=o_ref.at[to], dst_ref=o_new.at[me], send_sem=os_sem.at[to], recv_sem=or_sem.at[me],
            device_id={"sp": to}, device_id_type=pl.DeviceIdType.MESH)

    def o_keep():
        return pltpu.make_async_copy(o_ref.at[me], o_new.at[me], os_sem.at[me])

    def o_start(at):
        for t in range(nq):
            to = lax.rem(me // nq + at, steps) * nq + t

            @pl.when(to != me)
            def _():
                o_send(to).start()

            @pl.when(to == me)
            def _():
                o_keep().start()

    @pl.when(step == 0)
    def _():
        w_load = pltpu.make_async_copy(w_hbm.at[me], w_ref, w_sem)
        w_load.start()
        for k in range(steps):
            x_copy(k).start()
        meet(peers)
        for one in swaps:
            swap_start(*one, peers, hi=None if send_o else nq)
        dk_acc[...] = jnp.zeros_like(dk_acc)
        dv_acc[...] = jnp.zeros_like(dv_acc)
        q_pad[...] = jnp.zeros_like(q_pad)
        do_pad[...] = jnp.zeros_like(do_pad)
        mine = lax.broadcasted_iota(jnp.int32, (peers, dim), 0) == me
        for k in range(3):
            row = jnp.sum(jnp.where(mine, b_ref[k], 0.0), axis=0, keepdims=True)
            b_rep[k * dim:(k + 1) * dim, :] = spread(jnp.concatenate([row, jnp.zeros((1, pad), F32)], axis=1))[0:dim]
        w_load.wait()

        @pl.loop(0, steps)
        def _(k):
            rows = pl.ds(pl.multiple_of(k * blk, blk), blk)
            x_copy(k).wait()
            shift = jnp.concatenate([b_rep[...]] * (blk // 128), axis=1)
            qkvt_ref[:, rows] = (lax.dot_general(w_ref[...], x_buf[rows, :], NT, preferred_element_type=F32) + shift).astype(BF16)

            @pl.loop(0, blk // 128)
            def _(t):
                cols = pl.ds(pl.multiple_of(k * blk + t * 128, 128), 128)
                for base, dst in ((dim, k_tok), (2 * dim, v_tok)):
                    part = qkvt_ref[base:base + dim, cols].astype(F32)
                    whole = jnp.concatenate([part, jnp.zeros((pad, 128), F32)], axis=0)
                    dst[cols, :] = jnp.transpose(whole).astype(BF16)
                lanes = pl.ds(pl.multiple_of((t % sub) * 128, 128), 128)
                pos = marks_ref[k * nq + t // sub, which:which + 1, lanes].astype(F32)
                keep = marks_ref[k * nq + t // sub, batch + which:batch + which + 1, lanes]
                posk_ref[cols, :] = spread(jnp.where(keep > 0, pos, MASKED))

    if send_o:
        @pl.when(step > 0)
        def _():
            o_start(step - 1)
    else:
        for k in range(1, steps):
            @pl.when(step == k)
            def _():
                for one in swaps:
                    swap_some(*one, peers, k * nq, (k + 1) * nq)

    qcols = pl.ds(pl.multiple_of(i * blk, blk), blk)
    q_pad[0:dim, :] = qkvt_ref[0:dim, qcols]
    for t in range(nq):
        do_pad[0:dim, t * tok:(t + 1) * tok] = dot_ref[i * nq + t]
    slope2 = jnp.exp2(jnp.full((1, 128), -8.0 / peers, F32) * (me + 1).astype(F32)) * LOG2E
    ref_pos = jnp.broadcast_to(marks_ref[i * nq, which:which + 1, 0:128][:, 0:1].astype(F32), (1, 128))
    c = scale * LOG2E

    def scores(j, carry, diag):
        m, l8 = carry
        for sub in range(2):
            rows = pl.ds(pl.multiple_of(j * blk + sub * half, half), half)
            st = jnp.dot(k_tok[rows, :], q_pad[...], preferred_element_type=F32)
            bias = (posk_ref[rows, :] - ref_pos) * slope2
            st = st * c + jnp.concatenate([bias] * (blk // 128), axis=1)
            if diag:
                key = lax.broadcasted_iota(jnp.int32, (half, blk), 0) + sub * half
                qry = lax.broadcasted_iota(jnp.int32, (half, blk), 1)
                st = jnp.where(key <= qry, st, MASKED)
            m_new = jnp.maximum(m, jnp.max(st, axis=0, keepdims=True))
            e = jnp.exp2(st - m_new)
            s_buf[rows, :] = e
            m_buf[2 * j + sub] = jnp.broadcast_to(m_new, (8, blk))
            l8 = l8 * jnp.exp2(m - m_new) + jnp.sum(e.reshape(half // 8, 8, blk), axis=0)
            m = m_new
        return m, l8

    start = (jnp.full((1, blk), MASKED, F32), jnp.zeros((8, blk), F32))
    m, l8 = scores(i, lax.fori_loop(0, i, lambda j, carry: scores(j, carry, False), start), True)
    inv = 1.0 / jnp.sum(l8, axis=0, keepdims=True)
    o_acc[...] = jnp.zeros_like(o_acc)
    dq_acc[...] = jnp.zeros_like(dq_acc)

    def values(j, _):
        rows = pl.ds(pl.multiple_of(j * blk, blk), blk)
        pbs = []
        for sub in range(2):
            part = pl.ds(pl.multiple_of(j * blk + sub * half, half), half)
            p = s_buf[part, :] * (jnp.exp2(m_buf[2 * j + sub][0:1, :] - m) * inv)
            s_buf[part, :] = p
            pbs.append(p.astype(BF16))
        pb = jnp.concatenate(pbs, axis=0)
        o_acc[...] += jnp.dot(qkvt_ref[2 * dim:3 * dim, rows], pb, preferred_element_type=F32)
        dv_acc[:, rows] += lax.dot_general(do_pad[0:dim, :], pb, NT, preferred_element_type=F32)
        return 0

    lax.fori_loop(0, i + 1, values, 0)
    o_lo = o_acc[...].astype(BF16)
    do_f = do_pad[0:dim, :].astype(F32)
    r = jnp.sum(do_f * o_lo.astype(F32), axis=0, keepdims=True)

    def grads(j, _):
        rows = pl.ds(pl.multiple_of(j * blk, blk), blk)
        g = jnp.dot(v_tok[rows, :], do_pad[...], preferred_element_type=F32)
        ds = (s_buf[rows, :] * (g - r)).astype(BF16)
        dq_acc[...] += jnp.dot(qkvt_ref[dim:2 * dim, rows], ds, preferred_element_type=F32)
        dk_acc[:, rows] += lax.dot_general(q_pad[0:dim, :], ds, NT, preferred_element_type=F32)
        return 0

    lax.fori_loop(0, i + 1, grads, 0)
    dq_lo = (dq_acc[...] * scale).astype(BF16)
    for t in range(nq):
        o_ref[i * nq + t] = o_lo[:, t * tok:(t + 1) * tok]
        dqkv_ref[i * nq + t, 0:dim] = dq_lo[:, t * tok:(t + 1) * tok]

    @pl.when(step == steps - 1)
    def _():
        @pl.loop(0, seq // tok)
        def _(t):
            cols = pl.ds(pl.multiple_of(t * tok, tok), tok)
            dqkv_ref[t, dim:2 * dim] = (dk_acc[:, cols] * scale).astype(BF16)
            dqkv_ref[t, 2 * dim:3 * dim] = dv_acc[:, cols].astype(BF16)

        if send_o:
            o_start(step)
        for k, ref in enumerate((gwa_ref, gwb_ref, gb_ref)):
            ref[...] = gw_old[k][...] if n_old else jnp.zeros_like(ref)
        ones = jnp.ones((blk, 128), BF16)

        @pl.loop(0, steps)
        def _(j):
            rows = pl.ds(pl.multiple_of(j * blk, blk), blk)
            for ref, lo, hi in ((gwa_ref, 0, lead), (gwb_ref, lead, 3 * dim)):
                lhs = jnp.concatenate([dqkv_ref[j * nq + t, lo:hi] for t in range(nq)], axis=1)
                ref[...] += jnp.dot(lhs, x_buf[rows, :], preferred_element_type=F32)
                gb_ref[lo:hi, :] += jnp.dot(lhs, ones, preferred_element_type=F32)

        gbt_ref[...] = jnp.zeros_like(gbt_ref)
        for k in range(3):
            part = jnp.concatenate([gb_ref[k * dim:(k + 1) * dim, :], jnp.zeros((pad, 128), F32)], axis=0)
            gbt_ref[k:k + 1, :] = jnp.transpose(part)[0:1, :]

        if send_o:
            o_keep().wait()
            for d in range(1, peers):
                frm = lax.rem(me + d, peers)
                o_send(frm).wait_send()
                pltpu.make_async_remote_copy(
                    src_ref=o_ref.at[frm], dst_ref=o_new.at[frm], send_sem=os_sem.at[frm], recv_sem=or_sem.at[frm],
                    device_id={"sp": frm}, device_id_type=pl.DeviceIdType.MESH).wait_recv()
        for one in swaps:
            swap_wait(*one, peers)


def attention(w_all, b_all, dot_, marks, x, gw, old, *, blk, tok, which, batch, lead, send_o, collective_id):
    blocks, dim, _ = dot_.shape
    seq, hidden = blocks * tok, w_all.shape[2]
    wide = 128 * pl.cdiv(dim, 128)
    hbm = pl.BlockSpec(memory_space=pltpu.HBM)
    full = lambda a: pl.BlockSpec(a.shape, lambda i: (0,) * len(a.shape), pipeline_mode=pl.Buffered(1))
    like = lambda a: jax.ShapeDtypeStruct(a.shape, a.dtype)
    outs = [jax.ShapeDtypeStruct((blocks, 3 * dim, tok), BF16), jax.ShapeDtypeStruct((lead, hidden), F32),
            jax.ShapeDtypeStruct((3 * dim - lead, hidden), F32), jax.ShapeDtypeStruct((3 * dim, 128), F32), jax.ShapeDtypeStruct((8, 128), F32)]
    pairs = (seq // blk) * (seq // blk + 1) // 2
    dma = pltpu.SemaphoreType.DMA
    res = pl.pallas_call(
        functools.partial(attn_body, blk=blk, tok=tok, which=which, batch=batch, n_swap=len(old), n_old=len(gw), send_o=send_o),
        name="attention",
        out_shape=outs + [like(dot_)] + [like(a) for a in old],
        grid=(seq // blk,),
        in_specs=[hbm, full(b_all), full(dot_), full(marks), hbm] + [full(a) for a in gw] + [hbm] * len(old),
        out_specs=[full(a) for a in outs] + [hbm if send_o else full(dot_)] + [hbm] * len(old),
        scratch_shapes=[
            pltpu.VMEM((seq, hidden), BF16),
            pltpu.VMEM(w_all.shape[1:], BF16), pltpu.VMEM((3 * dim, 128), F32), pltpu.VMEM((3 * dim, seq), BF16),
            pltpu.VMEM((seq, wide), BF16), pltpu.VMEM((seq, wide), BF16), pltpu.VMEM((seq, 128), F32),
            pltpu.VMEM((seq, blk), F32), pltpu.VMEM((2 * seq // blk, 8, blk), F32),
            pltpu.VMEM((wide, blk), BF16), pltpu.VMEM((wide, blk), BF16),
            pltpu.VMEM((dim, blk), F32), pltpu.VMEM((dim, blk), F32),
            pltpu.VMEM((dim, seq), F32), pltpu.VMEM((dim, seq), F32), dma((seq // blk,)), dma]
        + sum((swap_scratch(a) for a in old), []) + ([pltpu.VMEM(dot_.shape, BF16), dma((blocks,)), dma((blocks,))] if send_o else []),
        cost_estimate=pl.CostEstimate(flops=pairs * 6 * 2 * blk * blk * 256, bytes_accessed=24 << 20, transcendentals=pairs * blk * blk),
        compiler_params=pltpu.CompilerParams(dimension_semantics=("arbitrary",), vmem_limit_bytes=VMEM_LIMIT,
                                             collective_id=collective_id, has_side_effects=True),
    )(w_all, b_all, dot_, marks, x, *gw, *old)
    return res[0], res[1:4], res[4], res[5], res[6:]


def peer_at(d, peers):
    return {"sp": lax.rem(lax.axis_index("sp") + d, peers)}


def greet(peers):
    barrier = pltpu.get_barrier_semaphore()
    for d in range(1, peers):
        pl.semaphore_signal(barrier, inc=1, device_id=peer_at(d, peers), device_id_type=pl.DeviceIdType.MESH)
    return lambda: pl.semaphore_wait(barrier, peers - 1)


def meet(peers):
    greet(peers)()


def swap_copies(x_ref, out_ref, send_sem, recv_sem, peers, lo=0, hi=None):
    me = lax.axis_index("sp")
    order = [d for near in range(peers // 2) for d in sorted({peers // 2 - near, peers // 2 + near})]
    return [pltpu.make_async_remote_copy(
        src_ref=x_ref.at[lax.rem(me + d, peers)], dst_ref=out_ref.at[me], send_sem=send_sem.at[d - 1], recv_sem=recv_sem.at[d - 1],
        device_id=peer_at(d, peers), device_id_type=pl.DeviceIdType.MESH) for d in order[lo:hi]]


def swap_some(x_ref, out_ref, own, send_sem, recv_sem, own_sem, peers, lo, hi):
    for copy in swap_copies(x_ref, out_ref, send_sem, recv_sem, peers, lo, hi):
        copy.start()


def swap_start(x_ref, out_ref, own, send_sem, recv_sem, own_sem, peers, hi=None):
    me = lax.axis_index("sp")
    swap_some(x_ref, out_ref, own, send_sem, recv_sem, own_sem, peers, 0, hi)
    take = pltpu.make_async_copy(x_ref.at[me], own, own_sem)
    take.start()
    take.wait()
    pltpu.make_async_copy(own, out_ref.at[me], own_sem).start()


def swap_wait(x_ref, out_ref, own, send_sem, recv_sem, own_sem, peers):
    pltpu.make_async_copy(own, out_ref.at[lax.axis_index("sp")], own_sem).wait()
    for copy in swap_copies(x_ref, out_ref, send_sem, recv_sem, peers):
        copy.wait()


def swap_scratch(x):
    peers = x.shape[0]
    return [pltpu.VMEM(x.shape[1:], x.dtype), pltpu.SemaphoreType.DMA((peers - 1,)), pltpu.SemaphoreType.DMA((peers - 1,)),
            pltpu.SemaphoreType.DMA]


STEP = (1, -1)


def hops(ring, s, w):
    return ring // 2 - (s != w)


def ring_gather(block, own, sems, peers, cuts):
    ring = peers // 2
    me = lax.axis_index("sp")
    z, c = me // 2, me % 2
    send_sem, recv_sem, over_sem, came_sem = sems
    turn = lambda k: lax.rem(z + k + 2 * ring, ring)
    lots = [(s, w, u) for u in range(cuts) for w in range(2) for s in range(2)]

    def copy(src, dst, one, two, to):
        return pltpu.make_async_remote_copy(src_ref=src, dst_ref=dst, send_sem=one, recv_sem=two, device_id={"sp": to},
                                            device_id_type=pl.DeviceIdType.MESH)

    def along(s, w, t, u):
        ref = block(turn(-STEP[s] * t), c, w, u)
        return copy(own(w, u) if t == 0 else ref, ref, send_sem.at[s, w, t, u], recv_sem.at[s, w, t, u], 2 * turn(STEP[s]) + c)

    def across(s, w, t, u, side):
        ref = block(turn(-STEP[s] * t), side, w, u)
        return copy(own(w, u) if t == 0 and side is c else ref, ref, over_sem.at[s, w, t, u], came_sem.at[s, w, t, u], 2 * z + 1 - c)

    home = [(0, w, 0, u) for u in range(cuts) for w in range(2)]
    moved = [(s, w, t, u) for t in range(1, ring // 2 + 1) for s, w, u in lots if t <= hops(ring, s, w)]

    def start(only=None):
        for s, w, u in lots:
            if only in (None, (w, u)):
                along(s, w, 0, u).start()
        for lot in home:
            if only in (None, (lot[1], lot[3])):
                across(*lot, c).start()

    def run(lo=1, hi=ring):
        for s, w, t, u in moved:
            if lo <= t < hi:
                along(s, w, t - 1, u).wait_recv()
                if t < hops(ring, s, w):
                    along(s, w, t, u).start()
                across(s, w, t, u, c).start()

    def finish():
        for s, w, t, u in moved:
            along(s, w, t - 1, u).wait_send()
        for lot in home + moved:
            across(*lot, c).wait_send()
            across(*lot, 1 - c).wait_recv()

    return start, run, finish


def ring_scratch(peers, cuts):
    dma = pltpu.SemaphoreType.DMA
    return [dma((2, 2, peers // 4, cuts))] * 2 + [dma((2, 2, peers // 4 + 1, cuts))] * 2


def opening_body(x_hbm, dy_hbm, wo_hbm, gain_ref, bias_ref, pos_ref, keep_ref, marks_all, do_t, x_all, *refs, peers, batch, cuts):
    x_out, do_out = refs[:batch - 1], refs[batch - 1:2 * batch - 2]
    x_ref, dy_ref, x_own, do_own, wo_ref, marks_ref, own, ds_sem, dr_sem, do_sem, ms_sem, mr_sem, in_sem = refs[2 * batch - 2:2 * batch + 11]
    ring_sems = refs[2 * batch + 11:]
    gain, bias = gain_ref[...].reshape(1, -1), bias_ref[...].reshape(1, -1)
    me = lax.axis_index("sp")
    tok, dim = x_own.shape[0], do_own.shape[1]
    lot = tok // 2 // cuts
    rows_of = lambda w, u: pl.ds((w * cuts + u) * lot, lot)
    arrived = greet(peers)
    loads = [pltpu.make_async_copy(x_hbm.at[b], x_ref.at[b], in_sem.at[b]) for b in range(batch)]
    loads += [pltpu.make_async_copy(dy_hbm, dy_ref, in_sem.at[batch]), pltpu.make_async_copy(wo_hbm, wo_ref, in_sem.at[batch + 1])]
    for load in loads:
        load.start()

    def norm_rows(b, out_ref, rows):
        x = x_ref[b, rows, :].astype(F32)
        cen = x - jnp.mean(x, axis=-1, keepdims=True)
        hat = cen * lax.rsqrt(jnp.mean(cen * cen, axis=-1, keepdims=True) + NORM_EPS)
        out_ref[rows, :] = (hat * gain + bias).astype(BF16)

    def norm(b, out_ref):
        loads[b].wait()

        @pl.loop(0, tok // 32)
        def _(k):
            norm_rows(b, out_ref, pl.ds(pl.multiple_of(k * 32, 32), 32))

    def product(b, out_ref):
        @pl.loop(0, peers // 4)
        def _(g):
            rows = pl.ds(pl.multiple_of(g * 4 * dim, 4 * dim), 4 * dim)
            out_ref[pl.ds(g * 4, 4)] = lax.dot_general(wo_ref[rows, :], dy_ref[b], NT, preferred_element_type=F32).astype(BF16).reshape(4, dim, tok)

    marks_ref[...] = jnp.zeros_like(marks_ref)
    marks_ref[0:batch, :] = pos_ref[...]
    marks_ref[batch:2 * batch, :] = keep_ref[...]
    block = lambda k, side, w, u: x_all.at[2 * k + side, rows_of(w, u)]
    start, run, finish = ring_gather(block, lambda w, u: x_own.at[rows_of(w, u)], ring_sems, peers, cuts)
    loads[0].wait()
    pieces = [(w, u) for u in range(cuts) for w in range(2)]
    for k, piece in enumerate(pieces):
        norm_rows(0, x_own, rows_of(*piece))
        if k == 1:
            arrived()
        if k:
            start(pieces[k - 1])
    start(pieces[-1])
    keep = pltpu.make_async_copy(x_own, x_all.at[me], in_sem.at[batch + 2])
    keep.start()
    marks = [pltpu.make_async_remote_copy(
        src_ref=marks_ref, dst_ref=marks_all.at[me], send_sem=ms_sem.at[d - 1], recv_sem=mr_sem.at[d - 1],
        device_id=peer_at(d, peers), device_id_type=pl.DeviceIdType.MESH) for d in range(1, peers)]
    for copy in marks:
        copy.start()
    marks_all[me] = marks_ref[...]
    loads[-2].wait()
    loads[-1].wait()
    product(0, do_own)
    swap = (do_own, do_t, own, ds_sem, dr_sem, do_sem, peers)
    third = (peers + 1) // 3
    swap_start(*swap, hi=third)
    for b in range(1, batch):
        norm(b, x_out[b - 1])
        product(b, do_out[b - 1])
    run(1, 2)
    swap_some(*swap, third, 2 * third)
    run(2, 3)
    swap_some(*swap, 2 * third, peers)
    run(3)
    keep.wait()
    for copy in marks:
        copy.wait()
    swap_wait(do_own, do_t, own, ds_sem, dr_sem, do_sem, peers)
    finish()


def opening(x, dy, w_out, gain, bias, pos, keep, peers, collective_id, cuts=4):
    batch, tok, hidden = x.shape
    dim = hidden // peers
    hbm, vmem = pl.BlockSpec(memory_space=pltpu.HBM), pl.BlockSpec(memory_space=pltpu.VMEM)
    dma = pltpu.SemaphoreType.DMA
    do_shape, x_shape = jax.ShapeDtypeStruct((peers, dim, tok), BF16), jax.ShapeDtypeStruct((tok, hidden), BF16)
    res = pl.pallas_call(
        functools.partial(opening_body, peers=peers, batch=batch, cuts=cuts),
        name="opening",
        out_shape=[jax.ShapeDtypeStruct((peers, 8, tok), pos.dtype), do_shape, jax.ShapeDtypeStruct((peers, tok, hidden), BF16)]
        + [x_shape] * (batch - 1) + [do_shape] * (batch - 1),
        in_specs=[hbm, hbm, hbm, vmem, vmem, vmem, vmem],
        out_specs=[vmem, hbm, hbm] + [vmem] * (2 * batch - 2),
        scratch_shapes=[pltpu.VMEM(x.shape, BF16), pltpu.VMEM(dy.shape, BF16), pltpu.VMEM(x_shape.shape, BF16), pltpu.VMEM(do_shape.shape, BF16),
                        pltpu.VMEM(w_out.shape, BF16), pltpu.VMEM((8, tok), pos.dtype)] + swap_scratch(do_shape)
        + [dma((peers - 1,)), dma((peers - 1,)), dma((batch + 3,))] + ring_scratch(peers, cuts),
        cost_estimate=pl.CostEstimate(flops=5 * 10**10, bytes_accessed=16 << 20, transcendentals=0),
        compiler_params=pltpu.CompilerParams(collective_id=collective_id, has_side_effects=True, vmem_limit_bytes=VMEM_LIMIT),
    )(x, dy, w_out, gain, bias, pos, keep)
    return res[0], res[1], res[2], res[3:2 + batch], res[2 + batch:]


TN = (((0,), (0,)), ((), ()))


def tail_a_body(dqkv_ref, oo_hbm, on_hbm, dy_hbm, x_hbm, wo_hbm, d_hbm, w_hbm, gain_ref, bo_ref, y_ref, gx_ref, part, rows_ref,
                o_old, o_new, dy_ref, x_ref, wo_ref, d_old, w_ref, d_new, dn, sums, bo_rep, both, mine, landed, own_d,
                ds_sem, dr_sem, do_sem, ps_sem, pr_sem, rs_sem, rr_sem, w_sem, *, peers, cuts):
    ring = peers // 2
    me = lax.axis_index("sp")
    z, c = me // 2, me % 2
    _, tok, hidden = x_ref.shape
    half, wide, few = hidden // 2, hidden // 3, part.shape[0] // cuts
    cols = (pl.ds(0, half), pl.ds(half, half))
    at = lambda zz, cc: {"sp": 2 * zz + cc}
    turn = lambda k: lax.rem(z + k + 2 * ring, ring)
    remote = functools.partial(pltpu.make_async_remote_copy, device_id_type=pl.DeviceIdType.MESH)
    span, group = d_old.shape[1], 8
    gain, b_out = gain_ref[...].reshape(1, hidden), bo_ref[...].reshape(1, hidden)
    pairs = ((oo_hbm, o_old), (on_hbm, o_new), (dy_hbm, dy_ref), (x_hbm, x_ref), (wo_hbm, wo_ref), (d_hbm, d_old), (w_hbm, w_ref))
    loads = [pltpu.make_async_copy(src, dst, w_sem.at[k]) for k, (src, dst) in enumerate(pairs)]
    swap = (dqkv_ref, d_new, own_d, ds_sem, dr_sem, do_sem, peers)
    arrived = greet(peers)
    for load in loads:
        load.start()
    arrived()
    third = (peers + 1) // 3
    swap_start(*swap, hi=third)
    for load in loads[:3]:
        load.wait()

    def product(put, side):
        @pl.loop(0, ring)
        def _(k):
            h = 2 * k + side
            put(k, jnp.dot(o_old[h], dy_ref[0], preferred_element_type=F32)
                + jnp.dot(o_new[h], dy_ref[1], preferred_element_type=F32))

    def put_other(k, value):
        both[k, 1 - c] = value

    def put_mine(k, value):
        mine[k] = value

    def forward(b, o_ref):
        o_t = o_ref[...].reshape(hidden, tok)

        @pl.loop(0, 3)
        def _(n):
            at_n = pl.ds(pl.multiple_of(n * wide, wide), wide)
            acc = lax.dot_general(o_t, wo_ref[:, at_n], TN, preferred_element_type=F32)
            y_ref[b, :, at_n] = (x_ref[b, :, at_n].astype(F32) + acc + bo_rep[0:1, at_n]).astype(BF16)

    def backward(b, d_ref):
        @pl.loop(0, 3)
        def _(n):
            at_n = pl.ds(pl.multiple_of(n * wide, wide), wide)
            acc = None
            for k in range(0, peers, group):
                lhs = d_ref[k:k + group].reshape(-1, tok)
                one = lax.dot_general(lhs, w_ref[k * span:(k + group) * span, at_n], TN, preferred_element_type=F32)
                acc = one if acc is None else acc + one
            dn[:, at_n] = acc

        @pl.loop(0, tok // 32)
        def _(k):
            rows = pl.ds(pl.multiple_of(k * 32, 32), 32)
            x = x_ref[b, rows, :].astype(F32)
            dy = dy_ref[b, rows, :].astype(F32)
            d = dn[rows, :]
            cen = x - jnp.mean(x, axis=-1, keepdims=True)
            inv = lax.rsqrt(jnp.mean(cen * cen, axis=-1, keepdims=True) + NORM_EPS)
            hat = cen * inv
            for n, one in enumerate((d * hat, d, dy)):
                sums[n] += jnp.sum(one.reshape(4, 8, hidden), axis=0)
            e = d * gain
            m1 = jnp.mean(e, axis=-1, keepdims=True)
            m2 = jnp.mean(e * hat, axis=-1, keepdims=True)
            gx_ref[b, rows, :] = (dy + inv * (e - m1 - hat * m2)).astype(BF16)

    bo_rep[...] = jnp.broadcast_to(b_out, bo_rep.shape)
    sums[...] = jnp.zeros_like(sums)
    product(put_other, 1 - c)
    pair_copy = lambda side: remote(src_ref=both.at[:, side], dst_ref=both.at[:, side], send_sem=ps_sem, recv_sem=pr_sem, device_id=at(z, 1 - c))
    product(put_mine, c)
    pair_copy(1 - c).start()
    pair_copy(1 - c).wait_send()
    pair_copy(c).wait_recv()

    @pl.loop(0, ring)
    def _(k):
        mine[k] = mine[k] + both[k, c]

    lots = [(s, w, u) for u in range(cuts) for w in range(2) for s in range(2)]

    def reduce_copy(s, w, t, u):
        return remote(src_ref=mine.at[turn(STEP[s] * (hops(ring, s, w) - t)), pl.ds(u * few, few), cols[w]], dst_ref=landed.at[s, w, t, u],
                      send_sem=rs_sem.at[s, w, t, u], recv_sem=rr_sem.at[s, w, t, u], device_id=at(turn(STEP[s]), c))

    def fold(s, w, t, u):
        reduce_copy(s, w, t, u).wait_recv()
        at_k = (turn(STEP[s] * (hops(ring, s, w) - t - 1)), pl.ds(u * few, few), cols[w])
        mine[at_k] = mine[at_k] + landed[s, w, t, u]

    def hop(t):
        for s, w, u in lots:
            if t < hops(ring, s, w):
                fold(s, w, t - 1, u)
                reduce_copy(s, w, t, u).start()

    for s, w, u in lots:
        reduce_copy(s, w, 0, u).start()
    swap_some(*swap, third, 2 * third)
    for load in loads[3:5]:
        load.wait()
    forward(0, o_old)
    forward(1, o_new)
    hop(1)
    swap_some(*swap, 2 * third, peers)
    for load in loads[5:]:
        load.wait()
    backward(0, d_old)
    for t in range(2, ring // 2 - 1):
        hop(t)
    swap_wait(*swap)
    backward(1, d_new)
    hop(ring // 2 - 1)
    rows_ref[...] = jnp.zeros_like(rows_ref)
    for n in range(3):
        rows_ref[n:n + 1, :] = jnp.sum(sums[n], axis=0, keepdims=True)
    for s, w, u in lots:
        fold(s, w, hops(ring, s, w) - 1, u)
    part[...] = mine[z]
    for s, w, u in lots:
        for t in range(hops(ring, s, w)):
            reduce_copy(s, w, t, u).wait_send()


def tail_a(dqkv, d_old, o_old, o_new, dy, x, w_flat, w_out, gain, b_out, collective_id, cuts=2):
    peers, dim, tok = o_old.shape
    ring = peers // 2
    hidden = dy.shape[-1]
    hbm, vmem = pl.BlockSpec(memory_space=pltpu.HBM), pl.BlockSpec(memory_space=pltpu.VMEM)
    dma = pltpu.SemaphoreType.DMA
    held = lambda a: pltpu.VMEM(a.shape, a.dtype)
    steps = (2, 2, ring // 2, cuts)
    return pl.pallas_call(
        functools.partial(tail_a_body, peers=peers, cuts=cuts),
        name="tail_a",
        out_shape=[jax.ShapeDtypeStruct(x.shape, BF16), jax.ShapeDtypeStruct(x.shape, BF16), jax.ShapeDtypeStruct((dim, hidden), F32),
                   jax.ShapeDtypeStruct((8, hidden), F32)],
        in_specs=[hbm] * 8 + [vmem] * 2,
        out_specs=[vmem] * 4,
        scratch_shapes=[held(a) for a in (o_old, o_new, dy, x, w_out, d_old, w_flat, dqkv)]
        + [pltpu.VMEM((tok, hidden), F32), pltpu.VMEM((3, 8, hidden), F32), pltpu.VMEM((8, hidden), F32),
           pltpu.VMEM((ring, 2, dim, hidden), F32), pltpu.VMEM((ring, dim, hidden), F32), pltpu.VMEM(steps + (dim // cuts, hidden // 2), F32),
           pltpu.VMEM(dqkv.shape[1:], BF16), dma((peers - 1,)), dma((peers - 1,)), dma, dma, dma, dma(steps), dma(steps), dma((7,))],
        cost_estimate=pl.CostEstimate(flops=10**11, bytes_accessed=64 << 20, transcendentals=0),
        compiler_params=pltpu.CompilerParams(collective_id=collective_id, has_side_effects=True, vmem_limit_bytes=VMEM_LIMIT),
    )(dqkv, o_old, o_new, dy, x, w_out, d_old, w_flat, gain, b_out)


def tail_b_body(part, rows_ref, gb_ref, full, total, gb_all, stage, xs_sem, xr_sem, *ring_sems, peers, cuts):
    ring = peers // 2
    me = lax.axis_index("sp")
    z, c = me // 2, me % 2
    hidden = part.shape[1]
    half, few = hidden // 2, part.shape[0] // cuts
    cols = (pl.ds(0, half), pl.ds(half, half))
    remote = functools.partial(pltpu.make_async_remote_copy, device_id_type=pl.DeviceIdType.MESH)
    arrived = greet(peers)
    full[z, c] = part[...]
    gb_all[me] = gb_ref[...]
    block = lambda k, side, w, u: full.at[k, side, pl.ds(u * few, few), cols[w]]
    start, run, finish = ring_gather(block, lambda w, u: block(z, c, w, u), ring_sems, peers, cuts)
    owners = hidden // 128
    lanes = lambda k: pl.ds(pl.multiple_of(k * 128, 128), 128)

    def small_copy(kind, frm, to):
        src, dst = ((rows_ref.at[:, lanes(to)], stage.at[frm]), (total.at[:, lanes(frm)],) * 2, (gb_ref, gb_all.at[frm]))[kind]
        return remote(src_ref=src, dst_ref=dst, send_sem=xs_sem.at[kind, to], recv_sem=xr_sem.at[kind, frm], device_id={"sp": to})

    def each(act, kind, only_to=False, only_from=False):
        @pl.loop(1, peers)
        def _(d):
            far = lax.rem(me + d, peers)

            def go():
                act(kind, far)

            if only_to:
                pl.when(far < owners)(go)
            elif only_from:
                pl.when(me < owners)(go)
            else:
                go()

    send = lambda kind, far: small_copy(kind, me, far).start()
    over = lambda kind, far: small_copy(kind, me, far).wait_send()
    came = lambda kind, far: small_copy(kind, far, me).wait_recv()

    @pl.when(me < owners)
    def _():
        stage[me] = rows_ref[:, lanes(me)]

    arrived()
    start()
    each(send, 0, only_to=True)
    each(send, 2)
    run(1, 2)
    each(came, 0, only_from=True)

    @pl.when(me < owners)
    def _():
        total[:, lanes(me)] = jnp.sum(stage[...], axis=0)

    each(send, 1, only_from=True)
    run(2)
    each(came, 1, only_to=True)
    each(came, 2)
    each(over, 0, only_to=True)
    each(over, 1, only_from=True)
    each(over, 2)
    finish()


def tail_b(part, rows, gb, peers, collective_id, cuts=2):
    ring = peers // 2
    vmem = pl.BlockSpec(memory_space=pltpu.VMEM)
    dma = pltpu.SemaphoreType.DMA
    return pl.pallas_call(
        functools.partial(tail_b_body, peers=peers, cuts=cuts),
        name="tail_b",
        out_shape=[jax.ShapeDtypeStruct((ring, 2) + part.shape, F32), jax.ShapeDtypeStruct(rows.shape, F32),
                   jax.ShapeDtypeStruct((peers,) + gb.shape, F32)],
        in_specs=[vmem] * 3,
        out_specs=[vmem] * 3,
        scratch_shapes=[pltpu.VMEM((peers, 8, 128), F32), dma((3, peers)), dma((3, peers))] + ring_scratch(peers, cuts),
        cost_estimate=pl.CostEstimate(flops=5 * 10**10, bytes_accessed=10 << 20, transcendentals=0),
        compiler_params=pltpu.CompilerParams(collective_id=collective_id, has_side_effects=True, vmem_limit_bytes=32 << 20),
    )(part, rows, gb)


def settle_body(*refs, n_in, first, n_plain, n_held):
    x_ref, plain, held = refs[0], refs[1:1 + n_plain], refs[1 + n_plain:1 + n_plain + n_held]
    outs = refs[n_in:n_in + 1 + n_plain + n_held]
    buf, in_sem, out_sem, in_plain, out_plain, *rooms = refs[n_in + 1 + n_plain + n_held:]
    heads, n = x_ref.shape[:2]
    copy = pltpu.make_async_copy
    reads = [copy(x_ref.at[h], buf.at[h], in_sem.at[h]) for h in range(heads)]
    writes = [copy(buf.at[h], outs[0].at[h, pl.ds(first, n)], out_sem.at[h]) for h in range(heads)]
    reads += [copy(plain[k], rooms[k], in_plain.at[k]) for k in range(n_plain)]
    writes += [copy(rooms[k], outs[1 + k], out_plain.at[k]) for k in range(n_plain)]
    flat = [copy(held[k], outs[1 + n_plain + k], out_plain.at[n_plain + k]) for k in range(n_held)]
    for one in reads + flat:
        one.start()
    for read, write in zip(reads, writes):
        read.wait()
        write.start()
    for one in writes + flat:
        one.wait()


def settle(x, into, plain, held, span, first):
    heads, n, hidden = x.shape
    hbm, vmem = pl.BlockSpec(memory_space=pltpu.HBM), pl.BlockSpec(memory_space=pltpu.VMEM)
    pin = lambda a: pltpu.with_memory_space_constraint(a, pltpu.HBM)
    args = (pin(x), *[pin(a) for a in plain], *held) + (() if into is None else (into,))
    dma = pltpu.SemaphoreType.DMA
    extra = max(len(plain) + len(held), 1)
    return pl.pallas_call(
        functools.partial(settle_body, n_in=len(args), first=first, n_plain=len(plain), n_held=len(held)), name="settle",
        out_shape=[jax.ShapeDtypeStruct((heads, span, hidden), x.dtype)] + [jax.ShapeDtypeStruct(a.shape, a.dtype) for a in (*plain, *held)],
        in_specs=[hbm] * (1 + len(plain)) + [vmem] * len(held) + [hbm] * (into is not None),
        out_specs=[hbm] * (1 + len(plain) + len(held)),
        input_output_aliases={} if into is None else {len(args) - 1: 0},
        scratch_shapes=[pltpu.VMEM(x.shape, x.dtype), dma((heads,)), dma((heads,)), dma((extra,)), dma((extra,))]
        + [pltpu.VMEM(a.shape, a.dtype) for a in plain],
        cost_estimate=pl.CostEstimate(flops=10**9, bytes_accessed=8 * x.size, transcendentals=0),
        compiler_params=pltpu.CompilerParams(vmem_limit_bytes=24 << 20))(*args)


def lay_body(go_ref, total, gb_all, go_out, gb_out, *refs):
    vectors, sem = refs[:-1], refs[-1]
    copies = [pltpu.make_async_copy(go_ref.at[k], go_out.at[k], sem.at[k]) for k in range(go_ref.shape[0])]
    for copy in copies:
        copy.start()
    for k in range(3):
        gb_out[k] = gb_all[:, k, 0:gb_out.shape[2]]
        vectors[k][...] = total[k]
    for copy in copies:
        copy.wait()


def lay_down(go, total, gb_all):
    hbm, vmem = pl.BlockSpec(memory_space=pltpu.HBM), pl.BlockSpec(memory_space=pltpu.VMEM)
    ring, _, dim, hidden = go.shape
    return pl.pallas_call(
        lay_body, name="lay_down",
        out_shape=[jax.ShapeDtypeStruct(go.shape, F32), jax.ShapeDtypeStruct((3, 2 * ring, dim), F32)] + [jax.ShapeDtypeStruct((hidden,), F32)] * 3,
        in_specs=[vmem] * 3, out_specs=[hbm] + [vmem] * 4,
        scratch_shapes=[pltpu.SemaphoreType.DMA((ring,))],
        cost_estimate=pl.CostEstimate(flops=10**9, bytes_accessed=8 * go.size, transcendentals=0),
        compiler_params=pltpu.CompilerParams(vmem_limit_bytes=24 << 20))(go, total, gb_all)


def solution(mesh):
    peers = mesh.shape["sp"]

    def block_fn(x_blk, pos_blk, keep_blk, ln_gain, ln_bias, w_qkv, b_qkv, w_out, b_out, dy_blk):
        batch, tok, hidden = x_blk.shape
        heads, dim = w_qkv.shape[1], w_qkv.shape[3]
        assert heads == peers
        seq = tok * peers
        blk = 2 * tok
        w_all = jnp.transpose(w_qkv, (1, 2, 3, 0)).reshape(heads, 3 * dim, hidden)
        b_all = jnp.transpose(b_qkv, (1, 0, 2))
        marks, do_first, x_first, x_rest, do_rest = opening(x_blk, dy_blk, w_out, ln_gain, ln_bias, pos_blk, keep_blk, peers, 1)
        xs = [x_first.reshape(seq, hidden)] + [lax.all_gather(one, "sp", axis=0, tiled=True) for one in x_rest]
        do_t = [do_first]
        lead = 5 * dim // 3
        gw, att = (), []
        for b in range(batch):
            old = list(do_rest[b:b + 1]) if b + 1 < batch else att
            att_d, gw, gb, att_o, swapped = attention(w_all, b_all, do_t[b], marks, xs[b], gw, old, blk=blk, tok=tok, which=b, batch=batch, lead=lead,
                                                      send_o=b + 1 == batch, collective_id=4 + b)
            if b + 1 < batch:
                do_t.append(swapped[0])
            att = [att_o, att_d]
        o_old, d_old = swapped
        gw_all = [lax.all_gather(one, "sp", axis=0, tiled=True).reshape(heads, -1, hidden) for one in gw[:2]]
        y, gx, part, rows = tail_a(att_d, d_old, o_old, att_o, dy_blk, x_blk, w_all.reshape(3 * hidden, hidden), w_out, ln_gain, b_out, 2)
        first, _ = lax.optimization_barrier((gw_all[0], y))
        gw_out, y, gx = settle(first, None, (y, gx), (), 3 * dim, 0)
        part, gw_out, y, gx = lax.optimization_barrier((part, gw_out, y, gx))
        go_all, gb_all, g_gain, g_bias, g_out = lay_down(*tail_b(part, rows, gb, peers, 3))
        second, gw_out, go_all = lax.optimization_barrier((gw_all[1], gw_out, go_all))
        gw_out, = settle(second, gw_out, (), (), 3 * dim, lead)
        gw_out = jnp.transpose(gw_out.reshape(heads, 3, dim, hidden), (3, 0, 1, 2))
        return y, gx, gw_out, jnp.transpose(gb_all, (1, 0, 2)), go_all.reshape(hidden, hidden), g_out, g_gain, g_bias

    act_spec = P("dp", "sp", None)
    tok_spec = P("dp", "sp")
    in_specs = (act_spec, tok_spec, tok_spec, P(), P(), P(), P(), P(), P(), act_spec)
    out_specs = (act_spec, act_spec, P("dp", None, None, None), P("dp", None, None), P("dp", None), P("dp"), P("dp"), P("dp"))
    return jax.shard_map(block_fn, mesh=mesh, in_specs=in_specs, out_specs=out_specs, check_vma=False)
```

```python
import functools
import jax
import jax.numpy as jnp
from jax import lax
from jax.experimental import pallas as pl
from jax.experimental.pallas import tpu as pltpu
from jax.sharding import PartitionSpec as P

NORM_EPS = 1e-5

LOG2E = 1.4426950408889634
MASKED = -1e30
VMEM_LIMIT = 62 << 20
F32, BF16 = jnp.float32, jnp.bfloat16
NT = (((1,), (1,)), ((), ()))


def attn_body(w_hbm, b_ref, dot_ref, marks_ref, x_ref, *refs, blk, tok, which, batch, n_swap, n_old, send_o):
    peers = dot_ref.shape[0]
    gw_old, old, refs = refs[:n_old], refs[n_old:n_old + n_swap], refs[n_old + n_swap:]
    (dqkv_ref, gwa_ref, gwb_ref, gb_ref, gbt_ref, o_out), got, refs = refs[:6], refs[6:6 + n_swap], refs[6 + n_swap:]
    x_buf, refs = refs[0], refs[1:]
    w_ref, b_rep, qkvt_ref, k_tok, v_tok, posk_ref, s_buf, m_buf, q_pad, do_pad, o_acc, dq_acc, dk_acc, dv_acc, x_sem, w_sem = refs[:16]
    swaps = [(old[k], got[k]) + refs[16 + 4 * k:20 + 4 * k] for k in range(n_swap)]
    if send_o:
        o_ref, os_sem, or_sem = refs[-3:]
        o_new = o_out
    else:
        o_ref = o_out
    dim, lead = dot_ref.shape[1], gwa_ref.shape[0]
    seq = dot_ref.shape[0] * tok
    pad = k_tok.shape[1] - dim
    nq = blk // tok
    steps = seq // blk
    scale = dim ** -0.5
    me = lax.axis_index("sp")
    step = pl.program_id(0)
    i = lax.rem(me // nq + step, steps)
    half = blk // 2
    sub = tok // 128

    def spread(row):
        return jnp.transpose(jnp.broadcast_to(row, (128, 128)))

    def x_copy(k):
        rows = pl.ds(pl.multiple_of(k * blk, blk), blk)
        return pltpu.make_async_copy(x_ref.at[rows], x_buf.at[rows], x_sem.at[k])

    def o_send(to):
        return pltpu.make_async_remote_copy(
            src_ref=o_ref.at[to], dst_ref=o_new.at[me], send_sem=os_sem.at[to], recv_sem=or_sem.at[me],
            device_id={"sp": to}, device_id_type=pl.DeviceIdType.MESH)

    def o_keep():
        return pltpu.make_async_copy(o_ref.at[me], o_new.at[me], os_sem.at[me])

    def o_start(at):
        for t in range(nq):
            to = lax.rem(me // nq + at, steps) * nq + t

            @pl.when(to != me)
            def _():
                o_send(to).start()

            @pl.when(to == me)
            def _():
                o_keep().start()

    @pl.when(step == 0)
    def _():
        w_load = pltpu.make_async_copy(w_hbm.at[me], w_ref, w_sem)
        w_load.start()
        for k in range(steps):
            x_copy(k).start()
        meet(peers)
        for one in swaps:
            swap_start(*one, peers)
        dk_acc[...] = jnp.zeros_like(dk_acc)
        dv_acc[...] = jnp.zeros_like(dv_acc)
        q_pad[...] = jnp.zeros_like(q_pad)
        do_pad[...] = jnp.zeros_like(do_pad)
        mine = lax.broadcasted_iota(jnp.int32, (peers, dim), 0) == me
        for k in range(3):
            row = jnp.sum(jnp.where(mine, b_ref[k], 0.0), axis=0, keepdims=True)
            b_rep[k * dim:(k + 1) * dim, :] = spread(jnp.concatenate([row, jnp.zeros((1, pad), F32)], axis=1))[0:dim]
        w_load.wait()

        @pl.loop(0, steps)
        def _(k):
            rows = pl.ds(pl.multiple_of(k * blk, blk), blk)
            x_copy(k).wait()
            shift = jnp.concatenate([b_rep[...]] * (blk // 128), axis=1)
            qkvt_ref[:, rows] = (lax.dot_general(w_ref[...], x_buf[rows, :], NT, preferred_element_type=F32) + shift).astype(BF16)

            for t in range(blk // 128):
                cols = pl.ds(pl.multiple_of(k * blk + t * 128, 128), 128)
                for base, dst in ((dim, k_tok), (2 * dim, v_tok)):
                    part = qkvt_ref[base:base + dim, cols].astype(F32)
                    whole = jnp.concatenate([part, jnp.zeros((pad, 128), F32)], axis=0)
                    dst[cols, :] = jnp.transpose(whole).astype(BF16)
                mark = marks_ref[k * nq + t // sub, which * sub + t % sub:which * sub + t % sub + 1, :]
                pos, keep = lax.shift_right_logical(mark, 1).astype(F32), mark & 1
                posk_ref[cols, :] = spread(jnp.where(keep > 0, pos, MASKED))

    if send_o:
        @pl.when(step > 0)
        def _():
            o_start(step - 1)

    qcols = pl.ds(pl.multiple_of(i * blk, blk), blk)
    q_pad[0:dim, :] = qkvt_ref[0:dim, qcols]
    for t in range(nq):
        do_pad[0:dim, t * tok:(t + 1) * tok] = dot_ref[i * nq + t]
    slope2 = jnp.exp2(jnp.full((1, 128), -8.0 / peers, F32) * (me + 1).astype(F32)) * LOG2E
    first = lax.shift_right_logical(marks_ref[i * nq, which * sub:which * sub + 1, :], 1).astype(F32)
    ref_pos = jnp.broadcast_to(first[:, 0:1], (1, 128))
    c = scale * LOG2E

    def scores(j, carry, diag):
        m, l8 = carry
        for sub in range(2):
            rows = pl.ds(pl.multiple_of(j * blk + sub * half, half), half)
            st = jnp.dot(k_tok[rows, :], q_pad[...], preferred_element_type=F32)
            bias = (posk_ref[rows, :] - ref_pos) * slope2
            st = st * c + jnp.concatenate([bias] * (blk // 128), axis=1)
            if diag:
                key = lax.broadcasted_iota(jnp.int32, (half, blk), 0) + sub * half
                qry = lax.broadcasted_iota(jnp.int32, (half, blk), 1)
                st = jnp.where(key <= qry, st, MASKED)
            m_new = jnp.maximum(m, jnp.max(st, axis=0, keepdims=True))
            e = jnp.exp2(st - m_new)
            s_buf[rows, :] = e
            m_buf[2 * j + sub] = jnp.broadcast_to(m_new, (8, blk))
            l8 = l8 * jnp.exp2(m - m_new) + jnp.sum(e.reshape(half // 8, 8, blk), axis=0)
            m = m_new
        return m, l8

    start = (jnp.full((1, blk), MASKED, F32), jnp.zeros((8, blk), F32))
    m, l8 = scores(i, lax.fori_loop(0, i, lambda j, carry: scores(j, carry, False), start), True)
    inv = 1.0 / jnp.sum(l8, axis=0, keepdims=True)
    o_acc[...] = jnp.zeros_like(o_acc)
    dq_acc[...] = jnp.zeros_like(dq_acc)

    def values(j, _):
        rows = pl.ds(pl.multiple_of(j * blk, blk), blk)
        pbs = []
        for sub in range(2):
            part = pl.ds(pl.multiple_of(j * blk + sub * half, half), half)
            p = s_buf[part, :] * (jnp.exp2(m_buf[2 * j + sub][0:1, :] - m) * inv)
            s_buf[part, :] = p
            pbs.append(p.astype(BF16))
        pb = jnp.concatenate(pbs, axis=0)
        o_acc[...] += jnp.dot(qkvt_ref[2 * dim:3 * dim, rows], pb, preferred_element_type=F32)
        dv_acc[:, rows] += lax.dot_general(do_pad[0:dim, :], pb, NT, preferred_element_type=F32)
        return 0

    lax.fori_loop(0, i + 1, values, 0)
    o_lo = o_acc[...].astype(BF16)
    do_f = do_pad[0:dim, :].astype(F32)
    r = jnp.sum(do_f * o_lo.astype(F32), axis=0, keepdims=True)

    def grads(j, _):
        rows = pl.ds(pl.multiple_of(j * blk, blk), blk)
        g = jnp.dot(v_tok[rows, :], do_pad[...], preferred_element_type=F32)
        ds = (s_buf[rows, :] * (g - r)).astype(BF16)
        dq_acc[...] += jnp.dot(qkvt_ref[dim:2 * dim, rows], ds, preferred_element_type=F32)
        dk_acc[:, rows] += lax.dot_general(q_pad[0:dim, :], ds, NT, preferred_element_type=F32)
        return 0

    lax.fori_loop(0, i + 1, grads, 0)
    dq_lo = (dq_acc[...] * scale).astype(BF16)
    for t in range(nq):
        o_ref[i * nq + t] = o_lo[:, t * tok:(t + 1) * tok]
        dqkv_ref[i * nq + t, 0:dim] = dq_lo[:, t * tok:(t + 1) * tok]

    @pl.when(step == steps - 1)
    def _():
        @pl.loop(0, seq // tok)
        def _(t):
            cols = pl.ds(pl.multiple_of(t * tok, tok), tok)
            dqkv_ref[t, dim:2 * dim] = (dk_acc[:, cols] * scale).astype(BF16)
            dqkv_ref[t, 2 * dim:3 * dim] = dv_acc[:, cols].astype(BF16)

        if send_o:
            o_start(step)
        for k, ref in enumerate((gwa_ref, gwb_ref, gb_ref)):
            ref[...] = gw_old[k][...] if n_old else jnp.zeros_like(ref)
        ones = jnp.ones((blk, 128), BF16)

        @pl.loop(0, steps)
        def _(j):
            rows = pl.ds(pl.multiple_of(j * blk, blk), blk)
            for ref, lo, hi in ((gwa_ref, 0, lead), (gwb_ref, lead, 3 * dim)):
                lhs = jnp.concatenate([dqkv_ref[j * nq + t, lo:hi] for t in range(nq)], axis=1)
                ref[...] += jnp.dot(lhs, x_buf[rows, :], preferred_element_type=F32)
                gb_ref[lo:hi, :] += jnp.dot(lhs, ones, preferred_element_type=F32)

        gbt_ref[...] = jnp.zeros_like(gbt_ref)
        for k in range(3):
            part = jnp.concatenate([gb_ref[k * dim:(k + 1) * dim, :], jnp.zeros((pad, 128), F32)], axis=0)
            gbt_ref[k:k + 1, :] = jnp.transpose(part)[0:1, :]

        if send_o:
            o_keep().wait()
            for d in range(1, peers):
                frm = lax.rem(me + d, peers)
                o_send(frm).wait_send()
                pltpu.make_async_remote_copy(
                    src_ref=o_ref.at[frm], dst_ref=o_new.at[frm], send_sem=os_sem.at[frm], recv_sem=or_sem.at[frm],
                    device_id={"sp": frm}, device_id_type=pl.DeviceIdType.MESH).wait_recv()
        for one in swaps:
            swap_wait(*one, peers)


def attention(w_all, b_all, dot_, marks, x, gw, old, *, blk, tok, which, batch, lead, send_o, collective_id):
    blocks, dim, _ = dot_.shape
    seq, hidden = blocks * tok, w_all.shape[2]
    wide = 128 * pl.cdiv(dim, 128)
    hbm = pl.BlockSpec(memory_space=pltpu.HBM)
    full = lambda a: pl.BlockSpec(a.shape, lambda i: (0,) * len(a.shape), pipeline_mode=pl.Buffered(1))
    like = lambda a: jax.ShapeDtypeStruct(a.shape, a.dtype)
    outs = [jax.ShapeDtypeStruct((blocks, 3 * dim, tok), BF16), jax.ShapeDtypeStruct((lead, hidden), F32),
            jax.ShapeDtypeStruct((3 * dim - lead, hidden), F32), jax.ShapeDtypeStruct((3 * dim, 128), F32), jax.ShapeDtypeStruct((8, 128), F32)]
    pairs = (seq // blk) * (seq // blk + 1) // 2
    dma = pltpu.SemaphoreType.DMA
    res = pl.pallas_call(
        functools.partial(attn_body, blk=blk, tok=tok, which=which, batch=batch, n_swap=len(old), n_old=len(gw), send_o=send_o),
        name="attention",
        out_shape=outs + [like(dot_)] + [like(a) for a in old],
        grid=(seq // blk,),
        in_specs=[hbm, full(b_all), full(dot_), full(marks), hbm] + [full(a) for a in gw] + [hbm] * len(old),
        out_specs=[full(a) for a in outs] + [hbm if send_o else full(dot_)] + [hbm] * len(old),
        scratch_shapes=[
            pltpu.VMEM((seq, hidden), BF16),
            pltpu.VMEM(w_all.shape[1:], BF16), pltpu.VMEM((3 * dim, 128), F32), pltpu.VMEM((3 * dim, seq), BF16),
            pltpu.VMEM((seq, wide), BF16), pltpu.VMEM((seq, wide), BF16), pltpu.VMEM((seq, 128), F32),
            pltpu.VMEM((seq, blk), F32), pltpu.VMEM((2 * seq // blk, 8, blk), F32),
            pltpu.VMEM((wide, blk), BF16), pltpu.VMEM((wide, blk), BF16),
            pltpu.VMEM((dim, blk), F32), pltpu.VMEM((dim, blk), F32),
            pltpu.VMEM((dim, seq), F32), pltpu.VMEM((dim, seq), F32), dma((seq // blk,)), dma]
        + sum((swap_scratch(a) for a in old), []) + ([pltpu.VMEM(dot_.shape, BF16), dma((blocks,)), dma((blocks,))] if send_o else []),
        cost_estimate=pl.CostEstimate(flops=pairs * 6 * 2 * blk * blk * 256, bytes_accessed=24 << 20, transcendentals=pairs * blk * blk),
        compiler_params=pltpu.CompilerParams(dimension_semantics=("arbitrary",), vmem_limit_bytes=VMEM_LIMIT,
                                             collective_id=collective_id, has_side_effects=True),
    )(w_all, b_all, dot_, marks, x, *gw, *old)
    return res[0], res[1:4], res[4], res[5], res[6:]


def peer_at(d, peers):
    return {"sp": lax.rem(lax.axis_index("sp") + d, peers)}


def greet(peers):
    barrier = pltpu.get_barrier_semaphore()
    for d in range(1, peers):
        pl.semaphore_signal(barrier, inc=1, device_id=peer_at(d, peers), device_id_type=pl.DeviceIdType.MESH)
    return lambda: pl.semaphore_wait(barrier, peers - 1)


def meet(peers):
    greet(peers)()


def swap_copies(x_ref, out_ref, send_sem, recv_sem, peers):
    me = lax.axis_index("sp")
    order = [d for near in range(peers // 2) for d in sorted({peers // 2 - near, peers // 2 + near})]
    return [pltpu.make_async_remote_copy(
        src_ref=x_ref.at[lax.rem(me + d, peers)], dst_ref=out_ref.at[me], send_sem=send_sem.at[d - 1], recv_sem=recv_sem.at[d - 1],
        device_id=peer_at(d, peers), device_id_type=pl.DeviceIdType.MESH) for d in order]


def swap_start(x_ref, out_ref, own, send_sem, recv_sem, own_sem, peers):
    me = lax.axis_index("sp")
    for copy in swap_copies(x_ref, out_ref, send_sem, recv_sem, peers):
        copy.start()
    take = pltpu.make_async_copy(x_ref.at[me], own, own_sem)
    take.start()
    take.wait()
    pltpu.make_async_copy(own, out_ref.at[me], own_sem).start()


def swap_wait(x_ref, out_ref, own, send_sem, recv_sem, own_sem, peers):
    pltpu.make_async_copy(own, out_ref.at[lax.axis_index("sp")], own_sem).wait()
    for copy in swap_copies(x_ref, out_ref, send_sem, recv_sem, peers):
        copy.wait()


def swap_scratch(x):
    peers = x.shape[0]
    return [pltpu.VMEM(x.shape[1:], x.dtype), pltpu.SemaphoreType.DMA((peers - 1,)), pltpu.SemaphoreType.DMA((peers - 1,)),
            pltpu.SemaphoreType.DMA]


STEP = (1, -1)


def hops(ring, s, w):
    return ring // 2 - (s != w)


def ring_gather(block, own, sems, peers, cuts):
    ring = peers // 2
    me = lax.axis_index("sp")
    z, c = me // 2, me % 2
    send_sem, recv_sem, over_sem, came_sem = sems
    turn = lambda k: lax.rem(z + k + 2 * ring, ring)
    lots = [(s, w, u) for u in range(cuts) for w in range(2) for s in range(2)]

    def copy(src, dst, one, two, to):
        return pltpu.make_async_remote_copy(src_ref=src, dst_ref=dst, send_sem=one, recv_sem=two, device_id={"sp": to},
                                            device_id_type=pl.DeviceIdType.MESH)

    def along(s, w, t, u):
        ref = block(turn(-STEP[s] * t), c, w, u)
        return copy(own(w, u) if t == 0 else ref, ref, send_sem.at[s, w, t, u], recv_sem.at[s, w, t, u], 2 * turn(STEP[s]) + c)

    def across(s, w, t, u, side):
        ref = block(turn(-STEP[s] * t), side, w, u)
        return copy(own(w, u) if t == 0 and side is c else ref, ref, over_sem.at[s, w, t, u], came_sem.at[s, w, t, u], 2 * z + 1 - c)

    home = [(0, w, 0, u) for u in range(cuts) for w in range(2)]
    moved = [(s, w, t, u) for t in range(1, ring // 2 + 1) for s, w, u in lots if t <= hops(ring, s, w)]

    def start(only=None):
        for s, w, u in lots:
            if only in (None, (w, u)):
                along(s, w, 0, u).start()
        for lot in home:
            if only in (None, (lot[1], lot[3])):
                across(*lot, c).start()

    def run(lo=1, hi=ring):
        for s, w, t, u in moved:
            if lo <= t < hi:
                along(s, w, t - 1, u).wait_recv()
                if t < hops(ring, s, w):
                    along(s, w, t, u).start()
                across(s, w, t, u, c).start()

    def finish():
        for s, w, t, u in moved:
            along(s, w, t - 1, u).wait_send()
        for lot in home + moved:
            across(*lot, c).wait_send()
            across(*lot, 1 - c).wait_recv()

    return start, run, finish


def ring_scratch(peers, cuts):
    dma = pltpu.SemaphoreType.DMA
    return [dma((2, 2, peers // 4, cuts))] * 2 + [dma((2, 2, peers // 4 + 1, cuts))] * 2


def opening_body(x_hbm, dy_hbm, wo_hbm, gain_ref, bias_ref, pos_ref, keep_ref, marks_all, do_t, x_all, *refs, peers, batch, cuts):
    x_out, do_out = refs[:batch - 1], refs[batch - 1:2 * batch - 2]
    x_ref, dy_ref, x_own, do_own, wo_ref, marks_ref, own, ds_sem, dr_sem, do_sem, ms_sem, mr_sem, in_sem = refs[2 * batch - 2:2 * batch + 11]
    ring_sems = refs[2 * batch + 11:]
    gain, bias = gain_ref[...].reshape(1, -1), bias_ref[...].reshape(1, -1)
    me = lax.axis_index("sp")
    tok, dim = x_own.shape[0], do_own.shape[1]
    lot = tok // 2 // cuts
    rows_of = lambda w, u: pl.ds((w * cuts + u) * lot, lot)
    arrived = greet(peers)
    loads = [pltpu.make_async_copy(x_hbm.at[b], x_ref.at[b], in_sem.at[b]) for b in range(batch)]
    loads += [pltpu.make_async_copy(dy_hbm, dy_ref, in_sem.at[batch]), pltpu.make_async_copy(wo_hbm, wo_ref, in_sem.at[batch + 1])]
    for load in loads:
        load.start()

    def norm_rows(b, out_ref, rows):
        x = x_ref[b, rows, :].astype(F32)
        cen = x - jnp.mean(x, axis=-1, keepdims=True)
        hat = cen * lax.rsqrt(jnp.mean(cen * cen, axis=-1, keepdims=True) + NORM_EPS)
        out_ref[rows, :] = (hat * gain + bias).astype(BF16)

    def norm(b, out_ref):
        loads[b].wait()

        @pl.loop(0, tok // 32)
        def _(k):
            norm_rows(b, out_ref, pl.ds(pl.multiple_of(k * 32, 32), 32))

    def product(b, out_ref):
        @pl.loop(0, peers // 4)
        def _(g):
            rows = pl.ds(pl.multiple_of(g * 4 * dim, 4 * dim), 4 * dim)
            out_ref[pl.ds(g * 4, 4)] = lax.dot_general(wo_ref[rows, :], dy_ref[b], NT, preferred_element_type=F32).astype(BF16).reshape(4, dim, tok)

    marks_ref[...] = jnp.zeros_like(marks_ref)
    packed = 2 * pos_ref[...] + keep_ref[...]
    sub = tok // 128
    for b in range(batch):
        for k in range(sub):
            marks_ref[b * sub + k:b * sub + k + 1, :] = packed[b:b + 1, k * 128:(k + 1) * 128]
    block = lambda k, side, w, u: x_all.at[2 * k + side, rows_of(w, u)]
    start, run, finish = ring_gather(block, lambda w, u: x_own.at[rows_of(w, u)], ring_sems, peers, cuts)
    loads[0].wait()
    pieces = [(w, u) for u in range(cuts) for w in range(2)]
    for k, piece in enumerate(pieces):
        norm_rows(0, x_own, rows_of(*piece))
        if k == 1:
            arrived()
        if k:
            start(pieces[k - 1])
    start(pieces[-1])
    keep = pltpu.make_async_copy(x_own, x_all.at[me], in_sem.at[batch + 2])
    keep.start()
    marks = [pltpu.make_async_remote_copy(
        src_ref=marks_ref, dst_ref=marks_all.at[me], send_sem=ms_sem.at[d - 1], recv_sem=mr_sem.at[d - 1],
        device_id=peer_at(d, peers), device_id_type=pl.DeviceIdType.MESH) for d in range(1, peers)]
    for copy in marks:
        copy.start()
    marks_all[me] = marks_ref[...]
    loads[-2].wait()
    loads[-1].wait()
    product(0, do_own)
    for b in range(1, batch):
        norm(b, x_out[b - 1])
    swap_start(do_own, do_t, own, ds_sem, dr_sem, do_sem, peers)
    for b in range(1, batch):
        product(b, do_out[b - 1])
    run()
    keep.wait()
    for copy in marks:
        copy.wait()
    swap_wait(do_own, do_t, own, ds_sem, dr_sem, do_sem, peers)
    finish()


def opening(x, dy, w_out, gain, bias, pos, keep, peers, collective_id, cuts=4):
    batch, tok, hidden = x.shape
    dim = hidden // peers
    hbm, vmem = pl.BlockSpec(memory_space=pltpu.HBM), pl.BlockSpec(memory_space=pltpu.VMEM)
    dma = pltpu.SemaphoreType.DMA
    do_shape, x_shape = jax.ShapeDtypeStruct((peers, dim, tok), BF16), jax.ShapeDtypeStruct((tok, hidden), BF16)
    res = pl.pallas_call(
        functools.partial(opening_body, peers=peers, batch=batch, cuts=cuts),
        name="opening",
        out_shape=[jax.ShapeDtypeStruct((peers, 8, 128), pos.dtype), do_shape, jax.ShapeDtypeStruct((peers, tok, hidden), BF16)]
        + [x_shape] * (batch - 1) + [do_shape] * (batch - 1),
        in_specs=[hbm, hbm, hbm, vmem, vmem, vmem, vmem],
        out_specs=[vmem, hbm, hbm] + [vmem] * (2 * batch - 2),
        scratch_shapes=[pltpu.VMEM(x.shape, BF16), pltpu.VMEM(dy.shape, BF16), pltpu.VMEM(x_shape.shape, BF16), pltpu.VMEM(do_shape.shape, BF16),
                        pltpu.VMEM(w_out.shape, BF16), pltpu.VMEM((8, 128), pos.dtype)] + swap_scratch(do_shape)
        + [dma((peers - 1,)), dma((peers - 1,)), dma((batch + 3,))] + ring_scratch(peers, cuts),
        cost_estimate=pl.CostEstimate(flops=5 * 10**10, bytes_accessed=16 << 20, transcendentals=0),
        compiler_params=pltpu.CompilerParams(collective_id=collective_id, has_side_effects=True, vmem_limit_bytes=VMEM_LIMIT),
    )(x, dy, w_out, gain, bias, pos, keep)
    return res[0], res[1], res[2], res[3:2 + batch], res[2 + batch:]


TN = (((0,), (0,)), ((), ()))


def tail_a_body(dqkv_ref, oo_hbm, on_hbm, dy_hbm, x_hbm, wo_hbm, d_hbm, w_hbm, gain_ref, bo_ref, y_ref, gx_ref, part, rows_ref,
                o_old, o_new, dy_ref, x_ref, wo_ref, d_old, w_ref, d_new, dn, sums, bo_rep, both, mine, landed, own_d,
                ds_sem, dr_sem, do_sem, ps_sem, pr_sem, rs_sem, rr_sem, w_sem, *, peers, cuts):
    ring = peers // 2
    me = lax.axis_index("sp")
    z, c = me // 2, me % 2
    _, tok, hidden = x_ref.shape
    half, wide, few = hidden // 2, hidden // 3, part.shape[0] // cuts
    cols = (pl.ds(0, half), pl.ds(half, half))
    at = lambda zz, cc: {"sp": 2 * zz + cc}
    turn = lambda k: lax.rem(z + k + 2 * ring, ring)
    remote = functools.partial(pltpu.make_async_remote_copy, device_id_type=pl.DeviceIdType.MESH)
    span, group = d_old.shape[1], 8
    gain, b_out = gain_ref[...].reshape(1, hidden), bo_ref[...].reshape(1, hidden)
    pairs = ((oo_hbm, o_old), (on_hbm, o_new), (dy_hbm, dy_ref), (x_hbm, x_ref), (wo_hbm, wo_ref), (d_hbm, d_old), (w_hbm, w_ref))
    loads = [pltpu.make_async_copy(src, dst, w_sem.at[k]) for k, (src, dst) in enumerate(pairs)]
    swap = (dqkv_ref, d_new, own_d, ds_sem, dr_sem, do_sem, peers)
    arrived = greet(peers)
    for load in loads:
        load.start()
    arrived()
    swap_start(*swap)
    for load in loads[:3]:
        load.wait()

    def product(put, side):
        @pl.loop(0, ring)
        def _(k):
            h = 2 * k + side
            put(k, jnp.dot(o_old[h], dy_ref[0], preferred_element_type=F32)
                + jnp.dot(o_new[h], dy_ref[1], preferred_element_type=F32))

    def put_other(k, value):
        both[k, 1 - c] = value

    def put_mine(k, value):
        mine[k] = value

    def forward(b, o_ref):
        o_t = o_ref[...].reshape(hidden, tok)

        @pl.loop(0, 3)
        def _(n):
            at_n = pl.ds(pl.multiple_of(n * wide, wide), wide)
            acc = lax.dot_general(o_t, wo_ref[:, at_n], TN, preferred_element_type=F32)
            y_ref[b, :, at_n] = (x_ref[b, :, at_n].astype(F32) + acc + bo_rep[0:1, at_n]).astype(BF16)

    def backward(b, d_ref):
        @pl.loop(0, 3)
        def _(n):
            at_n = pl.ds(pl.multiple_of(n * wide, wide), wide)
            acc = None
            for k in range(0, peers, group):
                lhs = d_ref[k:k + group].reshape(-1, tok)
                one = lax.dot_general(lhs, w_ref[k * span:(k + group) * span, at_n], TN, preferred_element_type=F32)
                acc = one if acc is None else acc + one
            dn[:, at_n] = acc

        @pl.loop(0, tok // 32)
        def _(k):
            rows = pl.ds(pl.multiple_of(k * 32, 32), 32)
            x = x_ref[b, rows, :].astype(F32)
            dy = dy_ref[b, rows, :].astype(F32)
            d = dn[rows, :]
            cen = x - jnp.mean(x, axis=-1, keepdims=True)
            inv = lax.rsqrt(jnp.mean(cen * cen, axis=-1, keepdims=True) + NORM_EPS)
            hat = cen * inv
            for n, one in enumerate((d * hat, d, dy)):
                sums[n] += jnp.sum(one.reshape(4, 8, hidden), axis=0)
            e = d * gain
            m1 = jnp.mean(e, axis=-1, keepdims=True)
            m2 = jnp.mean(e * hat, axis=-1, keepdims=True)
            gx_ref[b, rows, :] = (dy + inv * (e - m1 - hat * m2)).astype(BF16)

    bo_rep[...] = jnp.broadcast_to(b_out, bo_rep.shape)
    sums[...] = jnp.zeros_like(sums)
    product(put_other, 1 - c)
    pair_copy = lambda side: remote(src_ref=both.at[:, side], dst_ref=both.at[:, side], send_sem=ps_sem, recv_sem=pr_sem, device_id=at(z, 1 - c))
    product(put_mine, c)
    pair_copy(1 - c).start()
    pair_copy(1 - c).wait_send()
    pair_copy(c).wait_recv()

    @pl.loop(0, ring)
    def _(k):
        mine[k] = mine[k] + both[k, c]

    lots = [(s, w, u) for u in range(cuts) for w in range(2) for s in range(2)]

    def reduce_copy(s, w, t, u):
        return remote(src_ref=mine.at[turn(STEP[s] * (hops(ring, s, w) - t)), pl.ds(u * few, few), cols[w]], dst_ref=landed.at[s, w, t, u],
                      send_sem=rs_sem.at[s, w, t, u], recv_sem=rr_sem.at[s, w, t, u], device_id=at(turn(STEP[s]), c))

    def fold(s, w, t, u):
        reduce_copy(s, w, t, u).wait_recv()
        at_k = (turn(STEP[s] * (hops(ring, s, w) - t - 1)), pl.ds(u * few, few), cols[w])
        mine[at_k] = mine[at_k] + landed[s, w, t, u]

    def hop(t):
        for s, w, u in lots:
            if t < hops(ring, s, w):
                fold(s, w, t - 1, u)
                reduce_copy(s, w, t, u).start()

    for s, w, u in lots:
        reduce_copy(s, w, 0, u).start()
    for load in loads[3:5]:
        load.wait()
    forward(0, o_old)
    forward(1, o_new)
    for load in loads[5:]:
        load.wait()
    backward(0, d_old)
    for t in range(1, ring // 2 - 1):
        hop(t)
    swap_wait(*swap)
    backward(1, d_new)
    hop(ring // 2 - 1)
    rows_ref[...] = jnp.zeros_like(rows_ref)
    for n in range(3):
        rows_ref[n:n + 1, :] = jnp.sum(sums[n], axis=0, keepdims=True)
    for s, w, u in lots:
        fold(s, w, hops(ring, s, w) - 1, u)
    part[...] = mine[z]
    for s, w, u in lots:
        for t in range(hops(ring, s, w)):
            reduce_copy(s, w, t, u).wait_send()


def tail_a(dqkv, d_old, o_old, o_new, dy, x, w_flat, w_out, gain, b_out, collective_id, cuts=2):
    peers, dim, tok = o_old.shape
    ring = peers // 2
    hidden = dy.shape[-1]
    hbm, vmem = pl.BlockSpec(memory_space=pltpu.HBM), pl.BlockSpec(memory_space=pltpu.VMEM)
    dma = pltpu.SemaphoreType.DMA
    held = lambda a: pltpu.VMEM(a.shape, a.dtype)
    steps = (2, 2, ring // 2, cuts)
    return pl.pallas_call(
        functools.partial(tail_a_body, peers=peers, cuts=cuts),
        name="tail_a",
        out_shape=[jax.ShapeDtypeStruct(x.shape, BF16), jax.ShapeDtypeStruct(x.shape, BF16), jax.ShapeDtypeStruct((dim, hidden), F32),
                   jax.ShapeDtypeStruct((8, hidden), F32)],
        in_specs=[hbm] * 8 + [vmem] * 2,
        out_specs=[vmem] * 4,
        scratch_shapes=[held(a) for a in (o_old, o_new, dy, x, w_out, d_old, w_flat, dqkv)]
        + [pltpu.VMEM((tok, hidden), F32), pltpu.VMEM((3, 8, hidden), F32), pltpu.VMEM((8, hidden), F32),
           pltpu.VMEM((ring, 2, dim, hidden), F32), pltpu.VMEM((ring, dim, hidden), F32), pltpu.VMEM(steps + (dim // cuts, hidden // 2), F32),
           pltpu.VMEM(dqkv.shape[1:], BF16), dma((peers - 1,)), dma((peers - 1,)), dma, dma, dma, dma(steps), dma(steps), dma((7,))],
        cost_estimate=pl.CostEstimate(flops=10**11, bytes_accessed=64 << 20, transcendentals=0),
        compiler_params=pltpu.CompilerParams(collective_id=collective_id, has_side_effects=True, vmem_limit_bytes=VMEM_LIMIT),
    )(dqkv, o_old, o_new, dy, x, w_out, d_old, w_flat, gain, b_out)


def tail_b_body(part, rows_ref, gb_ref, full, total, gb_all, stage, xs_sem, xr_sem, *ring_sems, peers, cuts):
    ring = peers // 2
    me = lax.axis_index("sp")
    z, c = me // 2, me % 2
    hidden = part.shape[1]
    half, few = hidden // 2, part.shape[0] // cuts
    cols = (pl.ds(0, half), pl.ds(half, half))
    remote = functools.partial(pltpu.make_async_remote_copy, device_id_type=pl.DeviceIdType.MESH)
    arrived = greet(peers)
    full[z, c] = part[...]
    gb_all[me] = gb_ref[...]
    block = lambda k, side, w, u: full.at[k, side, pl.ds(u * few, few), cols[w]]
    start, run, finish = ring_gather(block, lambda w, u: block(z, c, w, u), ring_sems, peers, cuts)
    owners = hidden // 128
    lanes = lambda k: pl.ds(pl.multiple_of(k * 128, 128), 128)

    def small_copy(kind, frm, to):
        src, dst = ((rows_ref.at[:, lanes(to)], stage.at[frm]), (total.at[:, lanes(frm)],) * 2, (gb_ref, gb_all.at[frm]))[kind]
        return remote(src_ref=src, dst_ref=dst, send_sem=xs_sem.at[kind, to], recv_sem=xr_sem.at[kind, frm], device_id={"sp": to})

    def each(act, kind, only_to=False, only_from=False):
        @pl.loop(1, peers)
        def _(d):
            far = lax.rem(me + d, peers)

            def go():
                act(kind, far)

            if only_to:
                pl.when(far < owners)(go)
            elif only_from:
                pl.when(me < owners)(go)
            else:
                go()

    send = lambda kind, far: small_copy(kind, me, far).start()
    over = lambda kind, far: small_copy(kind, me, far).wait_send()
    came = lambda kind, far: small_copy(kind, far, me).wait_recv()

    @pl.when(me < owners)
    def _():
        stage[me] = rows_ref[:, lanes(me)]

    arrived()
    start()
    each(send, 0, only_to=True)
    each(send, 2)
    run(1, 2)
    each(came, 0, only_from=True)

    @pl.when(me < owners)
    def _():
        total[:, lanes(me)] = jnp.sum(stage[...], axis=0)

    each(send, 1, only_from=True)
    run(2)
    each(came, 1, only_to=True)
    each(came, 2)
    each(over, 0, only_to=True)
    each(over, 1, only_from=True)
    each(over, 2)
    finish()


def tail_b(part, rows, gb, peers, collective_id, cuts=2):
    ring = peers // 2
    vmem = pl.BlockSpec(memory_space=pltpu.VMEM)
    dma = pltpu.SemaphoreType.DMA
    return pl.pallas_call(
        functools.partial(tail_b_body, peers=peers, cuts=cuts),
        name="tail_b",
        out_shape=[jax.ShapeDtypeStruct((ring, 2) + part.shape, F32), jax.ShapeDtypeStruct(rows.shape, F32),
                   jax.ShapeDtypeStruct((peers,) + gb.shape, F32)],
        in_specs=[vmem] * 3,
        out_specs=[vmem] * 3,
        scratch_shapes=[pltpu.VMEM((peers, 8, 128), F32), dma((3, peers)), dma((3, peers))] + ring_scratch(peers, cuts),
        cost_estimate=pl.CostEstimate(flops=5 * 10**10, bytes_accessed=10 << 20, transcendentals=0),
        compiler_params=pltpu.CompilerParams(collective_id=collective_id, has_side_effects=True, vmem_limit_bytes=32 << 20),
    )(part, rows, gb)


def settle_body(*refs, n_in, first, n_plain, n_held):
    x_ref, plain, held = refs[0], refs[1:1 + n_plain], refs[1 + n_plain:1 + n_plain + n_held]
    outs = refs[n_in:n_in + 1 + n_plain + n_held]
    buf, in_sem, out_sem, in_plain, out_plain, *rooms = refs[n_in + 1 + n_plain + n_held:]
    heads, n = x_ref.shape[:2]
    copy = pltpu.make_async_copy
    reads = [copy(x_ref.at[h], buf.at[h], in_sem.at[h]) for h in range(heads)]
    writes = [copy(buf.at[h], outs[0].at[h, pl.ds(first, n)], out_sem.at[h]) for h in range(heads)]
    reads += [copy(plain[k], rooms[k], in_plain.at[k]) for k in range(n_plain)]
    writes += [copy(rooms[k], outs[1 + k], out_plain.at[k]) for k in range(n_plain)]
    flat = [copy(held[k], outs[1 + n_plain + k], out_plain.at[n_plain + k]) for k in range(n_held)]
    for one in reads + flat:
        one.start()
    for read, write in zip(reads, writes):
        read.wait()
        write.start()
    for one in writes + flat:
        one.wait()


def settle(x, into, plain, held, span, first):
    heads, n, hidden = x.shape
    hbm, vmem = pl.BlockSpec(memory_space=pltpu.HBM), pl.BlockSpec(memory_space=pltpu.VMEM)
    pin = lambda a: pltpu.with_memory_space_constraint(a, pltpu.HBM)
    args = (pin(x), *[pin(a) for a in plain], *held) + (() if into is None else (into,))
    dma = pltpu.SemaphoreType.DMA
    extra = max(len(plain) + len(held), 1)
    return pl.pallas_call(
        functools.partial(settle_body, n_in=len(args), first=first, n_plain=len(plain), n_held=len(held)), name="settle",
        out_shape=[jax.ShapeDtypeStruct((heads, span, hidden), x.dtype)] + [jax.ShapeDtypeStruct(a.shape, a.dtype) for a in (*plain, *held)],
        in_specs=[hbm] * (1 + len(plain)) + [vmem] * len(held) + [hbm] * (into is not None),
        out_specs=[hbm] * (1 + len(plain) + len(held)),
        input_output_aliases={} if into is None else {len(args) - 1: 0},
        scratch_shapes=[pltpu.VMEM(x.shape, x.dtype), dma((heads,)), dma((heads,)), dma((extra,)), dma((extra,))]
        + [pltpu.VMEM(a.shape, a.dtype) for a in plain],
        cost_estimate=pl.CostEstimate(flops=10**9, bytes_accessed=8 * x.size, transcendentals=0),
        compiler_params=pltpu.CompilerParams(vmem_limit_bytes=24 << 20))(*args)


def lay_body(go_ref, total, gb_all, go_out, gb_out, *refs):
    vectors, sem = refs[:-1], refs[-1]
    copies = [pltpu.make_async_copy(go_ref.at[k], go_out.at[k], sem.at[k]) for k in range(go_ref.shape[0])]
    for copy in copies:
        copy.start()
    for k in range(3):
        gb_out[k] = gb_all[:, k, 0:gb_out.shape[2]]
        vectors[k][...] = total[k]
    for copy in copies:
        copy.wait()


def lay_down(go, total, gb_all):
    hbm, vmem = pl.BlockSpec(memory_space=pltpu.HBM), pl.BlockSpec(memory_space=pltpu.VMEM)
    ring, _, dim, hidden = go.shape
    return pl.pallas_call(
        lay_body, name="lay_down",
        out_shape=[jax.ShapeDtypeStruct(go.shape, F32), jax.ShapeDtypeStruct((3, 2 * ring, dim), F32)] + [jax.ShapeDtypeStruct((hidden,), F32)] * 3,
        in_specs=[vmem] * 3, out_specs=[hbm] + [vmem] * 4,
        scratch_shapes=[pltpu.SemaphoreType.DMA((ring,))],
        cost_estimate=pl.CostEstimate(flops=10**9, bytes_accessed=8 * go.size, transcendentals=0),
        compiler_params=pltpu.CompilerParams(vmem_limit_bytes=24 << 20))(go, total, gb_all)


def solution(mesh):
    peers = mesh.shape["sp"]

    def block_fn(x_blk, pos_blk, keep_blk, ln_gain, ln_bias, w_qkv, b_qkv, w_out, b_out, dy_blk):
        batch, tok, hidden = x_blk.shape
        heads, dim = w_qkv.shape[1], w_qkv.shape[3]
        assert heads == peers
        seq = tok * peers
        blk = 2 * tok
        w_all = jnp.transpose(w_qkv, (1, 2, 3, 0)).reshape(heads, 3 * dim, hidden)
        b_all = jnp.transpose(b_qkv, (1, 0, 2))
        marks, do_first, x_first, x_rest, do_rest = opening(x_blk, dy_blk, w_out, ln_gain, ln_bias, pos_blk, keep_blk, peers, 1)
        xs = [x_first.reshape(seq, hidden)] + [lax.all_gather(one, "sp", axis=0, tiled=True) for one in x_rest]
        do_t = [do_first]
        lead = 13 * dim // 6
        gw, att = (), []
        for b in range(batch):
            old = list(do_rest[b:b + 1]) if b + 1 < batch else att
            att_d, gw, gb, att_o, swapped = attention(w_all, b_all, do_t[b], marks, xs[b], gw, old, blk=blk, tok=tok, which=b, batch=batch, lead=lead,
                                                      send_o=b + 1 == batch, collective_id=4 + b)
            if b + 1 < batch:
                do_t.append(swapped[0])
            att = [att_o, att_d]
        o_old, d_old = swapped
        gw_all = [lax.all_gather(one, "sp", axis=0, tiled=True).reshape(heads, -1, hidden) for one in gw[:2]]
        y, gx, part, rows = tail_a(att_d, d_old, o_old, att_o, dy_blk, x_blk, w_all.reshape(3 * hidden, hidden), w_out, ln_gain, b_out, 2)
        go_all, gb_all, g_gain, g_bias, g_out = lay_down(*tail_b(part, rows, gb, peers, 3))
        first, y, gx, go_all = lax.optimization_barrier((gw_all[0], y, gx, go_all))
        gw_out, y, gx = settle(first, None, (y, gx), (), 3 * dim, 0)
        second, gw_out, go_all = lax.optimization_barrier((gw_all[1], gw_out, go_all))
        gw_out, = settle(second, gw_out, (), (), 3 * dim, lead)
        gw_out = jnp.transpose(gw_out.reshape(heads, 3, dim, hidden), (3, 0, 1, 2))
        return y, gx, gw_out, jnp.transpose(gb_all, (1, 0, 2)), go_all.reshape(hidden, hidden), g_out, g_gain, g_bias

    act_spec = P("dp", "sp", None)
    tok_spec = P("dp", "sp")
    in_specs = (act_spec, tok_spec, tok_spec, P(), P(), P(), P(), P(), P(), act_spec)
    out_specs = (act_spec, act_spec, P("dp", None, None, None), P("dp", None, None), P("dp", None), P("dp"), P("dp"), P("dp"))
    return jax.shard_map(block_fn, mesh=mesh, in_specs=in_specs, out_specs=out_specs, check_vma=False)
```

```python
import functools
import jax
import jax.numpy as jnp
from jax import lax
from jax.experimental import pallas as pl
from jax.experimental.pallas import tpu as pltpu
from jax.sharding import PartitionSpec as P

NORM_EPS = 1e-5

LOG2E = 1.4426950408889634
MASKED = -1e30
VMEM_LIMIT = 62 << 20
F32, BF16 = jnp.float32, jnp.bfloat16
NT = (((1,), (1,)), ((), ()))


def attn_body(w_hbm, b_ref, dot_ref, marks_ref, x_ref, *refs, blk, tok, which, batch, n_swap, n_old, send_o):
    peers = dot_ref.shape[0]
    gw_old, old, refs = refs[:n_old], refs[n_old:n_old + n_swap], refs[n_old + n_swap:]
    (dqkv_ref, gwa_ref, gwb_ref, gb_ref, gbt_ref, o_out), got, refs = refs[:6], refs[6:6 + n_swap], refs[6 + n_swap:]
    x_buf, refs = refs[0], refs[1:]
    w_ref, b_rep, qkvt_ref, k_tok, v_tok, posk_ref, s_buf, m_buf, q_pad, do_pad, o_acc, dq_acc, dk_acc, dv_acc, x_sem, w_sem = refs[:16]
    swaps = [(old[k], got[k]) + refs[16 + 4 * k:20 + 4 * k] for k in range(n_swap)]
    if send_o:
        o_ref, os_sem, or_sem = refs[-3:]
        o_new = o_out
    else:
        o_ref = o_out
    dim, lead = dot_ref.shape[1], gwa_ref.shape[0]
    seq = dot_ref.shape[0] * tok
    pad = k_tok.shape[1] - dim
    nq = blk // tok
    steps = seq // blk
    scale = dim ** -0.5
    me = lax.axis_index("sp")
    step = pl.program_id(0)
    i = lax.rem(me // nq + step, steps)
    half = blk // 2
    sub = tok // 128

    def spread(row):
        return jnp.transpose(jnp.broadcast_to(row, (128, 128)))

    def x_copy(k):
        rows = pl.ds(pl.multiple_of(k * blk, blk), blk)
        return pltpu.make_async_copy(x_ref.at[rows], x_buf.at[rows], x_sem.at[k])

    def o_send(to):
        return pltpu.make_async_remote_copy(
            src_ref=o_ref.at[to], dst_ref=o_new.at[me], send_sem=os_sem.at[to], recv_sem=or_sem.at[me],
            device_id={"sp": to}, device_id_type=pl.DeviceIdType.MESH)

    def o_keep():
        return pltpu.make_async_copy(o_ref.at[me], o_new.at[me], os_sem.at[me])

    def o_start(at):
        for t in range(nq):
            to = lax.rem(me // nq + at, steps) * nq + t

            @pl.when(to != me)
            def _():
                o_send(to).start()

            @pl.when(to == me)
            def _():
                o_keep().start()

    @pl.when(step == 0)
    def _():
        w_load = pltpu.make_async_copy(w_hbm.at[me], w_ref, w_sem)
        w_load.start()
        for k in range(steps):
            x_copy(k).start()
        meet(peers)
        for one in swaps:
            swap_start(*one, peers)
        dk_acc[...] = jnp.zeros_like(dk_acc)
        dv_acc[...] = jnp.zeros_like(dv_acc)
        q_pad[...] = jnp.zeros_like(q_pad)
        do_pad[...] = jnp.zeros_like(do_pad)
        mine = lax.broadcasted_iota(jnp.int32, (peers, dim), 0) == me
        for k in range(3):
            row = jnp.sum(jnp.where(mine, b_ref[k], 0.0), axis=0, keepdims=True)
            b_rep[k * dim:(k + 1) * dim, :] = spread(jnp.concatenate([row, jnp.zeros((1, pad), F32)], axis=1))[0:dim]
        w_load.wait()

        @pl.loop(0, steps)
        def _(k):
            rows = pl.ds(pl.multiple_of(k * blk, blk), blk)
            x_copy(k).wait()
            shift = jnp.concatenate([b_rep[...]] * (blk // 128), axis=1)
            qkvt_ref[:, rows] = (lax.dot_general(w_ref[...], x_buf[rows, :], NT, preferred_element_type=F32) + shift).astype(BF16)

            for t in range(blk // 128):
                cols = pl.ds(pl.multiple_of(k * blk + t * 128, 128), 128)
                for base, dst in ((dim, k_tok), (2 * dim, v_tok)):
                    part = qkvt_ref[base:base + dim, cols].astype(F32)
                    whole = jnp.concatenate([part, jnp.zeros((pad, 128), F32)], axis=0)
                    dst[cols, :] = jnp.transpose(whole).astype(BF16)
                mark = marks_ref[k * nq + t // sub, which * sub + t % sub:which * sub + t % sub + 1, :]
                pos, keep = lax.shift_right_logical(mark, 1).astype(F32), mark & 1
                posk_ref[cols, :] = spread(jnp.where(keep > 0, pos, MASKED))

    if send_o:
        @pl.when(step > 0)
        def _():
            o_start(step - 1)

    qcols = pl.ds(pl.multiple_of(i * blk, blk), blk)
    q_pad[0:dim, :] = qkvt_ref[0:dim, qcols]
    for t in range(nq):
        do_pad[0:dim, t * tok:(t + 1) * tok] = dot_ref[i * nq + t]
    slope2 = jnp.exp2(jnp.full((1, 128), -8.0 / peers, F32) * (me + 1).astype(F32)) * LOG2E
    first = lax.shift_right_logical(marks_ref[i * nq, which * sub:which * sub + 1, :], 1).astype(F32)
    ref_pos = jnp.broadcast_to(first[:, 0:1], (1, 128))
    c = scale * LOG2E

    def scores(j, carry, diag):
        m, l8 = carry
        for sub in range(2):
            rows = pl.ds(pl.multiple_of(j * blk + sub * half, half), half)
            st = jnp.dot(k_tok[rows, :], q_pad[...], preferred_element_type=F32)
            bias = (posk_ref[rows, :] - ref_pos) * slope2
            st = st * c + jnp.concatenate([bias] * (blk // 128), axis=1)
            if diag:
                key = lax.broadcasted_iota(jnp.int32, (half, blk), 0) + sub * half
                qry = lax.broadcasted_iota(jnp.int32, (half, blk), 1)
                st = jnp.where(key <= qry, st, MASKED)
            m_new = jnp.maximum(m, jnp.max(st, axis=0, keepdims=True))
            e = jnp.exp2(st - m_new)
            s_buf[rows, :] = e
            m_buf[2 * j + sub] = jnp.broadcast_to(m_new, (8, blk))
            l8 = l8 * jnp.exp2(m - m_new) + jnp.sum(e.reshape(half // 8, 8, blk), axis=0)
            m = m_new
        return m, l8

    start = (jnp.full((1, blk), MASKED, F32), jnp.zeros((8, blk), F32))
    m, l8 = scores(i, lax.fori_loop(0, i, lambda j, carry: scores(j, carry, False), start), True)
    inv = 1.0 / jnp.sum(l8, axis=0, keepdims=True)
    o_acc[...] = jnp.zeros_like(o_acc)
    dq_acc[...] = jnp.zeros_like(dq_acc)

    def values(j, _):
        rows = pl.ds(pl.multiple_of(j * blk, blk), blk)
        pbs = []
        for sub in range(2):
            part = pl.ds(pl.multiple_of(j * blk + sub * half, half), half)
            p = s_buf[part, :] * (jnp.exp2(m_buf[2 * j + sub][0:1, :] - m) * inv)
            s_buf[part, :] = p
            pbs.append(p.astype(BF16))
        pb = jnp.concatenate(pbs, axis=0)
        o_acc[...] += jnp.dot(qkvt_ref[2 * dim:3 * dim, rows], pb, preferred_element_type=F32)
        dv_acc[:, rows] += lax.dot_general(do_pad[0:dim, :], pb, NT, preferred_element_type=F32)
        return 0

    lax.fori_loop(0, i + 1, values, 0)
    o_lo = o_acc[...].astype(BF16)
    do_f = do_pad[0:dim, :].astype(F32)
    r = jnp.sum(do_f * o_lo.astype(F32), axis=0, keepdims=True)

    def grads(j, _):
        rows = pl.ds(pl.multiple_of(j * blk, blk), blk)
        g = jnp.dot(v_tok[rows, :], do_pad[...], preferred_element_type=F32)
        ds = (s_buf[rows, :] * (g - r)).astype(BF16)
        dq_acc[...] += jnp.dot(qkvt_ref[dim:2 * dim, rows], ds, preferred_element_type=F32)
        dk_acc[:, rows] += lax.dot_general(q_pad[0:dim, :], ds, NT, preferred_element_type=F32)
        return 0

    lax.fori_loop(0, i + 1, grads, 0)
    dq_lo = (dq_acc[...] * scale).astype(BF16)
    for t in range(nq):
        o_ref[i * nq + t] = o_lo[:, t * tok:(t + 1) * tok]
        dqkv_ref[i * nq + t, 0:dim] = dq_lo[:, t * tok:(t + 1) * tok]

    @pl.when(step == steps - 1)
    def _():
        @pl.loop(0, seq // tok)
        def _(t):
            cols = pl.ds(pl.multiple_of(t * tok, tok), tok)
            dqkv_ref[t, dim:2 * dim] = (dk_acc[:, cols] * scale).astype(BF16)
            dqkv_ref[t, 2 * dim:3 * dim] = dv_acc[:, cols].astype(BF16)

        if send_o:
            o_start(step)
        for k, ref in enumerate((gwa_ref, gwb_ref, gb_ref)):
            ref[...] = gw_old[k][...] if n_old else jnp.zeros_like(ref)
        ones = jnp.ones((blk, 128), BF16)

        @pl.loop(0, steps)
        def _(j):
            rows = pl.ds(pl.multiple_of(j * blk, blk), blk)
            for ref, lo, hi in ((gwa_ref, 0, lead), (gwb_ref, lead, 3 * dim)):
                lhs = jnp.concatenate([dqkv_ref[j * nq + t, lo:hi] for t in range(nq)], axis=1)
                ref[...] += jnp.dot(lhs, x_buf[rows, :], preferred_element_type=F32)
                gb_ref[lo:hi, :] += jnp.dot(lhs, ones, preferred_element_type=F32)

        gbt_ref[...] = jnp.zeros_like(gbt_ref)
        for k in range(3):
            part = jnp.concatenate([gb_ref[k * dim:(k + 1) * dim, :], jnp.zeros((pad, 128), F32)], axis=0)
            gbt_ref[k:k + 1, :] = jnp.transpose(part)[0:1, :]

        if send_o:
            o_keep().wait()
            for d in range(1, peers):
                frm = lax.rem(me + d, peers)
                o_send(frm).wait_send()
                pltpu.make_async_remote_copy(
                    src_ref=o_ref.at[frm], dst_ref=o_new.at[frm], send_sem=os_sem.at[frm], recv_sem=or_sem.at[frm],
                    device_id={"sp": frm}, device_id_type=pl.DeviceIdType.MESH).wait_recv()
        for one in swaps:
            swap_wait(*one, peers)


def attention(w_all, b_all, dot_, marks, x, gw, old, *, blk, tok, which, batch, lead, send_o, collective_id):
    blocks, dim, _ = dot_.shape
    seq, hidden = blocks * tok, w_all.shape[2]
    wide = 128 * pl.cdiv(dim, 128)
    hbm = pl.BlockSpec(memory_space=pltpu.HBM)
    full = lambda a: pl.BlockSpec(a.shape, lambda i: (0,) * len(a.shape), pipeline_mode=pl.Buffered(1))
    like = lambda a: jax.ShapeDtypeStruct(a.shape, a.dtype)
    outs = [jax.ShapeDtypeStruct((blocks, 3 * dim, tok), BF16), jax.ShapeDtypeStruct((lead, hidden), F32),
            jax.ShapeDtypeStruct((3 * dim - lead, hidden), F32), jax.ShapeDtypeStruct((3 * dim, 128), F32), jax.ShapeDtypeStruct((8, 128), F32)]
    pairs = (seq // blk) * (seq // blk + 1) // 2
    dma = pltpu.SemaphoreType.DMA
    res = pl.pallas_call(
        functools.partial(attn_body, blk=blk, tok=tok, which=which, batch=batch, n_swap=len(old), n_old=len(gw), send_o=send_o),
        name="attention",
        out_shape=outs + [like(dot_)] + [like(a) for a in old],
        grid=(seq // blk,),
        in_specs=[hbm, full(b_all), full(dot_), full(marks), hbm] + [full(a) for a in gw] + [hbm] * len(old),
        out_specs=[full(a) for a in outs] + [hbm if send_o else full(dot_)] + [hbm] * len(old),
        scratch_shapes=[
            pltpu.VMEM((seq, hidden), BF16),
            pltpu.VMEM(w_all.shape[1:], BF16), pltpu.VMEM((3 * dim, 128), F32), pltpu.VMEM((3 * dim, seq), BF16),
            pltpu.VMEM((seq, wide), BF16), pltpu.VMEM((seq, wide), BF16), pltpu.VMEM((seq, 128), F32),
            pltpu.VMEM((seq, blk), F32), pltpu.VMEM((2 * seq // blk, 8, blk), F32),
            pltpu.VMEM((wide, blk), BF16), pltpu.VMEM((wide, blk), BF16),
            pltpu.VMEM((dim, blk), F32), pltpu.VMEM((dim, blk), F32),
            pltpu.VMEM((dim, seq), F32), pltpu.VMEM((dim, seq), F32), dma((seq // blk,)), dma]
        + sum((swap_scratch(a) for a in old), []) + ([pltpu.VMEM(dot_.shape, BF16), dma((blocks,)), dma((blocks,))] if send_o else []),
        cost_estimate=pl.CostEstimate(flops=pairs * 6 * 2 * blk * blk * 256, bytes_accessed=24 << 20, transcendentals=pairs * blk * blk),
        compiler_params=pltpu.CompilerParams(dimension_semantics=("arbitrary",), vmem_limit_bytes=VMEM_LIMIT,
                                             collective_id=collective_id, has_side_effects=True),
    )(w_all, b_all, dot_, marks, x, *gw, *old)
    return res[0], res[1:4], res[4], res[5], res[6:]


def peer_at(d, peers):
    return {"sp": lax.rem(lax.axis_index("sp") + d, peers)}


def greet(peers):
    barrier = pltpu.get_barrier_semaphore()
    for d in range(1, peers):
        pl.semaphore_signal(barrier, inc=1, device_id=peer_at(d, peers), device_id_type=pl.DeviceIdType.MESH)
    return lambda: pl.semaphore_wait(barrier, peers - 1)


def meet(peers):
    greet(peers)()


def swap_copies(x_ref, out_ref, send_sem, recv_sem, peers):
    me = lax.axis_index("sp")
    order = [d for near in range(peers // 2) for d in sorted({peers // 2 - near, peers // 2 + near})]
    return [pltpu.make_async_remote_copy(
        src_ref=x_ref.at[lax.rem(me + d, peers)], dst_ref=out_ref.at[me], send_sem=send_sem.at[d - 1], recv_sem=recv_sem.at[d - 1],
        device_id=peer_at(d, peers), device_id_type=pl.DeviceIdType.MESH) for d in order]


def swap_start(x_ref, out_ref, own, send_sem, recv_sem, own_sem, peers):
    me = lax.axis_index("sp")
    for copy in swap_copies(x_ref, out_ref, send_sem, recv_sem, peers):
        copy.start()
    take = pltpu.make_async_copy(x_ref.at[me], own, own_sem)
    take.start()
    take.wait()
    pltpu.make_async_copy(own, out_ref.at[me], own_sem).start()


def swap_wait(x_ref, out_ref, own, send_sem, recv_sem, own_sem, peers):
    pltpu.make_async_copy(own, out_ref.at[lax.axis_index("sp")], own_sem).wait()
    for copy in swap_copies(x_ref, out_ref, send_sem, recv_sem, peers):
        copy.wait()


def swap_scratch(x):
    peers = x.shape[0]
    return [pltpu.VMEM(x.shape[1:], x.dtype), pltpu.SemaphoreType.DMA((peers - 1,)), pltpu.SemaphoreType.DMA((peers - 1,)),
            pltpu.SemaphoreType.DMA]


STEP = (1, -1)


def hops(ring, s, w):
    return ring // 2 - (s != w)


def ring_gather(block, own, sems, peers, cuts):
    ring = peers // 2
    me = lax.axis_index("sp")
    z, c = me // 2, me % 2
    send_sem, recv_sem, over_sem, came_sem = sems
    turn = lambda k: lax.rem(z + k + 2 * ring, ring)
    lots = [(s, w, u) for u in range(cuts) for w in range(2) for s in range(2)]

    def copy(src, dst, one, two, to):
        return pltpu.make_async_remote_copy(src_ref=src, dst_ref=dst, send_sem=one, recv_sem=two, device_id={"sp": to},
                                            device_id_type=pl.DeviceIdType.MESH)

    def along(s, w, t, u):
        ref = block(turn(-STEP[s] * t), c, w, u)
        return copy(own(w, u) if t == 0 else ref, ref, send_sem.at[s, w, t, u], recv_sem.at[s, w, t, u], 2 * turn(STEP[s]) + c)

    def across(s, w, t, u, side):
        ref = block(turn(-STEP[s] * t), side, w, u)
        return copy(own(w, u) if t == 0 and side is c else ref, ref, over_sem.at[s, w, t, u], came_sem.at[s, w, t, u], 2 * z + 1 - c)

    home = [(0, w, 0, u) for u in range(cuts) for w in range(2)]
    moved = [(s, w, t, u) for t in range(1, ring // 2 + 1) for s, w, u in lots if t <= hops(ring, s, w)]

    def start(only=None):
        for s, w, u in lots:
            if only in (None, (w, u)):
                along(s, w, 0, u).start()
        for lot in home:
            if only in (None, (lot[1], lot[3])):
                across(*lot, c).start()

    def run(lo=1, hi=ring):
        for s, w, t, u in moved:
            if lo <= t < hi:
                along(s, w, t - 1, u).wait_recv()
                if t < hops(ring, s, w):
                    along(s, w, t, u).start()
                across(s, w, t, u, c).start()

    def finish():
        for s, w, t, u in moved:
            along(s, w, t - 1, u).wait_send()
        for lot in home + moved:
            across(*lot, c).wait_send()
            across(*lot, 1 - c).wait_recv()

    return start, run, finish


def ring_scratch(peers, cuts):
    dma = pltpu.SemaphoreType.DMA
    return [dma((2, 2, peers // 4, cuts))] * 2 + [dma((2, 2, peers // 4 + 1, cuts))] * 2


def opening_body(x_hbm, dy_hbm, wo_hbm, gain_ref, bias_ref, pos_ref, keep_ref, marks_all, do_t, x_all, *refs, peers, batch, cuts):
    x_out, do_out = refs[:batch - 1], refs[batch - 1:2 * batch - 2]
    x_ref, dy_ref, x_own, do_own, wo_ref, marks_ref, own, ds_sem, dr_sem, do_sem, ms_sem, mr_sem, in_sem = refs[2 * batch - 2:2 * batch + 11]
    ring_sems = refs[2 * batch + 11:]
    gain, bias = gain_ref[...].reshape(1, -1), bias_ref[...].reshape(1, -1)
    me = lax.axis_index("sp")
    tok, dim = x_own.shape[0], do_own.shape[1]
    lot = tok // 2 // cuts
    rows_of = lambda w, u: pl.ds((w * cuts + u) * lot, lot)
    arrived = greet(peers)
    loads = [pltpu.make_async_copy(x_hbm.at[b], x_ref.at[b], in_sem.at[b]) for b in range(batch)]
    loads += [pltpu.make_async_copy(dy_hbm, dy_ref, in_sem.at[batch]), pltpu.make_async_copy(wo_hbm, wo_ref, in_sem.at[batch + 1])]
    for load in loads:
        load.start()

    def norm_rows(b, out_ref, rows):
        x = x_ref[b, rows, :].astype(F32)
        cen = x - jnp.mean(x, axis=-1, keepdims=True)
        hat = cen * lax.rsqrt(jnp.mean(cen * cen, axis=-1, keepdims=True) + NORM_EPS)
        out_ref[rows, :] = (hat * gain + bias).astype(BF16)

    def norm(b, out_ref):
        loads[b].wait()

        @pl.loop(0, tok // 32)
        def _(k):
            norm_rows(b, out_ref, pl.ds(pl.multiple_of(k * 32, 32), 32))

    def product(b, out_ref):
        @pl.loop(0, peers // 4)
        def _(g):
            rows = pl.ds(pl.multiple_of(g * 4 * dim, 4 * dim), 4 * dim)
            out_ref[pl.ds(g * 4, 4)] = lax.dot_general(wo_ref[rows, :], dy_ref[b], NT, preferred_element_type=F32).astype(BF16).reshape(4, dim, tok)

    marks_ref[...] = jnp.zeros_like(marks_ref)
    packed = 2 * pos_ref[...] + keep_ref[...]
    sub = tok // 128
    for b in range(batch):
        for k in range(sub):
            marks_ref[b * sub + k:b * sub + k + 1, :] = packed[b:b + 1, k * 128:(k + 1) * 128]
    block = lambda k, side, w, u: x_all.at[2 * k + side, rows_of(w, u)]
    start, run, finish = ring_gather(block, lambda w, u: x_own.at[rows_of(w, u)], ring_sems, peers, cuts)
    loads[0].wait()
    pieces = [(w, u) for u in range(cuts) for w in range(2)]
    for k, piece in enumerate(pieces):
        norm_rows(0, x_own, rows_of(*piece))
        if k == 1:
            arrived()
        if k:
            start(pieces[k - 1])
    start(pieces[-1])
    keep = pltpu.make_async_copy(x_own, x_all.at[me], in_sem.at[batch + 2])
    keep.start()
    marks = [pltpu.make_async_remote_copy(
        src_ref=marks_ref, dst_ref=marks_all.at[me], send_sem=ms_sem.at[d - 1], recv_sem=mr_sem.at[d - 1],
        device_id=peer_at(d, peers), device_id_type=pl.DeviceIdType.MESH) for d in range(1, peers)]
    for copy in marks:
        copy.start()
    marks_all[me] = marks_ref[...]
    loads[-2].wait()
    loads[-1].wait()
    product(0, do_own)
    for b in range(1, batch):
        norm(b, x_out[b - 1])
    swap_start(do_own, do_t, own, ds_sem, dr_sem, do_sem, peers)
    for b in range(1, batch):
        product(b, do_out[b - 1])
    run()
    keep.wait()
    for copy in marks:
        copy.wait()
    swap_wait(do_own, do_t, own, ds_sem, dr_sem, do_sem, peers)
    finish()


def opening(x, dy, w_out, gain, bias, pos, keep, peers, collective_id, cuts=8):
    batch, tok, hidden = x.shape
    dim = hidden // peers
    hbm, vmem = pl.BlockSpec(memory_space=pltpu.HBM), pl.BlockSpec(memory_space=pltpu.VMEM)
    dma = pltpu.SemaphoreType.DMA
    do_shape, x_shape = jax.ShapeDtypeStruct((peers, dim, tok), BF16), jax.ShapeDtypeStruct((tok, hidden), BF16)
    res = pl.pallas_call(
        functools.partial(opening_body, peers=peers, batch=batch, cuts=cuts),
        name="opening",
        out_shape=[jax.ShapeDtypeStruct((peers, 8, 128), pos.dtype), do_shape, jax.ShapeDtypeStruct((peers, tok, hidden), BF16)]
        + [x_shape] * (batch - 1) + [do_shape] * (batch - 1),
        in_specs=[hbm, hbm, hbm, vmem, vmem, vmem, vmem],
        out_specs=[vmem, hbm, hbm] + [vmem] * (2 * batch - 2),
        scratch_shapes=[pltpu.VMEM(x.shape, BF16), pltpu.VMEM(dy.shape, BF16), pltpu.VMEM(x_shape.shape, BF16), pltpu.VMEM(do_shape.shape, BF16),
                        pltpu.VMEM(w_out.shape, BF16), pltpu.VMEM((8, 128), pos.dtype)] + swap_scratch(do_shape)
        + [dma((peers - 1,)), dma((peers - 1,)), dma((batch + 3,))] + ring_scratch(peers, cuts),
        cost_estimate=pl.CostEstimate(flops=5 * 10**10, bytes_accessed=16 << 20, transcendentals=0),
        compiler_params=pltpu.CompilerParams(collective_id=collective_id, has_side_effects=True, vmem_limit_bytes=VMEM_LIMIT),
    )(x, dy, w_out, gain, bias, pos, keep)
    return res[0], res[1], res[2], res[3:2 + batch], res[2 + batch:]


TN = (((0,), (0,)), ((), ()))


def tail_a_body(dqkv_ref, oo_hbm, on_hbm, dy_hbm, x_hbm, wo_hbm, d_hbm, w_hbm, gain_ref, bo_ref, y_ref, gx_ref, part, rows_ref,
                o_old, o_new, dy_ref, x_ref, wo_ref, d_old, w_ref, d_new, dn, sums, bo_rep, both, mine, landed, own_d,
                ds_sem, dr_sem, do_sem, ps_sem, pr_sem, rs_sem, rr_sem, w_sem, *, peers, cuts):
    ring = peers // 2
    me = lax.axis_index("sp")
    z, c = me // 2, me % 2
    _, tok, hidden = x_ref.shape
    half, wide, few = hidden // 2, hidden // 3, part.shape[0] // cuts
    cols = (pl.ds(0, half), pl.ds(half, half))
    at = lambda zz, cc: {"sp": 2 * zz + cc}
    turn = lambda k: lax.rem(z + k + 2 * ring, ring)
    remote = functools.partial(pltpu.make_async_remote_copy, device_id_type=pl.DeviceIdType.MESH)
    span, group = d_old.shape[1], 8
    gain, b_out = gain_ref[...].reshape(1, hidden), bo_ref[...].reshape(1, hidden)
    pairs = ((oo_hbm, o_old), (on_hbm, o_new), (dy_hbm, dy_ref), (x_hbm, x_ref), (wo_hbm, wo_ref), (d_hbm, d_old), (w_hbm, w_ref))
    loads = [pltpu.make_async_copy(src, dst, w_sem.at[k]) for k, (src, dst) in enumerate(pairs)]
    swap = (dqkv_ref, d_new, own_d, ds_sem, dr_sem, do_sem, peers)
    arrived = greet(peers)
    for load in loads:
        load.start()
    arrived()
    swap_start(*swap)
    for load in loads[:3]:
        load.wait()

    def product(put, side):
        @pl.loop(0, ring)
        def _(k):
            h = 2 * k + side
            put(k, jnp.dot(o_old[h], dy_ref[0], preferred_element_type=F32)
                + jnp.dot(o_new[h], dy_ref[1], preferred_element_type=F32))

    def put_other(k, value):
        both[k, 1 - c] = value

    def put_mine(k, value):
        mine[k] = value

    def forward(b, o_ref):
        o_t = o_ref[...].reshape(hidden, tok)

        @pl.loop(0, 3)
        def _(n):
            at_n = pl.ds(pl.multiple_of(n * wide, wide), wide)
            acc = lax.dot_general(o_t, wo_ref[:, at_n], TN, preferred_element_type=F32)
            y_ref[b, :, at_n] = (x_ref[b, :, at_n].astype(F32) + acc + bo_rep[0:1, at_n]).astype(BF16)

    def backward(b, d_ref):
        @pl.loop(0, 3)
        def _(n):
            at_n = pl.ds(pl.multiple_of(n * wide, wide), wide)
            acc = None
            for k in range(0, peers, group):
                lhs = d_ref[k:k + group].reshape(-1, tok)
                one = lax.dot_general(lhs, w_ref[k * span:(k + group) * span, at_n], TN, preferred_element_type=F32)
                acc = one if acc is None else acc + one
            dn[:, at_n] = acc

        @pl.loop(0, tok // 32)
        def _(k):
            rows = pl.ds(pl.multiple_of(k * 32, 32), 32)
            x = x_ref[b, rows, :].astype(F32)
            dy = dy_ref[b, rows, :].astype(F32)
            d = dn[rows, :]
            cen = x - jnp.mean(x, axis=-1, keepdims=True)
            inv = lax.rsqrt(jnp.mean(cen * cen, axis=-1, keepdims=True) + NORM_EPS)
            hat = cen * inv
            for n, one in enumerate((d * hat, d, dy)):
                sums[n] += jnp.sum(one.reshape(4, 8, hidden), axis=0)
            e = d * gain
            m1 = jnp.mean(e, axis=-1, keepdims=True)
            m2 = jnp.mean(e * hat, axis=-1, keepdims=True)
            gx_ref[b, rows, :] = (dy + inv * (e - m1 - hat * m2)).astype(BF16)

    bo_rep[...] = jnp.broadcast_to(b_out, bo_rep.shape)
    sums[...] = jnp.zeros_like(sums)
    product(put_other, 1 - c)
    pair_copy = lambda side: remote(src_ref=both.at[:, side], dst_ref=both.at[:, side], send_sem=ps_sem, recv_sem=pr_sem, device_id=at(z, 1 - c))
    product(put_mine, c)
    pair_copy(1 - c).start()
    pair_copy(1 - c).wait_send()
    pair_copy(c).wait_recv()

    @pl.loop(0, ring)
    def _(k):
        mine[k] = mine[k] + both[k, c]

    lots = [(s, w, u) for u in range(cuts) for w in range(2) for s in range(2)]

    def reduce_copy(s, w, t, u):
        return remote(src_ref=mine.at[turn(STEP[s] * (hops(ring, s, w) - t)), pl.ds(u * few, few), cols[w]], dst_ref=landed.at[s, w, t, u],
                      send_sem=rs_sem.at[s, w, t, u], recv_sem=rr_sem.at[s, w, t, u], device_id=at(turn(STEP[s]), c))

    def fold(s, w, t, u):
        reduce_copy(s, w, t, u).wait_recv()
        at_k = (turn(STEP[s] * (hops(ring, s, w) - t - 1)), pl.ds(u * few, few), cols[w])
        mine[at_k] = mine[at_k] + landed[s, w, t, u]

    def hop(t):
        for s, w, u in lots:
            if t < hops(ring, s, w):
                fold(s, w, t - 1, u)
                reduce_copy(s, w, t, u).start()

    for s, w, u in lots:
        reduce_copy(s, w, 0, u).start()
    for load in loads[3:5]:
        load.wait()
    forward(0, o_old)
    forward(1, o_new)
    for load in loads[5:]:
        load.wait()
    backward(0, d_old)
    for t in range(1, ring // 2 - 1):
        hop(t)
    swap_wait(*swap)
    backward(1, d_new)
    hop(ring // 2 - 1)
    rows_ref[...] = jnp.zeros_like(rows_ref)
    for n in range(3):
        rows_ref[n:n + 1, :] = jnp.sum(sums[n], axis=0, keepdims=True)
    for s, w, u in lots:
        fold(s, w, hops(ring, s, w) - 1, u)
    part[...] = mine[z]
    for s, w, u in lots:
        for t in range(hops(ring, s, w)):
            reduce_copy(s, w, t, u).wait_send()


def tail_a(dqkv, d_old, o_old, o_new, dy, x, w_flat, w_out, gain, b_out, collective_id, cuts=4):
    peers, dim, tok = o_old.shape
    ring = peers // 2
    hidden = dy.shape[-1]
    hbm, vmem = pl.BlockSpec(memory_space=pltpu.HBM), pl.BlockSpec(memory_space=pltpu.VMEM)
    dma = pltpu.SemaphoreType.DMA
    held = lambda a: pltpu.VMEM(a.shape, a.dtype)
    steps = (2, 2, ring // 2, cuts)
    return pl.pallas_call(
        functools.partial(tail_a_body, peers=peers, cuts=cuts),
        name="tail_a",
        out_shape=[jax.ShapeDtypeStruct(x.shape, BF16), jax.ShapeDtypeStruct(x.shape, BF16), jax.ShapeDtypeStruct((dim, hidden), F32),
                   jax.ShapeDtypeStruct((8, hidden), F32)],
        in_specs=[hbm] * 8 + [vmem] * 2,
        out_specs=[vmem] * 4,
        scratch_shapes=[held(a) for a in (o_old, o_new, dy, x, w_out, d_old, w_flat, dqkv)]
        + [pltpu.VMEM((tok, hidden), F32), pltpu.VMEM((3, 8, hidden), F32), pltpu.VMEM((8, hidden), F32),
           pltpu.VMEM((ring, 2, dim, hidden), F32), pltpu.VMEM((ring, dim, hidden), F32), pltpu.VMEM(steps + (dim // cuts, hidden // 2), F32),
           pltpu.VMEM(dqkv.shape[1:], BF16), dma((peers - 1,)), dma((peers - 1,)), dma, dma, dma, dma(steps), dma(steps), dma((7,))],
        cost_estimate=pl.CostEstimate(flops=10**11, bytes_accessed=64 << 20, transcendentals=0),
        compiler_params=pltpu.CompilerParams(collective_id=collective_id, has_side_effects=True, vmem_limit_bytes=VMEM_LIMIT),
    )(dqkv, o_old, o_new, dy, x, w_out, d_old, w_flat, gain, b_out)


def tail_b_body(part, rows_ref, gb_ref, full, total, gb_all, stage, xs_sem, xr_sem, *ring_sems, peers, cuts):
    ring = peers // 2
    me = lax.axis_index("sp")
    z, c = me // 2, me % 2
    hidden = part.shape[1]
    half, few = hidden // 2, part.shape[0] // cuts
    cols = (pl.ds(0, half), pl.ds(half, half))
    remote = functools.partial(pltpu.make_async_remote_copy, device_id_type=pl.DeviceIdType.MESH)
    arrived = greet(peers)
    full[z, c] = part[...]
    gb_all[me] = gb_ref[...]
    block = lambda k, side, w, u: full.at[k, side, pl.ds(u * few, few), cols[w]]
    start, run, finish = ring_gather(block, lambda w, u: block(z, c, w, u), ring_sems, peers, cuts)
    owners = hidden // 128
    lanes = lambda k: pl.ds(pl.multiple_of(k * 128, 128), 128)

    def small_copy(kind, frm, to):
        src, dst = ((rows_ref.at[:, lanes(to)], stage.at[frm]), (total.at[:, lanes(frm)],) * 2, (gb_ref, gb_all.at[frm]))[kind]
        return remote(src_ref=src, dst_ref=dst, send_sem=xs_sem.at[kind, to], recv_sem=xr_sem.at[kind, frm], device_id={"sp": to})

    def each(act, kind, only_to=False, only_from=False):
        @pl.loop(1, peers)
        def _(d):
            far = lax.rem(me + d, peers)

            def go():
                act(kind, far)

            if only_to:
                pl.when(far < owners)(go)
            elif only_from:
                pl.when(me < owners)(go)
            else:
                go()

    send = lambda kind, far: small_copy(kind, me, far).start()
    over = lambda kind, far: small_copy(kind, me, far).wait_send()
    came = lambda kind, far: small_copy(kind, far, me).wait_recv()

    @pl.when(me < owners)
    def _():
        stage[me] = rows_ref[:, lanes(me)]

    arrived()
    start()
    each(send, 0, only_to=True)
    each(send, 2)
    run(1, 2)
    each(came, 0, only_from=True)

    @pl.when(me < owners)
    def _():
        total[:, lanes(me)] = jnp.sum(stage[...], axis=0)

    each(send, 1, only_from=True)
    run(2)
    each(came, 1, only_to=True)
    each(came, 2)
    each(over, 0, only_to=True)
    each(over, 1, only_from=True)
    each(over, 2)
    finish()


def tail_b(part, rows, gb, peers, collective_id, cuts=4):
    ring = peers // 2
    vmem = pl.BlockSpec(memory_space=pltpu.VMEM)
    dma = pltpu.SemaphoreType.DMA
    return pl.pallas_call(
        functools.partial(tail_b_body, peers=peers, cuts=cuts),
        name="tail_b",
        out_shape=[jax.ShapeDtypeStruct((ring, 2) + part.shape, F32), jax.ShapeDtypeStruct(rows.shape, F32),
                   jax.ShapeDtypeStruct((peers,) + gb.shape, F32)],
        in_specs=[vmem] * 3,
        out_specs=[vmem] * 3,
        scratch_shapes=[pltpu.VMEM((peers, 8, 128), F32), dma((3, peers)), dma((3, peers))] + ring_scratch(peers, cuts),
        cost_estimate=pl.CostEstimate(flops=5 * 10**10, bytes_accessed=10 << 20, transcendentals=0),
        compiler_params=pltpu.CompilerParams(collective_id=collective_id, has_side_effects=True, vmem_limit_bytes=32 << 20),
    )(part, rows, gb)


def settle_body(*refs, n_in, first, n_plain, n_held):
    x_ref, plain, held = refs[0], refs[1:1 + n_plain], refs[1 + n_plain:1 + n_plain + n_held]
    outs = refs[n_in:n_in + 1 + n_plain + n_held]
    buf, in_sem, out_sem, in_plain, out_plain, *rooms = refs[n_in + 1 + n_plain + n_held:]
    heads, n = x_ref.shape[:2]
    copy = pltpu.make_async_copy
    reads = [copy(x_ref.at[h], buf.at[h], in_sem.at[h]) for h in range(heads)]
    writes = [copy(buf.at[h], outs[0].at[h, pl.ds(first, n)], out_sem.at[h]) for h in range(heads)]
    reads += [copy(plain[k], rooms[k], in_plain.at[k]) for k in range(n_plain)]
    writes += [copy(rooms[k], outs[1 + k], out_plain.at[k]) for k in range(n_plain)]
    flat = [copy(held[k], outs[1 + n_plain + k], out_plain.at[n_plain + k]) for k in range(n_held)]
    for one in reads + flat:
        one.start()
    for read, write in zip(reads, writes):
        read.wait()
        write.start()
    for one in writes + flat:
        one.wait()


def settle(x, into, plain, held, span, first):
    heads, n, hidden = x.shape
    hbm, vmem = pl.BlockSpec(memory_space=pltpu.HBM), pl.BlockSpec(memory_space=pltpu.VMEM)
    pin = lambda a: pltpu.with_memory_space_constraint(a, pltpu.HBM)
    args = (pin(x), *[pin(a) for a in plain], *held) + (() if into is None else (into,))
    dma = pltpu.SemaphoreType.DMA
    extra = max(len(plain) + len(held), 1)
    return pl.pallas_call(
        functools.partial(settle_body, n_in=len(args), first=first, n_plain=len(plain), n_held=len(held)), name="settle",
        out_shape=[jax.ShapeDtypeStruct((heads, span, hidden), x.dtype)] + [jax.ShapeDtypeStruct(a.shape, a.dtype) for a in (*plain, *held)],
        in_specs=[hbm] * (1 + len(plain)) + [vmem] * len(held) + [hbm] * (into is not None),
        out_specs=[hbm] * (1 + len(plain) + len(held)),
        input_output_aliases={} if into is None else {len(args) - 1: 0},
        scratch_shapes=[pltpu.VMEM(x.shape, x.dtype), dma((heads,)), dma((heads,)), dma((extra,)), dma((extra,))]
        + [pltpu.VMEM(a.shape, a.dtype) for a in plain],
        cost_estimate=pl.CostEstimate(flops=10**9, bytes_accessed=8 * x.size, transcendentals=0),
        compiler_params=pltpu.CompilerParams(vmem_limit_bytes=24 << 20))(*args)


def lay_body(go_ref, total, gb_all, go_out, gb_out, *refs):
    vectors, sem = refs[:-1], refs[-1]
    copies = [pltpu.make_async_copy(go_ref.at[k], go_out.at[k], sem.at[k]) for k in range(go_ref.shape[0])]
    for copy in copies:
        copy.start()
    for k in range(3):
        gb_out[k] = gb_all[:, k, 0:gb_out.shape[2]]
        vectors[k][...] = total[k]
    for copy in copies:
        copy.wait()


def lay_down(go, total, gb_all):
    hbm, vmem = pl.BlockSpec(memory_space=pltpu.HBM), pl.BlockSpec(memory_space=pltpu.VMEM)
    ring, _, dim, hidden = go.shape
    return pl.pallas_call(
        lay_body, name="lay_down",
        out_shape=[jax.ShapeDtypeStruct(go.shape, F32), jax.ShapeDtypeStruct((3, 2 * ring, dim), F32)] + [jax.ShapeDtypeStruct((hidden,), F32)] * 3,
        in_specs=[vmem] * 3, out_specs=[hbm] + [vmem] * 4,
        scratch_shapes=[pltpu.SemaphoreType.DMA((ring,))],
        cost_estimate=pl.CostEstimate(flops=10**9, bytes_accessed=8 * go.size, transcendentals=0),
        compiler_params=pltpu.CompilerParams(vmem_limit_bytes=24 << 20))(go, total, gb_all)


def solution(mesh):
    peers = mesh.shape["sp"]

    def block_fn(x_blk, pos_blk, keep_blk, ln_gain, ln_bias, w_qkv, b_qkv, w_out, b_out, dy_blk):
        batch, tok, hidden = x_blk.shape
        heads, dim = w_qkv.shape[1], w_qkv.shape[3]
        assert heads == peers
        seq = tok * peers
        blk = 2 * tok
        w_all = jnp.transpose(w_qkv, (1, 2, 3, 0)).reshape(heads, 3 * dim, hidden)
        b_all = jnp.transpose(b_qkv, (1, 0, 2))
        marks, do_first, x_first, x_rest, do_rest = opening(x_blk, dy_blk, w_out, ln_gain, ln_bias, pos_blk, keep_blk, peers, 1)
        xs = [x_first.reshape(seq, hidden)] + [lax.all_gather(one, "sp", axis=0, tiled=True) for one in x_rest]
        do_t = [do_first]
        lead = 7 * dim // 3
        gw, att = (), []
        for b in range(batch):
            old = list(do_rest[b:b + 1]) if b + 1 < batch else att
            att_d, gw, gb, att_o, swapped = attention(w_all, b_all, do_t[b], marks, xs[b], gw, old, blk=blk, tok=tok, which=b, batch=batch, lead=lead,
                                                      send_o=b + 1 == batch, collective_id=4 + b)
            if b + 1 < batch:
                do_t.append(swapped[0])
            att = [att_o, att_d]
        o_old, d_old = swapped
        gw_all = [lax.all_gather(one, "sp", axis=0, tiled=True).reshape(heads, -1, hidden) for one in gw[:2]]
        y, gx, part, rows = tail_a(att_d, d_old, o_old, att_o, dy_blk, x_blk, w_all.reshape(3 * hidden, hidden), w_out, ln_gain, b_out, 2)
        go_all, gb_all, g_gain, g_bias, g_out = lay_down(*tail_b(part, rows, gb, peers, 3))
        first, y, gx, go_all = lax.optimization_barrier((gw_all[0], y, gx, go_all))
        gw_out, y, gx = settle(first, None, (y, gx), (), 3 * dim, 0)
        second, gw_out, go_all = lax.optimization_barrier((gw_all[1], gw_out, go_all))
        gw_out, = settle(second, gw_out, (), (), 3 * dim, lead)
        gw_out = jnp.transpose(gw_out.reshape(heads, 3, dim, hidden), (3, 0, 1, 2))
        return y, gx, gw_out, jnp.transpose(gb_all, (1, 0, 2)), go_all.reshape(hidden, hidden), g_out, g_gain, g_bias

    act_spec = P("dp", "sp", None)
    tok_spec = P("dp", "sp")
    in_specs = (act_spec, tok_spec, tok_spec, P(), P(), P(), P(), P(), P(), act_spec)
    out_specs = (act_spec, act_spec, P("dp", None, None, None), P("dp", None, None), P("dp", None), P("dp"), P("dp"), P("dp"))
    return jax.shard_map(block_fn, mesh=mesh, in_specs=in_specs, out_specs=out_specs, check_vma=False)
```

```python
import functools
import jax
import jax.numpy as jnp
from jax import lax
from jax.experimental import pallas as pl
from jax.experimental.pallas import tpu as pltpu
from jax.sharding import PartitionSpec as P

NORM_EPS = 1e-5

LOG2E = 1.4426950408889634
MASKED = -1e30
VMEM_LIMIT = 62 << 20
F32, BF16 = jnp.float32, jnp.bfloat16
NT = (((1,), (1,)), ((), ()))


def attn_body(w_hbm, b_ref, dot_ref, marks_ref, x_ref, *refs, blk, tok, which, batch, n_swap, n_old, send_o):
    peers = dot_ref.shape[0]
    gw_old, old, refs = refs[:n_old], refs[n_old:n_old + n_swap], refs[n_old + n_swap:]
    (dqkv_ref, gwa_ref, gwb_ref, gb_ref, gbt_ref, o_out), got, refs = refs[:6], refs[6:6 + n_swap], refs[6 + n_swap:]
    x_buf, refs = refs[0], refs[1:]
    w_ref, b_rep, qkvt_ref, k_tok, v_tok, posk_ref, s_buf, m_buf, q_pad, do_pad, o_acc, dq_acc, dk_acc, dv_acc, x_sem, w_sem = refs[:16]
    swaps = [(old[k], got[k]) + refs[16 + 4 * k:20 + 4 * k] for k in range(n_swap)]
    if send_o:
        o_ref, os_sem, or_sem, out_sem, o_new, *landed = refs[16 + 4 * n_swap:]
        swaps = [(one[0], land) + one[2:] for one, land in zip(swaps, landed)]
    else:
        o_ref = o_out
    dim, lead = dot_ref.shape[1], gwa_ref.shape[0]
    seq = dot_ref.shape[0] * tok
    pad = k_tok.shape[1] - dim
    nq = blk // tok
    steps = seq // blk
    scale = dim ** -0.5
    me = lax.axis_index("sp")
    step = pl.program_id(0)
    i = lax.rem(me // nq + step, steps)
    half = blk // 2
    sub = tok // 128

    def spread(row):
        return jnp.transpose(jnp.broadcast_to(row, (128, 128)))

    def x_copy(k):
        rows = pl.ds(pl.multiple_of(k * blk, blk), blk)
        return pltpu.make_async_copy(x_ref.at[rows], x_buf.at[rows], x_sem.at[k])

    def o_send(to):
        return pltpu.make_async_remote_copy(
            src_ref=o_ref.at[to], dst_ref=o_new.at[me], send_sem=os_sem.at[to], recv_sem=or_sem.at[me],
            device_id={"sp": to}, device_id_type=pl.DeviceIdType.MESH)

    def o_keep():
        return pltpu.make_async_copy(o_ref.at[me], o_new.at[me], os_sem.at[me])

    def o_start(at):
        for t in range(nq):
            to = lax.rem(me // nq + at, steps) * nq + t

            @pl.when(to != me)
            def _():
                o_send(to).start()

            @pl.when(to == me)
            def _():
                o_keep().start()

    @pl.when(step == 0)
    def _():
        w_load = pltpu.make_async_copy(w_hbm.at[me], w_ref, w_sem)
        w_load.start()
        for k in range(steps):
            x_copy(k).start()
        meet(peers)
        for one in swaps:
            swap_start(*one, peers)
        dk_acc[...] = jnp.zeros_like(dk_acc)
        dv_acc[...] = jnp.zeros_like(dv_acc)
        q_pad[...] = jnp.zeros_like(q_pad)
        do_pad[...] = jnp.zeros_like(do_pad)
        mine = lax.broadcasted_iota(jnp.int32, (peers, dim), 0) == me
        for k in range(3):
            row = jnp.sum(jnp.where(mine, b_ref[k], 0.0), axis=0, keepdims=True)
            b_rep[k * dim:(k + 1) * dim, :] = spread(jnp.concatenate([row, jnp.zeros((1, pad), F32)], axis=1))[0:dim]
        w_load.wait()

        @pl.loop(0, steps)
        def _(k):
            rows = pl.ds(pl.multiple_of(k * blk, blk), blk)
            x_copy(k).wait()
            shift = jnp.concatenate([b_rep[...]] * (blk // 128), axis=1)
            qkvt_ref[:, rows] = (lax.dot_general(w_ref[...], x_buf[rows, :], NT, preferred_element_type=F32) + shift).astype(BF16)

            for t in range(blk // 128):
                cols = pl.ds(pl.multiple_of(k * blk + t * 128, 128), 128)
                for base, dst in ((dim, k_tok), (2 * dim, v_tok)):
                    part = qkvt_ref[base:base + dim, cols].astype(F32)
                    whole = jnp.concatenate([part, jnp.zeros((pad, 128), F32)], axis=0)
                    dst[cols, :] = jnp.transpose(whole).astype(BF16)
                mark = marks_ref[k * nq + t // sub, which * sub + t % sub:which * sub + t % sub + 1, :]
                pos, keep = lax.shift_right_logical(mark, 1).astype(F32), mark & 1
                posk_ref[cols, :] = spread(jnp.where(keep > 0, pos, MASKED))

    if send_o:
        @pl.when(step > 0)
        def _():
            o_start(step - 1)

    qcols = pl.ds(pl.multiple_of(i * blk, blk), blk)
    q_pad[0:dim, :] = qkvt_ref[0:dim, qcols]
    for t in range(nq):
        do_pad[0:dim, t * tok:(t + 1) * tok] = dot_ref[i * nq + t]
    slope2 = jnp.exp2(jnp.full((1, 128), -8.0 / peers, F32) * (me + 1).astype(F32)) * LOG2E
    first = lax.shift_right_logical(marks_ref[i * nq, which * sub:which * sub + 1, :], 1).astype(F32)
    ref_pos = jnp.broadcast_to(first[:, 0:1], (1, 128))
    c = scale * LOG2E

    def scores(j, carry, diag):
        m, l8 = carry
        for sub in range(2):
            rows = pl.ds(pl.multiple_of(j * blk + sub * half, half), half)
            st = jnp.dot(k_tok[rows, :], q_pad[...], preferred_element_type=F32)
            bias = (posk_ref[rows, :] - ref_pos) * slope2
            st = st * c + jnp.concatenate([bias] * (blk // 128), axis=1)
            if diag:
                key = lax.broadcasted_iota(jnp.int32, (half, blk), 0) + sub * half
                qry = lax.broadcasted_iota(jnp.int32, (half, blk), 1)
                st = jnp.where(key <= qry, st, MASKED)
            m_new = jnp.maximum(m, jnp.max(st, axis=0, keepdims=True))
            e = jnp.exp2(st - m_new)
            s_buf[rows, :] = e
            m_buf[2 * j + sub] = jnp.broadcast_to(m_new, (8, blk))
            l8 = l8 * jnp.exp2(m - m_new) + jnp.sum(e.reshape(half // 8, 8, blk), axis=0)
            m = m_new
        return m, l8

    start = (jnp.full((1, blk), MASKED, F32), jnp.zeros((8, blk), F32))
    m, l8 = scores(i, lax.fori_loop(0, i, lambda j, carry: scores(j, carry, False), start), True)
    inv = 1.0 / jnp.sum(l8, axis=0, keepdims=True)
    o_acc[...] = jnp.zeros_like(o_acc)
    dq_acc[...] = jnp.zeros_like(dq_acc)

    def values(j, _):
        rows = pl.ds(pl.multiple_of(j * blk, blk), blk)
        pbs = []
        for sub in range(2):
            part = pl.ds(pl.multiple_of(j * blk + sub * half, half), half)
            p = s_buf[part, :] * (jnp.exp2(m_buf[2 * j + sub][0:1, :] - m) * inv)
            s_buf[part, :] = p
            pbs.append(p.astype(BF16))
        pb = jnp.concatenate(pbs, axis=0)
        o_acc[...] += jnp.dot(qkvt_ref[2 * dim:3 * dim, rows], pb, preferred_element_type=F32)
        dv_acc[:, rows] += lax.dot_general(do_pad[0:dim, :], pb, NT, preferred_element_type=F32)
        return 0

    lax.fori_loop(0, i + 1, values, 0)
    o_lo = o_acc[...].astype(BF16)
    do_f = do_pad[0:dim, :].astype(F32)
    r = jnp.sum(do_f * o_lo.astype(F32), axis=0, keepdims=True)

    def grads(j, _):
        rows = pl.ds(pl.multiple_of(j * blk, blk), blk)
        g = jnp.dot(v_tok[rows, :], do_pad[...], preferred_element_type=F32)
        ds = (s_buf[rows, :] * (g - r)).astype(BF16)
        dq_acc[...] += jnp.dot(qkvt_ref[dim:2 * dim, rows], ds, preferred_element_type=F32)
        dk_acc[:, rows] += lax.dot_general(q_pad[0:dim, :], ds, NT, preferred_element_type=F32)
        return 0

    lax.fori_loop(0, i + 1, grads, 0)
    dq_lo = (dq_acc[...] * scale).astype(BF16)
    for t in range(nq):
        o_ref[i * nq + t] = o_lo[:, t * tok:(t + 1) * tok]
        dqkv_ref[i * nq + t, 0:dim] = dq_lo[:, t * tok:(t + 1) * tok]

    @pl.when(step == steps - 1)
    def _():
        @pl.loop(0, seq // tok)
        def _(t):
            cols = pl.ds(pl.multiple_of(t * tok, tok), tok)
            dqkv_ref[t, dim:2 * dim] = (dk_acc[:, cols] * scale).astype(BF16)
            dqkv_ref[t, 2 * dim:3 * dim] = dv_acc[:, cols].astype(BF16)

        if send_o:
            o_start(step)
        for k, ref in enumerate((gwa_ref, gwb_ref, gb_ref)):
            ref[...] = gw_old[k][...] if n_old else jnp.zeros_like(ref)
        ones = jnp.ones((blk, 128), BF16)

        @pl.loop(0, steps)
        def _(j):
            rows = pl.ds(pl.multiple_of(j * blk, blk), blk)
            for ref, lo, hi in ((gwa_ref, 0, lead), (gwb_ref, lead, 3 * dim)):
                lhs = jnp.concatenate([dqkv_ref[j * nq + t, lo:hi] for t in range(nq)], axis=1)
                ref[...] += jnp.dot(lhs, x_buf[rows, :], preferred_element_type=F32)
                gb_ref[lo:hi, :] += jnp.dot(lhs, ones, preferred_element_type=F32)

        gbt_ref[...] = jnp.zeros_like(gbt_ref)
        for k in range(3):
            part = jnp.concatenate([gb_ref[k * dim:(k + 1) * dim, :], jnp.zeros((pad, 128), F32)], axis=0)
            gbt_ref[k:k + 1, :] = jnp.transpose(part)[0:1, :]

        if send_o:
            o_keep().wait()
            for d in range(1, peers):
                frm = lax.rem(me + d, peers)
                o_send(frm).wait_send()
                pltpu.make_async_remote_copy(
                    src_ref=o_ref.at[frm], dst_ref=o_new.at[frm], send_sem=os_sem.at[frm], recv_sem=or_sem.at[frm],
                    device_id={"sp": frm}, device_id_type=pl.DeviceIdType.MESH).wait_recv()
        for one in swaps:
            swap_wait(*one, peers)
        if send_o:
            outs = [pltpu.make_async_copy(src, dst, out_sem.at[k]) for k, (src, dst) in enumerate(zip((o_new, *landed), (o_out, *got)))]
            for copy in outs:
                copy.start()
            for copy in outs:
                copy.wait()


def attention(w_all, b_all, dot_, marks, x, gw, old, *, blk, tok, which, batch, lead, send_o, collective_id):
    blocks, dim, _ = dot_.shape
    seq, hidden = blocks * tok, w_all.shape[2]
    wide = 128 * pl.cdiv(dim, 128)
    hbm = pl.BlockSpec(memory_space=pltpu.HBM)
    full = lambda a: pl.BlockSpec(a.shape, lambda i: (0,) * len(a.shape), pipeline_mode=pl.Buffered(1))
    like = lambda a: jax.ShapeDtypeStruct(a.shape, a.dtype)
    outs = [jax.ShapeDtypeStruct((blocks, 3 * dim, tok), BF16), jax.ShapeDtypeStruct((lead, hidden), F32),
            jax.ShapeDtypeStruct((3 * dim - lead, hidden), F32), jax.ShapeDtypeStruct((3 * dim, 128), F32), jax.ShapeDtypeStruct((8, 128), F32)]
    pairs = (seq // blk) * (seq // blk + 1) // 2
    dma = pltpu.SemaphoreType.DMA
    res = pl.pallas_call(
        functools.partial(attn_body, blk=blk, tok=tok, which=which, batch=batch, n_swap=len(old), n_old=len(gw), send_o=send_o),
        name="attention",
        out_shape=outs + [like(dot_)] + [like(a) for a in old],
        grid=(seq // blk,),
        in_specs=[hbm, full(b_all), full(dot_), full(marks), hbm] + [full(a) for a in gw] + [hbm] * len(old),
        out_specs=[full(a) for a in outs] + [hbm if send_o else full(dot_)] + [hbm] * len(old),
        scratch_shapes=[
            pltpu.VMEM((seq, hidden), BF16),
            pltpu.VMEM(w_all.shape[1:], BF16), pltpu.VMEM((3 * dim, 128), F32), pltpu.VMEM((3 * dim, seq), BF16),
            pltpu.VMEM((seq, wide), BF16), pltpu.VMEM((seq, wide), BF16), pltpu.VMEM((seq, 128), F32),
            pltpu.VMEM((seq, blk), F32), pltpu.VMEM((2 * seq // blk, 8, blk), F32),
            pltpu.VMEM((wide, blk), BF16), pltpu.VMEM((wide, blk), BF16),
            pltpu.VMEM((dim, blk), F32), pltpu.VMEM((dim, blk), F32),
            pltpu.VMEM((dim, seq), F32), pltpu.VMEM((dim, seq), F32), dma((seq // blk,)), dma]
        + sum((swap_scratch(a) for a in old), []) + ([pltpu.VMEM(dot_.shape, BF16), dma((blocks,)), dma((blocks,)), dma((1 + len(old),)), pltpu.VMEM(dot_.shape, BF16)]
           + [pltpu.VMEM(a.shape, a.dtype) for a in old] if send_o else []),
        cost_estimate=pl.CostEstimate(flops=pairs * 6 * 2 * blk * blk * 256, bytes_accessed=24 << 20, transcendentals=pairs * blk * blk),
        compiler_params=pltpu.CompilerParams(dimension_semantics=("arbitrary",), vmem_limit_bytes=VMEM_LIMIT,
                                             collective_id=collective_id, has_side_effects=True),
    )(w_all, b_all, dot_, marks, x, *gw, *old)
    return res[0], res[1:4], res[4], res[5], res[6:]


def peer_at(d, peers):
    return {"sp": lax.rem(lax.axis_index("sp") + d, peers)}


def greet(peers):
    barrier = pltpu.get_barrier_semaphore()
    for d in range(1, peers):
        pl.semaphore_signal(barrier, inc=1, device_id=peer_at(d, peers), device_id_type=pl.DeviceIdType.MESH)
    return lambda: pl.semaphore_wait(barrier, peers - 1)


def meet(peers):
    greet(peers)()


def swap_copies(x_ref, out_ref, send_sem, recv_sem, peers):
    me = lax.axis_index("sp")
    order = [d for near in range(peers // 2) for d in sorted({peers // 2 - near, peers // 2 + near})]
    return [pltpu.make_async_remote_copy(
        src_ref=x_ref.at[lax.rem(me + d, peers)], dst_ref=out_ref.at[me], send_sem=send_sem.at[d - 1], recv_sem=recv_sem.at[d - 1],
        device_id=peer_at(d, peers), device_id_type=pl.DeviceIdType.MESH) for d in order]


def swap_start(x_ref, out_ref, own, send_sem, recv_sem, own_sem, peers):
    me = lax.axis_index("sp")
    for copy in swap_copies(x_ref, out_ref, send_sem, recv_sem, peers):
        copy.start()
    take = pltpu.make_async_copy(x_ref.at[me], own, own_sem)
    take.start()
    take.wait()
    pltpu.make_async_copy(own, out_ref.at[me], own_sem).start()


def swap_wait(x_ref, out_ref, own, send_sem, recv_sem, own_sem, peers):
    pltpu.make_async_copy(own, out_ref.at[lax.axis_index("sp")], own_sem).wait()
    for copy in swap_copies(x_ref, out_ref, send_sem, recv_sem, peers):
        copy.wait()


def swap_scratch(x):
    peers = x.shape[0]
    return [pltpu.VMEM(x.shape[1:], x.dtype), pltpu.SemaphoreType.DMA((peers - 1,)), pltpu.SemaphoreType.DMA((peers - 1,)),
            pltpu.SemaphoreType.DMA]


STEP = (1, -1)


def hops(ring, s, w):
    return ring // 2 - (s != w)


def ring_gather(block, own, sems, peers, cuts):
    ring = peers // 2
    me = lax.axis_index("sp")
    z, c = me // 2, me % 2
    send_sem, recv_sem, over_sem, came_sem = sems
    turn = lambda k: lax.rem(z + k + 2 * ring, ring)
    lots = [(s, w, u) for u in range(cuts) for w in range(2) for s in range(2)]

    def copy(src, dst, one, two, to):
        return pltpu.make_async_remote_copy(src_ref=src, dst_ref=dst, send_sem=one, recv_sem=two, device_id={"sp": to},
                                            device_id_type=pl.DeviceIdType.MESH)

    def along(s, w, t, u):
        ref = block(turn(-STEP[s] * t), c, w, u)
        return copy(own(w, u) if t == 0 else ref, ref, send_sem.at[s, w, t, u], recv_sem.at[s, w, t, u], 2 * turn(STEP[s]) + c)

    def across(s, w, t, u, side):
        ref = block(turn(-STEP[s] * t), side, w, u)
        return copy(own(w, u) if t == 0 and side is c else ref, ref, over_sem.at[s, w, t, u], came_sem.at[s, w, t, u], 2 * z + 1 - c)

    home = [(0, w, 0, u) for u in range(cuts) for w in range(2)]
    moved = [(s, w, t, u) for t in range(1, ring // 2 + 1) for s, w, u in lots if t <= hops(ring, s, w)]

    def start(only=None):
        for s, w, u in lots:
            if only in (None, (w, u)):
                along(s, w, 0, u).start()
        for lot in home:
            if only in (None, (lot[1], lot[3])):
                across(*lot, c).start()

    def run(lo=1, hi=ring):
        for s, w, t, u in moved:
            if lo <= t < hi:
                along(s, w, t - 1, u).wait_recv()
                if t < hops(ring, s, w):
                    along(s, w, t, u).start()
                across(s, w, t, u, c).start()

    def finish():
        for s, w, t, u in moved:
            along(s, w, t - 1, u).wait_send()
        for lot in home + moved:
            across(*lot, c).wait_send()
            across(*lot, 1 - c).wait_recv()

    return start, run, finish


def ring_scratch(peers, cuts):
    dma = pltpu.SemaphoreType.DMA
    return [dma((2, 2, peers // 4, cuts))] * 2 + [dma((2, 2, peers // 4 + 1, cuts))] * 2


def opening_body(x_hbm, dy_hbm, wo_hbm, gain_ref, bias_ref, pos_ref, keep_ref, marks_all, do_t, x_all, *refs, peers, batch, cuts):
    x_out, do_out = refs[:batch - 1], refs[batch - 1:2 * batch - 2]
    x_ref, dy_ref, x_own, do_own, wo_ref, marks_ref, own, ds_sem, dr_sem, do_sem, ms_sem, mr_sem, in_sem = refs[2 * batch - 2:2 * batch + 11]
    ring_sems = refs[2 * batch + 11:]
    gain, bias = gain_ref[...].reshape(1, -1), bias_ref[...].reshape(1, -1)
    me = lax.axis_index("sp")
    tok, dim = x_own.shape[0], do_own.shape[1]
    lot = tok // 2 // cuts
    rows_of = lambda w, u: pl.ds((w * cuts + u) * lot, lot)
    arrived = greet(peers)
    loads = [pltpu.make_async_copy(x_hbm.at[b], x_ref.at[b], in_sem.at[b]) for b in range(batch)]
    loads += [pltpu.make_async_copy(dy_hbm, dy_ref, in_sem.at[batch]), pltpu.make_async_copy(wo_hbm, wo_ref, in_sem.at[batch + 1])]
    for load in loads:
        load.start()

    def norm_rows(b, out_ref, rows):
        x = x_ref[b, rows, :].astype(F32)
        cen = x - jnp.mean(x, axis=-1, keepdims=True)
        hat = cen * lax.rsqrt(jnp.mean(cen * cen, axis=-1, keepdims=True) + NORM_EPS)
        out_ref[rows, :] = (hat * gain + bias).astype(BF16)

    def norm(b, out_ref):
        loads[b].wait()

        @pl.loop(0, tok // 32)
        def _(k):
            norm_rows(b, out_ref, pl.ds(pl.multiple_of(k * 32, 32), 32))

    def product(b, out_ref):
        @pl.loop(0, peers // 4)
        def _(g):
            rows = pl.ds(pl.multiple_of(g * 4 * dim, 4 * dim), 4 * dim)
            out_ref[pl.ds(g * 4, 4)] = lax.dot_general(wo_ref[rows, :], dy_ref[b], NT, preferred_element_type=F32).astype(BF16).reshape(4, dim, tok)

    marks_ref[...] = jnp.zeros_like(marks_ref)
    packed = 2 * pos_ref[...] + keep_ref[...]
    sub = tok // 128
    for b in range(batch):
        for k in range(sub):
            marks_ref[b * sub + k:b * sub + k + 1, :] = packed[b:b + 1, k * 128:(k + 1) * 128]
    block = lambda k, side, w, u: x_all.at[2 * k + side, rows_of(w, u)]
    start, run, finish = ring_gather(block, lambda w, u: x_own.at[rows_of(w, u)], ring_sems, peers, cuts)
    loads[0].wait()
    pieces = [(w, u) for u in range(cuts) for w in range(2)]
    for k, piece in enumerate(pieces):
        @pl.loop(0, lot // 32)
        def _(n):
            norm_rows(0, x_own, pl.ds(pl.multiple_of((piece[0] * cuts + piece[1]) * lot + n * 32, 32), 32))

        if k == 1:
            arrived()
        if k:
            start(pieces[k - 1])
    start(pieces[-1])
    keep = pltpu.make_async_copy(x_own, x_all.at[me], in_sem.at[batch + 2])
    keep.start()
    marks = [pltpu.make_async_remote_copy(
        src_ref=marks_ref, dst_ref=marks_all.at[me], send_sem=ms_sem.at[d - 1], recv_sem=mr_sem.at[d - 1],
        device_id=peer_at(d, peers), device_id_type=pl.DeviceIdType.MESH) for d in range(1, peers)]
    for copy in marks:
        copy.start()
    marks_all[me] = marks_ref[...]
    loads[-2].wait()
    loads[-1].wait()
    product(0, do_own)
    for b in range(1, batch):
        norm(b, x_out[b - 1])
    swap_start(do_own, do_t, own, ds_sem, dr_sem, do_sem, peers)
    for b in range(1, batch):
        product(b, do_out[b - 1])
    run()
    keep.wait()
    for copy in marks:
        copy.wait()
    swap_wait(do_own, do_t, own, ds_sem, dr_sem, do_sem, peers)
    finish()


def opening(x, dy, w_out, gain, bias, pos, keep, peers, collective_id, cuts=2):
    batch, tok, hidden = x.shape
    dim = hidden // peers
    hbm, vmem = pl.BlockSpec(memory_space=pltpu.HBM), pl.BlockSpec(memory_space=pltpu.VMEM)
    dma = pltpu.SemaphoreType.DMA
    do_shape, x_shape = jax.ShapeDtypeStruct((peers, dim, tok), BF16), jax.ShapeDtypeStruct((tok, hidden), BF16)
    res = pl.pallas_call(
        functools.partial(opening_body, peers=peers, batch=batch, cuts=cuts),
        name="opening",
        out_shape=[jax.ShapeDtypeStruct((peers, 8, 128), pos.dtype), do_shape, jax.ShapeDtypeStruct((peers, tok, hidden), BF16)]
        + [x_shape] * (batch - 1) + [do_shape] * (batch - 1),
        in_specs=[hbm, hbm, hbm, vmem, vmem, vmem, vmem],
        out_specs=[vmem, hbm, hbm] + [vmem] * (2 * batch - 2),
        scratch_shapes=[pltpu.VMEM(x.shape, BF16), pltpu.VMEM(dy.shape, BF16), pltpu.VMEM(x_shape.shape, BF16), pltpu.VMEM(do_shape.shape, BF16),
                        pltpu.VMEM(w_out.shape, BF16), pltpu.VMEM((8, 128), pos.dtype)] + swap_scratch(do_shape)
        + [dma((peers - 1,)), dma((peers - 1,)), dma((batch + 3,))] + ring_scratch(peers, cuts),
        cost_estimate=pl.CostEstimate(flops=5 * 10**10, bytes_accessed=16 << 20, transcendentals=0),
        compiler_params=pltpu.CompilerParams(collective_id=collective_id, has_side_effects=True, vmem_limit_bytes=VMEM_LIMIT),
    )(x, dy, w_out, gain, bias, pos, keep)
    return res[0], res[1], res[2], res[3:2 + batch], res[2 + batch:]


TN = (((0,), (0,)), ((), ()))


def tail_a_body(dqkv_ref, oo_hbm, on_hbm, dy_hbm, x_hbm, wo_hbm, d_hbm, w_hbm, gain_ref, bo_ref, y_ref, gx_ref, part, rows_ref,
                o_old, o_new, dy_ref, x_ref, wo_ref, d_old, w_ref, d_new, dn, sums, bo_rep, both, mine, landed, own_d,
                ds_sem, dr_sem, do_sem, ps_sem, pr_sem, rs_sem, rr_sem, w_sem, *, peers, cuts):
    ring = peers // 2
    me = lax.axis_index("sp")
    z, c = me // 2, me % 2
    _, tok, hidden = x_ref.shape
    half, wide, few = hidden // 2, hidden // 3, part.shape[0] // cuts
    cols = (pl.ds(0, half), pl.ds(half, half))
    at = lambda zz, cc: {"sp": 2 * zz + cc}
    turn = lambda k: lax.rem(z + k + 2 * ring, ring)
    remote = functools.partial(pltpu.make_async_remote_copy, device_id_type=pl.DeviceIdType.MESH)
    span, group = d_old.shape[1], 8
    gain, b_out = gain_ref[...].reshape(1, hidden), bo_ref[...].reshape(1, hidden)
    pairs = ((oo_hbm, o_old), (on_hbm, o_new), (dy_hbm, dy_ref), (x_hbm, x_ref), (wo_hbm, wo_ref), (d_hbm, d_old), (w_hbm, w_ref))
    loads = [pltpu.make_async_copy(src, dst, w_sem.at[k]) for k, (src, dst) in enumerate(pairs)]
    swap = (dqkv_ref, d_new, own_d, ds_sem, dr_sem, do_sem, peers)
    arrived = greet(peers)
    for load in loads:
        load.start()
    arrived()
    swap_start(*swap)
    for load in loads[:3]:
        load.wait()

    def product(put, side):
        @pl.loop(0, ring)
        def _(k):
            h = 2 * k + side
            put(k, jnp.dot(o_old[h], dy_ref[0], preferred_element_type=F32)
                + jnp.dot(o_new[h], dy_ref[1], preferred_element_type=F32))

    def put_other(k, value):
        both[k, 1 - c] = value

    def put_mine(k, value):
        mine[k] = value

    def forward(b, o_ref):
        o_t = o_ref[...].reshape(hidden, tok)

        @pl.loop(0, 3)
        def _(n):
            at_n = pl.ds(pl.multiple_of(n * wide, wide), wide)
            acc = lax.dot_general(o_t, wo_ref[:, at_n], TN, preferred_element_type=F32)
            y_ref[b, :, at_n] = (x_ref[b, :, at_n].astype(F32) + acc + bo_rep[0:1, at_n]).astype(BF16)

    def backward(b, d_ref):
        @pl.loop(0, 3)
        def _(n):
            at_n = pl.ds(pl.multiple_of(n * wide, wide), wide)
            acc = None
            for k in range(0, peers, group):
                lhs = d_ref[k:k + group].reshape(-1, tok)
                one = lax.dot_general(lhs, w_ref[k * span:(k + group) * span, at_n], TN, preferred_element_type=F32)
                acc = one if acc is None else acc + one
            dn[:, at_n] = acc

        @pl.loop(0, tok // 32)
        def _(k):
            rows = pl.ds(pl.multiple_of(k * 32, 32), 32)
            x = x_ref[b, rows, :].astype(F32)
            dy = dy_ref[b, rows, :].astype(F32)
            d = dn[rows, :]
            cen = x - jnp.mean(x, axis=-1, keepdims=True)
            inv = lax.rsqrt(jnp.mean(cen * cen, axis=-1, keepdims=True) + NORM_EPS)
            hat = cen * inv
            for n, one in enumerate((d * hat, d, dy)):
                sums[n] += jnp.sum(one.reshape(4, 8, hidden), axis=0)
            e = d * gain
            m1 = jnp.mean(e, axis=-1, keepdims=True)
            m2 = jnp.mean(e * hat, axis=-1, keepdims=True)
            gx_ref[b, rows, :] = (dy + inv * (e - m1 - hat * m2)).astype(BF16)

    bo_rep[...] = jnp.broadcast_to(b_out, bo_rep.shape)
    sums[...] = jnp.zeros_like(sums)
    product(put_other, 1 - c)
    pair_copy = lambda side: remote(src_ref=both.at[:, side], dst_ref=both.at[:, side], send_sem=ps_sem, recv_sem=pr_sem, device_id=at(z, 1 - c))
    product(put_mine, c)
    pair_copy(1 - c).start()
    pair_copy(1 - c).wait_send()
    pair_copy(c).wait_recv()

    @pl.loop(0, ring)
    def _(k):
        mine[k] = mine[k] + both[k, c]

    lots = [(s, w, u) for u in range(cuts) for w in range(2) for s in range(2)]

    def reduce_copy(s, w, t, u):
        return remote(src_ref=mine.at[turn(STEP[s] * (hops(ring, s, w) - t)), pl.ds(u * few, few), cols[w]], dst_ref=landed.at[s, w, t, u],
                      send_sem=rs_sem.at[s, w, t, u], recv_sem=rr_sem.at[s, w, t, u], device_id=at(turn(STEP[s]), c))

    def fold(s, w, t, u):
        reduce_copy(s, w, t, u).wait_recv()
        at_k = (turn(STEP[s] * (hops(ring, s, w) - t - 1)), pl.ds(u * few, few), cols[w])
        mine[at_k] = mine[at_k] + landed[s, w, t, u]

    def hop(t):
        for s, w, u in lots:
            if t < hops(ring, s, w):
                fold(s, w, t - 1, u)
                reduce_copy(s, w, t, u).start()

    for s, w, u in lots:
        reduce_copy(s, w, 0, u).start()
    for load in loads[3:5]:
        load.wait()
    forward(0, o_old)
    forward(1, o_new)
    for load in loads[5:]:
        load.wait()
    backward(0, d_old)
    for t in range(1, ring // 2 - 1):
        hop(t)
    swap_wait(*swap)
    backward(1, d_new)
    hop(ring // 2 - 1)
    rows_ref[...] = jnp.zeros_like(rows_ref)
    for n in range(3):
        rows_ref[n:n + 1, :] = jnp.sum(sums[n], axis=0, keepdims=True)
    for s, w, u in lots:
        fold(s, w, hops(ring, s, w) - 1, u)
    part[...] = mine[z]
    for s, w, u in lots:
        for t in range(hops(ring, s, w)):
            reduce_copy(s, w, t, u).wait_send()


def tail_a(dqkv, d_old, o_old, o_new, dy, x, w_flat, w_out, gain, b_out, collective_id, cuts=2):
    peers, dim, tok = o_old.shape
    ring = peers // 2
    hidden = dy.shape[-1]
    hbm, vmem = pl.BlockSpec(memory_space=pltpu.HBM), pl.BlockSpec(memory_space=pltpu.VMEM)
    dma = pltpu.SemaphoreType.DMA
    held = lambda a: pltpu.VMEM(a.shape, a.dtype)
    steps = (2, 2, ring // 2, cuts)
    return pl.pallas_call(
        functools.partial(tail_a_body, peers=peers, cuts=cuts),
        name="tail_a",
        out_shape=[jax.ShapeDtypeStruct(x.shape, BF16), jax.ShapeDtypeStruct(x.shape, BF16), jax.ShapeDtypeStruct((dim, hidden), F32),
                   jax.ShapeDtypeStruct((8, hidden), F32)],
        in_specs=[hbm] * 8 + [vmem] * 2,
        out_specs=[vmem] * 4,
        scratch_shapes=[held(a) for a in (o_old, o_new, dy, x, w_out, d_old, w_flat, dqkv)]
        + [pltpu.VMEM((tok, hidden), F32), pltpu.VMEM((3, 8, hidden), F32), pltpu.VMEM((8, hidden), F32),
           pltpu.VMEM((ring, 2, dim, hidden), F32), pltpu.VMEM((ring, dim, hidden), F32), pltpu.VMEM(steps + (dim // cuts, hidden // 2), F32),
           pltpu.VMEM(dqkv.shape[1:], BF16), dma((peers - 1,)), dma((peers - 1,)), dma, dma, dma, dma(steps), dma(steps), dma((7,))],
        cost_estimate=pl.CostEstimate(flops=10**11, bytes_accessed=64 << 20, transcendentals=0),
        compiler_params=pltpu.CompilerParams(collective_id=collective_id, has_side_effects=True, vmem_limit_bytes=VMEM_LIMIT),
    )(dqkv, o_old, o_new, dy, x, w_out, d_old, w_flat, gain, b_out)


def tail_b_body(part, rows_ref, gb_ref, full, total, gb_all, stage, xs_sem, xr_sem, *ring_sems, peers, cuts):
    ring = peers // 2
    me = lax.axis_index("sp")
    z, c = me // 2, me % 2
    hidden = part.shape[1]
    half, few = hidden // 2, part.shape[0] // cuts
    cols = (pl.ds(0, half), pl.ds(half, half))
    remote = functools.partial(pltpu.make_async_remote_copy, device_id_type=pl.DeviceIdType.MESH)
    arrived = greet(peers)
    full[z, c] = part[...]
    gb_all[me] = gb_ref[...]
    block = lambda k, side, w, u: full.at[k, side, pl.ds(u * few, few), cols[w]]
    start, run, finish = ring_gather(block, lambda w, u: block(z, c, w, u), ring_sems, peers, cuts)
    owners = hidden // 128
    lanes = lambda k: pl.ds(pl.multiple_of(k * 128, 128), 128)

    def small_copy(kind, frm, to):
        src, dst = ((rows_ref.at[:, lanes(to)], stage.at[frm]), (total.at[:, lanes(frm)],) * 2, (gb_ref, gb_all.at[frm]))[kind]
        return remote(src_ref=src, dst_ref=dst, send_sem=xs_sem.at[kind, to], recv_sem=xr_sem.at[kind, frm], device_id={"sp": to})

    def each(act, kind, only_to=False, only_from=False):
        @pl.loop(1, peers)
        def _(d):
            far = lax.rem(me + d, peers)

            def go():
                act(kind, far)

            if only_to:
                pl.when(far < owners)(go)
            elif only_from:
                pl.when(me < owners)(go)
            else:
                go()

    send = lambda kind, far: small_copy(kind, me, far).start()
    over = lambda kind, far: small_copy(kind, me, far).wait_send()
    came = lambda kind, far: small_copy(kind, far, me).wait_recv()

    @pl.when(me < owners)
    def _():
        stage[me] = rows_ref[:, lanes(me)]

    arrived()
    start()
    each(send, 0, only_to=True)
    each(send, 2)
    run(1, 2)
    each(came, 0, only_from=True)

    @pl.when(me < owners)
    def _():
        total[:, lanes(me)] = jnp.sum(stage[...], axis=0)

    each(send, 1, only_from=True)
    run(2)
    each(came, 1, only_to=True)
    each(came, 2)
    each(over, 0, only_to=True)
    each(over, 1, only_from=True)
    each(over, 2)
    finish()


def tail_b(part, rows, gb, peers, collective_id, cuts=2):
    ring = peers // 2
    vmem = pl.BlockSpec(memory_space=pltpu.VMEM)
    dma = pltpu.SemaphoreType.DMA
    return pl.pallas_call(
        functools.partial(tail_b_body, peers=peers, cuts=cuts),
        name="tail_b",
        out_shape=[jax.ShapeDtypeStruct((ring, 2) + part.shape, F32), jax.ShapeDtypeStruct(rows.shape, F32),
                   jax.ShapeDtypeStruct((peers,) + gb.shape, F32)],
        in_specs=[vmem] * 3,
        out_specs=[vmem] * 3,
        scratch_shapes=[pltpu.VMEM((peers, 8, 128), F32), dma((3, peers)), dma((3, peers))] + ring_scratch(peers, cuts),
        cost_estimate=pl.CostEstimate(flops=5 * 10**10, bytes_accessed=10 << 20, transcendentals=0),
        compiler_params=pltpu.CompilerParams(collective_id=collective_id, has_side_effects=True, vmem_limit_bytes=32 << 20),
    )(part, rows, gb)


def settle_body(*refs, n_in, first, n_plain, n_held):
    x_ref, plain, held = refs[0], refs[1:1 + n_plain], refs[1 + n_plain:1 + n_plain + n_held]
    outs = refs[n_in:n_in + 1 + n_plain + n_held]
    buf, in_sem, out_sem, in_plain, out_plain, *rooms = refs[n_in + 1 + n_plain + n_held:]
    heads, n = x_ref.shape[:2]
    copy = pltpu.make_async_copy
    reads = [copy(x_ref.at[h], buf.at[h], in_sem.at[h]) for h in range(heads)]
    writes = [copy(buf.at[h], outs[0].at[h, pl.ds(first, n)], out_sem.at[h]) for h in range(heads)]
    reads += [copy(plain[k], rooms[k], in_plain.at[k]) for k in range(n_plain)]
    writes += [copy(rooms[k], outs[1 + k], out_plain.at[k]) for k in range(n_plain)]
    flat = [copy(held[k], outs[1 + n_plain + k], out_plain.at[n_plain + k]) for k in range(n_held)]
    for one in reads + flat:
        one.start()
    for read, write in zip(reads, writes):
        read.wait()
        write.start()
    for one in writes + flat:
        one.wait()


def settle(x, into, plain, held, span, first):
    heads, n, hidden = x.shape
    hbm, vmem = pl.BlockSpec(memory_space=pltpu.HBM), pl.BlockSpec(memory_space=pltpu.VMEM)
    pin = lambda a: pltpu.with_memory_space_constraint(a, pltpu.HBM)
    args = (pin(x), *[pin(a) for a in plain], *held) + (() if into is None else (into,))
    dma = pltpu.SemaphoreType.DMA
    extra = max(len(plain) + len(held), 1)
    return pl.pallas_call(
        functools.partial(settle_body, n_in=len(args), first=first, n_plain=len(plain), n_held=len(held)), name="settle",
        out_shape=[jax.ShapeDtypeStruct((heads, span, hidden), x.dtype)] + [jax.ShapeDtypeStruct(a.shape, a.dtype) for a in (*plain, *held)],
        in_specs=[hbm] * (1 + len(plain)) + [vmem] * len(held) + [hbm] * (into is not None),
        out_specs=[hbm] * (1 + len(plain) + len(held)),
        input_output_aliases={} if into is None else {len(args) - 1: 0},
        scratch_shapes=[pltpu.VMEM(x.shape, x.dtype), dma((heads,)), dma((heads,)), dma((extra,)), dma((extra,))]
        + [pltpu.VMEM(a.shape, a.dtype) for a in plain],
        cost_estimate=pl.CostEstimate(flops=10**9, bytes_accessed=8 * x.size, transcendentals=0),
        compiler_params=pltpu.CompilerParams(vmem_limit_bytes=24 << 20))(*args)


def lay_body(go_ref, total, gb_all, go_out, gb_out, *refs):
    vectors, sem = refs[:-1], refs[-1]
    copies = [pltpu.make_async_copy(go_ref.at[k], go_out.at[k], sem.at[k]) for k in range(go_ref.shape[0])]
    for copy in copies:
        copy.start()
    for k in range(3):
        gb_out[k] = gb_all[:, k, 0:gb_out.shape[2]]
        vectors[k][...] = total[k]
    for copy in copies:
        copy.wait()


def lay_down(go, total, gb_all):
    hbm, vmem = pl.BlockSpec(memory_space=pltpu.HBM), pl.BlockSpec(memory_space=pltpu.VMEM)
    ring, _, dim, hidden = go.shape
    return pl.pallas_call(
        lay_body, name="lay_down",
        out_shape=[jax.ShapeDtypeStruct(go.shape, F32), jax.ShapeDtypeStruct((3, 2 * ring, dim), F32)] + [jax.ShapeDtypeStruct((hidden,), F32)] * 3,
        in_specs=[vmem] * 3, out_specs=[hbm] + [vmem] * 4,
        scratch_shapes=[pltpu.SemaphoreType.DMA((ring,))],
        cost_estimate=pl.CostEstimate(flops=10**9, bytes_accessed=8 * go.size, transcendentals=0),
        compiler_params=pltpu.CompilerParams(vmem_limit_bytes=24 << 20))(go, total, gb_all)


def solution(mesh):
    peers = mesh.shape["sp"]

    def block_fn(x_blk, pos_blk, keep_blk, ln_gain, ln_bias, w_qkv, b_qkv, w_out, b_out, dy_blk):
        batch, tok, hidden = x_blk.shape
        heads, dim = w_qkv.shape[1], w_qkv.shape[3]
        assert heads == peers
        seq = tok * peers
        blk = 2 * tok
        w_all = jnp.transpose(w_qkv, (1, 2, 3, 0)).reshape(heads, 3 * dim, hidden)
        b_all = jnp.transpose(b_qkv, (1, 0, 2))
        marks, do_first, x_first, x_rest, do_rest = opening(x_blk, dy_blk, w_out, ln_gain, ln_bias, pos_blk, keep_blk, peers, 1)
        xs = [x_first.reshape(seq, hidden)] + [lax.all_gather(one, "sp", axis=0, tiled=True) for one in x_rest]
        do_t = [do_first]
        lead = 13 * dim // 6
        gw, att = (), []
        for b in range(batch):
            old = list(do_rest[b:b + 1]) if b + 1 < batch else att
            att_d, gw, gb, att_o, swapped = attention(w_all, b_all, do_t[b], marks, xs[b], gw, old, blk=blk, tok=tok, which=b, batch=batch, lead=lead,
                                                      send_o=b + 1 == batch, collective_id=4 + b)
            if b + 1 < batch:
                do_t.append(swapped[0])
            att = [att_o, att_d]
        o_old, d_old = swapped
        gw_all = [lax.all_gather(one, "sp", axis=0, tiled=True).reshape(heads, -1, hidden) for one in gw[:2]]
        y, gx, part, rows = tail_a(att_d, d_old, o_old, att_o, dy_blk, x_blk, w_all.reshape(3 * hidden, hidden), w_out, ln_gain, b_out, 2)
        go_all, gb_all, g_gain, g_bias, g_out = lay_down(*tail_b(part, rows, gb, peers, 3))
        first, y, gx, go_all = lax.optimization_barrier((gw_all[0], y, gx, go_all))
        gw_out, y, gx = settle(first, None, (y, gx), (), 3 * dim, 0)
        second, gw_out, go_all = lax.optimization_barrier((gw_all[1], gw_out, go_all))
        gw_out, = settle(second, gw_out, (), (), 3 * dim, lead)
        gw_out = jnp.transpose(gw_out.reshape(heads, 3, dim, hidden), (3, 0, 1, 2))
        return y, gx, gw_out, jnp.transpose(gb_all, (1, 0, 2)), go_all.reshape(hidden, hidden), g_out, g_gain, g_bias

    act_spec = P("dp", "sp", None)
    tok_spec = P("dp", "sp")
    in_specs = (act_spec, tok_spec, tok_spec, P(), P(), P(), P(), P(), P(), act_spec)
    out_specs = (act_spec, act_spec, P("dp", None, None, None), P("dp", None, None), P("dp", None), P("dp"), P("dp"), P("dp"))
    return jax.shard_map(block_fn, mesh=mesh, in_specs=in_specs, out_specs=out_specs, check_vma=False)
```

```python
import functools
import jax
import jax.numpy as jnp
from jax import lax
from jax.experimental import pallas as pl
from jax.experimental.pallas import tpu as pltpu
from jax.sharding import PartitionSpec as P

NORM_EPS = 1e-5

LOG2E = 1.4426950408889634
MASKED = -1e30
VMEM_LIMIT = 62 << 20
F32, BF16 = jnp.float32, jnp.bfloat16
NT = (((1,), (1,)), ((), ()))


def attn_body(w_hbm, b_ref, dot_ref, marks_ref, x_ref, *refs, blk, tok, which, batch, n_swap, n_old, send_o):
    peers = dot_ref.shape[0]
    gw_old, old, refs = refs[:n_old], refs[n_old:n_old + n_swap], refs[n_old + n_swap:]
    (dqkv_ref, gwa_ref, gwb_ref, gb_ref, gbt_ref, o_out), got, refs = refs[:6], refs[6:6 + n_swap], refs[6 + n_swap:]
    x_buf, refs = refs[0], refs[1:]
    w_ref, b_rep, qkvt_ref, k_tok, v_tok, posk_ref, s_buf, m_buf, q_pad, do_pad, o_acc, dq_acc, dk_acc, dv_acc, x_sem, w_sem = refs[:16]
    swaps = [(old[k], got[k]) + refs[16 + 4 * k:20 + 4 * k] for k in range(n_swap)]
    if send_o:
        o_ref, os_sem, or_sem = refs[-3:]
        o_new = o_out
    else:
        o_ref = o_out
    dim, lead = dot_ref.shape[1], gwa_ref.shape[0]
    seq = dot_ref.shape[0] * tok
    pad = k_tok.shape[1] - dim
    nq = blk // tok
    steps = seq // blk
    scale = dim ** -0.5
    me = lax.axis_index("sp")
    step = pl.program_id(0)
    i = lax.rem(me // nq + step, steps)
    half = blk // 2
    sub = tok // 128

    def spread(row):
        return jnp.transpose(jnp.broadcast_to(row, (128, 128)))

    def x_copy(k):
        rows = pl.ds(pl.multiple_of(k * blk, blk), blk)
        return pltpu.make_async_copy(x_ref.at[rows], x_buf.at[rows], x_sem.at[k])

    def o_send(to):
        return pltpu.make_async_remote_copy(
            src_ref=o_ref.at[to], dst_ref=o_new.at[me], send_sem=os_sem.at[to], recv_sem=or_sem.at[me],
            device_id={"sp": to}, device_id_type=pl.DeviceIdType.MESH)

    def o_keep():
        return pltpu.make_async_copy(o_ref.at[me], o_new.at[me], os_sem.at[me])

    def o_start(at):
        for t in range(nq):
            to = lax.rem(me // nq + at, steps) * nq + t

            @pl.when(to != me)
            def _():
                o_send(to).start()

            @pl.when(to == me)
            def _():
                o_keep().start()

    @pl.when(step == 0)
    def _():
        w_load = pltpu.make_async_copy(w_hbm.at[me], w_ref, w_sem)
        w_load.start()
        for k in range(steps):
            x_copy(k).start()
        meet(peers)
        for one in swaps:
            swap_start(*one, peers)
        dk_acc[...] = jnp.zeros_like(dk_acc)
        dv_acc[...] = jnp.zeros_like(dv_acc)
        q_pad[...] = jnp.zeros_like(q_pad)
        do_pad[...] = jnp.zeros_like(do_pad)
        mine = lax.broadcasted_iota(jnp.int32, (peers, dim), 0) == me
        for k in range(3):
            row = jnp.sum(jnp.where(mine, b_ref[k], 0.0), axis=0, keepdims=True)
            b_rep[k * dim:(k + 1) * dim, :] = spread(jnp.concatenate([row, jnp.zeros((1, pad), F32)], axis=1))[0:dim]
        w_load.wait()

        @pl.loop(0, steps)
        def _(k):
            rows = pl.ds(pl.multiple_of(k * blk, blk), blk)
            x_copy(k).wait()
            shift = jnp.concatenate([b_rep[...]] * (blk // 128), axis=1)
            qkvt_ref[:, rows] = (lax.dot_general(w_ref[...], x_buf[rows, :], NT, preferred_element_type=F32) + shift).astype(BF16)

            for t in range(blk // 128):
                cols = pl.ds(pl.multiple_of(k * blk + t * 128, 128), 128)
                for base, dst in ((dim, k_tok), (2 * dim, v_tok)):
                    part = qkvt_ref[base:base + dim, cols].astype(F32)
                    whole = jnp.concatenate([part, jnp.zeros((pad, 128), F32)], axis=0)
                    dst[cols, :] = jnp.transpose(whole).astype(BF16)
                mark = marks_ref[k * nq + t // sub, which * sub + t % sub:which * sub + t % sub + 1, :]
                pos, keep = lax.shift_right_logical(mark, 1).astype(F32), mark & 1
                posk_ref[cols, :] = spread(jnp.where(keep > 0, pos, MASKED))

    if send_o:
        @pl.when(step > 0)
        def _():
            o_start(step - 1)

    qcols = pl.ds(pl.multiple_of(i * blk, blk), blk)
    q_pad[0:dim, :] = qkvt_ref[0:dim, qcols]
    for t in range(nq):
        do_pad[0:dim, t * tok:(t + 1) * tok] = dot_ref[i * nq + t]
    slope2 = jnp.exp2(jnp.full((1, 128), -8.0 / peers, F32) * (me + 1).astype(F32)) * LOG2E
    first = lax.shift_right_logical(marks_ref[i * nq, which * sub:which * sub + 1, :], 1).astype(F32)
    ref_pos = jnp.broadcast_to(first[:, 0:1], (1, 128))
    c = scale * LOG2E

    def scores(j, carry, diag):
        m, l8 = carry
        for sub in range(2):
            rows = pl.ds(pl.multiple_of(j * blk + sub * half, half), half)
            st = jnp.dot(k_tok[rows, :], q_pad[...], preferred_element_type=F32)
            bias = (posk_ref[rows, :] - ref_pos) * slope2
            st = st * c + jnp.concatenate([bias] * (blk // 128), axis=1)
            if diag:
                key = lax.broadcasted_iota(jnp.int32, (half, blk), 0) + sub * half
                qry = lax.broadcasted_iota(jnp.int32, (half, blk), 1)
                st = jnp.where(key <= qry, st, MASKED)
            m_new = jnp.maximum(m, jnp.max(st, axis=0, keepdims=True))
            e = jnp.exp2(st - m_new)
            s_buf[rows, :] = e
            m_buf[2 * j + sub] = jnp.broadcast_to(m_new, (8, blk))
            l8 = l8 * jnp.exp2(m - m_new) + jnp.sum(e.reshape(half // 8, 8, blk), axis=0)
            m = m_new
        return m, l8

    start = (jnp.full((1, blk), MASKED, F32), jnp.zeros((8, blk), F32))
    m, l8 = scores(i, lax.fori_loop(0, i, lambda j, carry: scores(j, carry, False), start), True)
    inv = 1.0 / jnp.sum(l8, axis=0, keepdims=True)
    o_acc[...] = jnp.zeros_like(o_acc)
    dq_acc[...] = jnp.zeros_like(dq_acc)

    def values(j, _):
        rows = pl.ds(pl.multiple_of(j * blk, blk), blk)
        pbs = []
        for sub in range(2):
            part = pl.ds(pl.multiple_of(j * blk + sub * half, half), half)
            p = s_buf[part, :] * (jnp.exp2(m_buf[2 * j + sub][0:1, :] - m) * inv)
            s_buf[part, :] = p
            pbs.append(p.astype(BF16))
        pb = jnp.concatenate(pbs, axis=0)
        o_acc[...] += jnp.dot(qkvt_ref[2 * dim:3 * dim, rows], pb, preferred_element_type=F32)
        dv_acc[:, rows] += lax.dot_general(do_pad[0:dim, :], pb, NT, preferred_element_type=F32)
        return 0

    lax.fori_loop(0, i + 1, values, 0)
    o_lo = o_acc[...].astype(BF16)
    do_f = do_pad[0:dim, :].astype(F32)
    r = jnp.sum(do_f * o_lo.astype(F32), axis=0, keepdims=True)

    def grads(j, _):
        rows = pl.ds(pl.multiple_of(j * blk, blk), blk)
        g = jnp.dot(v_tok[rows, :], do_pad[...], preferred_element_type=F32)
        ds = (s_buf[rows, :] * (g - r)).astype(BF16)
        dq_acc[...] += jnp.dot(qkvt_ref[dim:2 * dim, rows], ds, preferred_element_type=F32)
        dk_acc[:, rows] += lax.dot_general(q_pad[0:dim, :], ds, NT, preferred_element_type=F32)
        return 0

    lax.fori_loop(0, i + 1, grads, 0)
    dq_lo = (dq_acc[...] * scale).astype(BF16)
    for t in range(nq):
        o_ref[i * nq + t] = o_lo[:, t * tok:(t + 1) * tok]
        dqkv_ref[i * nq + t, 0:dim] = dq_lo[:, t * tok:(t + 1) * tok]

    @pl.when(step == steps - 1)
    def _():
        @pl.loop(0, seq // tok)
        def _(t):
            cols = pl.ds(pl.multiple_of(t * tok, tok), tok)
            dqkv_ref[t, dim:2 * dim] = (dk_acc[:, cols] * scale).astype(BF16)
            dqkv_ref[t, 2 * dim:3 * dim] = dv_acc[:, cols].astype(BF16)

        if send_o:
            o_start(step)
        for k, ref in enumerate((gwa_ref, gwb_ref, gb_ref)):
            ref[...] = gw_old[k][...] if n_old else jnp.zeros_like(ref)
        ones = jnp.ones((blk, 128), BF16)

        @pl.loop(0, steps)
        def _(j):
            rows = pl.ds(pl.multiple_of(j * blk, blk), blk)
            for ref, lo, hi in ((gwa_ref, 0, lead), (gwb_ref, lead, 3 * dim)):
                lhs = jnp.concatenate([dqkv_ref[j * nq + t, lo:hi] for t in range(nq)], axis=1)
                ref[...] += jnp.dot(lhs, x_buf[rows, :], preferred_element_type=F32)
                gb_ref[lo:hi, :] += jnp.dot(lhs, ones, preferred_element_type=F32)

        gbt_ref[...] = jnp.zeros_like(gbt_ref)
        for k in range(3):
            part = jnp.concatenate([gb_ref[k * dim:(k + 1) * dim, :], jnp.zeros((pad, 128), F32)], axis=0)
            gbt_ref[k:k + 1, :] = jnp.transpose(part)[0:1, :]

        if send_o:
            o_keep().wait()
            for d in range(1, peers):
                frm = lax.rem(me + d, peers)
                o_send(frm).wait_send()
                pltpu.make_async_remote_copy(
                    src_ref=o_ref.at[frm], dst_ref=o_new.at[frm], send_sem=os_sem.at[frm], recv_sem=or_sem.at[frm],
                    device_id={"sp": frm}, device_id_type=pl.DeviceIdType.MESH).wait_recv()
        for one in swaps:
            swap_wait(*one, peers)


def attention(w_all, b_all, dot_, marks, x, gw, old, *, blk, tok, which, batch, lead, send_o, collective_id):
    blocks, dim, _ = dot_.shape
    seq, hidden = blocks * tok, w_all.shape[2]
    wide = 128 * pl.cdiv(dim, 128)
    hbm = pl.BlockSpec(memory_space=pltpu.HBM)
    full = lambda a: pl.BlockSpec(a.shape, lambda i: (0,) * len(a.shape), pipeline_mode=pl.Buffered(1))
    like = lambda a: jax.ShapeDtypeStruct(a.shape, a.dtype)
    outs = [jax.ShapeDtypeStruct((blocks, 3 * dim, tok), BF16), jax.ShapeDtypeStruct((lead, hidden), F32),
            jax.ShapeDtypeStruct((3 * dim - lead, hidden), F32), jax.ShapeDtypeStruct((3 * dim, 128), F32), jax.ShapeDtypeStruct((8, 128), F32)]
    pairs = (seq // blk) * (seq // blk + 1) // 2
    dma = pltpu.SemaphoreType.DMA
    res = pl.pallas_call(
        functools.partial(attn_body, blk=blk, tok=tok, which=which, batch=batch, n_swap=len(old), n_old=len(gw), send_o=send_o),
        name="attention",
        out_shape=outs + [like(dot_)] + [like(a) for a in old],
        grid=(seq // blk,),
        in_specs=[hbm, full(b_all), full(dot_), full(marks), hbm] + [full(a) for a in gw] + [hbm] * len(old),
        out_specs=[full(a) for a in outs] + [hbm if send_o else full(dot_)] + [hbm] * len(old),
        scratch_shapes=[
            pltpu.VMEM((seq, hidden), BF16),
            pltpu.VMEM(w_all.shape[1:], BF16), pltpu.VMEM((3 * dim, 128), F32), pltpu.VMEM((3 * dim, seq), BF16),
            pltpu.VMEM((seq, wide), BF16), pltpu.VMEM((seq, wide), BF16), pltpu.VMEM((seq, 128), F32),
            pltpu.VMEM((seq, blk), F32), pltpu.VMEM((2 * seq // blk, 8, blk), F32),
            pltpu.VMEM((wide, blk), BF16), pltpu.VMEM((wide, blk), BF16),
            pltpu.VMEM((dim, blk), F32), pltpu.VMEM((dim, blk), F32),
            pltpu.VMEM((dim, seq), F32), pltpu.VMEM((dim, seq), F32), dma((seq // blk,)), dma]
        + sum((swap_scratch(a) for a in old), []) + ([pltpu.VMEM(dot_.shape, BF16), dma((blocks,)), dma((blocks,))] if send_o else []),
        cost_estimate=pl.CostEstimate(flops=pairs * 6 * 2 * blk * blk * 256, bytes_accessed=24 << 20, transcendentals=pairs * blk * blk),
        compiler_params=pltpu.CompilerParams(dimension_semantics=("arbitrary",), vmem_limit_bytes=VMEM_LIMIT,
                                             collective_id=collective_id, has_side_effects=True),
    )(w_all, b_all, dot_, marks, x, *gw, *old)
    return res[0], res[1:4], res[4], res[5], res[6:]


def peer_at(d, peers):
    return {"sp": lax.rem(lax.axis_index("sp") + d, peers)}


def greet(peers):
    barrier = pltpu.get_barrier_semaphore()
    for d in range(1, peers):
        pl.semaphore_signal(barrier, inc=1, device_id=peer_at(d, peers), device_id_type=pl.DeviceIdType.MESH)
    return lambda: pl.semaphore_wait(barrier, peers - 1)


def meet(peers):
    greet(peers)()


def swap_copies(x_ref, out_ref, send_sem, recv_sem, peers):
    me = lax.axis_index("sp")
    order = [d for near in range(peers // 2) for d in sorted({peers // 2 - near, peers // 2 + near})]
    return [pltpu.make_async_remote_copy(
        src_ref=x_ref.at[lax.rem(me + d, peers)], dst_ref=out_ref.at[me], send_sem=send_sem.at[d - 1], recv_sem=recv_sem.at[d - 1],
        device_id=peer_at(d, peers), device_id_type=pl.DeviceIdType.MESH) for d in order]


def swap_start(x_ref, out_ref, own, send_sem, recv_sem, own_sem, peers):
    me = lax.axis_index("sp")
    for copy in swap_copies(x_ref, out_ref, send_sem, recv_sem, peers):
        copy.start()
    take = pltpu.make_async_copy(x_ref.at[me], own, own_sem)
    take.start()
    take.wait()
    pltpu.make_async_copy(own, out_ref.at[me], own_sem).start()


def swap_wait(x_ref, out_ref, own, send_sem, recv_sem, own_sem, peers):
    pltpu.make_async_copy(own, out_ref.at[lax.axis_index("sp")], own_sem).wait()
    for copy in swap_copies(x_ref, out_ref, send_sem, recv_sem, peers):
        copy.wait()


def swap_scratch(x):
    peers = x.shape[0]
    return [pltpu.VMEM(x.shape[1:], x.dtype), pltpu.SemaphoreType.DMA((peers - 1,)), pltpu.SemaphoreType.DMA((peers - 1,)),
            pltpu.SemaphoreType.DMA]


STEP = (1, -1)


def hops(ring, s, w):
    return ring // 2 - (s != w)


def ring_gather(block, own, sems, peers, cuts):
    ring = peers // 2
    me = lax.axis_index("sp")
    z, c = me // 2, me % 2
    send_sem, recv_sem, over_sem, came_sem = sems
    turn = lambda k: lax.rem(z + k + 2 * ring, ring)
    lots = [(s, w, u) for u in range(cuts) for w in range(2) for s in range(2)]

    def copy(src, dst, one, two, to):
        return pltpu.make_async_remote_copy(src_ref=src, dst_ref=dst, send_sem=one, recv_sem=two, device_id={"sp": to},
                                            device_id_type=pl.DeviceIdType.MESH)

    def along(s, w, t, u):
        ref = block(turn(-STEP[s] * t), c, w, u)
        return copy(own(w, u) if t == 0 else ref, ref, send_sem.at[s, w, t, u], recv_sem.at[s, w, t, u], 2 * turn(STEP[s]) + c)

    def across(s, w, t, u, side):
        ref = block(turn(-STEP[s] * t), side, w, u)
        return copy(own(w, u) if t == 0 and side is c else ref, ref, over_sem.at[s, w, t, u], came_sem.at[s, w, t, u], 2 * z + 1 - c)

    home = [(0, w, 0, u) for u in range(cuts) for w in range(2)]
    moved = [(s, w, t, u) for t in range(1, ring // 2 + 1) for s, w, u in lots if t <= hops(ring, s, w)]

    def start(only=None):
        for s, w, u in lots:
            if only in (None, (w, u)):
                along(s, w, 0, u).start()
        for lot in home:
            if only in (None, (lot[1], lot[3])):
                across(*lot, c).start()

    def run(lo=1, hi=ring):
        for s, w, t, u in moved:
            if lo <= t < hi:
                along(s, w, t - 1, u).wait_recv()
                if t < hops(ring, s, w):
                    along(s, w, t, u).start()
                across(s, w, t, u, c).start()

    def finish():
        for s, w, t, u in moved:
            along(s, w, t - 1, u).wait_send()
        for lot in home + moved:
            across(*lot, c).wait_send()
            across(*lot, 1 - c).wait_recv()

    return start, run, finish


def ring_scratch(peers, cuts):
    dma = pltpu.SemaphoreType.DMA
    return [dma((2, 2, peers // 4, cuts))] * 2 + [dma((2, 2, peers // 4 + 1, cuts))] * 2


def opening_body(x_hbm, dy_hbm, wo_hbm, gain_ref, bias_ref, pos_ref, keep_ref, marks_all, do_t, x_all, *refs, peers, batch, cuts):
    x_out, do_out = refs[:batch - 1], refs[batch - 1:2 * batch - 2]
    x_ref, dy_ref, x_own, do_own, wo_ref, marks_ref, own, ds_sem, dr_sem, do_sem, ms_sem, mr_sem, in_sem = refs[2 * batch - 2:2 * batch + 11]
    ring_sems = refs[2 * batch + 11:]
    gain, bias = gain_ref[...].reshape(1, -1), bias_ref[...].reshape(1, -1)
    me = lax.axis_index("sp")
    tok, dim = x_own.shape[0], do_own.shape[1]
    lot = tok // 2 // cuts
    rows_of = lambda w, u: pl.ds((w * cuts + u) * lot, lot)
    arrived = greet(peers)
    loads = [pltpu.make_async_copy(x_hbm.at[b], x_ref.at[b], in_sem.at[b]) for b in range(batch)]
    loads += [pltpu.make_async_copy(dy_hbm, dy_ref, in_sem.at[batch]), pltpu.make_async_copy(wo_hbm, wo_ref, in_sem.at[batch + 1])]
    for load in loads:
        load.start()

    def norm_rows(b, out_ref, rows):
        x = x_ref[b, rows, :].astype(F32)
        cen = x - jnp.mean(x, axis=-1, keepdims=True)
        hat = cen * lax.rsqrt(jnp.mean(cen * cen, axis=-1, keepdims=True) + NORM_EPS)
        out_ref[rows, :] = (hat * gain + bias).astype(BF16)

    def norm(b, out_ref):
        loads[b].wait()

        @pl.loop(0, tok // 32)
        def _(k):
            norm_rows(b, out_ref, pl.ds(pl.multiple_of(k * 32, 32), 32))

    def product(b, out_ref):
        @pl.loop(0, peers // 4)
        def _(g):
            rows = pl.ds(pl.multiple_of(g * 4 * dim, 4 * dim), 4 * dim)
            out_ref[pl.ds(g * 4, 4)] = lax.dot_general(wo_ref[rows, :], dy_ref[b], NT, preferred_element_type=F32).astype(BF16).reshape(4, dim, tok)

    marks_ref[...] = jnp.zeros_like(marks_ref)
    packed = 2 * pos_ref[...] + keep_ref[...]
    sub = tok // 128
    for b in range(batch):
        for k in range(sub):
            marks_ref[b * sub + k:b * sub + k + 1, :] = packed[b:b + 1, k * 128:(k + 1) * 128]
    block = lambda k, side, w, u: x_all.at[2 * k + side, rows_of(w, u)]
    start, run, finish = ring_gather(block, lambda w, u: x_own.at[rows_of(w, u)], ring_sems, peers, cuts)
    loads[0].wait()
    pieces = [(w, u) for u in range(cuts) for w in range(2)]
    for k, piece in enumerate(pieces):
        @pl.loop(0, lot // 32)
        def _(n):
            norm_rows(0, x_own, pl.ds(pl.multiple_of((piece[0] * cuts + piece[1]) * lot + n * 32, 32), 32))

        if k == 1:
            arrived()
        if k:
            start(pieces[k - 1])
    start(pieces[-1])
    keep = pltpu.make_async_copy(x_own, x_all.at[me], in_sem.at[batch + 2])
    keep.start()
    marks = [pltpu.make_async_remote_copy(
        src_ref=marks_ref, dst_ref=marks_all.at[me], send_sem=ms_sem.at[d - 1], recv_sem=mr_sem.at[d - 1],
        device_id=peer_at(d, peers), device_id_type=pl.DeviceIdType.MESH) for d in range(1, peers)]
    for copy in marks:
        copy.start()
    marks_all[me] = marks_ref[...]
    loads[-2].wait()
    loads[-1].wait()
    product(0, do_own)
    for b in range(1, batch):
        norm(b, x_out[b - 1])
    swap_start(do_own, do_t, own, ds_sem, dr_sem, do_sem, peers)
    for b in range(1, batch):
        product(b, do_out[b - 1])
    run()
    keep.wait()
    for copy in marks:
        copy.wait()
    swap_wait(do_own, do_t, own, ds_sem, dr_sem, do_sem, peers)
    finish()


def opening(x, dy, w_out, gain, bias, pos, keep, peers, collective_id, cuts=2):
    batch, tok, hidden = x.shape
    dim = hidden // peers
    hbm, vmem = pl.BlockSpec(memory_space=pltpu.HBM), pl.BlockSpec(memory_space=pltpu.VMEM)
    dma = pltpu.SemaphoreType.DMA
    do_shape, x_shape = jax.ShapeDtypeStruct((peers, dim, tok), BF16), jax.ShapeDtypeStruct((tok, hidden), BF16)
    res = pl.pallas_call(
        functools.partial(opening_body, peers=peers, batch=batch, cuts=cuts),
        name="opening",
        out_shape=[jax.ShapeDtypeStruct((peers, 8, 128), pos.dtype), do_shape, jax.ShapeDtypeStruct((peers, tok, hidden), BF16)]
        + [x_shape] * (batch - 1) + [do_shape] * (batch - 1),
        in_specs=[hbm, hbm, hbm, vmem, vmem, vmem, vmem],
        out_specs=[vmem, hbm, hbm] + [vmem] * (2 * batch - 2),
        scratch_shapes=[pltpu.VMEM(x.shape, BF16), pltpu.VMEM(dy.shape, BF16), pltpu.VMEM(x_shape.shape, BF16), pltpu.VMEM(do_shape.shape, BF16),
                        pltpu.VMEM(w_out.shape, BF16), pltpu.VMEM((8, 128), pos.dtype)] + swap_scratch(do_shape)
        + [dma((peers - 1,)), dma((peers - 1,)), dma((batch + 3,))] + ring_scratch(peers, cuts),
        cost_estimate=pl.CostEstimate(flops=5 * 10**10, bytes_accessed=16 << 20, transcendentals=0),
        compiler_params=pltpu.CompilerParams(collective_id=collective_id, has_side_effects=True, vmem_limit_bytes=VMEM_LIMIT),
    )(x, dy, w_out, gain, bias, pos, keep)
    return res[0], res[1], res[2], res[3:2 + batch], res[2 + batch:]


TN = (((0,), (0,)), ((), ()))


def tail_a_body(dqkv_ref, oo_hbm, on_hbm, dy_hbm, x_hbm, wo_hbm, d_hbm, w_hbm, gain_ref, bo_ref, y_ref, gx_ref, part, rows_ref,
                o_old, o_new, dy_ref, x_ref, wo_ref, d_old, w_ref, d_new, dn, sums, bo_rep, both, mine, landed, own_d,
                ds_sem, dr_sem, do_sem, ps_sem, pr_sem, rs_sem, rr_sem, w_sem, *, peers, cuts):
    ring = peers // 2
    me = lax.axis_index("sp")
    z, c = me // 2, me % 2
    _, tok, hidden = x_ref.shape
    half, wide, few = hidden // 2, hidden // 3, part.shape[0] // cuts
    cols = (pl.ds(0, half), pl.ds(half, half))
    at = lambda zz, cc: {"sp": 2 * zz + cc}
    turn = lambda k: lax.rem(z + k + 2 * ring, ring)
    remote = functools.partial(pltpu.make_async_remote_copy, device_id_type=pl.DeviceIdType.MESH)
    span, group = d_old.shape[1], 8
    gain, b_out = gain_ref[...].reshape(1, hidden), bo_ref[...].reshape(1, hidden)
    pairs = ((oo_hbm, o_old), (on_hbm, o_new), (dy_hbm, dy_ref), (x_hbm, x_ref), (wo_hbm, wo_ref), (d_hbm, d_old), (w_hbm, w_ref))
    loads = [pltpu.make_async_copy(src, dst, w_sem.at[k]) for k, (src, dst) in enumerate(pairs)]
    swap = (dqkv_ref, d_new, own_d, ds_sem, dr_sem, do_sem, peers)
    arrived = greet(peers)
    for load in loads:
        load.start()
    arrived()
    swap_start(*swap)
    for load in loads[:3]:
        load.wait()

    def product(put, side):
        @pl.loop(0, ring)
        def _(k):
            h = 2 * k + side
            put(k, jnp.dot(o_old[h], dy_ref[0], preferred_element_type=F32)
                + jnp.dot(o_new[h], dy_ref[1], preferred_element_type=F32))

    def put_other(k, value):
        both[k, 1 - c] = value

    def put_mine(k, value):
        mine[k] = value

    def forward(b, o_ref):
        o_t = o_ref[...].reshape(hidden, tok)

        @pl.loop(0, 3)
        def _(n):
            at_n = pl.ds(pl.multiple_of(n * wide, wide), wide)
            acc = lax.dot_general(o_t, wo_ref[:, at_n], TN, preferred_element_type=F32)
            y_ref[b, :, at_n] = (x_ref[b, :, at_n].astype(F32) + acc + bo_rep[0:1, at_n]).astype(BF16)

    def backward(b, d_ref):
        @pl.loop(0, 3)
        def _(n):
            at_n = pl.ds(pl.multiple_of(n * wide, wide), wide)
            acc = None
            for k in range(0, peers, group):
                lhs = d_ref[k:k + group].reshape(-1, tok)
                one = lax.dot_general(lhs, w_ref[k * span:(k + group) * span, at_n], TN, preferred_element_type=F32)
                acc = one if acc is None else acc + one
            dn[:, at_n] = acc

        @pl.loop(0, tok // 32)
        def _(k):
            rows = pl.ds(pl.multiple_of(k * 32, 32), 32)
            x = x_ref[b, rows, :].astype(F32)
            dy = dy_ref[b, rows, :].astype(F32)
            d = dn[rows, :]
            cen = x - jnp.mean(x, axis=-1, keepdims=True)
            inv = lax.rsqrt(jnp.mean(cen * cen, axis=-1, keepdims=True) + NORM_EPS)
            hat = cen * inv
            for n, one in enumerate((d * hat, d, dy)):
                sums[n] += jnp.sum(one.reshape(4, 8, hidden), axis=0)
            e = d * gain
            m1 = jnp.mean(e, axis=-1, keepdims=True)
            m2 = jnp.mean(e * hat, axis=-1, keepdims=True)
            gx_ref[b, rows, :] = (dy + inv * (e - m1 - hat * m2)).astype(BF16)

    bo_rep[...] = jnp.broadcast_to(b_out, bo_rep.shape)
    sums[...] = jnp.zeros_like(sums)
    product(put_other, 1 - c)
    pair_copy = lambda side: remote(src_ref=both.at[:, side], dst_ref=both.at[:, side], send_sem=ps_sem, recv_sem=pr_sem, device_id=at(z, 1 - c))
    product(put_mine, c)
    pair_copy(1 - c).start()
    pair_copy(1 - c).wait_send()
    pair_copy(c).wait_recv()

    @pl.loop(0, ring)
    def _(k):
        mine[k] = mine[k] + both[k, c]

    lots = [(s, w, u) for u in range(cuts) for w in range(2) for s in range(2)]

    def reduce_copy(s, w, t, u):
        return remote(src_ref=mine.at[turn(STEP[s] * (hops(ring, s, w) - t)), pl.ds(u * few, few), cols[w]], dst_ref=landed.at[s, w, t, u],
                      send_sem=rs_sem.at[s, w, t, u], recv_sem=rr_sem.at[s, w, t, u], device_id=at(turn(STEP[s]), c))

    def fold(s, w, t, u):
        reduce_copy(s, w, t, u).wait_recv()
        at_k = (turn(STEP[s] * (hops(ring, s, w) - t - 1)), pl.ds(u * few, few), cols[w])
        mine[at_k] = mine[at_k] + landed[s, w, t, u]

    def hop(t):
        for s, w, u in lots:
            if t < hops(ring, s, w):
                fold(s, w, t - 1, u)
                reduce_copy(s, w, t, u).start()

    for s, w, u in lots:
        reduce_copy(s, w, 0, u).start()
    for load in loads[3:5]:
        load.wait()
    forward(0, o_old)
    forward(1, o_new)
    for load in loads[5:]:
        load.wait()
    backward(0, d_old)
    for t in range(1, ring // 2 - 1):
        hop(t)
    swap_wait(*swap)
    backward(1, d_new)
    hop(ring // 2 - 1)
    rows_ref[...] = jnp.zeros_like(rows_ref)
    for n in range(3):
        rows_ref[n:n + 1, :] = jnp.sum(sums[n], axis=0, keepdims=True)
    for s, w, u in lots:
        fold(s, w, hops(ring, s, w) - 1, u)
    part[...] = mine[z]
    for s, w, u in lots:
        for t in range(hops(ring, s, w)):
            reduce_copy(s, w, t, u).wait_send()


def tail_a(dqkv, d_old, o_old, o_new, dy, x, w_flat, w_out, gain, b_out, collective_id, cuts=1):
    peers, dim, tok = o_old.shape
    ring = peers // 2
    hidden = dy.shape[-1]
    hbm, vmem = pl.BlockSpec(memory_space=pltpu.HBM), pl.BlockSpec(memory_space=pltpu.VMEM)
    dma = pltpu.SemaphoreType.DMA
    held = lambda a: pltpu.VMEM(a.shape, a.dtype)
    steps = (2, 2, ring // 2, cuts)
    return pl.pallas_call(
        functools.partial(tail_a_body, peers=peers, cuts=cuts),
        name="tail_a",
        out_shape=[jax.ShapeDtypeStruct(x.shape, BF16), jax.ShapeDtypeStruct(x.shape, BF16), jax.ShapeDtypeStruct((dim, hidden), F32),
                   jax.ShapeDtypeStruct((8, hidden), F32)],
        in_specs=[hbm] * 8 + [vmem] * 2,
        out_specs=[vmem] * 4,
        scratch_shapes=[held(a) for a in (o_old, o_new, dy, x, w_out, d_old, w_flat, dqkv)]
        + [pltpu.VMEM((tok, hidden), F32), pltpu.VMEM((3, 8, hidden), F32), pltpu.VMEM((8, hidden), F32),
           pltpu.VMEM((ring, 2, dim, hidden), F32), pltpu.VMEM((ring, dim, hidden), F32), pltpu.VMEM(steps + (dim // cuts, hidden // 2), F32),
           pltpu.VMEM(dqkv.shape[1:], BF16), dma((peers - 1,)), dma((peers - 1,)), dma, dma, dma, dma(steps), dma(steps), dma((7,))],
        cost_estimate=pl.CostEstimate(flops=10**11, bytes_accessed=64 << 20, transcendentals=0),
        compiler_params=pltpu.CompilerParams(collective_id=collective_id, has_side_effects=True, vmem_limit_bytes=VMEM_LIMIT),
    )(dqkv, o_old, o_new, dy, x, w_out, d_old, w_flat, gain, b_out)


def tail_b_body(part, rows_ref, gb_ref, full, total, gb_all, stage, xs_sem, xr_sem, *ring_sems, peers, cuts):
    ring = peers // 2
    me = lax.axis_index("sp")
    z, c = me // 2, me % 2
    hidden = part.shape[1]
    half, few = hidden // 2, part.shape[0] // cuts
    cols = (pl.ds(0, half), pl.ds(half, half))
    remote = functools.partial(pltpu.make_async_remote_copy, device_id_type=pl.DeviceIdType.MESH)
    arrived = greet(peers)
    full[z, c] = part[...]
    gb_all[me] = gb_ref[...]
    block = lambda k, side, w, u: full.at[k, side, pl.ds(u * few, few), cols[w]]
    start, run, finish = ring_gather(block, lambda w, u: block(z, c, w, u), ring_sems, peers, cuts)
    owners = hidden // 128
    lanes = lambda k: pl.ds(pl.multiple_of(k * 128, 128), 128)

    def small_copy(kind, frm, to):
        src, dst = ((rows_ref.at[:, lanes(to)], stage.at[frm]), (total.at[:, lanes(frm)],) * 2, (gb_ref, gb_all.at[frm]))[kind]
        return remote(src_ref=src, dst_ref=dst, send_sem=xs_sem.at[kind, to], recv_sem=xr_sem.at[kind, frm], device_id={"sp": to})

    def each(act, kind, only_to=False, only_from=False):
        @pl.loop(1, peers)
        def _(d):
            far = lax.rem(me + d, peers)

            def go():
                act(kind, far)

            if only_to:
                pl.when(far < owners)(go)
            elif only_from:
                pl.when(me < owners)(go)
            else:
                go()

    send = lambda kind, far: small_copy(kind, me, far).start()
    over = lambda kind, far: small_copy(kind, me, far).wait_send()
    came = lambda kind, far: small_copy(kind, far, me).wait_recv()

    @pl.when(me < owners)
    def _():
        stage[me] = rows_ref[:, lanes(me)]

    arrived()
    start()
    each(send, 0, only_to=True)
    each(send, 2)
    run(1, 2)
    each(came, 0, only_from=True)

    @pl.when(me < owners)
    def _():
        total[:, lanes(me)] = jnp.sum(stage[...], axis=0)

    each(send, 1, only_from=True)
    run(2)
    each(came, 1, only_to=True)
    each(came, 2)
    each(over, 0, only_to=True)
    each(over, 1, only_from=True)
    each(over, 2)
    finish()


def tail_b(part, rows, gb, peers, collective_id, cuts=1):
    ring = peers // 2
    vmem = pl.BlockSpec(memory_space=pltpu.VMEM)
    dma = pltpu.SemaphoreType.DMA
    return pl.pallas_call(
        functools.partial(tail_b_body, peers=peers, cuts=cuts),
        name="tail_b",
        out_shape=[jax.ShapeDtypeStruct((ring, 2) + part.shape, F32), jax.ShapeDtypeStruct(rows.shape, F32),
                   jax.ShapeDtypeStruct((peers,) + gb.shape, F32)],
        in_specs=[vmem] * 3,
        out_specs=[vmem] * 3,
        scratch_shapes=[pltpu.VMEM((peers, 8, 128), F32), dma((3, peers)), dma((3, peers))] + ring_scratch(peers, cuts),
        cost_estimate=pl.CostEstimate(flops=5 * 10**10, bytes_accessed=10 << 20, transcendentals=0),
        compiler_params=pltpu.CompilerParams(collective_id=collective_id, has_side_effects=True, vmem_limit_bytes=32 << 20),
    )(part, rows, gb)


def settle_body(*refs, n_in, first, n_plain, n_held):
    x_ref, plain, held = refs[0], refs[1:1 + n_plain], refs[1 + n_plain:1 + n_plain + n_held]
    outs = refs[n_in:n_in + 1 + n_plain + n_held]
    buf, in_sem, out_sem, in_plain, out_plain, *rooms = refs[n_in + 1 + n_plain + n_held:]
    heads, n = x_ref.shape[:2]
    copy = pltpu.make_async_copy
    reads = [copy(x_ref.at[h], buf.at[h], in_sem.at[h]) for h in range(heads)]
    writes = [copy(buf.at[h], outs[0].at[h, pl.ds(first, n)], out_sem.at[h]) for h in range(heads)]
    reads += [copy(plain[k], rooms[k], in_plain.at[k]) for k in range(n_plain)]
    writes += [copy(rooms[k], outs[1 + k], out_plain.at[k]) for k in range(n_plain)]
    flat = [copy(held[k], outs[1 + n_plain + k], out_plain.at[n_plain + k]) for k in range(n_held)]
    for one in reads + flat:
        one.start()
    for read, write in zip(reads, writes):
        read.wait()
        write.start()
    for one in writes + flat:
        one.wait()


def settle(x, into, plain, held, span, first):
    heads, n, hidden = x.shape
    hbm, vmem = pl.BlockSpec(memory_space=pltpu.HBM), pl.BlockSpec(memory_space=pltpu.VMEM)
    pin = lambda a: pltpu.with_memory_space_constraint(a, pltpu.HBM)
    args = (pin(x), *[pin(a) for a in plain], *held) + (() if into is None else (into,))
    dma = pltpu.SemaphoreType.DMA
    extra = max(len(plain) + len(held), 1)
    return pl.pallas_call(
        functools.partial(settle_body, n_in=len(args), first=first, n_plain=len(plain), n_held=len(held)), name="settle",
        out_shape=[jax.ShapeDtypeStruct((heads, span, hidden), x.dtype)] + [jax.ShapeDtypeStruct(a.shape, a.dtype) for a in (*plain, *held)],
        in_specs=[hbm] * (1 + len(plain)) + [vmem] * len(held) + [hbm] * (into is not None),
        out_specs=[hbm] * (1 + len(plain) + len(held)),
        input_output_aliases={} if into is None else {len(args) - 1: 0},
        scratch_shapes=[pltpu.VMEM(x.shape, x.dtype), dma((heads,)), dma((heads,)), dma((extra,)), dma((extra,))]
        + [pltpu.VMEM(a.shape, a.dtype) for a in plain],
        cost_estimate=pl.CostEstimate(flops=10**9, bytes_accessed=8 * x.size, transcendentals=0),
        compiler_params=pltpu.CompilerParams(vmem_limit_bytes=24 << 20))(*args)


def lay_body(go_ref, total, gb_all, go_out, gb_out, *refs):
    vectors, sem = refs[:-1], refs[-1]
    copies = [pltpu.make_async_copy(go_ref.at[k], go_out.at[k], sem.at[k]) for k in range(go_ref.shape[0])]
    for copy in copies:
        copy.start()
    for k in range(3):
        gb_out[k] = gb_all[:, k, 0:gb_out.shape[2]]
        vectors[k][...] = total[k]
    for copy in copies:
        copy.wait()


def lay_down(go, total, gb_all):
    hbm, vmem = pl.BlockSpec(memory_space=pltpu.HBM), pl.BlockSpec(memory_space=pltpu.VMEM)
    ring, _, dim, hidden = go.shape
    return pl.pallas_call(
        lay_body, name="lay_down",
        out_shape=[jax.ShapeDtypeStruct(go.shape, F32), jax.ShapeDtypeStruct((3, 2 * ring, dim), F32)] + [jax.ShapeDtypeStruct((hidden,), F32)] * 3,
        in_specs=[vmem] * 3, out_specs=[hbm] + [vmem] * 4,
        scratch_shapes=[pltpu.SemaphoreType.DMA((ring,))],
        cost_estimate=pl.CostEstimate(flops=10**9, bytes_accessed=8 * go.size, transcendentals=0),
        compiler_params=pltpu.CompilerParams(vmem_limit_bytes=24 << 20))(go, total, gb_all)


def solution(mesh):
    peers = mesh.shape["sp"]

    def block_fn(x_blk, pos_blk, keep_blk, ln_gain, ln_bias, w_qkv, b_qkv, w_out, b_out, dy_blk):
        batch, tok, hidden = x_blk.shape
        heads, dim = w_qkv.shape[1], w_qkv.shape[3]
        assert heads == peers
        seq = tok * peers
        blk = 2 * tok
        w_all = jnp.transpose(w_qkv, (1, 2, 3, 0)).reshape(heads, 3 * dim, hidden)
        b_all = jnp.transpose(b_qkv, (1, 0, 2))
        marks, do_first, x_first, x_rest, do_rest = opening(x_blk, dy_blk, w_out, ln_gain, ln_bias, pos_blk, keep_blk, peers, 1)
        xs = [x_first.reshape(seq, hidden)] + [lax.all_gather(one, "sp", axis=0, tiled=True) for one in x_rest]
        do_t = [do_first]
        lead = 13 * dim // 6
        gw, att = (), []
        for b in range(batch):
            old = list(do_rest[b:b + 1]) if b + 1 < batch else att
            att_d, gw, gb, att_o, swapped = attention(w_all, b_all, do_t[b], marks, xs[b], gw, old, blk=blk, tok=tok, which=b, batch=batch, lead=lead,
                                                      send_o=b + 1 == batch, collective_id=4 + b)
            if b + 1 < batch:
                do_t.append(swapped[0])
            att = [att_o, att_d]
        o_old, d_old = swapped
        gw_all = [lax.all_gather(one, "sp", axis=0, tiled=True).reshape(heads, -1, hidden) for one in gw[:2]]
        y, gx, part, rows = tail_a(att_d, d_old, o_old, att_o, dy_blk, x_blk, w_all.reshape(3 * hidden, hidden), w_out, ln_gain, b_out, 2)
        go_all, gb_all, g_gain, g_bias, g_out = lay_down(*tail_b(part, rows, gb, peers, 3))
        first, y, gx, go_all = lax.optimization_barrier((gw_all[0], y, gx, go_all))
        gw_out, y, gx = settle(first, None, (y, gx), (), 3 * dim, 0)
        second, gw_out, go_all = lax.optimization_barrier((gw_all[1], gw_out, go_all))
        gw_out, = settle(second, gw_out, (), (), 3 * dim, lead)
        gw_out = jnp.transpose(gw_out.reshape(heads, 3, dim, hidden), (3, 0, 1, 2))
        return y, gx, gw_out, jnp.transpose(gb_all, (1, 0, 2)), go_all.reshape(hidden, hidden), g_out, g_gain, g_bias

    act_spec = P("dp", "sp", None)
    tok_spec = P("dp", "sp")
    in_specs = (act_spec, tok_spec, tok_spec, P(), P(), P(), P(), P(), P(), act_spec)
    out_specs = (act_spec, act_spec, P("dp", None, None, None), P("dp", None, None), P("dp", None), P("dp"), P("dp"), P("dp"))
    return jax.shard_map(block_fn, mesh=mesh, in_specs=in_specs, out_specs=out_specs, check_vma=False)
```

```python
import functools
import jax
import jax.numpy as jnp
from jax import lax
from jax.experimental import pallas as pl
from jax.experimental.pallas import tpu as pltpu
from jax.sharding import PartitionSpec as P

NORM_EPS = 1e-5

LOG2E = 1.4426950408889634
MASKED = -1e30
VMEM_LIMIT = 62 << 20
F32, BF16 = jnp.float32, jnp.bfloat16
NT = (((1,), (1,)), ((), ()))


def attn_body(w_hbm, b_ref, dot_ref, marks_ref, x_ref, *refs, blk, tok, which, batch, n_swap, n_old, send_o):
    peers = dot_ref.shape[0]
    gw_old, old, refs = refs[:n_old], refs[n_old:n_old + n_swap], refs[n_old + n_swap:]
    (dqkv_ref, gwa_ref, gwb_ref, gb_ref, gbt_ref, o_out), got, refs = refs[:6], refs[6:6 + n_swap], refs[6 + n_swap:]
    x_buf, refs = refs[0], refs[1:]
    w_ref, b_rep, qkvt_ref, k_tok, v_tok, posk_ref, s_buf, m_buf, q_pad, do_pad, o_acc, dq_acc, dk_acc, dv_acc, x_sem, w_sem = refs[:16]
    swaps = [(old[k], got[k]) + refs[16 + 4 * k:20 + 4 * k] for k in range(n_swap)]
    if send_o:
        o_ref, os_sem, or_sem = refs[-3:]
        o_new = o_out
    else:
        o_ref = o_out
    dim, lead = dot_ref.shape[1], gwa_ref.shape[0]
    seq = dot_ref.shape[0] * tok
    pad = k_tok.shape[1] - dim
    nq = blk // tok
    steps = seq // blk
    scale = dim ** -0.5
    me = lax.axis_index("sp")
    step = pl.program_id(0)
    i = lax.rem(me // nq + step, steps)
    half = blk // 2
    sub = tok // 128

    def spread(row):
        return jnp.transpose(jnp.broadcast_to(row, (128, 128)))

    def x_copy(k):
        rows = pl.ds(pl.multiple_of(k * blk, blk), blk)
        return pltpu.make_async_copy(x_ref.at[rows], x_buf.at[rows], x_sem.at[k])

    def o_send(to):
        return pltpu.make_async_remote_copy(
            src_ref=o_ref.at[to], dst_ref=o_new.at[me], send_sem=os_sem.at[to], recv_sem=or_sem.at[me],
            device_id={"sp": to}, device_id_type=pl.DeviceIdType.MESH)

    def o_keep():
        return pltpu.make_async_copy(o_ref.at[me], o_new.at[me], os_sem.at[me])

    def o_start(at):
        for t in range(nq):
            to = lax.rem(me // nq + at, steps) * nq + t

            @pl.when(to != me)
            def _():
                o_send(to).start()

            @pl.when(to == me)
            def _():
                o_keep().start()

    @pl.when(step == 0)
    def _():
        w_load = pltpu.make_async_copy(w_hbm.at[me], w_ref, w_sem)
        w_load.start()
        for k in range(steps):
            x_copy(k).start()
        meet(peers)
        for one in swaps:
            swap_start(*one, peers)
        dk_acc[...] = jnp.zeros_like(dk_acc)
        dv_acc[...] = jnp.zeros_like(dv_acc)
        q_pad[...] = jnp.zeros_like(q_pad)
        do_pad[...] = jnp.zeros_like(do_pad)
        mine = lax.broadcasted_iota(jnp.int32, (peers, dim), 0) == me
        for k in range(3):
            row = jnp.sum(jnp.where(mine, b_ref[k], 0.0), axis=0, keepdims=True)
            b_rep[k * dim:(k + 1) * dim, :] = spread(jnp.concatenate([row, jnp.zeros((1, pad), F32)], axis=1))[0:dim]
        w_load.wait()

        @pl.loop(0, steps)
        def _(k):
            rows = pl.ds(pl.multiple_of(k * blk, blk), blk)
            x_copy(k).wait()
            shift = jnp.concatenate([b_rep[...]] * (blk // 128), axis=1)
            qkvt_ref[:, rows] = (lax.dot_general(w_ref[...], x_buf[rows, :], NT, preferred_element_type=F32) + shift).astype(BF16)

            for t in range(blk // 128):
                cols = pl.ds(pl.multiple_of(k * blk + t * 128, 128), 128)
                for base, dst in ((dim, k_tok), (2 * dim, v_tok)):
                    part = qkvt_ref[base:base + dim, cols].astype(F32)
                    whole = jnp.concatenate([part, jnp.zeros((pad, 128), F32)], axis=0)
                    dst[cols, :] = jnp.transpose(whole).astype(BF16)
                mark = marks_ref[k * nq + t // sub, which * sub + t % sub:which * sub + t % sub + 1, :]
                pos, keep = lax.shift_right_logical(mark, 1).astype(F32), mark & 1
                posk_ref[cols, :] = spread(jnp.where(keep > 0, pos, MASKED))

    if send_o:
        @pl.when(step > 0)
        def _():
            o_start(step - 1)

    qcols = pl.ds(pl.multiple_of(i * blk, blk), blk)
    q_pad[0:dim, :] = qkvt_ref[0:dim, qcols]
    for t in range(nq):
        do_pad[0:dim, t * tok:(t + 1) * tok] = dot_ref[i * nq + t]
    slope2 = jnp.exp2(jnp.full((1, 128), -8.0 / peers, F32) * (me + 1).astype(F32)) * LOG2E
    first = lax.shift_right_logical(marks_ref[i * nq, which * sub:which * sub + 1, :], 1).astype(F32)
    ref_pos = jnp.broadcast_to(first[:, 0:1], (1, 128))
    c = scale * LOG2E

    def scores(j, carry, diag):
        m, l8 = carry
        for sub in range(2):
            rows = pl.ds(pl.multiple_of(j * blk + sub * half, half), half)
            st = jnp.dot(k_tok[rows, :], q_pad[...], preferred_element_type=F32)
            bias = (posk_ref[rows, :] - ref_pos) * slope2
            st = st * c + jnp.concatenate([bias] * (blk // 128), axis=1)
            if diag:
                key = lax.broadcasted_iota(jnp.int32, (half, blk), 0) + sub * half
                qry = lax.broadcasted_iota(jnp.int32, (half, blk), 1)
                st = jnp.where(key <= qry, st, MASKED)
            m_new = jnp.maximum(m, jnp.max(st, axis=0, keepdims=True))
            e = jnp.exp2(st - m_new)
            s_buf[rows, :] = e
            m_buf[2 * j + sub] = jnp.broadcast_to(m_new, (8, blk))
            l8 = l8 * jnp.exp2(m - m_new) + jnp.sum(e.reshape(half // 8, 8, blk), axis=0)
            m = m_new
        return m, l8

    start = (jnp.full((1, blk), MASKED, F32), jnp.zeros((8, blk), F32))
    m, l8 = scores(i, lax.fori_loop(0, i, lambda j, carry: scores(j, carry, False), start), True)
    inv = 1.0 / jnp.sum(l8, axis=0, keepdims=True)
    o_acc[...] = jnp.zeros_like(o_acc)
    dq_acc[...] = jnp.zeros_like(dq_acc)

    def values(j, _):
        rows = pl.ds(pl.multiple_of(j * blk, blk), blk)
        pbs = []
        for sub in range(2):
            part = pl.ds(pl.multiple_of(j * blk + sub * half, half), half)
            p = s_buf[part, :] * (jnp.exp2(m_buf[2 * j + sub][0:1, :] - m) * inv)
            s_buf[part, :] = p
            pbs.append(p.astype(BF16))
        pb = jnp.concatenate(pbs, axis=0)
        o_acc[...] += jnp.dot(qkvt_ref[2 * dim:3 * dim, rows], pb, preferred_element_type=F32)
        dv_acc[:, rows] += lax.dot_general(do_pad[0:dim, :], pb, NT, preferred_element_type=F32)
        return 0

    lax.fori_loop(0, i + 1, values, 0)
    o_lo = o_acc[...].astype(BF16)
    do_f = do_pad[0:dim, :].astype(F32)
    r = jnp.sum(do_f * o_lo.astype(F32), axis=0, keepdims=True)

    def grads(j, _):
        rows = pl.ds(pl.multiple_of(j * blk, blk), blk)
        g = jnp.dot(v_tok[rows, :], do_pad[...], preferred_element_type=F32)
        ds = (s_buf[rows, :] * (g - r)).astype(BF16)
        dq_acc[...] += jnp.dot(qkvt_ref[dim:2 * dim, rows], ds, preferred_element_type=F32)
        dk_acc[:, rows] += lax.dot_general(q_pad[0:dim, :], ds, NT, preferred_element_type=F32)
        return 0

    lax.fori_loop(0, i + 1, grads, 0)
    dq_lo = (dq_acc[...] * scale).astype(BF16)
    for t in range(nq):
        o_ref[i * nq + t] = o_lo[:, t * tok:(t + 1) * tok]
        dqkv_ref[i * nq + t, 0:dim] = dq_lo[:, t * tok:(t + 1) * tok]

    @pl.when(step == steps - 1)
    def _():
        @pl.loop(0, seq // tok)
        def _(t):
            cols = pl.ds(pl.multiple_of(t * tok, tok), tok)
            dqkv_ref[t, dim:2 * dim] = (dk_acc[:, cols] * scale).astype(BF16)
            dqkv_ref[t, 2 * dim:3 * dim] = dv_acc[:, cols].astype(BF16)

        if send_o:
            o_start(step)
        for k, ref in enumerate((gwa_ref, gwb_ref, gb_ref)):
            ref[...] = gw_old[k][...] if n_old else jnp.zeros_like(ref)
        ones = jnp.ones((blk, 128), BF16)

        @pl.loop(0, steps)
        def _(j):
            rows = pl.ds(pl.multiple_of(j * blk, blk), blk)
            for ref, lo, hi in ((gwa_ref, 0, lead), (gwb_ref, lead, 3 * dim)):
                lhs = jnp.concatenate([dqkv_ref[j * nq + t, lo:hi] for t in range(nq)], axis=1)
                ref[...] += jnp.dot(lhs, x_buf[rows, :], preferred_element_type=F32)
                gb_ref[lo:hi, :] += jnp.dot(lhs, ones, preferred_element_type=F32)

        gbt_ref[...] = jnp.zeros_like(gbt_ref)
        for k in range(3):
            part = jnp.concatenate([gb_ref[k * dim:(k + 1) * dim, :], jnp.zeros((pad, 128), F32)], axis=0)
            gbt_ref[k:k + 1, :] = jnp.transpose(part)[0:1, :]

        if send_o:
            o_keep().wait()
            for d in range(1, peers):
                frm = lax.rem(me + d, peers)
                o_send(frm).wait_send()
                pltpu.make_async_remote_copy(
                    src_ref=o_ref.at[frm], dst_ref=o_new.at[frm], send_sem=os_sem.at[frm], recv_sem=or_sem.at[frm],
                    device_id={"sp": frm}, device_id_type=pl.DeviceIdType.MESH).wait_recv()
        for one in swaps:
            swap_wait(*one, peers)


def attention(w_all, b_all, dot_, marks, x, gw, old, *, blk, tok, which, batch, lead, send_o, collective_id):
    blocks, dim, _ = dot_.shape
    seq, hidden = blocks * tok, w_all.shape[2]
    wide = 128 * pl.cdiv(dim, 128)
    hbm = pl.BlockSpec(memory_space=pltpu.HBM)
    full = lambda a: pl.BlockSpec(a.shape, lambda i: (0,) * len(a.shape), pipeline_mode=pl.Buffered(1))
    like = lambda a: jax.ShapeDtypeStruct(a.shape, a.dtype)
    outs = [jax.ShapeDtypeStruct((blocks, 3 * dim, tok), BF16), jax.ShapeDtypeStruct((lead, hidden), F32),
            jax.ShapeDtypeStruct((3 * dim - lead, hidden), F32), jax.ShapeDtypeStruct((3 * dim, 128), F32), jax.ShapeDtypeStruct((8, 128), F32)]
    pairs = (seq // blk) * (seq // blk + 1) // 2
    dma = pltpu.SemaphoreType.DMA
    res = pl.pallas_call(
        functools.partial(attn_body, blk=blk, tok=tok, which=which, batch=batch, n_swap=len(old), n_old=len(gw), send_o=send_o),
        name="attention",
        out_shape=outs + [like(dot_)] + [like(a) for a in old],
        grid=(seq // blk,),
        in_specs=[hbm, full(b_all), full(dot_), full(marks), hbm] + [full(a) for a in gw] + [hbm] * len(old),
        out_specs=[full(a) for a in outs] + [hbm if send_o else full(dot_)] + [hbm] * len(old),
        scratch_shapes=[
            pltpu.VMEM((seq, hidden), BF16),
            pltpu.VMEM(w_all.shape[1:], BF16), pltpu.VMEM((3 * dim, 128), F32), pltpu.VMEM((3 * dim, seq), BF16),
            pltpu.VMEM((seq, wide), BF16), pltpu.VMEM((seq, wide), BF16), pltpu.VMEM((seq, 128), F32),
            pltpu.VMEM((seq, blk), F32), pltpu.VMEM((2 * seq // blk, 8, blk), F32),
            pltpu.VMEM((wide, blk), BF16), pltpu.VMEM((wide, blk), BF16),
            pltpu.VMEM((dim, blk), F32), pltpu.VMEM((dim, blk), F32),
            pltpu.VMEM((dim, seq), F32), pltpu.VMEM((dim, seq), F32), dma((seq // blk,)), dma]
        + sum((swap_scratch(a) for a in old), []) + ([pltpu.VMEM(dot_.shape, BF16), dma((blocks,)), dma((blocks,))] if send_o else []),
        cost_estimate=pl.CostEstimate(flops=pairs * 6 * 2 * blk * blk * 256, bytes_accessed=24 << 20, transcendentals=pairs * blk * blk),
        compiler_params=pltpu.CompilerParams(dimension_semantics=("arbitrary",), vmem_limit_bytes=VMEM_LIMIT,
                                             collective_id=collective_id, has_side_effects=True),
    )(w_all, b_all, dot_, marks, x, *gw, *old)
    return res[0], res[1:4], res[4], res[5], res[6:]


def peer_at(d, peers):
    return {"sp": lax.rem(lax.axis_index("sp") + d, peers)}


def greet(peers):
    barrier = pltpu.get_barrier_semaphore()
    for d in range(1, peers):
        pl.semaphore_signal(barrier, inc=1, device_id=peer_at(d, peers), device_id_type=pl.DeviceIdType.MESH)
    return lambda: pl.semaphore_wait(barrier, peers - 1)


def meet(peers):
    greet(peers)()


def swap_copies(x_ref, out_ref, send_sem, recv_sem, peers):
    me = lax.axis_index("sp")
    order = [d for near in range(peers // 2) for d in sorted({peers // 2 - near, peers // 2 + near})]
    return [pltpu.make_async_remote_copy(
        src_ref=x_ref.at[lax.rem(me + d, peers)], dst_ref=out_ref.at[me], send_sem=send_sem.at[d - 1], recv_sem=recv_sem.at[d - 1],
        device_id=peer_at(d, peers), device_id_type=pl.DeviceIdType.MESH) for d in order]


def swap_start(x_ref, out_ref, own, send_sem, recv_sem, own_sem, peers):
    me = lax.axis_index("sp")
    for copy in swap_copies(x_ref, out_ref, send_sem, recv_sem, peers):
        copy.start()
    take = pltpu.make_async_copy(x_ref.at[me], own, own_sem)
    take.start()
    take.wait()
    pltpu.make_async_copy(own, out_ref.at[me], own_sem).start()


def swap_wait(x_ref, out_ref, own, send_sem, recv_sem, own_sem, peers):
    pltpu.make_async_copy(own, out_ref.at[lax.axis_index("sp")], own_sem).wait()
    for copy in swap_copies(x_ref, out_ref, send_sem, recv_sem, peers):
        copy.wait()


def swap_scratch(x):
    peers = x.shape[0]
    return [pltpu.VMEM(x.shape[1:], x.dtype), pltpu.SemaphoreType.DMA((peers - 1,)), pltpu.SemaphoreType.DMA((peers - 1,)),
            pltpu.SemaphoreType.DMA]


STEP = (1, -1)


def hops(ring, s, w):
    return ring // 2 - (s != w)


def ring_gather(block, own, sems, peers, cuts):
    ring = peers // 2
    me = lax.axis_index("sp")
    z, c = me // 2, me % 2
    send_sem, recv_sem, over_sem, came_sem = sems
    turn = lambda k: lax.rem(z + k + 2 * ring, ring)
    lots = [(s, w, u) for u in range(cuts) for w in range(2) for s in range(2)]

    def copy(src, dst, one, two, to):
        return pltpu.make_async_remote_copy(src_ref=src, dst_ref=dst, send_sem=one, recv_sem=two, device_id={"sp": to},
                                            device_id_type=pl.DeviceIdType.MESH)

    def along(s, w, t, u):
        ref = block(turn(-STEP[s] * t), c, w, u)
        return copy(own(w, u) if t == 0 else ref, ref, send_sem.at[s, w, t, u], recv_sem.at[s, w, t, u], 2 * turn(STEP[s]) + c)

    def across(s, w, t, u, side):
        ref = block(turn(-STEP[s] * t), side, w, u)
        return copy(own(w, u) if t == 0 and side is c else ref, ref, over_sem.at[s, w, t, u], came_sem.at[s, w, t, u], 2 * z + 1 - c)

    home = [(0, w, 0, u) for u in range(cuts) for w in range(2)]
    moved = [(s, w, t, u) for t in range(1, ring // 2 + 1) for s, w, u in lots if t <= hops(ring, s, w)]

    def start(only=None):
        for s, w, u in lots:
            if only in (None, (w, u)):
                along(s, w, 0, u).start()
        for lot in home:
            if only in (None, (lot[1], lot[3])):
                across(*lot, c).start()

    def run(lo=1, hi=ring):
        for s, w, t, u in moved:
            if lo <= t < hi:
                along(s, w, t - 1, u).wait_recv()
                if t < hops(ring, s, w):
                    along(s, w, t, u).start()
                across(s, w, t, u, c).start()

    def finish():
        for s, w, t, u in moved:
            along(s, w, t - 1, u).wait_send()
        for lot in home + moved:
            across(*lot, c).wait_send()
            across(*lot, 1 - c).wait_recv()

    return start, run, finish


def ring_scratch(peers, cuts):
    dma = pltpu.SemaphoreType.DMA
    return [dma((2, 2, peers // 4, cuts))] * 2 + [dma((2, 2, peers // 4 + 1, cuts))] * 2


def opening_body(x_hbm, dy_hbm, wo_hbm, gain_ref, bias_ref, pos_ref, keep_ref, marks_all, do_t, x_all, *refs, peers, batch, cuts):
    x_out, do_out = refs[:batch - 1], refs[batch - 1:2 * batch - 2]
    x_ref, dy_ref, x_own, do_own, wo_ref, marks_ref, own, ds_sem, dr_sem, do_sem, ms_sem, mr_sem, in_sem = refs[2 * batch - 2:2 * batch + 11]
    ring_sems = refs[2 * batch + 11:]
    gain, bias = gain_ref[...].reshape(1, -1), bias_ref[...].reshape(1, -1)
    me = lax.axis_index("sp")
    tok, dim = x_own.shape[0], do_own.shape[1]
    lot = tok // 2 // cuts
    rows_of = lambda w, u: pl.ds((w * cuts + u) * lot, lot)
    arrived = greet(peers)
    loads = [pltpu.make_async_copy(x_hbm.at[b], x_ref.at[b], in_sem.at[b]) for b in range(batch)]
    loads += [pltpu.make_async_copy(dy_hbm, dy_ref, in_sem.at[batch]), pltpu.make_async_copy(wo_hbm, wo_ref, in_sem.at[batch + 1])]
    for load in loads:
        load.start()

    def norm_rows(b, out_ref, rows):
        x = x_ref[b, rows, :].astype(F32)
        cen = x - jnp.mean(x, axis=-1, keepdims=True)
        hat = cen * lax.rsqrt(jnp.mean(cen * cen, axis=-1, keepdims=True) + NORM_EPS)
        out_ref[rows, :] = (hat * gain + bias).astype(BF16)

    def norm(b, out_ref):
        loads[b].wait()

        @pl.loop(0, tok // 32)
        def _(k):
            norm_rows(b, out_ref, pl.ds(pl.multiple_of(k * 32, 32), 32))

    def product(b, out_ref):
        @pl.loop(0, peers // 4)
        def _(g):
            rows = pl.ds(pl.multiple_of(g * 4 * dim, 4 * dim), 4 * dim)
            out_ref[pl.ds(g * 4, 4)] = lax.dot_general(wo_ref[rows, :], dy_ref[b], NT, preferred_element_type=F32).astype(BF16).reshape(4, dim, tok)

    marks_ref[...] = jnp.zeros_like(marks_ref)
    packed = 2 * pos_ref[...] + keep_ref[...]
    sub = tok // 128
    for b in range(batch):
        for k in range(sub):
            marks_ref[b * sub + k:b * sub + k + 1, :] = packed[b:b + 1, k * 128:(k + 1) * 128]
    block = lambda k, side, w, u: x_all.at[2 * k + side, rows_of(w, u)]
    start, run, finish = ring_gather(block, lambda w, u: x_own.at[rows_of(w, u)], ring_sems, peers, cuts)
    loads[0].wait()
    pieces = [(w, u) for u in range(cuts) for w in range(2)]
    for k, piece in enumerate(pieces):
        @pl.loop(0, lot // 32)
        def _(n):
            norm_rows(0, x_own, pl.ds(pl.multiple_of((piece[0] * cuts + piece[1]) * lot + n * 32, 32), 32))

        if k == 1:
            arrived()
        if k:
            start(pieces[k - 1])
    start(pieces[-1])
    keep = pltpu.make_async_copy(x_own, x_all.at[me], in_sem.at[batch + 2])
    keep.start()
    marks = [pltpu.make_async_remote_copy(
        src_ref=marks_ref, dst_ref=marks_all.at[me], send_sem=ms_sem.at[d - 1], recv_sem=mr_sem.at[d - 1],
        device_id=peer_at(d, peers), device_id_type=pl.DeviceIdType.MESH) for d in range(1, peers)]
    for copy in marks:
        copy.start()
    marks_all[me] = marks_ref[...]
    loads[-2].wait()
    loads[-1].wait()
    product(0, do_own)
    for b in range(1, batch):
        norm(b, x_out[b - 1])
    swap_start(do_own, do_t, own, ds_sem, dr_sem, do_sem, peers)
    for b in range(1, batch):
        product(b, do_out[b - 1])
    run()
    keep.wait()
    for copy in marks:
        copy.wait()
    swap_wait(do_own, do_t, own, ds_sem, dr_sem, do_sem, peers)
    finish()


def opening(x, dy, w_out, gain, bias, pos, keep, peers, collective_id, cuts=2):
    batch, tok, hidden = x.shape
    dim = hidden // peers
    hbm, vmem = pl.BlockSpec(memory_space=pltpu.HBM), pl.BlockSpec(memory_space=pltpu.VMEM)
    dma = pltpu.SemaphoreType.DMA
    do_shape, x_shape = jax.ShapeDtypeStruct((peers, dim, tok), BF16), jax.ShapeDtypeStruct((tok, hidden), BF16)
    res = pl.pallas_call(
        functools.partial(opening_body, peers=peers, batch=batch, cuts=cuts),
        name="opening",
        out_shape=[jax.ShapeDtypeStruct((peers, 8, 128), pos.dtype), do_shape, jax.ShapeDtypeStruct((peers, tok, hidden), BF16)]
        + [x_shape] * (batch - 1) + [do_shape] * (batch - 1),
        in_specs=[hbm, hbm, hbm, vmem, vmem, vmem, vmem],
        out_specs=[vmem, hbm, hbm] + [vmem] * (2 * batch - 2),
        scratch_shapes=[pltpu.VMEM(x.shape, BF16), pltpu.VMEM(dy.shape, BF16), pltpu.VMEM(x_shape.shape, BF16), pltpu.VMEM(do_shape.shape, BF16),
                        pltpu.VMEM(w_out.shape, BF16), pltpu.VMEM((8, 128), pos.dtype)] + swap_scratch(do_shape)
        + [dma((peers - 1,)), dma((peers - 1,)), dma((batch + 3,))] + ring_scratch(peers, cuts),
        cost_estimate=pl.CostEstimate(flops=5 * 10**10, bytes_accessed=16 << 20, transcendentals=0),
        compiler_params=pltpu.CompilerParams(collective_id=collective_id, has_side_effects=True, vmem_limit_bytes=VMEM_LIMIT),
    )(x, dy, w_out, gain, bias, pos, keep)
    return res[0], res[1], res[2], res[3:2 + batch], res[2 + batch:]


TN = (((0,), (0,)), ((), ()))


def tail_a_body(dqkv_ref, oo_hbm, on_hbm, dy_hbm, x_hbm, wo_hbm, d_hbm, w_hbm, gain_ref, bo_ref, y_ref, gx_ref, part, rows_ref,
                o_old, o_new, dy_ref, x_ref, wo_ref, d_old, w_ref, d_new, dn, sums, bo_rep, both, mine, landed, own_d,
                ds_sem, dr_sem, do_sem, ps_sem, pr_sem, rs_sem, rr_sem, w_sem, *, peers, cuts):
    ring = peers // 2
    me = lax.axis_index("sp")
    z, c = me // 2, me % 2
    _, tok, hidden = x_ref.shape
    half, wide, few = hidden // 2, hidden // 3, part.shape[0] // cuts
    cols = (pl.ds(0, half), pl.ds(half, half))
    at = lambda zz, cc: {"sp": 2 * zz + cc}
    turn = lambda k: lax.rem(z + k + 2 * ring, ring)
    remote = functools.partial(pltpu.make_async_remote_copy, device_id_type=pl.DeviceIdType.MESH)
    span, group = d_old.shape[1], 8
    gain, b_out = gain_ref[...].reshape(1, hidden), bo_ref[...].reshape(1, hidden)
    pairs = ((oo_hbm, o_old), (on_hbm, o_new), (dy_hbm, dy_ref), (x_hbm, x_ref), (wo_hbm, wo_ref), (d_hbm, d_old), (w_hbm, w_ref))
    loads = [pltpu.make_async_copy(src, dst, w_sem.at[k]) for k, (src, dst) in enumerate(pairs)]
    swap = (dqkv_ref, d_new, own_d, ds_sem, dr_sem, do_sem, peers)
    arrived = greet(peers)
    for load in loads:
        load.start()
    arrived()
    swap_start(*swap)
    for load in loads[:3]:
        load.wait()

    def product(put, side):
        @pl.loop(0, ring)
        def _(k):
            h = 2 * k + side
            put(k, jnp.dot(o_old[h], dy_ref[0], preferred_element_type=F32)
                + jnp.dot(o_new[h], dy_ref[1], preferred_element_type=F32))

    def put_other(k, value):
        both[k, 1 - c] = value

    def put_mine(k, value):
        mine[k] = value

    def forward(b, o_ref):
        o_t = o_ref[...].reshape(hidden, tok)

        @pl.loop(0, 3)
        def _(n):
            at_n = pl.ds(pl.multiple_of(n * wide, wide), wide)
            acc = lax.dot_general(o_t, wo_ref[:, at_n], TN, preferred_element_type=F32)
            y_ref[b, :, at_n] = (x_ref[b, :, at_n].astype(F32) + acc + bo_rep[0:1, at_n]).astype(BF16)

    def backward(b, d_ref):
        @pl.loop(0, 3)
        def _(n):
            at_n = pl.ds(pl.multiple_of(n * wide, wide), wide)
            acc = None
            for k in range(0, peers, group):
                lhs = d_ref[k:k + group].reshape(-1, tok)
                one = lax.dot_general(lhs, w_ref[k * span:(k + group) * span, at_n], TN, preferred_element_type=F32)
                acc = one if acc is None else acc + one
            dn[:, at_n] = acc

        @pl.loop(0, tok // 32)
        def _(k):
            rows = pl.ds(pl.multiple_of(k * 32, 32), 32)
            x = x_ref[b, rows, :].astype(F32)
            dy = dy_ref[b, rows, :].astype(F32)
            d = dn[rows, :]
            cen = x - jnp.mean(x, axis=-1, keepdims=True)
            inv = lax.rsqrt(jnp.mean(cen * cen, axis=-1, keepdims=True) + NORM_EPS)
            hat = cen * inv
            for n, one in enumerate((d * hat, d, dy)):
                sums[n] += jnp.sum(one.reshape(4, 8, hidden), axis=0)
            e = d * gain
            m1 = jnp.mean(e, axis=-1, keepdims=True)
            m2 = jnp.mean(e * hat, axis=-1, keepdims=True)
            gx_ref[b, rows, :] = (dy + inv * (e - m1 - hat * m2)).astype(BF16)

    bo_rep[...] = jnp.broadcast_to(b_out, bo_rep.shape)
    sums[...] = jnp.zeros_like(sums)
    product(put_other, 1 - c)
    pair_copy = lambda side: remote(src_ref=both.at[:, side], dst_ref=both.at[:, side], send_sem=ps_sem, recv_sem=pr_sem, device_id=at(z, 1 - c))
    product(put_mine, c)
    pair_copy(1 - c).start()
    pair_copy(1 - c).wait_send()
    pair_copy(c).wait_recv()

    @pl.loop(0, ring)
    def _(k):
        mine[k] = mine[k] + both[k, c]

    lots = [(s, w, u) for u in range(cuts) for w in range(2) for s in range(2)]

    def reduce_copy(s, w, t, u):
        return remote(src_ref=mine.at[turn(STEP[s] * (hops(ring, s, w) - t)), pl.ds(u * few, few), cols[w]], dst_ref=landed.at[s, w, t, u],
                      send_sem=rs_sem.at[s, w, t, u], recv_sem=rr_sem.at[s, w, t, u], device_id=at(turn(STEP[s]), c))

    def fold(s, w, t, u):
        reduce_copy(s, w, t, u).wait_recv()
        at_k = (turn(STEP[s] * (hops(ring, s, w) - t - 1)), pl.ds(u * few, few), cols[w])
        mine[at_k] = mine[at_k] + landed[s, w, t, u]

    def hop(t):
        for s, w, u in lots:
            if t < hops(ring, s, w):
                fold(s, w, t - 1, u)
                reduce_copy(s, w, t, u).start()

    for s, w, u in lots:
        reduce_copy(s, w, 0, u).start()
    for load in loads[3:5]:
        load.wait()
    forward(0, o_old)
    forward(1, o_new)
    for load in loads[5:]:
        load.wait()
    backward(0, d_old)
    for t in range(1, ring // 2 - 1):
        hop(t)
    swap_wait(*swap)
    backward(1, d_new)
    hop(ring // 2 - 1)
    rows_ref[...] = jnp.zeros_like(rows_ref)
    for n in range(3):
        rows_ref[n:n + 1, :] = jnp.sum(sums[n], axis=0, keepdims=True)
    for s, w, u in lots:
        fold(s, w, hops(ring, s, w) - 1, u)
    part[...] = mine[z]
    for s, w, u in lots:
        for t in range(hops(ring, s, w)):
            reduce_copy(s, w, t, u).wait_send()


def tail_a(dqkv, d_old, o_old, o_new, dy, x, w_flat, w_out, gain, b_out, collective_id, cuts=2):
    peers, dim, tok = o_old.shape
    ring = peers // 2
    hidden = dy.shape[-1]
    hbm, vmem = pl.BlockSpec(memory_space=pltpu.HBM), pl.BlockSpec(memory_space=pltpu.VMEM)
    dma = pltpu.SemaphoreType.DMA
    held = lambda a: pltpu.VMEM(a.shape, a.dtype)
    steps = (2, 2, ring // 2, cuts)
    return pl.pallas_call(
        functools.partial(tail_a_body, peers=peers, cuts=cuts),
        name="tail_a",
        out_shape=[jax.ShapeDtypeStruct(x.shape, BF16), jax.ShapeDtypeStruct(x.shape, BF16), jax.ShapeDtypeStruct((dim, hidden), F32),
                   jax.ShapeDtypeStruct((8, hidden), F32)],
        in_specs=[hbm] * 8 + [vmem] * 2,
        out_specs=[vmem] * 4,
        scratch_shapes=[held(a) for a in (o_old, o_new, dy, x, w_out, d_old, w_flat, dqkv)]
        + [pltpu.VMEM((tok, hidden), F32), pltpu.VMEM((3, 8, hidden), F32), pltpu.VMEM((8, hidden), F32),
           pltpu.VMEM((ring, 2, dim, hidden), F32), pltpu.VMEM((ring, dim, hidden), F32), pltpu.VMEM(steps + (dim // cuts, hidden // 2), F32),
           pltpu.VMEM(dqkv.shape[1:], BF16), dma((peers - 1,)), dma((peers - 1,)), dma, dma, dma, dma(steps), dma(steps), dma((7,))],
        cost_estimate=pl.CostEstimate(flops=10**11, bytes_accessed=64 << 20, transcendentals=0),
        compiler_params=pltpu.CompilerParams(collective_id=collective_id, has_side_effects=True, vmem_limit_bytes=VMEM_LIMIT),
    )(dqkv, o_old, o_new, dy, x, w_out, d_old, w_flat, gain, b_out)


def tail_b_body(part, rows_ref, gb_ref, full, total, gb_all, stage, xs_sem, xr_sem, *ring_sems, peers, cuts):
    ring = peers // 2
    me = lax.axis_index("sp")
    z, c = me // 2, me % 2
    hidden = part.shape[1]
    half, few = hidden // 2, part.shape[0] // cuts
    cols = (pl.ds(0, half), pl.ds(half, half))
    remote = functools.partial(pltpu.make_async_remote_copy, device_id_type=pl.DeviceIdType.MESH)
    arrived = greet(peers)
    full[z, c] = part[...]
    gb_all[me] = gb_ref[...]
    block = lambda k, side, w, u: full.at[k, side, pl.ds(u * few, few), cols[w]]
    start, run, finish = ring_gather(block, lambda w, u: block(z, c, w, u), ring_sems, peers, cuts)
    owners = hidden // 128
    lanes = lambda k: pl.ds(pl.multiple_of(k * 128, 128), 128)

    def small_copy(kind, frm, to):
        src, dst = ((rows_ref.at[:, lanes(to)], stage.at[frm]), (total.at[:, lanes(frm)],) * 2, (gb_ref, gb_all.at[frm]))[kind]
        return remote(src_ref=src, dst_ref=dst, send_sem=xs_sem.at[kind, to], recv_sem=xr_sem.at[kind, frm], device_id={"sp": to})

    def each(act, kind, only_to=False, only_from=False):
        @pl.loop(1, peers)
        def _(d):
            far = lax.rem(me + d, peers)

            def go():
                act(kind, far)

            if only_to:
                pl.when(far < owners)(go)
            elif only_from:
                pl.when(me < owners)(go)
            else:
                go()

    send = lambda kind, far: small_copy(kind, me, far).start()
    over = lambda kind, far: small_copy(kind, me, far).wait_send()
    came = lambda kind, far: small_copy(kind, far, me).wait_recv()

    @pl.when(me < owners)
    def _():
        stage[me] = rows_ref[:, lanes(me)]

    arrived()
    start()
    each(send, 0, only_to=True)
    each(send, 2)
    run(1, 2)
    each(came, 0, only_from=True)

    @pl.when(me < owners)
    def _():
        total[:, lanes(me)] = jnp.sum(stage[...], axis=0)

    each(send, 1, only_from=True)
    run(2)
    each(came, 1, only_to=True)
    each(came, 2)
    each(over, 0, only_to=True)
    each(over, 1, only_from=True)
    each(over, 2)
    finish()


def tail_b(part, rows, gb, peers, collective_id, cuts=2):
    ring = peers // 2
    vmem = pl.BlockSpec(memory_space=pltpu.VMEM)
    dma = pltpu.SemaphoreType.DMA
    return pl.pallas_call(
        functools.partial(tail_b_body, peers=peers, cuts=cuts),
        name="tail_b",
        out_shape=[jax.ShapeDtypeStruct((ring, 2) + part.shape, F32), jax.ShapeDtypeStruct(rows.shape, F32),
                   jax.ShapeDtypeStruct((peers,) + gb.shape, F32)],
        in_specs=[vmem] * 3,
        out_specs=[vmem] * 3,
        scratch_shapes=[pltpu.VMEM((peers, 8, 128), F32), dma((3, peers)), dma((3, peers))] + ring_scratch(peers, cuts),
        cost_estimate=pl.CostEstimate(flops=5 * 10**10, bytes_accessed=10 << 20, transcendentals=0),
        compiler_params=pltpu.CompilerParams(collective_id=collective_id, has_side_effects=True, vmem_limit_bytes=32 << 20),
    )(part, rows, gb)


def settle_body(*refs, n_in, first, n_plain, n_held):
    x_ref, plain, held = refs[0], refs[1:1 + n_plain], refs[1 + n_plain:1 + n_plain + n_held]
    outs = refs[n_in:n_in + 1 + n_plain + n_held]
    buf, in_sem, out_sem, in_plain, out_plain, *rooms = refs[n_in + 1 + n_plain + n_held:]
    heads, n = x_ref.shape[:2]
    copy = pltpu.make_async_copy
    reads = [copy(x_ref.at[h], buf.at[h], in_sem.at[h]) for h in range(heads)]
    writes = [copy(buf.at[h], outs[0].at[h, pl.ds(first, n)], out_sem.at[h]) for h in range(heads)]
    reads += [copy(plain[k], rooms[k], in_plain.at[k]) for k in range(n_plain)]
    writes += [copy(rooms[k], outs[1 + k], out_plain.at[k]) for k in range(n_plain)]
    flat = [copy(held[k], outs[1 + n_plain + k], out_plain.at[n_plain + k]) for k in range(n_held)]
    for one in reads + flat:
        one.start()
    for read, write in zip(reads, writes):
        read.wait()
        write.start()
    for one in writes + flat:
        one.wait()


def settle(x, into, plain, held, span, first):
    heads, n, hidden = x.shape
    hbm, vmem = pl.BlockSpec(memory_space=pltpu.HBM), pl.BlockSpec(memory_space=pltpu.VMEM)
    pin = lambda a: pltpu.with_memory_space_constraint(a, pltpu.HBM)
    args = (pin(x), *[pin(a) for a in plain], *held) + (() if into is None else (into,))
    dma = pltpu.SemaphoreType.DMA
    extra = max(len(plain) + len(held), 1)
    return pl.pallas_call(
        functools.partial(settle_body, n_in=len(args), first=first, n_plain=len(plain), n_held=len(held)), name="settle",
        out_shape=[jax.ShapeDtypeStruct((heads, span, hidden), x.dtype)] + [jax.ShapeDtypeStruct(a.shape, a.dtype) for a in (*plain, *held)],
        in_specs=[hbm] * (1 + len(plain)) + [vmem] * len(held) + [hbm] * (into is not None),
        out_specs=[hbm] * (1 + len(plain) + len(held)),
        input_output_aliases={} if into is None else {len(args) - 1: 0},
        scratch_shapes=[pltpu.VMEM(x.shape, x.dtype), dma((heads,)), dma((heads,)), dma((extra,)), dma((extra,))]
        + [pltpu.VMEM(a.shape, a.dtype) for a in plain],
        cost_estimate=pl.CostEstimate(flops=10**9, bytes_accessed=8 * x.size, transcendentals=0),
        compiler_params=pltpu.CompilerParams(vmem_limit_bytes=24 << 20))(*args)


def lay_body(go_ref, total, gb_all, go_out, gb_out, *refs):
    vectors, sem = refs[:-1], refs[-1]
    copies = [pltpu.make_async_copy(go_ref.at[k], go_out.at[k], sem.at[k]) for k in range(go_ref.shape[0])]
    for copy in copies:
        copy.start()
    for k in range(3):
        gb_out[k] = gb_all[:, k, 0:gb_out.shape[2]]
        vectors[k][...] = total[k]
    for copy in copies:
        copy.wait()


def lay_down(go, total, gb_all):
    hbm, vmem = pl.BlockSpec(memory_space=pltpu.HBM), pl.BlockSpec(memory_space=pltpu.VMEM)
    ring, _, dim, hidden = go.shape
    return pl.pallas_call(
        lay_body, name="lay_down",
        out_shape=[jax.ShapeDtypeStruct(go.shape, F32), jax.ShapeDtypeStruct((3, 2 * ring, dim), F32)] + [jax.ShapeDtypeStruct((hidden,), F32)] * 3,
        in_specs=[vmem] * 3, out_specs=[hbm] + [vmem] * 4,
        scratch_shapes=[pltpu.SemaphoreType.DMA((ring,))],
        cost_estimate=pl.CostEstimate(flops=10**9, bytes_accessed=8 * go.size, transcendentals=0),
        compiler_params=pltpu.CompilerParams(vmem_limit_bytes=24 << 20))(go, total, gb_all)


def solution(mesh):
    peers = mesh.shape["sp"]

    def block_fn(x_blk, pos_blk, keep_blk, ln_gain, ln_bias, w_qkv, b_qkv, w_out, b_out, dy_blk):
        batch, tok, hidden = x_blk.shape
        heads, dim = w_qkv.shape[1], w_qkv.shape[3]
        assert heads == peers
        seq = tok * peers
        blk = 2 * tok
        w_all = jnp.transpose(w_qkv, (1, 2, 3, 0)).reshape(heads, 3 * dim, hidden)
        b_all = jnp.transpose(b_qkv, (1, 0, 2))
        marks, do_first, x_first, x_rest, do_rest = opening(x_blk, dy_blk, w_out, ln_gain, ln_bias, pos_blk, keep_blk, peers, 1)
        xs = [x_first.reshape(seq, hidden)] + [lax.all_gather(one, "sp", axis=0, tiled=True) for one in x_rest]
        do_t = [do_first]
        lead = 13 * dim // 6
        gw, att = (), []
        for b in range(batch):
            old = list(do_rest[b:b + 1]) if b + 1 < batch else att
            att_d, gw, gb, att_o, swapped = attention(w_all, b_all, do_t[b], marks, xs[b], gw, old, blk=blk, tok=tok, which=b, batch=batch, lead=lead,
                                                      send_o=b + 1 == batch, collective_id=4 + b)
            if b + 1 < batch:
                do_t.append(swapped[0])
            att = [att_o, att_d]
        o_old, d_old = swapped
        gw_all = [lax.all_gather(one, "sp", axis=0, tiled=True).reshape(heads, -1, hidden) for one in gw[:2]]
        y, gx, part, rows = tail_a(att_d, d_old, o_old, att_o, dy_blk, x_blk, w_all.reshape(3 * hidden, hidden), w_out, ln_gain, b_out, 2)
        go_all, gb_all, g_gain, g_bias, g_out = lay_down(*tail_b(part, rows, gb, peers, 3))
        first, y, gx, go_all = lax.optimization_barrier((gw_all[0], y, gx, go_all))
        gw_out, y, gx = settle(first, None, (y, gx), (), 3 * dim, 0)
        second, gw_out, go_all = lax.optimization_barrier((gw_all[1], gw_out, go_all))
        gw_out, = settle(second, gw_out, (), (), 3 * dim, lead)
        gw_out = jnp.transpose(gw_out.reshape(heads, 3, dim, hidden), (3, 0, 1, 2))
        return y, gx, gw_out, jnp.transpose(gb_all, (1, 0, 2)), go_all.reshape(hidden, hidden), g_out, g_gain, g_bias

    act_spec = P("dp", "sp", None)
    tok_spec = P("dp", "sp")
    in_specs = (act_spec, tok_spec, tok_spec, P(), P(), P(), P(), P(), P(), act_spec)
    out_specs = (act_spec, act_spec, P("dp", None, None, None), P("dp", None, None), P("dp", None), P("dp"), P("dp"), P("dp"))
    return jax.shard_map(block_fn, mesh=mesh, in_specs=in_specs, out_specs=out_specs, check_vma=False)
```
